128 devices in a mesh: dp: 1, tp: 128 (over z, y, x, core).
Axes of the slice: x: 4, y: 4, z: 4, core: 2. Of those that a mesh axis runs over, the one named last changes fastest.
Arguments:
- hidden: bfloat16 [384, 3, 2048], P(('dp', 'tp'))
- w_head: bfloat16 [2048, 128256], P(None, 'tp')
- q_draft: float32 [384, 2, 128256], P(('dp', 'tp'))
- draft_tok: int32 [384, 2], P('dp')
Outputs:
- output 1: float32 [384, 2], P('dp')
- output 2: float32 [384], P('dp')
- output 3: float32 [384, 2, 128256], P('dp', None, 'tp')
- output 4: float32 [384, 128256], P('dp', 'tp')
All inputs are finite; a program needn't handle non-finite values.
Results may differ from the reference program's by a relative error of at most 0.001.
Values are sent between devices in bfloat16 or wider.
A program may use at most 1 GiB of HBM per device.

```python
import jax
import jax.numpy as jnp

SEQ_DEV = 3
GROUP_SIZE = 128
DRAFT_LEN = 2
MODEL_DIM = 2048
VOCAB_SIZE = 128256
BATCH = SEQ_DEV * GROUP_SIZE
INV_TEMP = 1.25
HEAD_SCALE = MODEL_DIM ** -0.5


def setup_inputs(seed: int = 0, part: int = 0) -> dict:
    part_key = jax.random.fold_in(jax.random.key(seed), part)
    key_hid, key_noise, key_tok = jax.random.split(part_key, 3)
    key_head = jax.random.key(seed + 1)
    hidden = jax.random.normal(key_hid, (BATCH, DRAFT_LEN + 1, MODEL_DIM), jnp.float32).astype(jnp.bfloat16)
    w_head = (jax.random.normal(key_head, (MODEL_DIM, VOCAB_SIZE), jnp.float32) * HEAD_SCALE).astype(jnp.bfloat16)
    target = jnp.dot(hidden[:, :DRAFT_LEN].reshape(BATCH * DRAFT_LEN, MODEL_DIM), w_head, preferred_element_type=jnp.float32)
    target = target.reshape(BATCH, DRAFT_LEN, VOCAB_SIZE) * INV_TEMP
    draft_noise = jax.random.normal(key_noise, (BATCH, DRAFT_LEN, VOCAB_SIZE), jnp.float32)
    q_draft = jax.nn.softmax(0.8 * target + 0.6 * draft_noise, axis=-1)
    draft_tok = jax.random.randint(key_tok, (BATCH, DRAFT_LEN), 0, VOCAB_SIZE, jnp.int32)
    draft_tok = draft_tok.at[0, 0].set(0).at[BATCH - 1, DRAFT_LEN - 1].set(VOCAB_SIZE - 1)
    return {'hidden': hidden, 'w_head': w_head, 'q_draft': q_draft, 'draft_tok': draft_tok}


def reference(hidden, w_head, q_draft, draft_tok):
    logits = jnp.dot(hidden.reshape(BATCH * (DRAFT_LEN + 1), MODEL_DIM), w_head, preferred_element_type=jnp.float32)
    logits = logits.reshape(BATCH, DRAFT_LEN + 1, VOCAB_SIZE) * INV_TEMP
    target_prob = jax.nn.softmax(logits, axis=-1)
    draft_part = target_prob[:, :DRAFT_LEN]
    p_pick = jnp.take_along_axis(draft_part, draft_tok[:, :, None], axis=2)[:, :, 0]
    q_pick = jnp.take_along_axis(q_draft, draft_tok[:, :, None], axis=2)[:, :, 0]
    accept = jnp.minimum(p_pick / q_pick, 1.0)
    expected = jnp.sum(jnp.cumprod(accept, axis=1), axis=1)
    excess = jnp.maximum(draft_part - q_draft, 0.0)
    residual = excess / jnp.sum(excess, axis=-1, keepdims=True)
    return accept, expected, residual, target_prob[:, DRAFT_LEN]
```

```python
import jax
import jax.numpy as jnp
from jax import lax
from jax.experimental import pallas as pl
from jax.experimental.layout import Layout, with_layout_constraint
from jax.experimental.pallas import tpu as pltpu
from jax.sharding import PartitionSpec as P

INV_TEMP = 1.25
DEV = 128
SEQ = 3
NPOS = 3
DRAFT = 2
BATCH = 384
DIM = 2048
VOCAB = 128256
SHARD = VOCAB // DEV
LANES = 128
TILES = VOCAB // LANES
CHUNKS = 8
TAIL = SHARD - (CHUNKS - 1) * LANES
ROWS_P = 1008
TAIL_P = ROWS_P - (CHUNKS - 1) * LANES
KC = DIM // LANES
HROWS = SEQ * NPOS * KC
COLS = NPOS * BATCH
COLS_P = 1280
CT = COLS // LANES
BT = BATCH // LANES
BLK = SEQ * CHUNKS
PITCH = 49
NEG = -1e30
STAT = 24
MESH = pl.DeviceIdType.MESH


def remote(src, dst, ssem, rsem, dev):
    return pltpu.make_async_remote_copy(
        src_ref=src, dst_ref=dst, send_sem=ssem, recv_sem=rsem,
        device_id={'tp': dev}, device_id_type=MESH)


def reduce_round(me, bufa, bufb, sa, ra, sb, rb, payload, combine):
    slot, grp = me % 8, me // 8
    bufa[slot] = payload
    copies = []
    for r in range(1, 8):
        cp = remote(bufa.at[slot], bufa.at[slot], sa.at[r - 1], ra.at[r - 1], grp * 8 + (slot + r) % 8)
        cp.start()
        copies.append(cp)
    for cp in copies:
        cp.wait()
    bufb[grp] = combine([bufa[k] for k in range(8)])
    copies = []
    for r in range(1, 16):
        cp = remote(bufb.at[grp], bufb.at[grp], sb.at[r - 1], rb.at[r - 1], ((grp + r) % 16) * 8 + slot)
        cp.start()
        copies.append(cp)
    for cp in copies:
        cp.wait()
    return combine([bufb[k] for k in range(16)])


def merge_max_sum(parts):
    m = parts[0][0:CT]
    for p in parts[1:]:
        m = jnp.maximum(m, p[0:CT])
    s = parts[0][CT:2 * CT] * jnp.exp(parts[0][0:CT] - m)
    for p in parts[1:]:
        s = s + p[CT:2 * CT] * jnp.exp(p[0:CT] - m)
    return jnp.concatenate([m, s, jnp.zeros((STAT - 2 * CT, LANES), jnp.float32)], axis=0)


def merge_add(parts):
    total = parts[0]
    for p in parts[1:]:
        total = total + p
    return total


def kernel(q_hbm, w_hbm, h_ref, tok_ref,
           ex_hbm, bo_hbm, fac_ref, mass_ref, acc_ref,
           qbuf, wbuf, hidb, bounce, hmat, z, send, recv, exbuf, stat, scale,
           a1, b1, a2, b2,
           lsem, ag_s, ag_r, d2d_s, d2d_r, qs_sem, qr_sem,
           sa1, ra1, sb1, rb1, sa2, ra2, sb2, rb2):
    me = lax.axis_index('tp')
    core = me % 2
    coord = (me // 32, (me // 8) % 4, (me // 2) % 4)

    qcp = pltpu.make_async_copy(q_hbm, qbuf.at[pl.ds(0, SEQ * TILES * DRAFT)], lsem.at[0])
    qcp.start()
    wcp = pltpu.make_async_copy(w_hbm, wbuf, lsem.at[1])
    wcp.start()
    hview = hidb.reshape(4, 4, 4, 2, SEQ, HROWS // SEQ, LANES)
    own = hview.at[coord[0], coord[1], coord[2], core]
    hcp = pltpu.make_async_copy(h_ref.reshape(SEQ, HROWS // SEQ, LANES), own, lsem.at[2])
    hcp.start()
    hcp.wait()

    def sel(j, phase):
        order = [(j + k) % 3 for k in range(3)]
        idx = [coord[0], coord[1], coord[2]]
        for d in order[:phase]:
            idx[d] = slice(None)
        return hview.at[idx[0], idx[1], idx[2], core, j], order[phase]

    def ag_phase(phase):
        out = []
        for j in range(3):
            view, dim = sel(j, phase)
            for r in (1, 3, 2):
                to = list(coord)
                to[dim] = (coord[dim] + r) % 4
                dev = ((to[0] * 4 + to[1]) * 4 + to[2]) * 2 + core
                cp = remote(view, view, ag_s.at[phase, j, r - 1], ag_r.at[phase, j, r - 1], dev)
                cp.start()
                out.append(cp)
        return out

    qrows = qbuf.reshape(qbuf.shape[0], LANES)
    lane = lax.broadcasted_iota(jnp.int32, (8, LANES), 1)

    def pack(k, carry):
        first = (SHARD * k) // LANES
        off = (SHARD * k) % LANES
        shift = (LANES - off) % LANES
        keep = lane < LANES - off
        for i in range(DRAFT):
            for s in range(SEQ):
                base = (s * TILES + first) * DRAFT + i
                lo = qrows[pl.ds(base, 8, stride=2), :]
                hi = qrows[pl.ds(base + 2, 8, stride=2), :]
                lo = pltpu.roll(lo, shift, 1)
                hi = pltpu.roll(hi, shift, 1)
                send[i, pl.ds(pl.multiple_of(k * BLK + s * 8, 8), 8), :] = jnp.where(keep, lo, hi)
        return carry

    c0 = ag_phase(0)
    qcp.wait()
    lax.fori_loop(0, DEV, pack, 0)
    for cp in c0:
        cp.wait_recv()
    c1 = ag_phase(1)
    for cp in c1:
        cp.wait_recv()
    c2 = ag_phase(2)

    def exchange(i):
        pltpu.make_async_copy(
            send.at[i, pl.ds(pl.multiple_of(me * BLK, 8), BLK)],
            recv.at[i, pl.ds(pl.multiple_of(me * BLK, 8), BLK)], qr_sem.at[i]).start()

        def one(n, carry):
            r = (n * 37) % DEV
            rz, ry, rx, rc = r // 32, (r // 8) % 4, (r // 2) % 4, r % 2
            dev = ((((coord[0] + rz) % 4) * 4 + (coord[1] + ry) % 4) * 4 + (coord[2] + rx) % 4) * 2 + (core + rc) % 2
            remote(send.at[i, pl.ds(pl.multiple_of(dev * BLK, 8), BLK)],
                   recv.at[i, pl.ds(pl.multiple_of(me * BLK, 8), BLK)],
                   qs_sem.at[i], qr_sem.at[i], dev).start()
            return carry

        lax.fori_loop(1, DEV, one, 0)

    exchange(0)

    d2d = []
    for j in range(3):
        for cp in c2[3 * j:3 * j + 3]:
            cp.wait_recv()
        view = hview.at[:, :, :, core, j]
        cp = remote(view, view, d2d_s.at[j], d2d_r.at[j], me - core + 1 - core)
        cp.start()
        d2d.append(cp)
    for cp in d2d:
        cp.wait_recv()
    for cp in c0 + c1 + c2 + d2d:
        cp.wait_send()

    def relayout(n, carry):
        def up(b, c):
            x = hidb[pl.ds(pl.multiple_of((48 * n + b) * 48, 16), 48), :]
            bounce[pl.ds(b * PITCH, 48), :] = x.astype(jnp.float32)
            return c

        lax.fori_loop(0, 48, up, 0, unroll=4)
        for g in range(NPOS):
            for u in range(3):
                for kc in range(KC):
                    y = bounce[pl.ds(16 * u * PITCH + g * KC + kc, 16, stride=PITCH), :]
                    hmat[pl.ds(pl.multiple_of(g * BATCH + 48 * n + 16 * u, 16), 16),
                         kc * LANES:(kc + 1) * LANES] = y.astype(jnp.bfloat16)
        return carry

    lax.fori_loop(0, 8, relayout, 0)
    wcp.wait()

    z[SHARD:ROWS_P, :] = jnp.full((ROWS_P - SHARD, COLS_P), NEG, jnp.float32)

    def head(n, carry):
        hb = hmat[pl.ds(pl.multiple_of(n * 256, 256), 256), :]
        zt = lax.dot_general(wbuf[...], hb, (((1,), (1,)), ((), ())), preferred_element_type=jnp.float32)
        z[0:SHARD, pl.ds(pl.multiple_of(n * 256, 256), 256)] = zt * INV_TEMP
        return carry

    lax.fori_loop(0, COLS_P // 256, head, 0)

    def local_stats(t, carry):
        cols = pl.ds(pl.multiple_of(t * LANES, LANES), LANES)

        def peak(n, m):
            x = z[pl.ds(pl.multiple_of(n * 112, 8), 112), cols]
            return jnp.maximum(m, jnp.max(x.reshape(14, 8, LANES), axis=0))

        m8 = lax.fori_loop(0, 9, peak, jnp.full((8, LANES), NEG, jnp.float32))
        m = jnp.max(m8, axis=0, keepdims=True)

        def expo(n, s):
            rows = pl.ds(pl.multiple_of(n * 112, 8), 112)
            x = jnp.exp(z[rows, cols] - m)
            z[rows, cols] = x
            return s + jnp.sum(x.reshape(14, 8, LANES), axis=0)

        s8 = lax.fori_loop(0, 9, expo, jnp.zeros((8, LANES), jnp.float32))
        stat[pl.ds(t, 1), :] = m
        stat[pl.ds(CT + t, 1), :] = jnp.sum(s8, axis=0, keepdims=True)
        return carry

    stat[...] = jnp.zeros_like(stat)
    lax.fori_loop(0, CT, local_stats, 0)
    bcp = pltpu.make_async_copy(z.at[:, DRAFT * BATCH:COLS], bo_hbm, lsem.at[2])
    bcp.start()

    local = stat[...]
    tot = reduce_round(me, a1, b1, sa1, ra1, sb1, rb1, local, merge_max_sum)
    exchange(1)
    fac = jnp.exp(local[0:CT] - tot[0:CT]) / tot[CT:2 * CT]
    scale[0:CT, :] = fac
    for t in range(BT):
        fac_ref[0:1, t * LANES:(t + 1) * LANES] = fac[DRAFT * BT + t:DRAFT * BT + t + 1]

    exrows = exbuf.reshape(exbuf.shape[0], LANES)
    first_id = me * SHARD
    stat[...] = jnp.zeros_like(stat)
    for i in range(DRAFT):
        pltpu.make_async_copy(recv.at[i], recv.at[i], qr_sem.at[i]).wait()
        for t in range(BT):
            row = i * BT + t
            sc = scale[row:row + 1, :]
            tok = tok_ref[i:i + 1, t * LANES:(t + 1) * LANES] - first_id
            col0 = i * BATCH + t * LANES

            def block(c, carry, size, valid):
                mass, pp, qp = carry
                q = recv[i, pl.ds(t * LANES * CHUNKS + c, LANES, stride=CHUNKS), :].T
                p = z[pl.ds(pl.multiple_of(c * LANES, LANES), size), col0:col0 + LANES] * sc
                ids = lax.broadcasted_iota(jnp.int32, (size, LANES), 0)
                q = q[0:size]
                if valid < size:
                    q = jnp.where(ids < valid, q, 0.0)
                x = jnp.maximum(p - q, 0.0)
                exrows[pl.ds(c * LANES * 6 + t * 2 + i, valid, stride=6), :] = x[0:valid]
                hit = ids == tok - c * LANES
                fold = lambda v: jnp.sum(v.reshape(size // 8, 8, LANES), axis=0)
                return (mass + fold(x), pp + fold(jnp.where(hit, p, 0.0)), qp + fold(jnp.where(hit, q, 0.0)))

            zero = jnp.zeros((8, LANES), jnp.float32)
            carry = lax.fori_loop(0, CHUNKS - 1, lambda c, v: block(c, v, LANES, LANES), (zero, zero, zero))
            mass, pp, qp = block(CHUNKS - 1, carry, TAIL_P, TAIL)
            stat[row:row + 1, :] = jnp.sum(mass, axis=0, keepdims=True)
            stat[6 + row:7 + row, :] = jnp.sum(pp, axis=0, keepdims=True)
            stat[12 + row:13 + row, :] = jnp.sum(qp, axis=0, keepdims=True)

    ecp = pltpu.make_async_copy(exbuf, ex_hbm, lsem.at[0])
    ecp.start()
    tot = reduce_round(me, a2, b2, sa2, ra2, sb2, rb2, stat[...], merge_add)
    acc = jnp.minimum(tot[6:12] / tot[12:18], 1.0)
    for i in range(DRAFT):
        for t in range(BT):
            row = i * BT + t
            mass_ref[i:i + 1, t * LANES:(t + 1) * LANES] = tot[row:row + 1]
            acc_ref[i:i + 1, t * LANES:(t + 1) * LANES] = acc[row:row + 1]
    ecp.wait()
    bcp.wait()
    for i in range(DRAFT):
        part = send.at[i, pl.ds(0, (DEV - 1) * BLK)]
        pltpu.make_async_copy(part, part, qs_sem.at[i]).wait()


def verify_local(hid, w_cols, q_rows, draft_tok):
    q = with_layout_constraint(q_rows.reshape(SEQ, DRAFT, TILES, LANES), Layout((0, 2, 1, 3)))
    q = q.transpose(0, 2, 1, 3).reshape(SEQ * TILES * DRAFT, 1, LANES)
    f32 = jnp.float32
    hbm = pl.BlockSpec(memory_space=pl.ANY)
    vmem = pl.BlockSpec(memory_space=pltpu.VMEM)
    dma = pltpu.SemaphoreType.DMA
    ex, bo, fac, mass, acc = pl.pallas_call(
        kernel,
        out_shape=[
            jax.ShapeDtypeStruct((SHARD * BT * DRAFT, 1, LANES), f32),
            jax.ShapeDtypeStruct((ROWS_P, BATCH), f32),
            jax.ShapeDtypeStruct((1, BATCH), f32),
            jax.ShapeDtypeStruct((DRAFT, BATCH), f32),
            jax.ShapeDtypeStruct((DRAFT, BATCH), f32),
        ],
        in_specs=[hbm, hbm, vmem, vmem],
        out_specs=[hbm, hbm, vmem, vmem, vmem],
        scratch_shapes=[
            pltpu.VMEM((SEQ * TILES * DRAFT + 20, 1, LANES), f32),
            pltpu.VMEM((SHARD, DIM), jnp.bfloat16),
            pltpu.VMEM((DEV * HROWS, LANES), jnp.bfloat16),
            pltpu.VMEM((48 * PITCH, LANES), f32),
            pltpu.VMEM((COLS_P, DIM), jnp.bfloat16),
            pltpu.VMEM((ROWS_P, COLS_P), f32),
            pltpu.VMEM((DRAFT, DEV * BLK, LANES), f32),
            pltpu.VMEM((DRAFT, DEV * BLK, LANES), f32),
            pltpu.VMEM((SHARD * BT * DRAFT, 1, LANES), f32),
            pltpu.VMEM((STAT, LANES), f32),
            pltpu.VMEM((16, LANES), f32),
            pltpu.VMEM((8, STAT, LANES), f32),
            pltpu.VMEM((16, STAT, LANES), f32),
            pltpu.VMEM((8, STAT, LANES), f32),
            pltpu.VMEM((16, STAT, LANES), f32),
            dma((3,)),
            dma((3, 3, 3)), dma((3, 3, 3)), dma((3,)), dma((3,)),
            dma((2,)), dma((2,)),
            dma((7,)), dma((7,)), dma((15,)), dma((15,)),
            dma((7,)), dma((7,)), dma((15,)), dma((15,)),
        ],
        compiler_params=pltpu.CompilerParams(vmem_limit_bytes=62 * 2 ** 20, has_side_effects=True),
    )(q, w_cols.T, hid.reshape(HROWS, LANES), draft_tok.T)
    ex = with_layout_constraint(ex.reshape(SHARD, BT, DRAFT, LANES).transpose(0, 2, 1, 3), Layout((0, 2, 1, 3)))
    residual = (ex.reshape(SHARD, DRAFT, BATCH) / mass[None]).transpose(2, 1, 0)
    bonus = (bo[:SHARD] * fac).T
    expected = acc[0] * (1.0 + acc[1])
    return acc.T, expected, residual, bonus


def solution(mesh):
    return jax.shard_map(
        verify_local,
        mesh=mesh,
        in_specs=(P(('dp', 'tp'), None, None), P(None, 'tp'), P(('dp', 'tp'), None, None), P('dp', None)),
        out_specs=(P('dp', None), P('dp'), P('dp', None, 'tp'), P('dp', 'tp')),
        check_vma=False,
    )
```

```python
import jax
import jax.numpy as jnp
from jax import lax
from jax.experimental import pallas as pl
from jax.experimental.layout import Layout, with_layout_constraint
from jax.experimental.pallas import tpu as pltpu
from jax.sharding import PartitionSpec as P

INV_TEMP = 1.25
DEV = 128
SEQ = 3
NPOS = 3
DRAFT = 2
BATCH = 384
DIM = 2048
VOCAB = 128256
SHARD = VOCAB // DEV
LANES = 128
TILES = VOCAB // LANES
CHUNKS = 8
TAIL = SHARD - (CHUNKS - 1) * LANES
ROWS_P = 1008
TAIL_P = ROWS_P - (CHUNKS - 1) * LANES
KC = DIM // LANES
HROWS = SEQ * NPOS * KC
COLS = NPOS * BATCH
COLS_P = 1280
CT = COLS // LANES
BT = BATCH // LANES
BLK = SEQ * CHUNKS
PITCH = 49
NEG = -1e30
STAT = 24
MESH = pl.DeviceIdType.MESH


def remote(src, dst, ssem, rsem, dev):
    return pltpu.make_async_remote_copy(
        src_ref=src, dst_ref=dst, send_sem=ssem, recv_sem=rsem,
        device_id={'tp': dev}, device_id_type=MESH)


def reduce_stage(buf, slot, count, ssem, rsem, device, payload):
    buf[slot] = payload
    copies = []
    for r in range(1, count):
        cp = remote(buf.at[slot], buf.at[slot], ssem.at[r - 1], rsem.at[r - 1], device((slot + r) % count))
        cp.start()
        copies.append(cp)
    return copies


def finish(copies):
    for cp in copies:
        cp.wait()


def merge_max_sum(parts):
    m = parts[0][0:CT]
    for p in parts[1:]:
        m = jnp.maximum(m, p[0:CT])
    s = parts[0][CT:2 * CT] * jnp.exp(parts[0][0:CT] - m)
    for p in parts[1:]:
        s = s + p[CT:2 * CT] * jnp.exp(p[0:CT] - m)
    return jnp.concatenate([m, s, jnp.zeros((STAT - 2 * CT, LANES), jnp.float32)], axis=0)


def merge_add(parts):
    total = parts[0]
    for p in parts[1:]:
        total = total + p
    return total


def kernel(q_hbm, w_hbm, h_hbm, tok_ref,
           ex_hbm, bo_hbm, fac_ref, mass_ref, acc_ref,
           qbuf, wbuf, hloc, hidb, bounce, hmat, z, send, recv, exbuf, stat, scale,
           a1, b1, a2, b2,
           lsem, ag_s, ag_r, d2d_s, d2d_r, qs_sem, qr_sem,
           sa1, ra1, sb1, rb1, sa2, ra2, sb2, rb2):
    scope = jax.named_scope
    me = lax.axis_index('tp')
    core = me % 2
    coord = (me // 32, (me // 8) % 4, (me // 2) % 4)
    unit = (32, 8, 2)
    partner = me + 1 - 2 * core
    hop = [[((coord[d] + r) % 4) * unit[d] for r in range(4)] for d in range(3)]

    def device(rz, ry, rx, rc):
        return hop[0][rz] + hop[1][ry] + hop[2][rx] + (core if rc == 0 else 1 - core)

    hcp = pltpu.make_async_copy(h_hbm, hloc, lsem.at[2])
    hcp.start()
    qcp = pltpu.make_async_copy(q_hbm, qbuf.at[pl.ds(0, SEQ * TILES * DRAFT)], lsem.at[0])
    qcp.start()
    wcp = pltpu.make_async_copy(w_hbm, wbuf, lsem.at[1])
    wcp.start()
    barrier = pltpu.get_barrier_semaphore()
    peers = [partner]
    for d in range(3):
        for r in range(1, 4):
            steps = [0, 0, 0]
            steps[d] = r
            peers.append(device(*steps, 0))
    for dev in peers:
        pl.semaphore_signal(barrier, inc=1, device_id={'tp': dev}, device_id_type=MESH)

    with scope('hid'):
        hcp.wait()
        for s in range(SEQ):
            x = hloc[s].astype(jnp.float32)
            for kc in range(KC):
                bounce[pl.ds(s * 48 + kc, NPOS, stride=KC), :] = x[:, kc * LANES:(kc + 1) * LANES]
        hidb[pl.ds(pl.multiple_of(me * HROWS, 16), HROWS), :] = bounce[0:HROWS, :].astype(jnp.bfloat16)
    with scope('barrier'):
        pl.semaphore_wait(barrier, len(peers))

    hview = hidb.reshape(4, 4, 4, 2, SEQ, HROWS // SEQ, LANES)

    def ag_phase(phase):
        out = []
        for j in range(3):
            order = [(j + k) % 3 for k in range(3)]
            idx = list(coord)
            for d in order[:phase]:
                idx[d] = slice(None)
            view = hview.at[idx[0], idx[1], idx[2], core, j]
            for r in (1, 3, 2):
                steps = [0, 0, 0]
                steps[order[phase]] = r
                cp = remote(view, view, ag_s.at[phase, j, r - 1], ag_r.at[phase, j, r - 1], device(*steps, 0))
                cp.start()
                out.append(cp)
        return out

    qrows = qbuf.reshape(qbuf.shape[0], LANES)
    lane = lax.broadcasted_iota(jnp.int32, (8, LANES), 1)

    def pack(k, carry):
        first = (SHARD * k) // LANES
        off = (SHARD * k) % LANES
        shift = (LANES - off) % LANES
        keep = lane < LANES - off
        for i in range(DRAFT):
            for s in range(SEQ):
                base = (s * TILES + first) * DRAFT + i
                lo = qrows[pl.ds(base, 8, stride=2), :]
                hi = qrows[pl.ds(base + 2, 8, stride=2), :]
                lo = pltpu.roll(lo, shift, 1)
                hi = pltpu.roll(hi, shift, 1)
                send[i, pl.ds(pl.multiple_of(k * BLK + s * 8, 8), 8), :] = jnp.where(keep, lo, hi)
        return carry

    mine = pl.ds(pl.multiple_of(me * BLK, 8), BLK)

    def to(i, dev):
        remote(send.at[i, pl.ds(pl.multiple_of(dev * BLK, 8), BLK)], recv.at[i, mine],
               qs_sem.at[i], qr_sem.at[i], dev).start()

    def step(d, n):
        return ((coord[d] + n) % 4) * unit[d]

    def class0(i):
        pltpu.make_async_copy(send.at[i, mine], recv.at[i, mine], qr_sem.at[i]).start()
        to(i, partner)

    def class1(i, rc):
        last = core if rc == 0 else 1 - core
        for r in (1, 3, 2):
            for d in range(3):
                steps = [0, 0, 0]
                steps[d] = r
                to(i, device(*steps, rc))

    def class2(i, rc):
        last = core if rc == 0 else 1 - core

        def body(n, carry):
            a, b = n // 3 + 1, n % 3 + 1
            to(i, step(0, a) + step(1, b) + hop[2][0] + last)
            to(i, hop[0][0] + step(1, a) + step(2, b) + last)
            to(i, step(0, b) + hop[1][0] + step(2, a) + last)
            return carry

        lax.fori_loop(0, 9, body, 0)

    def class3(i, rc):
        last = core if rc == 0 else 1 - core

        def body(n, carry):
            a, b = n // 3, n % 3
            for k in range(3):
                to(i, step(0, (a + k) % 3 + 1) + step(1, (b + k) % 3 + 1) + hop[2][k + 1] + last)
            return carry

        lax.fori_loop(0, 9, body, 0)

    c0 = ag_phase(0)
    with scope('qwait'):
        qcp.wait()
    with scope('pack'):
        lax.fori_loop(0, DEV, pack, 0, unroll=8)
    with scope('ag0'):
        for cp in c0:
            cp.wait_recv()
    c1 = ag_phase(1)
    with scope('ex0a'):
        class0(0)
        class1(0, 0)
        class1(0, 1)
        class2(0, 0)
    with scope('ag1'):
        for cp in c1:
            cp.wait_recv()
    c2 = ag_phase(2)
    with scope('ex0b'):
        class2(0, 1)
        class3(0, 0)
    d2d = []
    for j in range(3):
        with scope(f'ag2_{j}'):
            for cp in c2[3 * j:3 * j + 3]:
                cp.wait_recv()
        view = hview.at[:, :, :, core, j]
        cp = remote(view, view, d2d_s.at[j], d2d_r.at[j], partner)
        cp.start()
        d2d.append(cp)
    with scope('ex0c'):
        class3(0, 1)
    with scope('d2d'):
        for cp in d2d:
            cp.wait_recv()

    def relayout(n, carry):
        def up(b, c):
            x = hidb[pl.ds(pl.multiple_of((48 * n + b) * 48, 16), 48), :]
            bounce[pl.ds(b * PITCH, 48), :] = x.astype(jnp.float32)
            return c

        lax.fori_loop(0, 48, up, 0, unroll=4)
        for g in range(NPOS):
            for u in range(3):
                for kc in range(KC):
                    y = bounce[pl.ds(16 * u * PITCH + g * KC + kc, 16, stride=PITCH), :]
                    hmat[pl.ds(pl.multiple_of(g * BATCH + 48 * n + 16 * u, 16), 16),
                         kc * LANES:(kc + 1) * LANES] = y.astype(jnp.bfloat16)
        return carry

    with scope('relayout'):
        lax.fori_loop(0, 8, relayout, 0)
    wcp.wait()

    z[SHARD:ROWS_P, :] = jnp.full((ROWS_P - SHARD, COLS_P), NEG, jnp.float32)

    def head(n, carry):
        hb = hmat[pl.ds(pl.multiple_of(n * 256, 256), 256), :]
        zt = lax.dot_general(wbuf[...], hb, (((1,), (1,)), ((), ())), preferred_element_type=jnp.float32)
        z[0:SHARD, pl.ds(pl.multiple_of(n * 256, 256), 256)] = zt * INV_TEMP
        return carry

    with scope('head'):
        lax.fori_loop(0, COLS_P // 256, head, 0)

    def local_stats(t, carry):
        cols = pl.ds(pl.multiple_of(t * LANES, LANES), LANES)

        def peak(n, m):
            x = z[pl.ds(pl.multiple_of(n * 112, 8), 112), cols]
            return jnp.maximum(m, jnp.max(x.reshape(14, 8, LANES), axis=0))

        m8 = lax.fori_loop(0, 9, peak, jnp.full((8, LANES), NEG, jnp.float32))
        m = jnp.max(m8, axis=0, keepdims=True)

        def expo(n, s):
            rows = pl.ds(pl.multiple_of(n * 112, 8), 112)
            x = jnp.exp(z[rows, cols] - m)
            z[rows, cols] = x
            return s + jnp.sum(x.reshape(14, 8, LANES), axis=0)

        s8 = lax.fori_loop(0, 9, expo, jnp.zeros((8, LANES), jnp.float32))
        stat[pl.ds(t, 1), :] = m
        stat[pl.ds(CT + t, 1), :] = jnp.sum(s8, axis=0, keepdims=True)
        return carry

    stat[...] = jnp.zeros_like(stat)
    with scope('stats'):
        lax.fori_loop(0, CT, local_stats, 0)
    bcp = pltpu.make_async_copy(z.at[:, DRAFT * BATCH:COLS], bo_hbm, lsem.at[2])
    bcp.start()

    slot, grp = me % 8, me // 8
    near = lambda k: grp * 8 + k
    far = lambda k: k * 8 + slot
    local = stat[...]
    copies = reduce_stage(a1, slot, 8, sa1, ra1, near, local)
    with scope('ex1a'):
        class0(1)
        class1(1, 0)
        class1(1, 1)
        class2(1, 0)
    with scope('round1a'):
        finish(copies)
    copies = reduce_stage(b1, grp, 16, sb1, rb1, far, merge_max_sum([a1[k] for k in range(8)]))
    with scope('ex1b'):
        class2(1, 1)
        class3(1, 0)
        class3(1, 1)
    with scope('round1b'):
        finish(copies)
    tot = merge_max_sum([b1[k] for k in range(16)])
    fac = jnp.exp(local[0:CT] - tot[0:CT]) / tot[CT:2 * CT]
    scale[0:CT, :] = fac
    for t in range(BT):
        for i in range(DRAFT):
            fac_ref[i:i + 1, t * LANES:(t + 1) * LANES] = fac[DRAFT * BT + t:DRAFT * BT + t + 1]

    exrows = exbuf.reshape(exbuf.shape[0], LANES)
    first_id = me * SHARD
    stat[...] = jnp.zeros_like(stat)
    for i in range(DRAFT):
        with scope(f'a2a_{i}'):
            pltpu.make_async_copy(recv.at[i], recv.at[i], qr_sem.at[i]).wait()
        for t in range(BT):
            row = i * BT + t
            sc = scale[row:row + 1, :]
            tok = tok_ref[i:i + 1, t * LANES:(t + 1) * LANES] - first_id
            col0 = i * BATCH + t * LANES

            def block(c, carry, size, valid):
                mass, pp, qp = carry
                q = recv[i, pl.ds(t * LANES * CHUNKS + c, LANES, stride=CHUNKS), :].T
                p = z[pl.ds(pl.multiple_of(c * LANES, LANES), size), col0:col0 + LANES] * sc
                ids = lax.broadcasted_iota(jnp.int32, (size, LANES), 0)
                q = q[0:size]
                if valid < size:
                    q = jnp.where(ids < valid, q, 0.0)
                x = jnp.maximum(p - q, 0.0)
                exrows[pl.ds(c * LANES * 6 + t * 2 + i, valid, stride=6), :] = x[0:valid]
                hit = ids == tok - c * LANES
                fold = lambda v: jnp.sum(v.reshape(size // 8, 8, LANES), axis=0)
                return (mass + fold(x), pp + fold(jnp.where(hit, p, 0.0)), qp + fold(jnp.where(hit, q, 0.0)))

            zero = jnp.zeros((8, LANES), jnp.float32)
            carry = lax.fori_loop(0, CHUNKS - 1, lambda c, v: block(c, v, LANES, LANES), (zero, zero, zero))
            mass, pp, qp = block(CHUNKS - 1, carry, TAIL_P, TAIL)
            stat[row:row + 1, :] = jnp.sum(mass, axis=0, keepdims=True)
            stat[6 + row:7 + row, :] = jnp.sum(pp, axis=0, keepdims=True)
            stat[12 + row:13 + row, :] = jnp.sum(qp, axis=0, keepdims=True)

    ecp = pltpu.make_async_copy(exbuf, ex_hbm, lsem.at[0])
    ecp.start()
    copies = reduce_stage(a2, slot, 8, sa2, ra2, near, stat[...])
    with scope('round2a'):
        finish(copies)
    copies = reduce_stage(b2, grp, 16, sb2, rb2, far, merge_add([a2[k] for k in range(8)]))
    with scope('round2b'):
        finish(copies)
    tot = merge_add([b2[k] for k in range(16)])
    acc = jnp.minimum(tot[6:12] / tot[12:18], 1.0)
    for i in range(DRAFT):
        for t in range(BT):
            row = i * BT + t
            mass_ref[i:i + 1, t * LANES:(t + 1) * LANES] = tot[row:row + 1]
            acc_ref[i:i + 1, t * LANES:(t + 1) * LANES] = acc[row:row + 1]
    with scope('tail'):
        ecp.wait()
        bcp.wait()
        for cp in c0 + c1 + c2 + d2d:
            cp.wait_send()
        for i in range(DRAFT):
            part = send.at[i, pl.ds(0, (DEV - 1) * BLK)]
            pltpu.make_async_copy(part, part, qs_sem.at[i]).wait()


def verify_local(hid, w_cols, q_rows, draft_tok):
    q = with_layout_constraint(q_rows.reshape(SEQ, DRAFT, TILES, LANES), Layout((0, 2, 1, 3)))
    q = q.transpose(0, 2, 1, 3).reshape(SEQ * TILES * DRAFT, 1, LANES)
    f32 = jnp.float32
    hbm = pl.BlockSpec(memory_space=pl.ANY)
    vmem = pl.BlockSpec(memory_space=pltpu.VMEM)
    dma = pltpu.SemaphoreType.DMA
    ex, bo, fac, mass, acc = pl.pallas_call(
        kernel,
        out_shape=[
            jax.ShapeDtypeStruct((SHARD * BT * DRAFT, 1, LANES), f32),
            jax.ShapeDtypeStruct((ROWS_P, BATCH), f32),
            jax.ShapeDtypeStruct((DRAFT, BATCH), f32),
            jax.ShapeDtypeStruct((DRAFT, BATCH), f32),
            jax.ShapeDtypeStruct((DRAFT, BATCH), f32),
        ],
        in_specs=[pl.BlockSpec(memory_space=pltpu.HBM)] * 3 + [vmem],
        out_specs=[hbm, hbm, vmem, vmem, vmem],
        scratch_shapes=[
            pltpu.VMEM((SEQ * TILES * DRAFT + 20, 1, LANES), f32),
            pltpu.VMEM((SHARD, DIM), jnp.bfloat16),
            pltpu.VMEM((SEQ, NPOS, DIM), jnp.bfloat16),
            pltpu.VMEM((DEV * HROWS, LANES), jnp.bfloat16),
            pltpu.VMEM((48 * PITCH, LANES), f32),
            pltpu.VMEM((COLS_P, DIM), jnp.bfloat16),
            pltpu.VMEM((ROWS_P, COLS_P), f32),
            pltpu.VMEM((DRAFT, DEV * BLK, LANES), f32),
            pltpu.VMEM((DRAFT, DEV * BLK, LANES), f32),
            pltpu.VMEM((SHARD * BT * DRAFT, 1, LANES), f32),
            pltpu.VMEM((STAT, LANES), f32),
            pltpu.VMEM((16, LANES), f32),
            pltpu.VMEM((8, STAT, LANES), f32),
            pltpu.VMEM((16, STAT, LANES), f32),
            pltpu.VMEM((8, STAT, LANES), f32),
            pltpu.VMEM((16, STAT, LANES), f32),
            dma((3,)),
            dma((3, 3, 3)), dma((3, 3, 3)), dma((3,)), dma((3,)),
            dma((2,)), dma((2,)),
            dma((7,)), dma((7,)), dma((15,)), dma((15,)),
            dma((7,)), dma((7,)), dma((15,)), dma((15,)),
        ],
        compiler_params=pltpu.CompilerParams(vmem_limit_bytes=40 * 2 ** 20, has_side_effects=True, collective_id=0),
    )(*(pltpu.with_memory_space_constraint(x, pltpu.HBM) for x in (q, w_cols.T, hid, draft_tok.T)))
    ex = with_layout_constraint(ex.reshape(SHARD, BT, DRAFT, LANES).transpose(0, 2, 1, 3), Layout((0, 2, 1, 3)))
    residual = (ex.reshape(SHARD, DRAFT, BATCH) / mass[None]).transpose(2, 1, 0)
    bonus = (bo[:SHARD] * fac[:1]).T
    expected = acc[0] * (1.0 + acc[1])
    return acc.T, expected, residual, bonus


def solution(mesh):
    return jax.shard_map(
        verify_local,
        mesh=mesh,
        in_specs=(P(('dp', 'tp'), None, None), P(None, 'tp'), P(('dp', 'tp'), None, None), P('dp', None)),
        out_specs=(P('dp', None), P('dp'), P('dp', None, 'tp'), P('dp', 'tp')),
        check_vma=False,
    )
```

```python
import jax
import jax.numpy as jnp
from jax import lax
from jax.experimental import pallas as pl
from jax.experimental.layout import Layout, with_layout_constraint
from jax.experimental.pallas import tpu as pltpu
from jax.sharding import PartitionSpec as P

INV_TEMP = 1.25
DEV = 128
SEQ = 3
NPOS = 3
DRAFT = 2
BATCH = 384
DIM = 2048
VOCAB = 128256
SHARD = VOCAB // DEV
LANES = 128
TILES = VOCAB // LANES
CHUNKS = 8
TAIL = SHARD - (CHUNKS - 1) * LANES
ROWS_P = 1008
TAIL_P = ROWS_P - (CHUNKS - 1) * LANES
KC = DIM // LANES
HROWS = SEQ * NPOS * KC
COLS = NPOS * BATCH
COLS_P = 1280
CT = COLS // LANES
BT = BATCH // LANES
BLK = SEQ * CHUNKS
PITCH = 49
NEG = -1e30
STAT = 24
MESH = pl.DeviceIdType.MESH


def remote(src, dst, ssem, rsem, dev):
    return pltpu.make_async_remote_copy(
        src_ref=src, dst_ref=dst, send_sem=ssem, recv_sem=rsem,
        device_id={'tp': dev}, device_id_type=MESH)


def reduce_stage(buf, slot, count, ssem, rsem, device, payload):
    buf[slot] = payload
    copies = []
    for r in range(1, count):
        cp = remote(buf.at[slot], buf.at[slot], ssem.at[r - 1], rsem.at[r - 1], device((slot + r) % count))
        cp.start()
        copies.append(cp)
    return copies


def finish(copies):
    for cp in copies:
        cp.wait()


def merge_max_sum(parts):
    m = parts[0][0:CT]
    for p in parts[1:]:
        m = jnp.maximum(m, p[0:CT])
    s = parts[0][CT:2 * CT] * jnp.exp(parts[0][0:CT] - m)
    for p in parts[1:]:
        s = s + p[CT:2 * CT] * jnp.exp(p[0:CT] - m)
    return jnp.concatenate([m, s, jnp.zeros((STAT - 2 * CT, LANES), jnp.float32)], axis=0)


def merge_add(parts):
    total = parts[0]
    for p in parts[1:]:
        total = total + p
    return total


def kernel(q_hbm, w_hbm, h_hbm, tok_ref,
           ex_hbm, bo_hbm, fac_ref, mass_ref, acc_ref,
           qbuf, wbuf, hloc, hidb, bounce, hmat, z, send, recv, exbuf, stat, scale,
           a1, b1, a2, b2,
           lsem, ag_s, ag_r, d2d_s, d2d_r, qs_sem, qr_sem,
           sa1, ra1, sb1, rb1, sa2, ra2, sb2, rb2):
    scope = jax.named_scope
    me = lax.axis_index('tp')
    core = me % 2
    coord = (me // 32, (me // 8) % 4, (me // 2) % 4)
    unit = (32, 8, 2)
    partner = me + 1 - 2 * core
    hop = [[((coord[d] + r) % 4) * unit[d] for r in range(4)] for d in range(3)]

    def device(rz, ry, rx, rc):
        return hop[0][rz] + hop[1][ry] + hop[2][rx] + (core if rc == 0 else 1 - core)

    hcp = pltpu.make_async_copy(h_hbm, hloc, lsem.at[2])
    hcp.start()
    qcp = pltpu.make_async_copy(q_hbm, qbuf.at[pl.ds(0, SEQ * TILES * DRAFT)], lsem.at[0])
    qcp.start()
    wcp = pltpu.make_async_copy(w_hbm, wbuf, lsem.at[1])
    wcp.start()
    barrier = pltpu.get_barrier_semaphore()
    peers = [partner]
    for d in range(3):
        for r in range(1, 4):
            steps = [0, 0, 0]
            steps[d] = r
            peers.append(device(*steps, 0))
    for dev in peers:
        pl.semaphore_signal(barrier, inc=1, device_id={'tp': dev}, device_id_type=MESH)

    with scope('hid'):
        hcp.wait()
        for s in range(SEQ):
            x = hloc[s].astype(jnp.float32)
            for kc in range(KC):
                bounce[pl.ds(s * 48 + kc, NPOS, stride=KC), :] = x[:, kc * LANES:(kc + 1) * LANES]
        hidb[pl.ds(pl.multiple_of(me * HROWS, 16), HROWS), :] = bounce[0:HROWS, :].astype(jnp.bfloat16)
    with scope('barrier'):
        pl.semaphore_wait(barrier, len(peers))

    hview = hidb.reshape(4, 4, 4, 2, SEQ, HROWS // SEQ, LANES)

    def ag_phase(phase):
        out = []
        for j in range(3):
            order = [(j + k) % 3 for k in range(3)]
            idx = list(coord)
            for d in order[:phase]:
                idx[d] = slice(None)
            view = hview.at[idx[0], idx[1], idx[2], core, j]
            for r in (1, 3, 2):
                steps = [0, 0, 0]
                steps[order[phase]] = r
                cp = remote(view, view, ag_s.at[phase, j, r - 1], ag_r.at[phase, j, r - 1], device(*steps, 0))
                cp.start()
                out.append(cp)
        return out

    qrows = qbuf.reshape(qbuf.shape[0], LANES)
    lane = lax.broadcasted_iota(jnp.int32, (8, LANES), 1)

    def pack(k, carry):
        first = (SHARD * k) // LANES
        off = (SHARD * k) % LANES
        shift = (LANES - off) % LANES
        keep = lane < LANES - off
        for i in range(DRAFT):
            for s in range(SEQ):
                base = (s * TILES + first) * DRAFT + i
                lo = qrows[pl.ds(base, 8, stride=2), :]
                hi = qrows[pl.ds(base + 2, 8, stride=2), :]
                lo = pltpu.roll(lo, shift, 1)
                hi = pltpu.roll(hi, shift, 1)
                send[i, pl.ds(pl.multiple_of(k * BLK + s * 8, 8), 8), :] = jnp.where(keep, lo, hi)
        return carry

    mine = pl.ds(pl.multiple_of(me * BLK, 8), BLK)

    def to(i, dev):
        remote(send.at[i, pl.ds(pl.multiple_of(dev * BLK, 8), BLK)], recv.at[i, mine],
               qs_sem.at[i], qr_sem.at[i], dev).start()

    def step(d, n):
        return ((coord[d] + n) % 4) * unit[d]

    def class0(i):
        pltpu.make_async_copy(send.at[i, mine], recv.at[i, mine], qr_sem.at[i]).start()
        to(i, partner)

    def class1(i, rc):
        last = core if rc == 0 else 1 - core
        for r in (1, 3, 2):
            for d in range(3):
                steps = [0, 0, 0]
                steps[d] = r
                to(i, device(*steps, rc))

    def class2(i, rc):
        last = core if rc == 0 else 1 - core

        def body(n, carry):
            a, b = n // 3 + 1, n % 3 + 1
            to(i, step(0, a) + step(1, b) + hop[2][0] + last)
            to(i, hop[0][0] + step(1, a) + step(2, b) + last)
            to(i, step(0, b) + hop[1][0] + step(2, a) + last)
            return carry

        lax.fori_loop(0, 9, body, 0)

    def class3(i, rc):
        last = core if rc == 0 else 1 - core

        def body(n, carry):
            a, b = n // 3, n % 3
            for k in range(3):
                to(i, step(0, (a + k) % 3 + 1) + step(1, (b + k) % 3 + 1) + hop[2][k + 1] + last)
            return carry

        lax.fori_loop(0, 9, body, 0)

    c0 = ag_phase(0)
    with scope('qwait'):
        qcp.wait()
    with scope('pack'):
        lax.fori_loop(0, 88, pack, 0, unroll=8)
    with scope('ag0'):
        for cp in c0:
            cp.wait_recv()
    c1 = ag_phase(1)
    with scope('pack2'):
        lax.fori_loop(88, DEV, pack, 0, unroll=8)
    with scope('ex0a'):
        class0(0)
        class1(0, 0)
        class1(0, 1)
        class2(0, 0)
    with scope('ag1'):
        for cp in c1:
            cp.wait_recv()
    c2 = ag_phase(2)
    d2d = []
    for j in range(3):
        with scope(f'ag2_{j}'):
            for cp in c2[3 * j:3 * j + 3]:
                cp.wait_recv()
        view = hview.at[:, :, :, core, j]
        cp = remote(view, view, d2d_s.at[j], d2d_r.at[j], partner)
        cp.start()
        d2d.append(cp)
    with scope('ex0b'):
        class2(0, 1)
        class3(0, 0)
        class3(0, 1)
        class0(1)
        class1(1, 0)
        class1(1, 1)
        class2(1, 0)
    with scope('d2d'):
        for cp in d2d:
            cp.wait_recv()

    def relayout(n, carry):
        def up(b, c):
            x = hidb[pl.ds(pl.multiple_of((48 * n + b) * 48, 16), 48), :]
            bounce[pl.ds(b * PITCH, 48), :] = x.astype(jnp.float32)
            return c

        lax.fori_loop(0, 48, up, 0, unroll=4)
        for g in range(NPOS):
            for u in range(3):
                for kc in range(KC):
                    y = bounce[pl.ds(16 * u * PITCH + g * KC + kc, 16, stride=PITCH), :]
                    hmat[pl.ds(pl.multiple_of(g * BATCH + 48 * n + 16 * u, 16), 16),
                         kc * LANES:(kc + 1) * LANES] = y.astype(jnp.bfloat16)
        return carry

    with scope('relayout'):
        lax.fori_loop(0, 8, relayout, 0)
    wcp.wait()

    z[SHARD:ROWS_P, :] = jnp.full((ROWS_P - SHARD, COLS_P), NEG, jnp.float32)

    def head(n, carry):
        hb = hmat[pl.ds(pl.multiple_of(n * 256, 256), 256), :]
        zt = lax.dot_general(wbuf[...], hb, (((1,), (1,)), ((), ())), preferred_element_type=jnp.float32)
        z[0:SHARD, pl.ds(pl.multiple_of(n * 256, 256), 256)] = zt * INV_TEMP
        return carry

    with scope('head'):
        lax.fori_loop(0, COLS_P // 256, head, 0)

    def local_stats(t, carry):
        cols = pl.ds(pl.multiple_of(t * LANES, LANES), LANES)

        def peak(n, m):
            x = z[pl.ds(pl.multiple_of(n * 112, 8), 112), cols]
            return jnp.maximum(m, jnp.max(x.reshape(14, 8, LANES), axis=0))

        m8 = lax.fori_loop(0, 9, peak, jnp.full((8, LANES), NEG, jnp.float32))
        m = jnp.max(m8, axis=0, keepdims=True)

        def expo(n, s):
            rows = pl.ds(pl.multiple_of(n * 112, 8), 112)
            x = jnp.exp(z[rows, cols] - m)
            z[rows, cols] = x
            return s + jnp.sum(x.reshape(14, 8, LANES), axis=0)

        s8 = lax.fori_loop(0, 9, expo, jnp.zeros((8, LANES), jnp.float32))
        stat[pl.ds(t, 1), :] = m
        stat[pl.ds(CT + t, 1), :] = jnp.sum(s8, axis=0, keepdims=True)
        return carry

    stat[...] = jnp.zeros_like(stat)
    with scope('stats'):
        lax.fori_loop(0, CT, local_stats, 0)
    bcp = pltpu.make_async_copy(z.at[:, DRAFT * BATCH:COLS], bo_hbm, lsem.at[2])
    bcp.start()

    slot, grp = me % 8, me // 8
    near = lambda k: grp * 8 + k
    far = lambda k: k * 8 + slot
    local = stat[...]
    copies = reduce_stage(a1, slot, 8, sa1, ra1, near, local)
    with scope('ex1a'):
        class2(1, 1)
    with scope('round1a'):
        finish(copies)
    copies = reduce_stage(b1, grp, 16, sb1, rb1, far, merge_max_sum([a1[k] for k in range(8)]))
    with scope('ex1b'):
        class3(1, 0)
        class3(1, 1)
    with scope('round1b'):
        finish(copies)
    tot = merge_max_sum([b1[k] for k in range(16)])
    fac = jnp.exp(local[0:CT] - tot[0:CT]) / tot[CT:2 * CT]
    scale[0:CT, :] = fac
    for t in range(BT):
        for i in range(DRAFT):
            fac_ref[i:i + 1, t * LANES:(t + 1) * LANES] = fac[DRAFT * BT + t:DRAFT * BT + t + 1]

    exrows = exbuf.reshape(exbuf.shape[0], LANES)
    first_id = me * SHARD
    stat[...] = jnp.zeros_like(stat)
    for i in range(DRAFT):
        with scope(f'a2a_{i}'):
            pltpu.make_async_copy(recv.at[i], recv.at[i], qr_sem.at[i]).wait()
        for t in range(BT):
            row = i * BT + t
            sc = scale[row:row + 1, :]
            tok = tok_ref[i:i + 1, t * LANES:(t + 1) * LANES] - first_id
            col0 = i * BATCH + t * LANES

            def block(c, carry, size, valid):
                mass, pp, qp = carry
                q = recv[i, pl.ds(t * LANES * CHUNKS + c, LANES, stride=CHUNKS), :].T
                p = z[pl.ds(pl.multiple_of(c * LANES, LANES), size), col0:col0 + LANES] * sc
                ids = lax.broadcasted_iota(jnp.int32, (size, LANES), 0)
                q = q[0:size]
                if valid < size:
                    q = jnp.where(ids < valid, q, 0.0)
                x = jnp.maximum(p - q, 0.0)
                exrows[pl.ds(c * LANES * 6 + t * 2 + i, valid, stride=6), :] = x[0:valid]
                hit = ids == tok - c * LANES
                fold = lambda v: jnp.sum(v.reshape(size // 8, 8, LANES), axis=0)
                return (mass + fold(x), pp + fold(jnp.where(hit, p, 0.0)), qp + fold(jnp.where(hit, q, 0.0)))

            zero = jnp.zeros((8, LANES), jnp.float32)
            carry = lax.fori_loop(0, CHUNKS - 1, lambda c, v: block(c, v, LANES, LANES), (zero, zero, zero))
            mass, pp, qp = block(CHUNKS - 1, carry, TAIL_P, TAIL)
            stat[row:row + 1, :] = jnp.sum(mass, axis=0, keepdims=True)
            stat[6 + row:7 + row, :] = jnp.sum(pp, axis=0, keepdims=True)
            stat[12 + row:13 + row, :] = jnp.sum(qp, axis=0, keepdims=True)

    ecp = pltpu.make_async_copy(exbuf, ex_hbm, lsem.at[0])
    ecp.start()
    copies = reduce_stage(a2, slot, 8, sa2, ra2, near, stat[...])
    with scope('round2a'):
        finish(copies)
    copies = reduce_stage(b2, grp, 16, sb2, rb2, far, merge_add([a2[k] for k in range(8)]))
    with scope('round2b'):
        finish(copies)
    tot = merge_add([b2[k] for k in range(16)])
    acc = jnp.minimum(tot[6:12] / tot[12:18], 1.0)
    for i in range(DRAFT):
        for t in range(BT):
            row = i * BT + t
            mass_ref[i:i + 1, t * LANES:(t + 1) * LANES] = tot[row:row + 1]
            acc_ref[i:i + 1, t * LANES:(t + 1) * LANES] = acc[row:row + 1]
    with scope('tail'):
        ecp.wait()
        bcp.wait()
        for cp in c0 + c1 + c2 + d2d:
            cp.wait_send()
        for i in range(DRAFT):
            part = send.at[i, pl.ds(0, (DEV - 1) * BLK)]
            pltpu.make_async_copy(part, part, qs_sem.at[i]).wait()


def verify_local(hid, w_cols, q_rows, draft_tok):
    q = with_layout_constraint(q_rows.reshape(SEQ, DRAFT, TILES, LANES), Layout((0, 2, 1, 3)))
    q = q.transpose(0, 2, 1, 3).reshape(SEQ * TILES * DRAFT, 1, LANES)
    f32 = jnp.float32
    hbm = pl.BlockSpec(memory_space=pl.ANY)
    vmem = pl.BlockSpec(memory_space=pltpu.VMEM)
    dma = pltpu.SemaphoreType.DMA
    ex, bo, fac, mass, acc = pl.pallas_call(
        kernel,
        out_shape=[
            jax.ShapeDtypeStruct((SHARD * BT * DRAFT, 1, LANES), f32),
            jax.ShapeDtypeStruct((ROWS_P, BATCH), f32),
            jax.ShapeDtypeStruct((DRAFT, BATCH), f32),
            jax.ShapeDtypeStruct((DRAFT, BATCH), f32),
            jax.ShapeDtypeStruct((DRAFT, BATCH), f32),
        ],
        in_specs=[pl.BlockSpec(memory_space=pltpu.HBM)] * 3 + [vmem],
        out_specs=[hbm, hbm, vmem, vmem, vmem],
        scratch_shapes=[
            pltpu.VMEM((SEQ * TILES * DRAFT + 20, 1, LANES), f32),
            pltpu.VMEM((SHARD, DIM), jnp.bfloat16),
            pltpu.VMEM((SEQ, NPOS, DIM), jnp.bfloat16),
            pltpu.VMEM((DEV * HROWS, LANES), jnp.bfloat16),
            pltpu.VMEM((48 * PITCH, LANES), f32),
            pltpu.VMEM((COLS_P, DIM), jnp.bfloat16),
            pltpu.VMEM((ROWS_P, COLS_P), f32),
            pltpu.VMEM((DRAFT, DEV * BLK, LANES), f32),
            pltpu.VMEM((DRAFT, DEV * BLK, LANES), f32),
            pltpu.VMEM((SHARD * BT * DRAFT, 1, LANES), f32),
            pltpu.VMEM((STAT, LANES), f32),
            pltpu.VMEM((16, LANES), f32),
            pltpu.VMEM((8, STAT, LANES), f32),
            pltpu.VMEM((16, STAT, LANES), f32),
            pltpu.VMEM((8, STAT, LANES), f32),
            pltpu.VMEM((16, STAT, LANES), f32),
            dma((3,)),
            dma((3, 3, 3)), dma((3, 3, 3)), dma((3,)), dma((3,)),
            dma((2,)), dma((2,)),
            dma((7,)), dma((7,)), dma((15,)), dma((15,)),
            dma((7,)), dma((7,)), dma((15,)), dma((15,)),
        ],
        compiler_params=pltpu.CompilerParams(vmem_limit_bytes=40 * 2 ** 20, has_side_effects=True, collective_id=0),
    )(*(pltpu.with_memory_space_constraint(x, pltpu.HBM) for x in (q, w_cols.T, hid, draft_tok.T)))
    ex = with_layout_constraint(ex.reshape(SHARD, BT, DRAFT, LANES).transpose(0, 2, 1, 3), Layout((0, 2, 1, 3)))
    residual = (ex.reshape(SHARD, DRAFT, BATCH) / mass[None]).transpose(2, 1, 0)
    bonus = (bo[:SHARD] * fac[:1]).T
    expected = acc[0] * (1.0 + acc[1])
    return acc.T, expected, residual, bonus


def solution(mesh):
    return jax.shard_map(
        verify_local,
        mesh=mesh,
        in_specs=(P(('dp', 'tp'), None, None), P(None, 'tp'), P(('dp', 'tp'), None, None), P('dp', None)),
        out_specs=(P('dp', None), P('dp'), P('dp', None, 'tp'), P('dp', 'tp')),
        check_vma=False,
    )
```

```python
import jax
import jax.numpy as jnp
from jax import lax
from jax.experimental import pallas as pl
from jax.experimental.layout import Layout, with_layout_constraint
from jax.experimental.pallas import tpu as pltpu
from jax.sharding import PartitionSpec as P

INV_TEMP = 1.25
DEV = 128
SEQ = 3
NPOS = 3
DRAFT = 2
BATCH = 384
DIM = 2048
VOCAB = 128256
SHARD = VOCAB // DEV
LANES = 128
TILES = VOCAB // LANES
CHUNKS = 8
TAIL = SHARD - (CHUNKS - 1) * LANES
ROWS_P = 1008
TAIL_P = ROWS_P - (CHUNKS - 1) * LANES
KC = DIM // LANES
HROWS = SEQ * NPOS * KC
COLS = NPOS * BATCH
COLS_P = 1280
CT = COLS // LANES
BT = BATCH // LANES
BLK = SEQ * CHUNKS
PITCH = 49
NEG = -1e30
STAT = 18
MESH = pl.DeviceIdType.MESH


def remote(src, dst, ssem, rsem, dev):
    return pltpu.make_async_remote_copy(
        src_ref=src, dst_ref=dst, send_sem=ssem, recv_sem=rsem,
        device_id={'tp': dev}, device_id_type=MESH)


def reduce_stage(buf, slot, count, ssem, rsem, device, payload):
    buf.reshape(count * STAT, LANES)[pl.ds(slot * STAT, STAT), :] = payload
    here = buf.at[pl.ds(slot * STAT, STAT)]
    copies = []
    for r in range(1, count):
        cp = remote(here, here, ssem.at[r - 1], rsem.at[r - 1], device((slot + r) % count))
        cp.start()
        copies.append(cp)
    return copies


def finish(copies, buf):
    for cp in copies:
        cp.wait()
    count = len(copies) + 1
    rows = buf.reshape(count * STAT, LANES)
    return [rows[k * STAT:(k + 1) * STAT, :] for k in range(count)]


def merge_max_sum(parts):
    m = parts[0][0:CT]
    for p in parts[1:]:
        m = jnp.maximum(m, p[0:CT])
    s = parts[0][CT:2 * CT] * jnp.exp(parts[0][0:CT] - m)
    for p in parts[1:]:
        s = s + p[CT:2 * CT] * jnp.exp(p[0:CT] - m)
    return jnp.concatenate([m, s], axis=0)


def merge_add(parts):
    total = parts[0]
    for p in parts[1:]:
        total = total + p
    return total


def kernel(q_hbm, w_hbm, h_hbm, tok_ref,
           ex_hbm, bo_hbm, fac_ref, mass_ref, acc_ref,
           qbuf, wbuf, hloc, hidb, bounce, hmat, z, send, recv, exbuf, stat, scale,
           a1, b1, a2, b2,
           lsem, ag_s, ag_r, d2d_s, d2d_r, qs_sem, qr_sem,
           sa1, ra1, sb1, rb1, sa2, ra2, sb2, rb2):
    scope = jax.named_scope
    me = lax.axis_index('tp')
    core = me % 2
    coord = (me // 32, (me // 8) % 4, (me // 2) % 4)
    unit = (32, 8, 2)
    partner = me + 1 - 2 * core
    hop = [[((coord[d] + r) % 4) * unit[d] for r in range(4)] for d in range(3)]

    def device(rz, ry, rx, rc):
        return hop[0][rz] + hop[1][ry] + hop[2][rx] + (core if rc == 0 else 1 - core)

    hcp = pltpu.make_async_copy(h_hbm, hloc, lsem.at[2])
    hcp.start()
    qcp = pltpu.make_async_copy(q_hbm, qbuf.at[pl.ds(0, SEQ * TILES * DRAFT)], lsem.at[0])
    qcp.start()
    wcp = pltpu.make_async_copy(w_hbm, wbuf, lsem.at[1])
    wcp.start()
    barrier = pltpu.get_barrier_semaphore()
    peers = [partner]
    for d in range(3):
        for r in range(1, 4):
            steps = [0, 0, 0]
            steps[d] = r
            peers.append(device(*steps, 0))
    for dev in peers:
        pl.semaphore_signal(barrier, inc=1, device_id={'tp': dev}, device_id_type=MESH)

    with scope('hid'):
        hcp.wait()
        for s in range(SEQ):
            x = hloc[s].astype(jnp.float32)
            for kc in range(KC):
                bounce[pl.ds(s * 48 + kc, NPOS, stride=KC), :] = x[:, kc * LANES:(kc + 1) * LANES]
        hidb[pl.ds(pl.multiple_of(me * HROWS, 16), HROWS), :] = bounce[0:HROWS, :].astype(jnp.bfloat16)
    with scope('barrier'):
        pl.semaphore_wait(barrier, len(peers))

    hview = hidb.reshape(4, 4, 4, 2, SEQ, HROWS // SEQ, LANES)

    def ag_phase(phase):
        out = []
        for j in range(3):
            order = [(j + k) % 3 for k in range(3)]
            idx = list(coord)
            for d in order[:phase]:
                idx[d] = slice(None)
            view = hview.at[idx[0], idx[1], idx[2], core, j]
            for r in (1, 3, 2):
                steps = [0, 0, 0]
                steps[order[phase]] = r
                cp = remote(view, view, ag_s.at[phase, j, r - 1], ag_r.at[phase, j, r - 1], device(*steps, 0))
                cp.start()
                out.append(cp)
        return out

    qrows = qbuf.reshape(qbuf.shape[0], LANES)
    lane = lax.broadcasted_iota(jnp.int32, (8, LANES), 1)

    def pack(k, carry):
        first = (SHARD * k) // LANES
        off = (SHARD * k) % LANES
        shift = (LANES - off) % LANES
        keep = lane < LANES - off
        for i in range(DRAFT):
            for s in range(SEQ):
                base = (s * TILES + first) * DRAFT + i
                lo = qrows[pl.ds(base, 8, stride=2), :]
                hi = qrows[pl.ds(base + 2, 8, stride=2), :]
                lo = pltpu.roll(lo, shift, 1)
                hi = pltpu.roll(hi, shift, 1)
                send[i, pl.ds(pl.multiple_of(k * BLK + s * 8, 8), 8), :] = jnp.where(keep, lo, hi)
        return carry

    mine = pl.ds(pl.multiple_of(me * BLK, 8), BLK)

    def to(i, dev):
        remote(send.at[i, pl.ds(pl.multiple_of(dev * BLK, 8), BLK)], recv.at[i, mine],
               qs_sem.at[i], qr_sem.at[i], dev).start()

    def step(d, n):
        return ((coord[d] + n) % 4) * unit[d]

    def class0(i):
        pltpu.make_async_copy(send.at[i, mine], recv.at[i, mine], qr_sem.at[i]).start()
        to(i, partner)

    def class1(i, rc):
        last = core if rc == 0 else 1 - core
        for r in (1, 3, 2):
            for d in range(3):
                steps = [0, 0, 0]
                steps[d] = r
                to(i, device(*steps, rc))

    def class2(i, rc):
        last = core if rc == 0 else 1 - core

        def body(n, carry):
            a, b = n // 3 + 1, n % 3 + 1
            to(i, step(0, a) + step(1, b) + hop[2][0] + last)
            to(i, hop[0][0] + step(1, a) + step(2, b) + last)
            to(i, step(0, b) + hop[1][0] + step(2, a) + last)
            return carry

        lax.fori_loop(0, 9, body, 0)

    def class3(i, rc):
        last = core if rc == 0 else 1 - core

        def body(n, carry):
            a, b = n // 3, n % 3
            for k in range(3):
                to(i, step(0, (a + k) % 3 + 1) + step(1, (b + k) % 3 + 1) + hop[2][k + 1] + last)
            return carry

        lax.fori_loop(0, 9, body, 0)

    c0 = ag_phase(0)
    with scope('qwait'):
        qcp.wait()
    with scope('pack'):
        lax.fori_loop(0, DEV, pack, 0, unroll=8)
    with scope('ex0'):
        class0(0)
        class1(0, 0)
    with scope('ag0'):
        for cp in c0:
            cp.wait_recv()
    c1 = ag_phase(1)
    with scope('ex0a'):
        class1(0, 1)
        class2(0, 0)
    with scope('ag1'):
        for cp in c1:
            cp.wait_recv()
    c2 = ag_phase(2)
    d2d = []
    for j in range(3):
        with scope(f'ag2_{j}'):
            for cp in c2[3 * j:3 * j + 3]:
                cp.wait_recv()
        view = hview.at[:, :, :, core, j]
        cp = remote(view, view, d2d_s.at[j], d2d_r.at[j], partner)
        cp.start()
        d2d.append(cp)
    with scope('ex0b'):
        class2(0, 1)
        class3(0, 0)
        class3(0, 1)
        class0(1)
        class1(1, 0)
        class1(1, 1)
    with scope('d2d'):
        for cp in d2d:
            cp.wait_recv()

    def relayout(n, carry):
        def up(b, c):
            x = hidb[pl.ds(pl.multiple_of((48 * n + b) * 48, 16), 48), :]
            bounce[pl.ds(b * PITCH, 48), :] = x.astype(jnp.float32)
            return c

        lax.fori_loop(0, 48, up, 0, unroll=4)
        for g in range(NPOS):
            for u in range(3):
                for kc in range(KC):
                    y = bounce[pl.ds(16 * u * PITCH + g * KC + kc, 16, stride=PITCH), :]
                    hmat[pl.ds(pl.multiple_of(g * BATCH + 48 * n + 16 * u, 16), 16),
                         kc * LANES:(kc + 1) * LANES] = y.astype(jnp.bfloat16)
        return carry

    with scope('relayout'):
        lax.fori_loop(0, 8, relayout, 0)
    wcp.wait()

    z[SHARD:ROWS_P, :] = jnp.full((ROWS_P - SHARD, COLS_P), NEG, jnp.float32)

    def head(n, carry):
        hb = hmat[pl.ds(pl.multiple_of(n * 256, 256), 256), :]
        zt = lax.dot_general(wbuf[...], hb, (((1,), (1,)), ((), ())), preferred_element_type=jnp.float32)
        z[0:SHARD, pl.ds(pl.multiple_of(n * 256, 256), 256)] = zt * INV_TEMP
        return carry

    with scope('head'):
        lax.fori_loop(0, COLS_P // 256, head, 0)

    def local_stats(t, carry):
        cols = pl.ds(pl.multiple_of(t * LANES, LANES), LANES)

        def peak(n, m):
            x = z[pl.ds(pl.multiple_of(n * 112, 8), 112), cols]
            return jnp.maximum(m, jnp.max(x.reshape(14, 8, LANES), axis=0))

        m8 = lax.fori_loop(0, 9, peak, jnp.full((8, LANES), NEG, jnp.float32))
        m = jnp.max(m8, axis=0, keepdims=True)

        def expo(n, s):
            rows = pl.ds(pl.multiple_of(n * 112, 8), 112)
            x = jnp.exp(z[rows, cols] - m)
            z[rows, cols] = x
            return s + jnp.sum(x.reshape(14, 8, LANES), axis=0)

        s8 = lax.fori_loop(0, 9, expo, jnp.zeros((8, LANES), jnp.float32))
        stat[pl.ds(t, 1), :] = m
        stat[pl.ds(CT + t, 1), :] = jnp.sum(s8, axis=0, keepdims=True)
        return carry

    stat[...] = jnp.zeros_like(stat)
    with scope('stats'):
        lax.fori_loop(0, CT, local_stats, 0)
    bcp = pltpu.make_async_copy(z.at[:, DRAFT * BATCH:COLS], bo_hbm, lsem.at[2])
    bcp.start()

    slot, grp = me % 8, me // 8
    near = lambda k: grp * 8 + k
    far = lambda k: k * 8 + slot
    local = stat[0:STAT, :]
    copies = reduce_stage(a1, slot, 8, sa1, ra1, near, local)
    with scope('ex1a'):
        class2(1, 0)
    with scope('round1a'):
        parts = finish(copies, a1)
    copies = reduce_stage(b1, grp, 16, sb1, rb1, far, merge_max_sum(parts))
    with scope('ex1b'):
        class2(1, 1)
        class3(1, 0)
        class3(1, 1)
    with scope('round1b'):
        parts = finish(copies, b1)
    tot = merge_max_sum(parts)
    fac = jnp.exp(local[0:CT] - tot[0:CT]) / tot[CT:2 * CT]
    scale[0:CT, :] = fac
    for t in range(BT):
        for i in range(DRAFT):
            fac_ref[i:i + 1, t * LANES:(t + 1) * LANES] = fac[DRAFT * BT + t:DRAFT * BT + t + 1]

    exrows = exbuf.reshape(exbuf.shape[0], LANES)
    first_id = me * SHARD
    stat[...] = jnp.zeros_like(stat)
    for i in range(DRAFT):
        with scope(f'a2a_{i}'):
            pltpu.make_async_copy(recv.at[i], recv.at[i], qr_sem.at[i]).wait()
        for t in range(BT):
            row = i * BT + t
            sc = scale[row:row + 1, :]
            tok = tok_ref[i:i + 1, t * LANES:(t + 1) * LANES] - first_id
            col0 = i * BATCH + t * LANES

            def block(c, carry, size, valid):
                mass, pp, qp = carry
                q = recv[i, pl.ds(t * LANES * CHUNKS + c, LANES, stride=CHUNKS), :].T
                p = z[pl.ds(pl.multiple_of(c * LANES, LANES), size), col0:col0 + LANES] * sc
                ids = lax.broadcasted_iota(jnp.int32, (size, LANES), 0)
                q = q[0:size]
                if valid < size:
                    q = jnp.where(ids < valid, q, 0.0)
                x = jnp.maximum(p - q, 0.0)
                exrows[pl.ds(c * LANES * 6 + t * 2 + i, valid, stride=6), :] = x[0:valid]
                hit = ids == tok - c * LANES
                fold = lambda v: jnp.sum(v.reshape(size // 8, 8, LANES), axis=0)
                return (mass + fold(x), pp + fold(jnp.where(hit, p, 0.0)), qp + fold(jnp.where(hit, q, 0.0)))

            zero = jnp.zeros((8, LANES), jnp.float32)
            carry = lax.fori_loop(0, CHUNKS - 1, lambda c, v: block(c, v, LANES, LANES), (zero, zero, zero))
            mass, pp, qp = block(CHUNKS - 1, carry, TAIL_P, TAIL)
            stat[row:row + 1, :] = jnp.sum(mass, axis=0, keepdims=True)
            stat[6 + row:7 + row, :] = jnp.sum(pp, axis=0, keepdims=True)
            stat[12 + row:13 + row, :] = jnp.sum(qp, axis=0, keepdims=True)

    ecp = pltpu.make_async_copy(exbuf, ex_hbm, lsem.at[0])
    ecp.start()
    copies = reduce_stage(a2, slot, 8, sa2, ra2, near, stat[0:STAT, :])
    with scope('round2a'):
        parts = finish(copies, a2)
    copies = reduce_stage(b2, grp, 16, sb2, rb2, far, merge_add(parts))
    with scope('round2b'):
        parts = finish(copies, b2)
    tot = merge_add(parts)
    acc = jnp.minimum(tot[6:12] / tot[12:18], 1.0)
    for i in range(DRAFT):
        for t in range(BT):
            row = i * BT + t
            mass_ref[i:i + 1, t * LANES:(t + 1) * LANES] = tot[row:row + 1]
            acc_ref[i:i + 1, t * LANES:(t + 1) * LANES] = acc[row:row + 1]
    with scope('tail'):
        ecp.wait()
        bcp.wait()
        for cp in c0 + c1 + c2 + d2d:
            cp.wait_send()
        for i in range(DRAFT):
            part = send.at[i, pl.ds(0, (DEV - 1) * BLK)]
            pltpu.make_async_copy(part, part, qs_sem.at[i]).wait()


def verify_local(hid, w_cols, q_rows, draft_tok):
    q = with_layout_constraint(q_rows.reshape(SEQ, DRAFT, TILES, LANES), Layout((0, 2, 1, 3)))
    q = q.transpose(0, 2, 1, 3).reshape(SEQ * TILES * DRAFT, 1, LANES)
    f32 = jnp.float32
    hbm = pl.BlockSpec(memory_space=pl.ANY)
    vmem = pl.BlockSpec(memory_space=pltpu.VMEM)
    dma = pltpu.SemaphoreType.DMA
    ex, bo, fac, mass, acc = pl.pallas_call(
        kernel,
        out_shape=[
            jax.ShapeDtypeStruct((SHARD * BT * DRAFT, 1, LANES), f32),
            jax.ShapeDtypeStruct((ROWS_P, BATCH), f32),
            jax.ShapeDtypeStruct((DRAFT, BATCH), f32),
            jax.ShapeDtypeStruct((DRAFT, BATCH), f32),
            jax.ShapeDtypeStruct((DRAFT, BATCH), f32),
        ],
        in_specs=[pl.BlockSpec(memory_space=pltpu.HBM)] * 3 + [vmem],
        out_specs=[hbm, hbm, vmem, vmem, vmem],
        scratch_shapes=[
            pltpu.VMEM((SEQ * TILES * DRAFT + 20, 1, LANES), f32),
            pltpu.VMEM((SHARD, DIM), jnp.bfloat16),
            pltpu.VMEM((SEQ, NPOS, DIM), jnp.bfloat16),
            pltpu.VMEM((DEV * HROWS, LANES), jnp.bfloat16),
            pltpu.VMEM((48 * PITCH, LANES), f32),
            pltpu.VMEM((COLS_P, DIM), jnp.bfloat16),
            pltpu.VMEM((ROWS_P, COLS_P), f32),
            pltpu.VMEM((DRAFT, DEV * BLK, LANES), f32),
            pltpu.VMEM((DRAFT, DEV * BLK, LANES), f32),
            pltpu.VMEM((SHARD * BT * DRAFT, 1, LANES), f32),
            pltpu.VMEM((24, LANES), f32),
            pltpu.VMEM((16, LANES), f32),
            pltpu.VMEM((8 * STAT, 1, LANES), f32),
            pltpu.VMEM((16 * STAT, 1, LANES), f32),
            pltpu.VMEM((8 * STAT, 1, LANES), f32),
            pltpu.VMEM((16 * STAT, 1, LANES), f32),
            dma((3,)),
            dma((3, 3, 3)), dma((3, 3, 3)), dma((3,)), dma((3,)),
            dma((2,)), dma((2,)),
            dma((7,)), dma((7,)), dma((15,)), dma((15,)),
            dma((7,)), dma((7,)), dma((15,)), dma((15,)),
        ],
        compiler_params=pltpu.CompilerParams(vmem_limit_bytes=40 * 2 ** 20, has_side_effects=True, collective_id=0),
    )(*(pltpu.with_memory_space_constraint(x, pltpu.HBM) for x in (q, w_cols.T, hid, draft_tok.T)))
    ex = with_layout_constraint(ex.reshape(SHARD, BT, DRAFT, LANES).transpose(0, 2, 1, 3), Layout((0, 2, 1, 3)))
    residual = (ex.reshape(SHARD, DRAFT, BATCH) / mass[None]).transpose(2, 1, 0)
    bonus = (bo[:SHARD] * fac[:1]).T
    expected = acc[0] * (1.0 + acc[1])
    return acc.T, expected, residual, bonus


def solution(mesh):
    return jax.shard_map(
        verify_local,
        mesh=mesh,
        in_specs=(P(('dp', 'tp'), None, None), P(None, 'tp'), P(('dp', 'tp'), None, None), P('dp', None)),
        out_specs=(P('dp', None), P('dp'), P('dp', None, 'tp'), P('dp', 'tp')),
        check_vma=False,
    )
```

```python
import jax
import jax.numpy as jnp
from jax import lax
from jax.experimental import pallas as pl
from jax.experimental.layout import Layout, with_layout_constraint
from jax.experimental.pallas import tpu as pltpu
from jax.sharding import PartitionSpec as P

INV_TEMP = 1.25
DEV = 128
SEQ = 3
NPOS = 3
DRAFT = 2
BATCH = 384
DIM = 2048
VOCAB = 128256
SHARD = VOCAB // DEV
LANES = 128
TILES = VOCAB // LANES
CHUNKS = 8
TAIL = SHARD - (CHUNKS - 1) * LANES
ROWS_P = 1008
TAIL_P = ROWS_P - (CHUNKS - 1) * LANES
KC = DIM // LANES
HROWS = SEQ * NPOS * KC
COLS = NPOS * BATCH
COLS_P = 1280
CT = COLS // LANES
BT = BATCH // LANES
BLK = SEQ * CHUNKS
PITCH = 49
NEG = -1e30
STAT = 18
MESH = pl.DeviceIdType.MESH


def remote(src, dst, ssem, rsem, dev):
    return pltpu.make_async_remote_copy(
        src_ref=src, dst_ref=dst, send_sem=ssem, recv_sem=rsem,
        device_id={'tp': dev}, device_id_type=MESH)


def reduce_stage(buf, slot, count, ssem, rsem, device, payload):
    buf.reshape(count * STAT, LANES)[pl.ds(slot * STAT, STAT), :] = payload
    here = buf.at[pl.ds(slot * STAT, STAT)]
    copies = []
    for r in range(1, count):
        cp = remote(here, here, ssem.at[r - 1], rsem.at[r - 1], device((slot + r) % count))
        cp.start()
        copies.append(cp)
    return copies


def finish(copies, buf):
    for cp in copies:
        cp.wait()
    count = len(copies) + 1
    rows = buf.reshape(count * STAT, LANES)
    return [rows[k * STAT:(k + 1) * STAT, :] for k in range(count)]


def merge_max_sum(parts):
    m = parts[0][0:CT]
    for p in parts[1:]:
        m = jnp.maximum(m, p[0:CT])
    s = parts[0][CT:2 * CT] * jnp.exp(parts[0][0:CT] - m)
    for p in parts[1:]:
        s = s + p[CT:2 * CT] * jnp.exp(p[0:CT] - m)
    return jnp.concatenate([m, s], axis=0)


def merge_add(parts):
    total = parts[0]
    for p in parts[1:]:
        total = total + p
    return total


def kernel(q_hbm, w_hbm, h_hbm, tok_hbm,
           ex_hbm, bo_hbm, out_ref,
           tok_ref, qbuf, wbuf, hloc, hidb, bounce, hmat, z, send, recv, exbuf, stat, scale,
           a1, b1, a2, b2,
           lsem, ag_s, ag_r, d2d_s, d2d_r, qs_sem, qr_sem,
           sa1, ra1, sb1, rb1, sa2, ra2, sb2, rb2):
    scope = jax.named_scope
    me = lax.axis_index('tp')
    core = me % 2
    coord = (me // 32, (me // 8) % 4, (me // 2) % 4)
    unit = (32, 8, 2)
    partner = me + 1 - 2 * core
    hop = [[((coord[d] + r) % 4) * unit[d] for r in range(4)] for d in range(3)]

    def device(rz, ry, rx, rc):
        return hop[0][rz] + hop[1][ry] + hop[2][rx] + (core if rc == 0 else 1 - core)

    hcp = pltpu.make_async_copy(h_hbm, hloc, lsem.at[2])
    hcp.start()
    qcp = pltpu.make_async_copy(q_hbm, qbuf.at[pl.ds(0, SEQ * TILES * DRAFT)], lsem.at[0])
    qcp.start()
    wcp = pltpu.make_async_copy(w_hbm, wbuf, lsem.at[1])
    wcp.start()
    tcp = pltpu.make_async_copy(tok_hbm, tok_ref, lsem.at[3])
    tcp.start()
    barrier = pltpu.get_barrier_semaphore()
    peers = [partner]
    for d in range(3):
        for r in range(1, 4):
            steps = [0, 0, 0]
            steps[d] = r
            peers.append(device(*steps, 0))
    for dev in peers:
        pl.semaphore_signal(barrier, inc=1, device_id={'tp': dev}, device_id_type=MESH)

    with scope('hid'):
        hcp.wait()
        for s in range(SEQ):
            x = hloc[s].astype(jnp.float32)
            for kc in range(KC):
                bounce[pl.ds(s * 48 + kc, NPOS, stride=KC), :] = x[:, kc * LANES:(kc + 1) * LANES]
        hidb[pl.ds(pl.multiple_of(me * HROWS, 16), HROWS), :] = bounce[0:HROWS, :].astype(jnp.bfloat16)
    with scope('barrier'):
        pl.semaphore_wait(barrier, len(peers))

    hview = hidb.reshape(4, 4, 4, 2, SEQ, HROWS // SEQ, LANES)

    def ag_phase(phase):
        out = []
        for j in range(3):
            order = [(j + k) % 3 for k in range(3)]
            idx = list(coord)
            for d in order[:phase]:
                idx[d] = slice(None)
            view = hview.at[idx[0], idx[1], idx[2], core, j]
            for r in (1, 3, 2):
                steps = [0, 0, 0]
                steps[order[phase]] = r
                cp = remote(view, view, ag_s.at[phase, j, r - 1], ag_r.at[phase, j, r - 1], device(*steps, 0))
                cp.start()
                out.append(cp)
        return out

    qrows = qbuf.reshape(qbuf.shape[0], LANES)
    lane = lax.broadcasted_iota(jnp.int32, (8, LANES), 1)

    def pack(k, carry):
        first = (SHARD * k) // LANES
        off = (SHARD * k) % LANES
        shift = (LANES - off) % LANES
        keep = lane < LANES - off
        for i in range(DRAFT):
            for s in range(SEQ):
                base = (s * TILES + first) * DRAFT + i
                lo = qrows[pl.ds(base, 8, stride=2), :]
                hi = qrows[pl.ds(base + 2, 8, stride=2), :]
                lo = pltpu.roll(lo, shift, 1)
                hi = pltpu.roll(hi, shift, 1)
                send[i, pl.ds(pl.multiple_of(k * BLK + s * 8, 8), 8), :] = jnp.where(keep, lo, hi)
        return carry

    mine = pl.ds(pl.multiple_of(me * BLK, 8), BLK)

    def to(i, dev):
        remote(send.at[i, pl.ds(pl.multiple_of(dev * BLK, 8), BLK)], recv.at[i, mine],
               qs_sem.at[i], qr_sem.at[i], dev).start()

    def step(d, n):
        return ((coord[d] + n) % 4) * unit[d]

    def class0(i):
        pltpu.make_async_copy(send.at[i, mine], recv.at[i, mine], qr_sem.at[i]).start()
        to(i, partner)

    def class1(i, rc):
        last = core if rc == 0 else 1 - core
        for r in (1, 3, 2):
            for d in range(3):
                steps = [0, 0, 0]
                steps[d] = r
                to(i, device(*steps, rc))

    def class2(i, rc):
        last = core if rc == 0 else 1 - core

        def body(n, carry):
            a, b = n // 3 + 1, n % 3 + 1
            to(i, step(0, a) + step(1, b) + hop[2][0] + last)
            to(i, hop[0][0] + step(1, a) + step(2, b) + last)
            to(i, step(0, b) + hop[1][0] + step(2, a) + last)
            return carry

        lax.fori_loop(0, 9, body, 0)

    def class3(i, rc):
        last = core if rc == 0 else 1 - core

        def body(n, carry):
            a, b = n // 3, n % 3
            for k in range(3):
                to(i, step(0, (a + k) % 3 + 1) + step(1, (b + k) % 3 + 1) + hop[2][k + 1] + last)
            return carry

        lax.fori_loop(0, 9, body, 0)

    c0 = ag_phase(0)
    with scope('qwait'):
        qcp.wait()
    with scope('pack'):
        lax.fori_loop(0, DEV, pack, 0, unroll=8)
    with scope('ex0'):
        class0(0)
        class1(0, 0)
    with scope('ag0'):
        for cp in c0:
            cp.wait_recv()
    c1 = ag_phase(1)
    with scope('ex0a'):
        class1(0, 1)
        class2(0, 0)
    with scope('ag1'):
        for cp in c1:
            cp.wait_recv()
    c2 = ag_phase(2)
    with scope('ex0'):
        class2(0, 1)
    d2d = []
    for j in range(3):
        with scope(f'ag2_{j}'):
            for cp in c2[3 * j:3 * j + 3]:
                cp.wait_recv()
        view = hview.at[:, :, :, core, j]
        cp = remote(view, view, d2d_s.at[j], d2d_r.at[j], partner)
        cp.start()
        d2d.append(cp)
    with scope('ex0b'):
        class3(0, 0)
        class3(0, 1)
        class0(1)
        class1(1, 0)
        class1(1, 1)
    with scope('d2d'):
        for cp in d2d:
            cp.wait_recv()

    def relayout(n, carry):
        def up(b, c):
            x = hidb[pl.ds(pl.multiple_of((48 * n + b) * 48, 16), 48), :]
            bounce[pl.ds(b * PITCH, 48), :] = x.astype(jnp.float32)
            return c

        lax.fori_loop(0, 48, up, 0, unroll=4)
        for g in range(NPOS):
            for u in range(3):
                for kc in range(KC):
                    y = bounce[pl.ds(16 * u * PITCH + g * KC + kc, 16, stride=PITCH), :]
                    hmat[pl.ds(pl.multiple_of(g * BATCH + 48 * n + 16 * u, 16), 16),
                         kc * LANES:(kc + 1) * LANES] = y.astype(jnp.bfloat16)
        return carry

    with scope('relayout'):
        lax.fori_loop(0, 8, relayout, 0)
    wcp.wait()
    tcp.wait()

    z[SHARD:ROWS_P, :] = jnp.full((ROWS_P - SHARD, COLS_P), NEG, jnp.float32)

    def head(n, carry):
        hb = hmat[pl.ds(pl.multiple_of(n * 256, 256), 256), :]
        zt = lax.dot_general(wbuf[...], hb, (((1,), (1,)), ((), ())), preferred_element_type=jnp.float32)
        z[0:SHARD, pl.ds(pl.multiple_of(n * 256, 256), 256)] = zt * INV_TEMP
        return carry

    with scope('head'):
        lax.fori_loop(0, COLS_P // 256, head, 0)

    def local_stats(t, carry):
        cols = pl.ds(pl.multiple_of(t * LANES, LANES), LANES)

        def peak(n, m):
            x = z[pl.ds(pl.multiple_of(n * 112, 8), 112), cols]
            return jnp.maximum(m, jnp.max(x.reshape(14, 8, LANES), axis=0))

        m8 = lax.fori_loop(0, 9, peak, jnp.full((8, LANES), NEG, jnp.float32))
        m = jnp.max(m8, axis=0, keepdims=True)

        def expo(n, s):
            rows = pl.ds(pl.multiple_of(n * 112, 8), 112)
            x = jnp.exp(z[rows, cols] - m)
            z[rows, cols] = x
            return s + jnp.sum(x.reshape(14, 8, LANES), axis=0)

        s8 = lax.fori_loop(0, 9, expo, jnp.zeros((8, LANES), jnp.float32))
        stat[pl.ds(t, 1), :] = m
        stat[pl.ds(CT + t, 1), :] = jnp.sum(s8, axis=0, keepdims=True)
        return carry

    stat[...] = jnp.zeros_like(stat)
    with scope('stats'):
        lax.fori_loop(0, CT, local_stats, 0)
    bcp = pltpu.make_async_copy(z.at[:, DRAFT * BATCH:COLS], bo_hbm, lsem.at[2])
    bcp.start()

    slot, grp = me % 8, me // 8
    near = lambda k: grp * 8 + k
    far = lambda k: k * 8 + slot
    local = stat[0:STAT, :]
    copies = reduce_stage(a1, slot, 8, sa1, ra1, near, local)
    with scope('ex1a'):
        class2(1, 0)
    with scope('round1a'):
        parts = finish(copies, a1)
    copies = reduce_stage(b1, grp, 16, sb1, rb1, far, merge_max_sum(parts))
    with scope('ex1b'):
        class2(1, 1)
    with scope('round1b'):
        parts = finish(copies, b1)
    with scope('ex1c'):
        class3(1, 0)
        class3(1, 1)
    tot = merge_max_sum(parts)
    fac = jnp.exp(local[0:CT] - tot[0:CT]) / tot[CT:2 * CT]
    scale[0:CT, :] = fac
    out_ref[12:16, :] = jnp.concatenate([fac[DRAFT * BT:CT], fac[0:1]], axis=0)

    exrows = exbuf.reshape(exbuf.shape[0], LANES)
    first_id = me * SHARD
    stat[...] = jnp.zeros_like(stat)
    for i in range(DRAFT):
        with scope(f'a2a_{i}'):
            pltpu.make_async_copy(recv.at[i], recv.at[i], qr_sem.at[i]).wait()
        for t in range(BT):
            row = i * BT + t
            sc = scale[row:row + 1, :]
            tok = tok_ref[i:i + 1, t * LANES:(t + 1) * LANES] - first_id
            col0 = i * BATCH + t * LANES

            def block(c, carry, size, valid):
                mass, pp, qp = carry
                q = recv[i, pl.ds(t * LANES * CHUNKS + c, LANES, stride=CHUNKS), :].T
                p = z[pl.ds(pl.multiple_of(c * LANES, LANES), size), col0:col0 + LANES] * sc
                ids = lax.broadcasted_iota(jnp.int32, (size, LANES), 0)
                q = q[0:size]
                if valid < size:
                    q = jnp.where(ids < valid, q, 0.0)
                x = jnp.maximum(p - q, 0.0)
                exrows[pl.ds(c * LANES * 6 + t * 2 + i, valid, stride=6), :] = x[0:valid]
                hit = ids == tok - c * LANES
                fold = lambda v: jnp.sum(v.reshape(size // 8, 8, LANES), axis=0)
                return (mass + fold(x), pp + fold(jnp.where(hit, p, 0.0)), qp + fold(jnp.where(hit, q, 0.0)))

            zero = jnp.zeros((8, LANES), jnp.float32)
            carry = lax.fori_loop(0, CHUNKS - 1, lambda c, v: block(c, v, LANES, LANES), (zero, zero, zero))
            mass, pp, qp = block(CHUNKS - 1, carry, TAIL_P, TAIL)
            stat[row:row + 1, :] = jnp.sum(mass, axis=0, keepdims=True)
            stat[6 + row:7 + row, :] = jnp.sum(pp, axis=0, keepdims=True)
            stat[12 + row:13 + row, :] = jnp.sum(qp, axis=0, keepdims=True)

    ecp = pltpu.make_async_copy(exbuf, ex_hbm, lsem.at[0])
    ecp.start()
    copies = reduce_stage(a2, slot, 8, sa2, ra2, near, stat[0:STAT, :])
    with scope('round2a'):
        parts = finish(copies, a2)
    copies = reduce_stage(b2, grp, 16, sb2, rb2, far, merge_add(parts))
    with scope('round2b'):
        parts = finish(copies, b2)
    tot = merge_add(parts)
    out_ref[0:6, :] = tot[0:6]
    out_ref[6:12, :] = jnp.minimum(tot[6:12] / tot[12:18], 1.0)
    with scope('tail'):
        ecp.wait()
        bcp.wait()
        for cp in c0 + c1 + c2 + d2d:
            cp.wait_send()
        for i in range(DRAFT):
            part = send.at[i, pl.ds(0, (DEV - 1) * BLK)]
            pltpu.make_async_copy(part, part, qs_sem.at[i]).wait()


def finish_kernel(ex_ref, bo_ref, stat_ref, res_hbm, bonus_hbm, acc_ref, exp_ref, res, bonus, sems):
    rows = ex_ref.reshape(ex_ref.shape[0], LANES)
    out = res.reshape(res.shape[0], LANES)
    copies = []
    fac = jnp.concatenate([stat_ref[12 + t:13 + t, :] for t in range(BT)], axis=1)
    step = 256
    for n in range(4):
        size = min(step, SHARD - n * step)
        bonus[n * step:n * step + size, :] = bo_ref[n * step:n * step + size, :] * fac
    cp = pltpu.make_async_copy(bonus, bonus_hbm, sems.at[0])
    cp.start()
    copies.append(cp)
    mass = jnp.concatenate([stat_ref[i * BT + t:i * BT + t + 1, :] for t in range(BT) for i in range(DRAFT)], axis=0)
    mass = jnp.concatenate([mass] * 4, axis=0)
    for n in range(5):
        def body(k, carry):
            at = pl.ds(pl.multiple_of(n * 1200 + k * 24, 8), 24)
            out[at, :] = rows[at, :] / mass
            return carry

        lax.fori_loop(0, 50, body, 0, unroll=5)
        size = 1200
        if n == 4:
            out[6000:6012, :] = rows[6000:6012, :] / mass[0:12]
            size = 1212
        cp = pltpu.make_async_copy(res.at[pl.ds(n * 1200, size)], res_hbm.at[pl.ds(n * 1200, size)], sems.at[1 + n])
        cp.start()
        copies.append(cp)
    acc = stat_ref[6:12, :]
    more = acc[0:BT] * (1.0 + acc[BT:2 * BT])
    for t in range(BT):
        cols = slice(t * LANES, (t + 1) * LANES)
        exp_ref[cols] = more[t]
        for i in range(DRAFT):
            acc_ref[i:i + 1, cols] = acc[i * BT + t:i * BT + t + 1]
    for cp in copies:
        cp.wait()


def verify_local(hid, w_cols, q_rows, draft_tok):
    q = with_layout_constraint(q_rows.reshape(SEQ, DRAFT, TILES, LANES), Layout((0, 2, 1, 3)))
    q = q.transpose(0, 2, 1, 3).reshape(SEQ * TILES * DRAFT, 1, LANES)
    f32 = jnp.float32
    hbm = pl.BlockSpec(memory_space=pl.ANY)
    vmem = pl.BlockSpec(memory_space=pltpu.VMEM)
    dma = pltpu.SemaphoreType.DMA
    ex, bo, st = pl.pallas_call(
        kernel,
        out_shape=[
            jax.ShapeDtypeStruct((SHARD * BT * DRAFT, 1, LANES), f32),
            jax.ShapeDtypeStruct((ROWS_P, BATCH), f32),
            jax.ShapeDtypeStruct((16, LANES), f32),
        ],
        in_specs=[pl.BlockSpec(memory_space=pltpu.HBM)] * 4,
        out_specs=[hbm, hbm, vmem],
        scratch_shapes=[
            pltpu.VMEM((DRAFT, BATCH), jnp.int32),
            pltpu.VMEM((SEQ * TILES * DRAFT + 20, 1, LANES), f32),
            pltpu.VMEM((SHARD, DIM), jnp.bfloat16),
            pltpu.VMEM((SEQ, NPOS, DIM), jnp.bfloat16),
            pltpu.VMEM((DEV * HROWS, LANES), jnp.bfloat16),
            pltpu.VMEM((48 * PITCH, LANES), f32),
            pltpu.VMEM((COLS_P, DIM), jnp.bfloat16),
            pltpu.VMEM((ROWS_P, COLS_P), f32),
            pltpu.VMEM((DRAFT, DEV * BLK, LANES), f32),
            pltpu.VMEM((DRAFT, DEV * BLK, LANES), f32),
            pltpu.VMEM((SHARD * BT * DRAFT, 1, LANES), f32),
            pltpu.VMEM((24, LANES), f32),
            pltpu.VMEM((16, LANES), f32),
            pltpu.VMEM((8 * STAT, 1, LANES), f32),
            pltpu.VMEM((16 * STAT, 1, LANES), f32),
            pltpu.VMEM((8 * STAT, 1, LANES), f32),
            pltpu.VMEM((16 * STAT, 1, LANES), f32),
            dma((4,)),
            dma((3, 3, 3)), dma((3, 3, 3)), dma((3,)), dma((3,)),
            dma((2,)), dma((2,)),
            dma((7,)), dma((7,)), dma((15,)), dma((15,)),
            dma((7,)), dma((7,)), dma((15,)), dma((15,)),
        ],
        compiler_params=pltpu.CompilerParams(vmem_limit_bytes=40 * 2 ** 20, has_side_effects=True, collective_id=0),
    )(*(pltpu.with_memory_space_constraint(x, pltpu.HBM) for x in (q, w_cols.T, hid, draft_tok.T)))
    res, bonus, acc, expected = pl.pallas_call(
        finish_kernel,
        out_shape=[
            jax.ShapeDtypeStruct((SHARD * BT * DRAFT, 1, LANES), f32),
            jax.ShapeDtypeStruct((SHARD, BATCH), f32),
            jax.ShapeDtypeStruct((DRAFT, BATCH), f32),
            jax.ShapeDtypeStruct((BATCH,), f32),
        ],
        in_specs=[vmem] * 3,
        out_specs=[hbm, hbm, vmem, vmem],
        scratch_shapes=[
            pltpu.VMEM((SHARD * BT * DRAFT, 1, LANES), f32),
            pltpu.VMEM((SHARD, BATCH), f32),
            dma((6,)),
        ],
        compiler_params=pltpu.CompilerParams(vmem_limit_bytes=12 * 2 ** 20),
    )(ex, bo, st)
    res = with_layout_constraint(res.reshape(SHARD, BT, DRAFT, LANES).transpose(0, 2, 1, 3), Layout((0, 2, 1, 3)))
    residual = res.reshape(SHARD, DRAFT, BATCH).transpose(2, 1, 0)
    return acc.T, expected, residual, bonus.T


def solution(mesh):
    return jax.shard_map(
        verify_local,
        mesh=mesh,
        in_specs=(P(('dp', 'tp'), None, None), P(None, 'tp'), P(('dp', 'tp'), None, None), P('dp', None)),
        out_specs=(P('dp', None), P('dp'), P('dp', None, 'tp'), P('dp', 'tp')),
        check_vma=False,
    )
```

```python
import jax
import jax.numpy as jnp
from jax import lax
from jax.experimental import pallas as pl
from jax.experimental.layout import Layout, with_layout_constraint
from jax.experimental.pallas import tpu as pltpu
from jax.sharding import PartitionSpec as P

INV_TEMP = 1.25
DEV = 128
SEQ = 3
NPOS = 3
DRAFT = 2
BATCH = 384
DIM = 2048
VOCAB = 128256
SHARD = VOCAB // DEV
LANES = 128
TILES = VOCAB // LANES
CHUNKS = 8
TAIL = SHARD - (CHUNKS - 1) * LANES
ROWS_P = 1008
TAIL_P = ROWS_P - (CHUNKS - 1) * LANES
KC = DIM // LANES
HROWS = SEQ * NPOS * KC
COLS = NPOS * BATCH
COLS_P = 1280
CT = COLS // LANES
BT = BATCH // LANES
BLK = SEQ * CHUNKS
PITCH = 49
NEG = -1e30
STAT = 18
MESH = pl.DeviceIdType.MESH


def remote(src, dst, ssem, rsem, dev):
    return pltpu.make_async_remote_copy(
        src_ref=src, dst_ref=dst, send_sem=ssem, recv_sem=rsem,
        device_id={'tp': dev}, device_id_type=MESH)


def reduce_stage(buf, slot, count, ssem, rsem, device, payload):
    buf.reshape(count * STAT, LANES)[pl.ds(slot * STAT, STAT), :] = payload
    here = buf.at[pl.ds(slot * STAT, STAT)]
    copies = []
    for r in range(1, count):
        cp = remote(here, here, ssem.at[r - 1], rsem.at[r - 1], device((slot + r) % count))
        cp.start()
        copies.append(cp)
    return copies


def finish(copies, buf):
    for cp in copies:
        cp.wait()
    count = len(copies) + 1
    rows = buf.reshape(count * STAT, LANES)
    return [rows[k * STAT:(k + 1) * STAT, :] for k in range(count)]


def merge_max_sum(parts):
    m = parts[0][0:CT]
    for p in parts[1:]:
        m = jnp.maximum(m, p[0:CT])
    s = parts[0][CT:2 * CT] * jnp.exp(parts[0][0:CT] - m)
    for p in parts[1:]:
        s = s + p[CT:2 * CT] * jnp.exp(p[0:CT] - m)
    return jnp.concatenate([m, s], axis=0)


def merge_add(parts):
    total = parts[0]
    for p in parts[1:]:
        total = total + p
    return total


def kernel(q_hbm, w_hbm, h_hbm, tok_hbm,
           ex_hbm, bo_hbm, out_ref,
           tok_ref, qbuf, wbuf, hloc, hidb, bounce, hmat, z, send, recv, exbuf, stat, peak, scale,
           a1, b1, a2, b2,
           lsem, ag_s, ag_r, d2d_s, d2d_r, qs_sem, qr_sem,
           sa1, ra1, sb1, rb1, sa2, ra2, sb2, rb2):
    scope = jax.named_scope
    me = lax.axis_index('tp')
    core = me % 2
    coord = (me // 32, (me // 8) % 4, (me // 2) % 4)
    unit = (32, 8, 2)
    partner = me + 1 - 2 * core
    hop = [[((coord[d] + r) % 4) * unit[d] for r in range(4)] for d in range(3)]

    def device(rz, ry, rx, rc):
        return hop[0][rz] + hop[1][ry] + hop[2][rx] + (core if rc == 0 else 1 - core)

    hcp = pltpu.make_async_copy(h_hbm, hloc, lsem.at[2])
    hcp.start()
    qcp = pltpu.make_async_copy(q_hbm, qbuf.at[pl.ds(0, SEQ * TILES * DRAFT)], lsem.at[0])
    qcp.start()
    wcp = pltpu.make_async_copy(w_hbm, wbuf, lsem.at[1])
    wcp.start()
    tcp = pltpu.make_async_copy(tok_hbm, tok_ref, lsem.at[3])
    tcp.start()
    barrier = pltpu.get_barrier_semaphore()
    peers = [partner]
    for d in range(3):
        for r in range(1, 4):
            steps = [0, 0, 0]
            steps[d] = r
            peers.append(device(*steps, 0))
    for dev in peers:
        pl.semaphore_signal(barrier, inc=1, device_id={'tp': dev}, device_id_type=MESH)

    with scope('hid'):
        hcp.wait()
        for s in range(SEQ):
            x = hloc[s].astype(jnp.float32)
            for kc in range(KC):
                bounce[pl.ds(s * 48 + kc, NPOS, stride=KC), :] = x[:, kc * LANES:(kc + 1) * LANES]
        hidb[pl.ds(pl.multiple_of(me * HROWS, 16), HROWS), :] = bounce[0:HROWS, :].astype(jnp.bfloat16)
    with scope('barrier'):
        pl.semaphore_wait(barrier, len(peers))

    hview = hidb.reshape(4, 4, 4, 2, SEQ, HROWS // SEQ, LANES)

    def ag_phase(phase):
        out = []
        for j in range(3):
            order = [(j + k) % 3 for k in range(3)]
            idx = list(coord)
            for d in order[:phase]:
                idx[d] = slice(None)
            view = hview.at[idx[0], idx[1], idx[2], core, j]
            for r in (1, 3, 2):
                steps = [0, 0, 0]
                steps[order[phase]] = r
                cp = remote(view, view, ag_s.at[phase, j, r - 1], ag_r.at[phase, j, r - 1], device(*steps, 0))
                cp.start()
                out.append(cp)
        return out

    qrows = qbuf.reshape(qbuf.shape[0], LANES)
    lane = lax.broadcasted_iota(jnp.int32, (8, LANES), 1)

    def pack(k, carry):
        first = (SHARD * k) // LANES
        off = (SHARD * k) % LANES
        shift = (LANES - off) % LANES
        keep = lane < LANES - off
        for i in range(DRAFT):
            for s in range(SEQ):
                base = (s * TILES + first) * DRAFT + i
                lo = qrows[pl.ds(base, 8, stride=2), :]
                hi = qrows[pl.ds(base + 2, 8, stride=2), :]
                lo = pltpu.roll(lo, shift, 1)
                hi = pltpu.roll(hi, shift, 1)
                send[i, pl.ds(pl.multiple_of(k * BLK + s * 8, 8), 8), :] = jnp.where(keep, lo, hi)
        return carry

    mine = pl.ds(pl.multiple_of(me * BLK, 8), BLK)

    def to(i, dev):
        remote(send.at[i, pl.ds(pl.multiple_of(dev * BLK, 8), BLK)], recv.at[i, mine],
               qs_sem.at[i], qr_sem.at[i], dev).start()

    def step(d, n):
        return ((coord[d] + n) % 4) * unit[d]

    def class0(i):
        pltpu.make_async_copy(send.at[i, mine], recv.at[i, mine], qr_sem.at[i]).start()
        to(i, partner)

    def class1(i, rc):
        last = core if rc == 0 else 1 - core
        for r in (1, 3, 2):
            for d in range(3):
                steps = [0, 0, 0]
                steps[d] = r
                to(i, device(*steps, rc))

    def class2(i, rc, lo=0, hi=9):
        last = core if rc == 0 else 1 - core

        def body(n, carry):
            a, b = n // 3 + 1, n % 3 + 1
            to(i, step(0, a) + step(1, b) + hop[2][0] + last)
            to(i, hop[0][0] + step(1, a) + step(2, b) + last)
            to(i, step(0, b) + hop[1][0] + step(2, a) + last)
            return carry

        lax.fori_loop(lo, hi, body, 0)

    def class3(i, rc):
        last = core if rc == 0 else 1 - core

        def body(n, carry):
            a, b = n // 3, n % 3
            for k in range(3):
                to(i, step(0, (a + k) % 3 + 1) + step(1, (b + k) % 3 + 1) + hop[2][k + 1] + last)
            return carry

        lax.fori_loop(0, 9, body, 0)

    c0 = ag_phase(0)
    with scope('qwait'):
        qcp.wait()
    with scope('pack'):
        lax.fori_loop(0, DEV, pack, 0, unroll=8)
    with scope('ex0'):
        for i in range(DRAFT):
            class0(i)
            class1(i, 0)
    with scope('ag0'):
        for cp in c0:
            cp.wait_recv()
    c1 = ag_phase(1)
    with scope('ag1'):
        for cp in c1:
            cp.wait_recv()
    c2 = ag_phase(2)
    d2d = []
    for j in range(3):
        with scope(f'ag2_{j}'):
            for cp in c2[3 * j:3 * j + 3]:
                cp.wait_recv()
        view = hview.at[:, :, :, core, j]
        cp = remote(view, view, d2d_s.at[j], d2d_r.at[j], partner)
        cp.start()
        d2d.append(cp)
    with scope('ex0b'):
        class1(0, 1)
        class2(0, 0)
        class2(0, 1)
        class3(0, 0)
        class3(0, 1)
        class1(1, 1)
    with scope('d2d'):
        for cp in d2d:
            cp.wait_recv()

    def relayout(n, carry):
        def up(b, c):
            x = hidb[pl.ds(pl.multiple_of((48 * n + b) * 48, 16), 48), :]
            bounce[pl.ds(b * PITCH, 48), :] = x.astype(jnp.float32)
            return c

        lax.fori_loop(0, 48, up, 0, unroll=4)
        for g in range(NPOS):
            for u in range(3):
                for kc in range(KC):
                    y = bounce[pl.ds(16 * u * PITCH + g * KC + kc, 16, stride=PITCH), :]
                    hmat[pl.ds(pl.multiple_of(g * BATCH + 48 * n + 16 * u, 16), 16),
                         kc * LANES:(kc + 1) * LANES] = y.astype(jnp.bfloat16)
        return carry

    with scope('relayout'):
        lax.fori_loop(0, 8, relayout, 0)
    wcp.wait()
    tcp.wait()

    z[SHARD:ROWS_P, :] = jnp.full((ROWS_P - SHARD, COLS_P), NEG, jnp.float32)

    def head(n, carry):
        hb = hmat[pl.ds(pl.multiple_of(n * 256, 256), 256), :]
        zt = lax.dot_general(wbuf[...], hb, (((1,), (1,)), ((), ())), preferred_element_type=jnp.float32)
        zt = zt * INV_TEMP
        z[0:SHARD, pl.ds(pl.multiple_of(n * 256, 256), 256)] = zt
        top = jnp.max(zt, axis=0, keepdims=True)
        peak[pl.ds(2 * n, 1), :] = top[:, 0:LANES]
        peak[pl.ds(2 * n + 1, 1), :] = top[:, LANES:]
        return carry

    with scope('head'):
        lax.fori_loop(0, COLS_P // 256, head, 0)

    def local_stats(t, carry):
        cols = pl.ds(pl.multiple_of(t * LANES, LANES), LANES)

        m = peak[pl.ds(t, 1), :]

        def expo(n, s):
            rows = pl.ds(pl.multiple_of(n * 112, 8), 112)
            x = jnp.exp(z[rows, cols] - m)
            z[rows, cols] = x
            return s + jnp.sum(x.reshape(14, 8, LANES), axis=0)

        s8 = lax.fori_loop(0, 9, expo, jnp.zeros((8, LANES), jnp.float32))
        stat[pl.ds(t, 1), :] = m
        stat[pl.ds(CT + t, 1), :] = jnp.sum(s8, axis=0, keepdims=True)
        return carry

    stat[...] = jnp.zeros_like(stat)
    with scope('stats'):
        lax.fori_loop(0, CT, local_stats, 0)
    bcp = pltpu.make_async_copy(z.at[:, DRAFT * BATCH:COLS], bo_hbm, lsem.at[2])
    bcp.start()

    slot, grp = me % 8, me // 8
    near = lambda k: grp * 8 + k
    far = lambda k: k * 8 + slot
    local = stat[0:STAT, :]
    copies = reduce_stage(a1, slot, 8, sa1, ra1, near, local)
    with scope('ex1a'):
        class2(1, 0, 0, 3)
    with scope('round1a'):
        parts = finish(copies, a1)
    copies = reduce_stage(b1, grp, 16, sb1, rb1, far, merge_max_sum(parts))
    with scope('ex1b'):
        class2(1, 0, 3, 9)
    with scope('round1b'):
        parts = finish(copies, b1)
    with scope('ex1c'):
        class2(1, 1)
        class3(1, 0)
        class3(1, 1)
    tot = merge_max_sum(parts)
    fac = jnp.exp(local[0:CT] - tot[0:CT]) / tot[CT:2 * CT]
    scale[0:CT, :] = fac
    out_ref[12:16, :] = jnp.concatenate([fac[DRAFT * BT:CT], fac[0:1]], axis=0)

    exrows = exbuf.reshape(exbuf.shape[0], LANES)
    first_id = me * SHARD
    stat[...] = jnp.zeros_like(stat)
    for i in range(DRAFT):
        with scope(f'a2a_{i}'):
            pltpu.make_async_copy(recv.at[i], recv.at[i], qr_sem.at[i]).wait()
        for t in range(BT):
            row = i * BT + t
            sc = scale[row:row + 1, :]
            tok = tok_ref[i:i + 1, t * LANES:(t + 1) * LANES] - first_id
            col0 = i * BATCH + t * LANES

            def block(c, carry, size, valid):
                mass, pp, qp = carry
                q = recv[i, pl.ds(t * LANES * CHUNKS + c, LANES, stride=CHUNKS), :].T
                p = z[pl.ds(pl.multiple_of(c * LANES, LANES), size), col0:col0 + LANES] * sc
                ids = lax.broadcasted_iota(jnp.int32, (size, LANES), 0)
                q = q[0:size]
                if valid < size:
                    q = jnp.where(ids < valid, q, 0.0)
                x = jnp.maximum(p - q, 0.0)
                exrows[pl.ds(c * LANES * 6 + t * 2 + i, valid, stride=6), :] = x[0:valid]
                hit = ids == tok - c * LANES
                fold = lambda v: jnp.sum(v.reshape(size // 8, 8, LANES), axis=0)
                return (mass + fold(x), pp + fold(jnp.where(hit, p, 0.0)), qp + fold(jnp.where(hit, q, 0.0)))

            zero = jnp.zeros((8, LANES), jnp.float32)
            carry = lax.fori_loop(0, CHUNKS - 1, lambda c, v: block(c, v, LANES, LANES), (zero, zero, zero))
            mass, pp, qp = block(CHUNKS - 1, carry, TAIL_P, TAIL)
            stat[row:row + 1, :] = jnp.sum(mass, axis=0, keepdims=True)
            stat[6 + row:7 + row, :] = jnp.sum(pp, axis=0, keepdims=True)
            stat[12 + row:13 + row, :] = jnp.sum(qp, axis=0, keepdims=True)

    ecp = pltpu.make_async_copy(exbuf, ex_hbm, lsem.at[0])
    ecp.start()
    copies = reduce_stage(a2, slot, 8, sa2, ra2, near, stat[0:STAT, :])
    with scope('round2a'):
        parts = finish(copies, a2)
    copies = reduce_stage(b2, grp, 16, sb2, rb2, far, merge_add(parts))
    with scope('round2b'):
        parts = finish(copies, b2)
    tot = merge_add(parts)
    out_ref[0:6, :] = tot[0:6]
    out_ref[6:12, :] = jnp.minimum(tot[6:12] / tot[12:18], 1.0)
    with scope('tail'):
        ecp.wait()
        bcp.wait()
        for cp in c0 + c1 + c2 + d2d:
            cp.wait_send()
        for i in range(DRAFT):
            part = send.at[i, pl.ds(0, (DEV - 1) * BLK)]
            pltpu.make_async_copy(part, part, qs_sem.at[i]).wait()


def finish_kernel(ex_ref, bo_ref, stat_ref, res_hbm, bonus_hbm, acc_ref, exp_ref, res, bonus, sems):
    rows = ex_ref.reshape(ex_ref.shape[0], LANES)
    out = res.reshape(res.shape[0], LANES)
    copies = []
    fac = jnp.concatenate([stat_ref[12 + t:13 + t, :] for t in range(BT)], axis=1)
    step = 256
    for n in range(4):
        size = min(step, SHARD - n * step)
        bonus[n * step:n * step + size, :] = bo_ref[n * step:n * step + size, :] * fac
    cp = pltpu.make_async_copy(bonus, bonus_hbm, sems.at[0])
    cp.start()
    copies.append(cp)
    mass = jnp.concatenate([stat_ref[i * BT + t:i * BT + t + 1, :] for t in range(BT) for i in range(DRAFT)], axis=0)
    mass = jnp.concatenate([mass] * 4, axis=0)
    for n in range(5):
        def body(k, carry):
            at = pl.ds(pl.multiple_of(n * 1200 + k * 24, 8), 24)
            out[at, :] = rows[at, :] / mass
            return carry

        lax.fori_loop(0, 50, body, 0, unroll=5)
        size = 1200
        if n == 4:
            out[6000:6012, :] = rows[6000:6012, :] / mass[0:12]
            size = 1212
        cp = pltpu.make_async_copy(res.at[pl.ds(n * 1200, size)], res_hbm.at[pl.ds(n * 1200, size)], sems.at[1 + n])
        cp.start()
        copies.append(cp)
    acc = stat_ref[6:12, :]
    more = acc[0:BT] * (1.0 + acc[BT:2 * BT])
    for t in range(BT):
        cols = slice(t * LANES, (t + 1) * LANES)
        exp_ref[cols] = more[t]
        for i in range(DRAFT):
            acc_ref[i:i + 1, cols] = acc[i * BT + t:i * BT + t + 1]
    for cp in copies:
        cp.wait()


def verify_local(hid, w_cols, q_rows, draft_tok):
    q = with_layout_constraint(q_rows.reshape(SEQ, DRAFT, TILES, LANES), Layout((0, 2, 1, 3)))
    q = q.transpose(0, 2, 1, 3).reshape(SEQ * TILES * DRAFT, 1, LANES)
    f32 = jnp.float32
    hbm = pl.BlockSpec(memory_space=pl.ANY)
    vmem = pl.BlockSpec(memory_space=pltpu.VMEM)
    dma = pltpu.SemaphoreType.DMA
    ex, bo, st = pl.pallas_call(
        kernel,
        out_shape=[
            jax.ShapeDtypeStruct((SHARD * BT * DRAFT, 1, LANES), f32),
            jax.ShapeDtypeStruct((ROWS_P, BATCH), f32),
            jax.ShapeDtypeStruct((16, LANES), f32),
        ],
        in_specs=[pl.BlockSpec(memory_space=pltpu.HBM)] * 4,
        out_specs=[hbm, hbm, vmem],
        scratch_shapes=[
            pltpu.VMEM((DRAFT, BATCH), jnp.int32),
            pltpu.VMEM((SEQ * TILES * DRAFT + 20, 1, LANES), f32),
            pltpu.VMEM((SHARD, DIM), jnp.bfloat16),
            pltpu.VMEM((SEQ, NPOS, DIM), jnp.bfloat16),
            pltpu.VMEM((DEV * HROWS, LANES), jnp.bfloat16),
            pltpu.VMEM((48 * PITCH, LANES), f32),
            pltpu.VMEM((COLS_P, DIM), jnp.bfloat16),
            pltpu.VMEM((ROWS_P, COLS_P), f32),
            pltpu.VMEM((DRAFT, DEV * BLK, LANES), f32),
            pltpu.VMEM((DRAFT, DEV * BLK, LANES), f32),
            pltpu.VMEM((SHARD * BT * DRAFT, 1, LANES), f32),
            pltpu.VMEM((24, LANES), f32),
            pltpu.VMEM((16, LANES), f32),
            pltpu.VMEM((16, LANES), f32),
            pltpu.VMEM((8 * STAT, 1, LANES), f32),
            pltpu.VMEM((16 * STAT, 1, LANES), f32),
            pltpu.VMEM((8 * STAT, 1, LANES), f32),
            pltpu.VMEM((16 * STAT, 1, LANES), f32),
            dma((4,)),
            dma((3, 3, 3)), dma((3, 3, 3)), dma((3,)), dma((3,)),
            dma((2,)), dma((2,)),
            dma((7,)), dma((7,)), dma((15,)), dma((15,)),
            dma((7,)), dma((7,)), dma((15,)), dma((15,)),
        ],
        compiler_params=pltpu.CompilerParams(vmem_limit_bytes=40 * 2 ** 20, has_side_effects=True, collective_id=0),
    )(*(pltpu.with_memory_space_constraint(x, pltpu.HBM) for x in (q, w_cols.T, hid, draft_tok.T)))
    res, bonus, acc, expected = pl.pallas_call(
        finish_kernel,
        out_shape=[
            jax.ShapeDtypeStruct((SHARD * BT * DRAFT, 1, LANES), f32),
            jax.ShapeDtypeStruct((SHARD, BATCH), f32),
            jax.ShapeDtypeStruct((DRAFT, BATCH), f32),
            jax.ShapeDtypeStruct((BATCH,), f32),
        ],
        in_specs=[vmem] * 3,
        out_specs=[hbm, hbm, vmem, vmem],
        scratch_shapes=[
            pltpu.VMEM((SHARD * BT * DRAFT, 1, LANES), f32),
            pltpu.VMEM((SHARD, BATCH), f32),
            dma((6,)),
        ],
        compiler_params=pltpu.CompilerParams(vmem_limit_bytes=12 * 2 ** 20),
    )(ex, bo, st)
    res = with_layout_constraint(res.reshape(SHARD, BT, DRAFT, LANES).transpose(0, 2, 1, 3), Layout((0, 2, 1, 3)))
    residual = res.reshape(SHARD, DRAFT, BATCH).transpose(2, 1, 0)
    return acc.T, expected, residual, bonus.T


def solution(mesh):
    return jax.shard_map(
        verify_local,
        mesh=mesh,
        in_specs=(P(('dp', 'tp'), None, None), P(None, 'tp'), P(('dp', 'tp'), None, None), P('dp', None)),
        out_specs=(P('dp', None), P('dp'), P('dp', None, 'tp'), P('dp', 'tp')),
        check_vma=False,
    )
```

```python
import jax
import jax.numpy as jnp
from jax import lax
from jax.experimental import pallas as pl
from jax.experimental.layout import Layout, with_layout_constraint
from jax.experimental.pallas import tpu as pltpu
from jax.sharding import PartitionSpec as P

INV_TEMP = 1.25
DEV = 128
SEQ = 3
NPOS = 3
DRAFT = 2
BATCH = 384
DIM = 2048
VOCAB = 128256
SHARD = VOCAB // DEV
LANES = 128
TILES = VOCAB // LANES
CHUNKS = 8
TAIL = SHARD - (CHUNKS - 1) * LANES
ROWS_P = 1008
TAIL_P = ROWS_P - (CHUNKS - 1) * LANES
KC = DIM // LANES
HROWS = SEQ * NPOS * KC
COLS = NPOS * BATCH
COLS_P = 1280
CT = COLS // LANES
BT = BATCH // LANES
BLK = SEQ * CHUNKS
PITCH = 49
NEG = -1e30
STAT = 18
WINDOW = 16
CUTS = (7, 16, 22, 46, 52, 60)
HEAD = 3
MESH = pl.DeviceIdType.MESH


def remote(src, dst, ssem, rsem, dev):
    return pltpu.make_async_remote_copy(
        src_ref=src, dst_ref=dst, send_sem=ssem, recv_sem=rsem,
        device_id={'tp': dev}, device_id_type=MESH)


def reduce_stage(buf, slot, count, ssem, rsem, device, payload):
    buf.reshape(count * STAT, LANES)[pl.ds(slot * STAT, STAT), :] = payload
    here = buf.at[pl.ds(slot * STAT, STAT)]
    copies = []
    for r in range(1, count):
        cp = remote(here, here, ssem.at[r - 1], rsem.at[r - 1], device((slot + r) % count))
        cp.start()
        copies.append(cp)
    return copies


def finish(copies, buf):
    for cp in copies:
        cp.wait()
    count = len(copies) + 1
    rows = buf.reshape(count * STAT, LANES)
    return [rows[k * STAT:(k + 1) * STAT, :] for k in range(count)]


def merge_max_sum(parts):
    m = parts[0][0:CT]
    for p in parts[1:]:
        m = jnp.maximum(m, p[0:CT])
    s = parts[0][CT:2 * CT] * jnp.exp(parts[0][0:CT] - m)
    for p in parts[1:]:
        s = s + p[CT:2 * CT] * jnp.exp(p[0:CT] - m)
    return jnp.concatenate([m, s], axis=0)


def merge_add(parts):
    total = parts[0]
    for p in parts[1:]:
        total = total + p
    return total


def kernel(q_hbm, w_hbm, h_hbm, tok_hbm,
           ex_hbm, bo_hbm, out_ref,
           tok_ref, qbuf, wbuf, hloc, hidb, bounce, hmat, z, send, recv, exbuf, stat, peak, scale,
           a1, b1, a2, b2,
           lsem, ag_s, ag_r, d2d_s, d2d_r, qs_sem, qr_sem,
           sa1, ra1, sb1, rb1, sa2, ra2, sb2, rb2):
    scope = jax.named_scope
    me = lax.axis_index('tp')
    core = me % 2
    coord = (me // 32, (me // 8) % 4, (me // 2) % 4)
    unit = (32, 8, 2)
    partner = me + 1 - 2 * core
    hop = [[((coord[d] + r) % 4) * unit[d] for r in range(4)] for d in range(3)]

    def device(rz, ry, rx, rc):
        return hop[0][rz] + hop[1][ry] + hop[2][rx] + (core if rc == 0 else 1 - core)

    hcp = pltpu.make_async_copy(h_hbm, hloc, lsem.at[2])
    hcp.start()
    qcp = pltpu.make_async_copy(q_hbm, qbuf.at[pl.ds(0, SEQ * TILES * DRAFT)], lsem.at[0])
    qcp.start()
    wcp = pltpu.make_async_copy(w_hbm, wbuf, lsem.at[1])
    wcp.start()
    tcp = pltpu.make_async_copy(tok_hbm, tok_ref, lsem.at[3])
    tcp.start()
    barrier = pltpu.get_barrier_semaphore()
    peers = [partner]
    for d in range(3):
        for r in range(1, 4):
            steps = [0, 0, 0]
            steps[d] = r
            peers.append(device(*steps, 0))
    for dev in peers:
        pl.semaphore_signal(barrier, inc=1, device_id={'tp': dev}, device_id_type=MESH)

    with scope('hid'):
        hcp.wait()
        for s in range(SEQ):
            x = hloc[s].astype(jnp.float32)
            for kc in range(KC):
                bounce[pl.ds(s * 48 + kc, NPOS, stride=KC), :] = x[:, kc * LANES:(kc + 1) * LANES]
        hidb[pl.ds(pl.multiple_of(me * HROWS, 16), HROWS), :] = bounce[0:HROWS, :].astype(jnp.bfloat16)
    with scope('barrier'):
        pl.semaphore_wait(barrier, len(peers))

    hview = hidb.reshape(4, 4, 4, 2, SEQ, HROWS // SEQ, LANES)

    def ag_phase(phase):
        out = []
        for j in range(3):
            order = [(j + k) % 3 for k in range(3)]
            idx = list(coord)
            for d in order[:phase]:
                idx[d] = slice(None)
            view = hview.at[idx[0], idx[1], idx[2], core, j]
            for r in (1, 3, 2):
                steps = [0, 0, 0]
                steps[order[phase]] = r
                cp = remote(view, view, ag_s.at[phase, j, r - 1], ag_r.at[phase, j, r - 1], device(*steps, 0))
                cp.start()
                out.append(cp)
        return out

    qrows = qbuf.reshape(qbuf.shape[0], LANES)
    lane = lax.broadcasted_iota(jnp.int32, (8, LANES), 1)

    def pack(k, carry):
        first = (SHARD * k) // LANES
        off = (SHARD * k) % LANES
        shift = (LANES - off) % LANES
        keep = lane < LANES - off
        for i in range(DRAFT):
            for s in range(SEQ):
                base = (s * TILES + first) * DRAFT + i
                lo = qrows[pl.ds(base, 8, stride=2), :]
                hi = qrows[pl.ds(base + 2, 8, stride=2), :]
                lo = pltpu.roll(lo, shift, 1)
                hi = pltpu.roll(hi, shift, 1)
                send[i, pl.ds(pl.multiple_of(k * BLK + s * 8, 8), 8), :] = jnp.where(keep, lo, hi)
        return carry

    mine = pl.ds(pl.multiple_of(me * BLK, 8), BLK)

    def to(i, dev, n):
        cp = remote(send.at[i, pl.ds(pl.multiple_of(dev * BLK, 8), BLK)], recv.at[i, mine],
                    qs_sem.at[n % WINDOW], qr_sem.at[i], dev)
        if not isinstance(n, int) or n >= WINDOW:
            cp.wait_send()
        cp.start()

    def step(d, n):
        return ((coord[d] + n) % 4) * unit[d]

    def triples(lo, hi):
        def body(n, carry):
            i, u = n // 36, n % 36
            three, rc, v = u // 18, (u // 9) % 2, u % 9
            last = core + rc - 2 * core * rc
            a, b = v // 3, v % 3
            two = ((a + 1, b + 1, 0), (0, a + 1, b + 1), (b + 1, 0, a + 1))
            for k in range(3):
                full = ((a + k) % 3 + 1, (b + k) % 3 + 1, k + 1)
                r = [(1 - three) * two[k][d] + three * full[d] for d in range(3)]
                to(i, step(0, r[0]) + step(1, r[1]) + step(2, r[2]) + last, 38 + 3 * n + k)
            return carry

        lax.fori_loop(lo, hi, body, 0)

    def lines(rc, first):
        n = first
        for r in (1, 3, 2):
            for i in range(DRAFT):
                for d in range(3):
                    steps = [0, 0, 0]
                    steps[d] = r
                    to(i, device(*steps, rc), n)
                    n += 1

    c0 = ag_phase(0)
    with scope('qwait'):
        qcp.wait()
    with scope('pack'):
        lax.fori_loop(0, DEV, pack, 0, unroll=8)
    with scope('ex0'):
        for i in range(DRAFT):
            pltpu.make_async_copy(send.at[i, mine], recv.at[i, mine], qr_sem.at[i]).start()
            to(i, partner, i)
        lines(0, 2)
    with scope('ag0'):
        for cp in c0:
            cp.wait_recv()
    c1 = ag_phase(1)
    with scope('exag1'):
        lines(1, 20)
        triples(0, CUTS[0])
    with scope('ag1'):
        for cp in c1:
            cp.wait_recv()
    c2 = ag_phase(2)
    with scope('exag2'):
        triples(CUTS[0], CUTS[1])
    d2d = []
    for j in range(3):
        with scope(f'ag2_{j}'):
            for cp in c2[3 * j:3 * j + 3]:
                cp.wait_recv()
        view = hview.at[:, :, :, core, j]
        cp = remote(view, view, d2d_s.at[j], d2d_r.at[j], partner)
        cp.start()
        d2d.append(cp)
    with scope('exd2d'):
        triples(CUTS[1], CUTS[2])
    with scope('d2d'):
        for cp in d2d:
            cp.wait_recv()

    def relayout(n, carry):
        def up(b, c):
            x = hidb[pl.ds(pl.multiple_of((48 * n + b) * 48, 16), 48), :]
            bounce[pl.ds(b * PITCH, 48), :] = x.astype(jnp.float32)
            return c

        lax.fori_loop(0, 48, up, 0, unroll=4)
        for g in range(NPOS):
            for u in range(3):
                for kc in range(KC):
                    y = bounce[pl.ds(16 * u * PITCH + g * KC + kc, 16, stride=PITCH), :]
                    hmat[pl.ds(pl.multiple_of(g * BATCH + 48 * n + 16 * u, 16), 16),
                         kc * LANES:(kc + 1) * LANES] = y.astype(jnp.bfloat16)
        return carry

    with scope('relayout'):
        def spread(n, carry):
            lax.fori_loop(2 * n, 2 * n + 2, relayout, 0)
            triples(CUTS[2] + n, CUTS[2] + n + 1)
            return carry

        lax.fori_loop(0, 4, spread, 0)
    wcp.wait()
    tcp.wait()

    z[SHARD:ROWS_P, :] = jnp.full((ROWS_P - SHARD, COLS_P), NEG, jnp.float32)

    def head(n, carry):
        triples(CUTS[2] + 4 + HEAD * n, CUTS[2] + 4 + HEAD * (n + 1))
        hb = hmat[pl.ds(pl.multiple_of(n * 256, 256), 256), :]
        zt = lax.dot_general(wbuf[...], hb, (((1,), (1,)), ((), ())), preferred_element_type=jnp.float32)
        zt = zt * INV_TEMP
        z[0:SHARD, pl.ds(pl.multiple_of(n * 256, 256), 256)] = zt
        top = jnp.max(zt, axis=0, keepdims=True)
        peak[pl.ds(2 * n, 1), :] = top[:, 0:LANES]
        peak[pl.ds(2 * n + 1, 1), :] = top[:, LANES:]
        return carry

    with scope('head'):
        lax.fori_loop(0, COLS_P // 256, head, 0)

    def local_stats(t, carry):
        cols = pl.ds(pl.multiple_of(t * LANES, LANES), LANES)

        m = peak[pl.ds(t, 1), :]

        def expo(n, s):
            rows = pl.ds(pl.multiple_of(n * 112, 8), 112)
            x = jnp.exp(z[rows, cols] - m)
            z[rows, cols] = x
            return s + jnp.sum(x.reshape(14, 8, LANES), axis=0)

        s8 = lax.fori_loop(0, 9, expo, jnp.zeros((8, LANES), jnp.float32))
        stat[pl.ds(t, 1), :] = m
        stat[pl.ds(CT + t, 1), :] = jnp.sum(s8, axis=0, keepdims=True)
        return carry

    stat[...] = jnp.zeros_like(stat)
    done = CUTS[2] + 4 + HEAD * (COLS_P // 256)
    with scope('exst'):
        triples(done, CUTS[3])
    with scope('stats'):
        lax.fori_loop(0, CT, local_stats, 0)
    bcp = pltpu.make_async_copy(z.at[:, DRAFT * BATCH:COLS], bo_hbm, lsem.at[2])
    bcp.start()

    slot, grp = me % 8, me // 8
    near = lambda k: grp * 8 + k
    far = lambda k: k * 8 + slot
    local = stat[0:STAT, :]
    copies = reduce_stage(a1, slot, 8, sa1, ra1, near, local)
    with scope('ex1a'):
        triples(CUTS[3], CUTS[4])
    with scope('round1a'):
        parts = finish(copies, a1)
    copies = reduce_stage(b1, grp, 16, sb1, rb1, far, merge_max_sum(parts))
    with scope('ex1b'):
        triples(CUTS[4], CUTS[5])
    with scope('round1b'):
        parts = finish(copies, b1)
    with scope('ex1c'):
        triples(CUTS[5], 72)
    tot = merge_max_sum(parts)
    fac = jnp.exp(local[0:CT] - tot[0:CT]) / tot[CT:2 * CT]
    scale[0:CT, :] = fac
    out_ref[12:16, :] = jnp.concatenate([fac[DRAFT * BT:CT], fac[0:1]], axis=0)

    exrows = exbuf.reshape(exbuf.shape[0], LANES)
    first_id = me * SHARD
    stat[...] = jnp.zeros_like(stat)
    for i in range(DRAFT):
        with scope(f'a2a_{i}'):
            pltpu.make_async_copy(recv.at[i], recv.at[i], qr_sem.at[i]).wait()
        for t in range(BT):
            row = i * BT + t
            sc = scale[row:row + 1, :]
            tok = tok_ref[i:i + 1, t * LANES:(t + 1) * LANES] - first_id
            col0 = i * BATCH + t * LANES

            def block(c, carry, size, valid):
                mass, pp, qp = carry
                q = recv[i, pl.ds(t * LANES * CHUNKS + c, LANES, stride=CHUNKS), :].T
                p = z[pl.ds(pl.multiple_of(c * LANES, LANES), size), col0:col0 + LANES] * sc
                ids = lax.broadcasted_iota(jnp.int32, (size, LANES), 0)
                q = q[0:size]
                if valid < size:
                    q = jnp.where(ids < valid, q, 0.0)
                x = jnp.maximum(p - q, 0.0)
                exrows[pl.ds(c * LANES * 6 + t * 2 + i, valid, stride=6), :] = x[0:valid]
                hit = ids == tok - c * LANES
                fold = lambda v: jnp.sum(v.reshape(size // 8, 8, LANES), axis=0)
                return (mass + fold(x), pp + fold(jnp.where(hit, p, 0.0)), qp + fold(jnp.where(hit, q, 0.0)))

            zero = jnp.zeros((8, LANES), jnp.float32)
            carry = lax.fori_loop(0, CHUNKS - 1, lambda c, v: block(c, v, LANES, LANES), (zero, zero, zero))
            mass, pp, qp = block(CHUNKS - 1, carry, TAIL_P, TAIL)
            stat[row:row + 1, :] = jnp.sum(mass, axis=0, keepdims=True)
            stat[6 + row:7 + row, :] = jnp.sum(pp, axis=0, keepdims=True)
            stat[12 + row:13 + row, :] = jnp.sum(qp, axis=0, keepdims=True)

    ecp = pltpu.make_async_copy(exbuf, ex_hbm, lsem.at[0])
    ecp.start()
    copies = reduce_stage(a2, slot, 8, sa2, ra2, near, stat[0:STAT, :])
    with scope('round2a'):
        parts = finish(copies, a2)
    copies = reduce_stage(b2, grp, 16, sb2, rb2, far, merge_add(parts))
    with scope('round2b'):
        parts = finish(copies, b2)
    tot = merge_add(parts)
    out_ref[0:6, :] = tot[0:6]
    out_ref[6:12, :] = jnp.minimum(tot[6:12] / tot[12:18], 1.0)
    with scope('tail'):
        ecp.wait()
        bcp.wait()
        for cp in c0 + c1 + c2 + d2d:
            cp.wait_send()
        for n in range(WINDOW):
            remote(send.at[0, pl.ds(0, BLK)], recv.at[0, mine], qs_sem.at[n], qr_sem.at[0], partner).wait_send()


def finish_kernel(ex_ref, bo_ref, stat_ref, res_hbm, bonus_hbm, acc_ref, exp_ref, res, bonus, sems):
    rows = ex_ref.reshape(ex_ref.shape[0], LANES)
    out = res.reshape(res.shape[0], LANES)
    copies = []
    fac = jnp.concatenate([stat_ref[12 + t:13 + t, :] for t in range(BT)], axis=1)
    step = 256
    for n in range(4):
        size = min(step, SHARD - n * step)
        bonus[n * step:n * step + size, :] = bo_ref[n * step:n * step + size, :] * fac
    cp = pltpu.make_async_copy(bonus, bonus_hbm, sems.at[0])
    cp.start()
    copies.append(cp)
    mass = jnp.concatenate([stat_ref[i * BT + t:i * BT + t + 1, :] for t in range(BT) for i in range(DRAFT)], axis=0)
    mass = jnp.concatenate([mass] * 4, axis=0)
    for n in range(5):
        def body(k, carry):
            at = pl.ds(pl.multiple_of(n * 1200 + k * 24, 8), 24)
            out[at, :] = rows[at, :] / mass
            return carry

        lax.fori_loop(0, 50, body, 0, unroll=5)
        size = 1200
        if n == 4:
            out[6000:6012, :] = rows[6000:6012, :] / mass[0:12]
            size = 1212
        cp = pltpu.make_async_copy(res.at[pl.ds(n * 1200, size)], res_hbm.at[pl.ds(n * 1200, size)], sems.at[1 + n])
        cp.start()
        copies.append(cp)
    acc = stat_ref[6:12, :]
    more = acc[0:BT] * (1.0 + acc[BT:2 * BT])
    for t in range(BT):
        cols = slice(t * LANES, (t + 1) * LANES)
        exp_ref[cols] = more[t]
        for i in range(DRAFT):
            acc_ref[i:i + 1, cols] = acc[i * BT + t:i * BT + t + 1]
    for cp in copies:
        cp.wait()


def verify_local(hid, w_cols, q_rows, draft_tok):
    q = with_layout_constraint(q_rows.reshape(SEQ, DRAFT, TILES, LANES), Layout((0, 2, 1, 3)))
    q = q.transpose(0, 2, 1, 3).reshape(SEQ * TILES * DRAFT, 1, LANES)
    f32 = jnp.float32
    hbm = pl.BlockSpec(memory_space=pl.ANY)
    vmem = pl.BlockSpec(memory_space=pltpu.VMEM)
    dma = pltpu.SemaphoreType.DMA
    ex, bo, st = pl.pallas_call(
        kernel,
        out_shape=[
            jax.ShapeDtypeStruct((SHARD * BT * DRAFT, 1, LANES), f32),
            jax.ShapeDtypeStruct((ROWS_P, BATCH), f32),
            jax.ShapeDtypeStruct((16, LANES), f32),
        ],
        in_specs=[pl.BlockSpec(memory_space=pltpu.HBM)] * 4,
        out_specs=[hbm, hbm, vmem],
        scratch_shapes=[
            pltpu.VMEM((DRAFT, BATCH), jnp.int32),
            pltpu.VMEM((SEQ * TILES * DRAFT + 20, 1, LANES), f32),
            pltpu.VMEM((SHARD, DIM), jnp.bfloat16),
            pltpu.VMEM((SEQ, NPOS, DIM), jnp.bfloat16),
            pltpu.VMEM((DEV * HROWS, LANES), jnp.bfloat16),
            pltpu.VMEM((48 * PITCH, LANES), f32),
            pltpu.VMEM((COLS_P, DIM), jnp.bfloat16),
            pltpu.VMEM((ROWS_P, COLS_P), f32),
            pltpu.VMEM((DRAFT, DEV * BLK, LANES), f32),
            pltpu.VMEM((DRAFT, DEV * BLK, LANES), f32),
            pltpu.VMEM((SHARD * BT * DRAFT, 1, LANES), f32),
            pltpu.VMEM((24, LANES), f32),
            pltpu.VMEM((16, LANES), f32),
            pltpu.VMEM((16, LANES), f32),
            pltpu.VMEM((8 * STAT, 1, LANES), f32),
            pltpu.VMEM((16 * STAT, 1, LANES), f32),
            pltpu.VMEM((8 * STAT, 1, LANES), f32),
            pltpu.VMEM((16 * STAT, 1, LANES), f32),
            dma((4,)),
            dma((3, 3, 3)), dma((3, 3, 3)), dma((3,)), dma((3,)),
            dma((WINDOW,)), dma((2,)),
            dma((7,)), dma((7,)), dma((15,)), dma((15,)),
            dma((7,)), dma((7,)), dma((15,)), dma((15,)),
        ],
        compiler_params=pltpu.CompilerParams(vmem_limit_bytes=40 * 2 ** 20, has_side_effects=True, collective_id=0),
    )(*(pltpu.with_memory_space_constraint(x, pltpu.HBM) for x in (q, w_cols.T, hid, draft_tok.T)))
    res, bonus, acc, expected = pl.pallas_call(
        finish_kernel,
        out_shape=[
            jax.ShapeDtypeStruct((SHARD * BT * DRAFT, 1, LANES), f32),
            jax.ShapeDtypeStruct((SHARD, BATCH), f32),
            jax.ShapeDtypeStruct((DRAFT, BATCH), f32),
            jax.ShapeDtypeStruct((BATCH,), f32),
        ],
        in_specs=[vmem] * 3,
        out_specs=[hbm, hbm, vmem, vmem],
        scratch_shapes=[
            pltpu.VMEM((SHARD * BT * DRAFT, 1, LANES), f32),
            pltpu.VMEM((SHARD, BATCH), f32),
            dma((6,)),
        ],
        compiler_params=pltpu.CompilerParams(vmem_limit_bytes=12 * 2 ** 20),
    )(ex, bo, st)
    res = with_layout_constraint(res.reshape(SHARD, BT, DRAFT, LANES).transpose(0, 2, 1, 3), Layout((0, 2, 1, 3)))
    residual = res.reshape(SHARD, DRAFT, BATCH).transpose(2, 1, 0)
    return acc.T, expected, residual, bonus.T


def solution(mesh):
    return jax.shard_map(
        verify_local,
        mesh=mesh,
        in_specs=(P(('dp', 'tp'), None, None), P(None, 'tp'), P(('dp', 'tp'), None, None), P('dp', None)),
        out_specs=(P('dp', None), P('dp'), P('dp', None, 'tp'), P('dp', 'tp')),
        check_vma=False,
    )
```

```python
import jax
import jax.numpy as jnp
from jax import lax
from jax.experimental import pallas as pl
from jax.experimental.layout import Layout, with_layout_constraint
from jax.experimental.pallas import tpu as pltpu
from jax.sharding import PartitionSpec as P

INV_TEMP = 1.25
DEV = 128
SEQ = 3
NPOS = 3
DRAFT = 2
BATCH = 384
DIM = 2048
VOCAB = 128256
SHARD = VOCAB // DEV
LANES = 128
TILES = VOCAB // LANES
CHUNKS = 8
TAIL = SHARD - (CHUNKS - 1) * LANES
ROWS_P = 1008
TAIL_P = ROWS_P - (CHUNKS - 1) * LANES
KC = DIM // LANES
HROWS = SEQ * NPOS * KC
COLS = NPOS * BATCH
COLS_P = 1280
CT = COLS // LANES
BT = BATCH // LANES
BLK = SEQ * CHUNKS
PITCH = 49
NEG = -1e30
STAT = 18
WINDOW = 16
CUTS = (7, 16, 22, 46, 56, 70)
HEAD = 3
MESH = pl.DeviceIdType.MESH


def remote(src, dst, ssem, rsem, dev):
    return pltpu.make_async_remote_copy(
        src_ref=src, dst_ref=dst, send_sem=ssem, recv_sem=rsem,
        device_id={'tp': dev}, device_id_type=MESH)


def reduce_stage(buf, slot, count, ssem, rsem, device, payload):
    buf.reshape(count * STAT, LANES)[pl.ds(slot * STAT, STAT), :] = payload
    here = buf.at[pl.ds(slot * STAT, STAT)]
    copies = []
    for r in range(1, count):
        cp = remote(here, here, ssem.at[r - 1], rsem.at[r - 1], device((slot + r) % count))
        cp.start()
        copies.append(cp)
    return copies


def finish(copies, buf):
    for cp in copies:
        cp.wait()
    count = len(copies) + 1
    rows = buf.reshape(count * STAT, LANES)
    return [rows[k * STAT:(k + 1) * STAT, :] for k in range(count)]


def merge_max_sum(parts):
    m = parts[0][0:CT]
    for p in parts[1:]:
        m = jnp.maximum(m, p[0:CT])
    s = parts[0][CT:2 * CT] * jnp.exp(parts[0][0:CT] - m)
    for p in parts[1:]:
        s = s + p[CT:2 * CT] * jnp.exp(p[0:CT] - m)
    return jnp.concatenate([m, s], axis=0)


def merge_add(parts):
    total = parts[0]
    for p in parts[1:]:
        total = total + p
    return total


def kernel(q_hbm, w_hbm, h_hbm, tok_hbm,
           ex_hbm, bo_hbm, out_ref,
           tok_ref, qbuf, wbuf, hloc, hidb, bounce, hmat, z, send, recv, exbuf, stat, peak, scale,
           a1, b1, a2, b2,
           lsem, ag_s, ag_r, d2d_s, d2d_r, qs_sem, qr_sem,
           sa1, ra1, sb1, rb1, sa2, ra2, sb2, rb2):
    scope = jax.named_scope
    me = lax.axis_index('tp')
    core = me % 2
    coord = (me // 32, (me // 8) % 4, (me // 2) % 4)
    unit = (32, 8, 2)
    partner = me + 1 - 2 * core
    hop = [[((coord[d] + r) % 4) * unit[d] for r in range(4)] for d in range(3)]

    def device(rz, ry, rx, rc):
        return hop[0][rz] + hop[1][ry] + hop[2][rx] + (core if rc == 0 else 1 - core)

    hcp = pltpu.make_async_copy(h_hbm, hloc, lsem.at[2])
    hcp.start()
    qcp = pltpu.make_async_copy(q_hbm, qbuf.at[pl.ds(0, SEQ * TILES * DRAFT)], lsem.at[0])
    qcp.start()
    wcp = pltpu.make_async_copy(w_hbm, wbuf, lsem.at[1])
    wcp.start()
    tcp = pltpu.make_async_copy(tok_hbm, tok_ref, lsem.at[3])
    tcp.start()
    barrier = pltpu.get_barrier_semaphore()
    peers = [partner]
    for d in range(3):
        for r in range(1, 4):
            steps = [0, 0, 0]
            steps[d] = r
            peers.append(device(*steps, 0))
    for dev in peers:
        pl.semaphore_signal(barrier, inc=1, device_id={'tp': dev}, device_id_type=MESH)

    with scope('hid'):
        hcp.wait()
        for s in range(SEQ):
            x = hloc[s].astype(jnp.float32)
            for kc in range(KC):
                bounce[pl.ds(s * 48 + kc, NPOS, stride=KC), :] = x[:, kc * LANES:(kc + 1) * LANES]
        hidb[pl.ds(pl.multiple_of(me * HROWS, 16), HROWS), :] = bounce[0:HROWS, :].astype(jnp.bfloat16)
    with scope('barrier'):
        pl.semaphore_wait(barrier, len(peers))

    hview = hidb.reshape(4, 4, 4, 2, SEQ, HROWS // SEQ, LANES)

    def ag_phase(phase):
        out = []
        for j in range(3):
            order = [(j + k) % 3 for k in range(3)]
            idx = list(coord)
            for d in order[:phase]:
                idx[d] = slice(None)
            view = hview.at[idx[0], idx[1], idx[2], core, j]
            for r in (1, 3, 2):
                steps = [0, 0, 0]
                steps[order[phase]] = r
                cp = remote(view, view, ag_s.at[phase, j, r - 1], ag_r.at[phase, j, r - 1], device(*steps, 0))
                cp.start()
                out.append(cp)
        return out

    qrows = qbuf.reshape(qbuf.shape[0], LANES)
    lane = lax.broadcasted_iota(jnp.int32, (8, LANES), 1)

    def pack(k, carry):
        first = (SHARD * k) // LANES
        off = (SHARD * k) % LANES
        shift = (LANES - off) % LANES
        keep = lane < LANES - off
        for i in range(DRAFT):
            for s in range(SEQ):
                base = (s * TILES + first) * DRAFT + i
                lo = qrows[pl.ds(base, 8, stride=2), :]
                hi = qrows[pl.ds(base + 2, 8, stride=2), :]
                lo = pltpu.roll(lo, shift, 1)
                hi = pltpu.roll(hi, shift, 1)
                send[i, pl.ds(pl.multiple_of(k * BLK + s * 8, 8), 8), :] = jnp.where(keep, lo, hi)
        return carry

    mine = pl.ds(pl.multiple_of(me * BLK, 8), BLK)

    def to(i, dev, n):
        cp = remote(send.at[i, pl.ds(pl.multiple_of(dev * BLK, 8), BLK)], recv.at[i, mine],
                    qs_sem.at[n % WINDOW], qr_sem.at[i], dev)
        if not isinstance(n, int) or n >= WINDOW:
            cp.wait_send()
        cp.start()

    def step(d, n):
        return ((coord[d] + n) % 4) * unit[d]

    def triples(lo, hi):
        def body(n, carry):
            i, u = n // 36, n % 36
            three, rc, v = u // 18, (u // 9) % 2, u % 9
            last = core + rc - 2 * core * rc
            a, b = v // 3, v % 3
            two = ((a + 1, b + 1, 0), (0, a + 1, b + 1), (b + 1, 0, a + 1))
            for k in range(3):
                full = ((a + k) % 3 + 1, (b + k) % 3 + 1, k + 1)
                r = [(1 - three) * two[k][d] + three * full[d] for d in range(3)]
                to(i, step(0, r[0]) + step(1, r[1]) + step(2, r[2]) + last, 38 + 3 * n + k)
            return carry

        lax.fori_loop(lo, hi, body, 0)

    def lines(rc, first):
        n = first
        for r in (1, 3, 2):
            for i in range(DRAFT):
                for d in range(3):
                    steps = [0, 0, 0]
                    steps[d] = r
                    to(i, device(*steps, rc), n)
                    n += 1

    c0 = ag_phase(0)
    with scope('qwait'):
        qcp.wait()
    with scope('pack'):
        lax.fori_loop(0, DEV, pack, 0, unroll=8)
    with scope('ex0'):
        for i in range(DRAFT):
            pltpu.make_async_copy(send.at[i, mine], recv.at[i, mine], qr_sem.at[i]).start()
            to(i, partner, i)
        lines(0, 2)
    with scope('ag0'):
        for cp in c0:
            cp.wait_recv()
    c1 = ag_phase(1)
    with scope('exag1'):
        lines(1, 20)
        triples(0, CUTS[0])
    with scope('ag1'):
        for cp in c1:
            cp.wait_recv()
    c2 = ag_phase(2)
    with scope('exag2'):
        triples(CUTS[0], CUTS[1])
    d2d = []
    for j in range(3):
        with scope(f'ag2_{j}'):
            for cp in c2[3 * j:3 * j + 3]:
                cp.wait_recv()
        view = hview.at[:, :, :, core, j]
        cp = remote(view, view, d2d_s.at[j], d2d_r.at[j], partner)
        cp.start()
        d2d.append(cp)
    with scope('exd2d'):
        triples(CUTS[1], CUTS[2])
    with scope('d2d'):
        for cp in d2d:
            cp.wait_recv()

    def relayout(n, carry):
        def up(b, c):
            x = hidb[pl.ds(pl.multiple_of((48 * n + b) * 48, 16), 48), :]
            bounce[pl.ds(b * PITCH, 48), :] = x.astype(jnp.float32)
            return c

        lax.fori_loop(0, 48, up, 0, unroll=4)
        for g in range(NPOS):
            for u in range(3):
                for kc in range(KC):
                    y = bounce[pl.ds(16 * u * PITCH + g * KC + kc, 16, stride=PITCH), :]
                    hmat[pl.ds(pl.multiple_of(g * BATCH + 48 * n + 16 * u, 16), 16),
                         kc * LANES:(kc + 1) * LANES] = y.astype(jnp.bfloat16)
        return carry

    with scope('relayout'):
        def spread(n, carry):
            lax.fori_loop(2 * n, 2 * n + 2, relayout, 0)
            triples(CUTS[2] + n, CUTS[2] + n + 1)
            return carry

        lax.fori_loop(0, 4, spread, 0)
    wcp.wait()
    tcp.wait()

    z[SHARD:ROWS_P, :] = jnp.full((ROWS_P - SHARD, COLS_P), NEG, jnp.float32)

    def head(n, carry):
        triples(CUTS[2] + 4 + HEAD * n, CUTS[2] + 4 + HEAD * (n + 1))
        hb = hmat[pl.ds(pl.multiple_of(n * 256, 256), 256), :]
        zt = lax.dot_general(wbuf[...], hb, (((1,), (1,)), ((), ())), preferred_element_type=jnp.float32)
        zt = zt * INV_TEMP
        z[0:SHARD, pl.ds(pl.multiple_of(n * 256, 256), 256)] = zt
        top = jnp.max(zt, axis=0, keepdims=True)
        peak[pl.ds(2 * n, 1), :] = top[:, 0:LANES]
        peak[pl.ds(2 * n + 1, 1), :] = top[:, LANES:]
        return carry

    with scope('head'):
        lax.fori_loop(0, COLS_P // 256, head, 0)

    def local_stats(t, carry):
        cols = pl.ds(pl.multiple_of(t * LANES, LANES), LANES)

        m = peak[pl.ds(t, 1), :]

        def expo(n, s):
            rows = pl.ds(pl.multiple_of(n * 112, 8), 112)
            x = jnp.exp(z[rows, cols] - m)
            z[rows, cols] = x
            return s + jnp.sum(x.reshape(14, 8, LANES), axis=0)

        s8 = lax.fori_loop(0, 9, expo, jnp.zeros((8, LANES), jnp.float32))
        stat[pl.ds(t, 1), :] = m
        stat[pl.ds(CT + t, 1), :] = jnp.sum(s8, axis=0, keepdims=True)
        return carry

    stat[...] = jnp.zeros_like(stat)
    done = CUTS[2] + 4 + HEAD * (COLS_P // 256)
    with scope('exst'):
        triples(done, CUTS[3])
    with scope('stats'):
        lax.fori_loop(0, CT, local_stats, 0)
    bcp = pltpu.make_async_copy(z.at[:, DRAFT * BATCH:COLS], bo_hbm, lsem.at[2])
    bcp.start()

    slot, grp = me % 8, me // 8
    near = lambda k: grp * 8 + k
    far = lambda k: k * 8 + slot
    local = stat[0:STAT, :]
    copies = reduce_stage(a1, slot, 8, sa1, ra1, near, local)
    with scope('ex1a'):
        triples(CUTS[3], CUTS[4])
    with scope('round1a'):
        parts = finish(copies, a1)
    copies = reduce_stage(b1, grp, 16, sb1, rb1, far, merge_max_sum(parts))
    with scope('ex1b'):
        triples(CUTS[4], CUTS[5])
    with scope('round1b'):
        parts = finish(copies, b1)
    with scope('ex1c'):
        triples(CUTS[5], 72)
    tot = merge_max_sum(parts)
    fac = jnp.exp(local[0:CT] - tot[0:CT]) / tot[CT:2 * CT]
    scale[0:CT, :] = fac
    out_ref[12:16, :] = jnp.concatenate([fac[DRAFT * BT:CT], fac[0:1]], axis=0)

    exrows = exbuf.reshape(exbuf.shape[0], LANES)
    first_id = me * SHARD
    stat[...] = jnp.zeros_like(stat)
    for i in range(DRAFT):
        with scope(f'a2a_{i}'):
            pltpu.make_async_copy(recv.at[i], recv.at[i], qr_sem.at[i]).wait()
        for t in range(BT):
            row = i * BT + t
            sc = scale[row:row + 1, :]
            tok = tok_ref[i:i + 1, t * LANES:(t + 1) * LANES] - first_id
            col0 = i * BATCH + t * LANES

            def block(c, carry, size, valid):
                mass, pp, qp = carry
                q = recv[i, pl.ds(t * LANES * CHUNKS + c, LANES, stride=CHUNKS), :].T
                p = z[pl.ds(pl.multiple_of(c * LANES, LANES), size), col0:col0 + LANES] * sc
                ids = lax.broadcasted_iota(jnp.int32, (size, LANES), 0)
                q = q[0:size]
                if valid < size:
                    q = jnp.where(ids < valid, q, 0.0)
                x = jnp.maximum(p - q, 0.0)
                exrows[pl.ds(c * LANES * 6 + t * 2 + i, valid, stride=6), :] = x[0:valid]
                hit = ids == tok - c * LANES
                fold = lambda v: jnp.sum(v.reshape(size // 8, 8, LANES), axis=0)
                return (mass + fold(x), pp + fold(jnp.where(hit, p, 0.0)), qp + fold(jnp.where(hit, q, 0.0)))

            zero = jnp.zeros((8, LANES), jnp.float32)
            carry = lax.fori_loop(0, CHUNKS - 1, lambda c, v: block(c, v, LANES, LANES), (zero, zero, zero))
            mass, pp, qp = block(CHUNKS - 1, carry, TAIL_P, TAIL)
            stat[row:row + 1, :] = jnp.sum(mass, axis=0, keepdims=True)
            stat[6 + row:7 + row, :] = jnp.sum(pp, axis=0, keepdims=True)
            stat[12 + row:13 + row, :] = jnp.sum(qp, axis=0, keepdims=True)

    ecp = pltpu.make_async_copy(exbuf, ex_hbm, lsem.at[0])
    ecp.start()
    copies = reduce_stage(a2, slot, 8, sa2, ra2, near, stat[0:STAT, :])
    with scope('round2a'):
        parts = finish(copies, a2)
    copies = reduce_stage(b2, grp, 16, sb2, rb2, far, merge_add(parts))
    with scope('round2b'):
        parts = finish(copies, b2)
    tot = merge_add(parts)
    out_ref[0:6, :] = tot[0:6]
    out_ref[6:12, :] = jnp.minimum(tot[6:12] / tot[12:18], 1.0)
    with scope('tail'):
        ecp.wait()
        bcp.wait()
        for cp in c0 + c1 + c2 + d2d:
            cp.wait_send()
        for n in range(WINDOW):
            remote(send.at[0, pl.ds(0, BLK)], recv.at[0, mine], qs_sem.at[n], qr_sem.at[0], partner).wait_send()


def finish_kernel(ex_ref, bo_ref, stat_ref, res_hbm, bonus_hbm, acc_ref, exp_ref, res, bonus, sems):
    rows = ex_ref.reshape(ex_ref.shape[0], LANES)
    out = res.reshape(res.shape[0], LANES)
    copies = []
    fac = jnp.concatenate([stat_ref[12 + t:13 + t, :] for t in range(BT)], axis=1)
    step = 256
    for n in range(4):
        size = min(step, SHARD - n * step)
        bonus[n * step:n * step + size, :] = bo_ref[n * step:n * step + size, :] * fac
    cp = pltpu.make_async_copy(bonus, bonus_hbm, sems.at[0])
    cp.start()
    copies.append(cp)
    mass = jnp.concatenate([stat_ref[i * BT + t:i * BT + t + 1, :] for t in range(BT) for i in range(DRAFT)], axis=0)
    mass = jnp.concatenate([mass] * 4, axis=0)
    for n in range(5):
        def body(k, carry):
            at = pl.ds(pl.multiple_of(n * 1200 + k * 24, 8), 24)
            out[at, :] = rows[at, :] / mass
            return carry

        lax.fori_loop(0, 50, body, 0, unroll=5)
        size = 1200
        if n == 4:
            out[6000:6012, :] = rows[6000:6012, :] / mass[0:12]
            size = 1212
        cp = pltpu.make_async_copy(res.at[pl.ds(n * 1200, size)], res_hbm.at[pl.ds(n * 1200, size)], sems.at[1 + n])
        cp.start()
        copies.append(cp)
    acc = stat_ref[6:12, :]
    more = acc[0:BT] * (1.0 + acc[BT:2 * BT])
    for t in range(BT):
        cols = slice(t * LANES, (t + 1) * LANES)
        exp_ref[cols] = more[t]
        for i in range(DRAFT):
            acc_ref[i:i + 1, cols] = acc[i * BT + t:i * BT + t + 1]
    for cp in copies:
        cp.wait()


def verify_local(hid, w_cols, q_rows, draft_tok):
    q = with_layout_constraint(q_rows.reshape(SEQ, DRAFT, TILES, LANES), Layout((0, 2, 1, 3)))
    q = q.transpose(0, 2, 1, 3).reshape(SEQ * TILES * DRAFT, 1, LANES)
    f32 = jnp.float32
    hbm = pl.BlockSpec(memory_space=pl.ANY)
    vmem = pl.BlockSpec(memory_space=pltpu.VMEM)
    dma = pltpu.SemaphoreType.DMA
    ex, bo, st = pl.pallas_call(
        kernel,
        out_shape=[
            jax.ShapeDtypeStruct((SHARD * BT * DRAFT, 1, LANES), f32),
            jax.ShapeDtypeStruct((ROWS_P, BATCH), f32),
            jax.ShapeDtypeStruct((16, LANES), f32),
        ],
        in_specs=[pl.BlockSpec(memory_space=pltpu.HBM)] * 4,
        out_specs=[hbm, hbm, vmem],
        scratch_shapes=[
            pltpu.VMEM((DRAFT, BATCH), jnp.int32),
            pltpu.VMEM((SEQ * TILES * DRAFT + 20, 1, LANES), f32),
            pltpu.VMEM((SHARD, DIM), jnp.bfloat16),
            pltpu.VMEM((SEQ, NPOS, DIM), jnp.bfloat16),
            pltpu.VMEM((DEV * HROWS, LANES), jnp.bfloat16),
            pltpu.VMEM((48 * PITCH, LANES), f32),
            pltpu.VMEM((COLS_P, DIM), jnp.bfloat16),
            pltpu.VMEM((ROWS_P, COLS_P), f32),
            pltpu.VMEM((DRAFT, DEV * BLK, LANES), f32),
            pltpu.VMEM((DRAFT, DEV * BLK, LANES), f32),
            pltpu.VMEM((SHARD * BT * DRAFT, 1, LANES), f32),
            pltpu.VMEM((24, LANES), f32),
            pltpu.VMEM((16, LANES), f32),
            pltpu.VMEM((16, LANES), f32),
            pltpu.VMEM((8 * STAT, 1, LANES), f32),
            pltpu.VMEM((16 * STAT, 1, LANES), f32),
            pltpu.VMEM((8 * STAT, 1, LANES), f32),
            pltpu.VMEM((16 * STAT, 1, LANES), f32),
            dma((4,)),
            dma((3, 3, 3)), dma((3, 3, 3)), dma((3,)), dma((3,)),
            dma((WINDOW,)), dma((2,)),
            dma((7,)), dma((7,)), dma((15,)), dma((15,)),
            dma((7,)), dma((7,)), dma((15,)), dma((15,)),
        ],
        compiler_params=pltpu.CompilerParams(vmem_limit_bytes=40 * 2 ** 20, has_side_effects=True, collective_id=0),
    )(*(pltpu.with_memory_space_constraint(x, pltpu.HBM) for x in (q, w_cols.T, hid, draft_tok.T)))
    res, bonus, acc, expected = pl.pallas_call(
        finish_kernel,
        out_shape=[
            jax.ShapeDtypeStruct((SHARD * BT * DRAFT, 1, LANES), f32),
            jax.ShapeDtypeStruct((SHARD, BATCH), f32),
            jax.ShapeDtypeStruct((DRAFT, BATCH), f32),
            jax.ShapeDtypeStruct((BATCH,), f32),
        ],
        in_specs=[vmem] * 3,
        out_specs=[hbm, hbm, vmem, vmem],
        scratch_shapes=[
            pltpu.VMEM((SHARD * BT * DRAFT, 1, LANES), f32),
            pltpu.VMEM((SHARD, BATCH), f32),
            dma((6,)),
        ],
        compiler_params=pltpu.CompilerParams(vmem_limit_bytes=12 * 2 ** 20),
    )(ex, bo, st)
    res = with_layout_constraint(res.reshape(SHARD, BT, DRAFT, LANES).transpose(0, 2, 1, 3), Layout((0, 2, 1, 3)))
    residual = res.reshape(SHARD, DRAFT, BATCH).transpose(2, 1, 0)
    return acc.T, expected, residual, bonus.T


def solution(mesh):
    return jax.shard_map(
        verify_local,
        mesh=mesh,
        in_specs=(P(('dp', 'tp'), None, None), P(None, 'tp'), P(('dp', 'tp'), None, None), P('dp', None)),
        out_specs=(P('dp', None), P('dp'), P('dp', None, 'tp'), P('dp', 'tp')),
        check_vma=False,
    )
```

```python
import jax
import jax.numpy as jnp
from jax import lax
from jax.experimental import pallas as pl
from jax.experimental.layout import Layout, with_layout_constraint
from jax.experimental.pallas import tpu as pltpu
from jax.sharding import PartitionSpec as P

INV_TEMP = 1.25
DEV = 128
SEQ = 3
NPOS = 3
DRAFT = 2
BATCH = 384
DIM = 2048
VOCAB = 128256
SHARD = VOCAB // DEV
LANES = 128
TILES = VOCAB // LANES
CHUNKS = 8
TAIL = SHARD - (CHUNKS - 1) * LANES
ROWS_P = 1008
TAIL_P = ROWS_P - (CHUNKS - 1) * LANES
KC = DIM // LANES
HROWS = SEQ * NPOS * KC
COLS = NPOS * BATCH
COLS_P = 1280
CT = COLS // LANES
BT = BATCH // LANES
BLK = SEQ * CHUNKS
PITCH = 49
NEG = -1e30
STAT = 18
MESH = pl.DeviceIdType.MESH


def remote(src, dst, ssem, rsem, dev):
    return pltpu.make_async_remote_copy(
        src_ref=src, dst_ref=dst, send_sem=ssem, recv_sem=rsem,
        device_id={'tp': dev}, device_id_type=MESH)


def reduce_stage(buf, slot, count, ssem, rsem, device, payload):
    buf.reshape(count * STAT, LANES)[pl.ds(slot * STAT, STAT), :] = payload
    here = buf.at[pl.ds(slot * STAT, STAT)]
    copies = []
    for r in range(1, count):
        cp = remote(here, here, ssem.at[r - 1], rsem.at[r - 1], device((slot + r) % count))
        cp.start()
        copies.append(cp)
    return copies


def finish(copies, buf):
    for cp in copies:
        cp.wait()
    count = len(copies) + 1
    rows = buf.reshape(count * STAT, LANES)
    return [rows[k * STAT:(k + 1) * STAT, :] for k in range(count)]


def merge_max_sum(parts):
    m = parts[0][0:CT]
    for p in parts[1:]:
        m = jnp.maximum(m, p[0:CT])
    s = parts[0][CT:2 * CT] * jnp.exp(parts[0][0:CT] - m)
    for p in parts[1:]:
        s = s + p[CT:2 * CT] * jnp.exp(p[0:CT] - m)
    return jnp.concatenate([m, s], axis=0)


def merge_add(parts):
    total = parts[0]
    for p in parts[1:]:
        total = total + p
    return total


def kernel(q_hbm, w_hbm, h_hbm, tok_hbm,
           ex_hbm, bo_hbm, out_ref,
           tok_ref, qbuf, wbuf, hloc, hidb, bounce, hmat, z, send, recv, exbuf, stat, peak, scale,
           a1, b1, a2, b2,
           lsem, ag_s, ag_r, d2d_s, d2d_r, qs_sem, qr_sem,
           sa1, ra1, sb1, rb1, sa2, ra2, sb2, rb2):
    scope = jax.named_scope
    me = lax.axis_index('tp')
    core = me % 2
    coord = (me // 32, (me // 8) % 4, (me // 2) % 4)
    unit = (32, 8, 2)
    partner = me + 1 - 2 * core
    hop = [[((coord[d] + r) % 4) * unit[d] for r in range(4)] for d in range(3)]

    def device(rz, ry, rx, rc):
        return hop[0][rz] + hop[1][ry] + hop[2][rx] + (core if rc == 0 else 1 - core)

    hcp = pltpu.make_async_copy(h_hbm, hloc, lsem.at[2])
    hcp.start()
    qcp = pltpu.make_async_copy(q_hbm, qbuf.at[pl.ds(0, SEQ * TILES * DRAFT)], lsem.at[0])
    qcp.start()
    wcp = pltpu.make_async_copy(w_hbm, wbuf, lsem.at[1])
    wcp.start()
    tcp = pltpu.make_async_copy(tok_hbm, tok_ref, lsem.at[3])
    tcp.start()
    barrier = pltpu.get_barrier_semaphore()
    peers = [partner]
    for d in range(3):
        for r in range(1, 4):
            steps = [0, 0, 0]
            steps[d] = r
            peers.append(device(*steps, 0))
    for dev in peers:
        pl.semaphore_signal(barrier, inc=1, device_id={'tp': dev}, device_id_type=MESH)

    with scope('hid'):
        hcp.wait()
        for s in range(SEQ):
            x = hloc[s].astype(jnp.float32)
            for kc in range(KC):
                bounce[pl.ds(s * 48 + kc, NPOS, stride=KC), :] = x[:, kc * LANES:(kc + 1) * LANES]
        hidb[pl.ds(pl.multiple_of(me * HROWS, 16), HROWS), :] = bounce[0:HROWS, :].astype(jnp.bfloat16)
    with scope('barrier'):
        pl.semaphore_wait(barrier, len(peers))

    hview = hidb.reshape(4, 4, 4, 2, SEQ, HROWS // SEQ, LANES)

    def ag_phase(phase):
        out = []
        for j in range(3):
            order = [(j + k) % 3 for k in range(3)]
            idx = list(coord)
            for d in order[:phase]:
                idx[d] = slice(None)
            view = hview.at[idx[0], idx[1], idx[2], core, j]
            for r in (1, 3, 2):
                steps = [0, 0, 0]
                steps[order[phase]] = r
                cp = remote(view, view, ag_s.at[phase, j, r - 1], ag_r.at[phase, j, r - 1], device(*steps, 0))
                cp.start()
                out.append(cp)
        return out

    qrows = qbuf.reshape(qbuf.shape[0], LANES)
    lane = lax.broadcasted_iota(jnp.int32, (8, LANES), 1)

    def pack(k, carry):
        first = (SHARD * k) // LANES
        off = (SHARD * k) % LANES
        shift = (LANES - off) % LANES
        keep = lane < LANES - off
        for i in range(DRAFT):
            for s in range(SEQ):
                base = (s * TILES + first) * DRAFT + i
                lo = qrows[pl.ds(base, 8, stride=2), :]
                hi = qrows[pl.ds(base + 2, 8, stride=2), :]
                lo = pltpu.roll(lo, shift, 1)
                hi = pltpu.roll(hi, shift, 1)
                send[i, pl.ds(pl.multiple_of(k * BLK + s * 8, 8), 8), :] = jnp.where(keep, lo, hi)
        return carry

    mine = pl.ds(pl.multiple_of(me * BLK, 8), BLK)

    def to(i, dev):
        remote(send.at[i, pl.ds(pl.multiple_of(dev * BLK, 8), BLK)], recv.at[i, mine],
               qs_sem.at[i], qr_sem.at[i], dev).start()

    def step(d, n):
        return ((coord[d] + n) % 4) * unit[d]

    def class0(i):
        pltpu.make_async_copy(send.at[i, mine], recv.at[i, mine], qr_sem.at[i]).start()
        to(i, partner)

    def class1(i, rc):
        last = core if rc == 0 else 1 - core
        for r in (1, 3, 2):
            for d in range(3):
                steps = [0, 0, 0]
                steps[d] = r
                to(i, device(*steps, rc))

    def class2(i, rc, lo=0, hi=9):
        last = core if rc == 0 else 1 - core

        def body(n, carry):
            a, b = n // 3 + 1, n % 3 + 1
            to(i, step(0, a) + step(1, b) + hop[2][0] + last)
            to(i, hop[0][0] + step(1, a) + step(2, b) + last)
            to(i, step(0, b) + hop[1][0] + step(2, a) + last)
            return carry

        lax.fori_loop(lo, hi, body, 0)

    def class3(i, rc):
        last = core if rc == 0 else 1 - core

        def body(n, carry):
            a, b = n // 3, n % 3
            for k in range(3):
                to(i, step(0, (a + k) % 3 + 1) + step(1, (b + k) % 3 + 1) + hop[2][k + 1] + last)
            return carry

        lax.fori_loop(0, 9, body, 0)

    c0 = ag_phase(0)
    with scope('qwait'):
        qcp.wait()
    with scope('pack'):
        lax.fori_loop(0, DEV, pack, 0, unroll=8)
    with scope('ex0'):
        class0(0)
        class1(0, 0)
    with scope('ag0'):
        for cp in c0:
            cp.wait_recv()
    c1 = ag_phase(1)
    with scope('ex0a'):
        class1(0, 1)
        class2(0, 0)
    with scope('ag1'):
        for cp in c1:
            cp.wait_recv()
    c2 = ag_phase(2)
    d2d = []
    for j in range(3):
        with scope(f'ag2_{j}'):
            for cp in c2[3 * j:3 * j + 3]:
                cp.wait_recv()
        view = hview.at[:, :, :, core, j]
        cp = remote(view, view, d2d_s.at[j], d2d_r.at[j], partner)
        cp.start()
        d2d.append(cp)
    with scope('ex0b'):
        class2(0, 1)
        class3(0, 0)
        class3(0, 1)
        class3(1, 0)
    with scope('d2d'):
        for cp in d2d:
            cp.wait_recv()

    def relayout(n, carry):
        def up(b, c):
            x = hidb[pl.ds(pl.multiple_of((48 * n + b) * 48, 16), 48), :]
            bounce[pl.ds(b * PITCH, 48), :] = x.astype(jnp.float32)
            return c

        lax.fori_loop(0, 48, up, 0, unroll=4)
        for g in range(NPOS):
            for u in range(3):
                for kc in range(KC):
                    y = bounce[pl.ds(16 * u * PITCH + g * KC + kc, 16, stride=PITCH), :]
                    hmat[pl.ds(pl.multiple_of(g * BATCH + 48 * n + 16 * u, 16), 16),
                         kc * LANES:(kc + 1) * LANES] = y.astype(jnp.bfloat16)
        return carry

    with scope('relayout'):
        lax.fori_loop(0, 8, relayout, 0)
    wcp.wait()
    tcp.wait()

    z[SHARD:ROWS_P, :] = jnp.full((ROWS_P - SHARD, COLS_P), NEG, jnp.float32)

    def head(n, carry):
        hb = hmat[pl.ds(pl.multiple_of(n * 256, 256), 256), :]
        zt = lax.dot_general(wbuf[...], hb, (((1,), (1,)), ((), ())), preferred_element_type=jnp.float32)
        zt = zt * INV_TEMP
        z[0:SHARD, pl.ds(pl.multiple_of(n * 256, 256), 256)] = zt
        top = jnp.max(zt, axis=0, keepdims=True)
        peak[pl.ds(2 * n, 1), :] = top[:, 0:LANES]
        peak[pl.ds(2 * n + 1, 1), :] = top[:, LANES:]
        return carry

    with scope('head'):
        lax.fori_loop(0, COLS_P // 256, head, 0)

    def local_stats(t, carry):
        cols = pl.ds(pl.multiple_of(t * LANES, LANES), LANES)

        m = peak[pl.ds(t, 1), :]

        def expo(n, s):
            rows = pl.ds(pl.multiple_of(n * 112, 8), 112)
            x = jnp.exp(z[rows, cols] - m)
            z[rows, cols] = x
            return s + jnp.sum(x.reshape(14, 8, LANES), axis=0)

        s8 = lax.fori_loop(0, 9, expo, jnp.zeros((8, LANES), jnp.float32))
        stat[pl.ds(t, 1), :] = m
        stat[pl.ds(CT + t, 1), :] = jnp.sum(s8, axis=0, keepdims=True)
        return carry

    stat[...] = jnp.zeros_like(stat)
    with scope('stats'):
        lax.fori_loop(0, CT, local_stats, 0)
    bcp = pltpu.make_async_copy(z.at[:, DRAFT * BATCH:COLS], bo_hbm, lsem.at[2])
    bcp.start()

    slot, grp = me % 8, me // 8
    near = lambda k: grp * 8 + k
    far = lambda k: k * 8 + slot
    local = stat[0:STAT, :]
    copies = reduce_stage(a1, slot, 8, sa1, ra1, near, local)
    with scope('ex1a'):
        class3(1, 1)
    with scope('round1a'):
        parts = finish(copies, a1)
    copies = reduce_stage(b1, grp, 16, sb1, rb1, far, merge_max_sum(parts))
    with scope('ex1b'):
        class2(1, 1)
        class2(1, 0)
        class1(1, 1)
        class1(1, 0)
        class0(1)
    with scope('round1b'):
        parts = finish(copies, b1)
    tot = merge_max_sum(parts)
    fac = jnp.exp(local[0:CT] - tot[0:CT]) / tot[CT:2 * CT]
    scale[0:CT, :] = fac
    out_ref[12:16, :] = jnp.concatenate([fac[DRAFT * BT:CT], fac[0:1]], axis=0)

    exrows = exbuf.reshape(exbuf.shape[0], LANES)
    first_id = me * SHARD
    stat[...] = jnp.zeros_like(stat)
    for i in range(DRAFT):
        with scope(f'a2a_{i}'):
            pltpu.make_async_copy(recv.at[i], recv.at[i], qr_sem.at[i]).wait()
        for t in range(BT):
            row = i * BT + t
            sc = scale[row:row + 1, :]
            tok = tok_ref[i:i + 1, t * LANES:(t + 1) * LANES] - first_id
            col0 = i * BATCH + t * LANES

            def block(c, carry, size, valid):
                mass, pp, qp = carry
                q = recv[i, pl.ds(t * LANES * CHUNKS + c, LANES, stride=CHUNKS), :].T
                p = z[pl.ds(pl.multiple_of(c * LANES, LANES), size), col0:col0 + LANES] * sc
                ids = lax.broadcasted_iota(jnp.int32, (size, LANES), 0)
                q = q[0:size]
                if valid < size:
                    q = jnp.where(ids < valid, q, 0.0)
                x = jnp.maximum(p - q, 0.0)
                exrows[pl.ds(c * LANES * 6 + t * 2 + i, valid, stride=6), :] = x[0:valid]
                hit = ids == tok - c * LANES
                fold = lambda v: jnp.sum(v.reshape(size // 8, 8, LANES), axis=0)
                return (mass + fold(x), pp + fold(jnp.where(hit, p, 0.0)), qp + fold(jnp.where(hit, q, 0.0)))

            zero = jnp.zeros((8, LANES), jnp.float32)
            carry = lax.fori_loop(0, CHUNKS - 1, lambda c, v: block(c, v, LANES, LANES), (zero, zero, zero))
            mass, pp, qp = block(CHUNKS - 1, carry, TAIL_P, TAIL)
            stat[row:row + 1, :] = jnp.sum(mass, axis=0, keepdims=True)
            stat[6 + row:7 + row, :] = jnp.sum(pp, axis=0, keepdims=True)
            stat[12 + row:13 + row, :] = jnp.sum(qp, axis=0, keepdims=True)

    ecp = pltpu.make_async_copy(exbuf, ex_hbm, lsem.at[0])
    ecp.start()
    copies = reduce_stage(a2, slot, 8, sa2, ra2, near, stat[0:STAT, :])
    with scope('round2a'):
        parts = finish(copies, a2)
    copies = reduce_stage(b2, grp, 16, sb2, rb2, far, merge_add(parts))
    with scope('round2b'):
        parts = finish(copies, b2)
    tot = merge_add(parts)
    out_ref[0:6, :] = tot[0:6]
    out_ref[6:12, :] = jnp.minimum(tot[6:12] / tot[12:18], 1.0)
    with scope('tail'):
        ecp.wait()
        bcp.wait()
        for cp in c0 + c1 + c2 + d2d:
            cp.wait_send()
        for i in range(DRAFT):
            part = send.at[i, pl.ds(0, (DEV - 1) * BLK)]
            pltpu.make_async_copy(part, part, qs_sem.at[i]).wait()


def finish_kernel(ex_ref, bo_ref, stat_ref, res_hbm, bonus_hbm, acc_ref, exp_ref, res, bonus, sems):
    rows = ex_ref.reshape(ex_ref.shape[0], LANES)
    out = res.reshape(res.shape[0], LANES)
    copies = []
    fac = jnp.concatenate([stat_ref[12 + t:13 + t, :] for t in range(BT)], axis=1)
    step = 256
    for n in range(4):
        size = min(step, SHARD - n * step)
        bonus[n * step:n * step + size, :] = bo_ref[n * step:n * step + size, :] * fac
    cp = pltpu.make_async_copy(bonus, bonus_hbm, sems.at[0])
    cp.start()
    copies.append(cp)
    mass = jnp.concatenate([stat_ref[i * BT + t:i * BT + t + 1, :] for t in range(BT) for i in range(DRAFT)], axis=0)
    mass = jnp.concatenate([mass] * 4, axis=0)
    for n in range(5):
        def body(k, carry):
            at = pl.ds(pl.multiple_of(n * 1200 + k * 24, 8), 24)
            out[at, :] = rows[at, :] / mass
            return carry

        lax.fori_loop(0, 50, body, 0, unroll=5)
        size = 1200
        if n == 4:
            out[6000:6012, :] = rows[6000:6012, :] / mass[0:12]
            size = 1212
        cp = pltpu.make_async_copy(res.at[pl.ds(n * 1200, size)], res_hbm.at[pl.ds(n * 1200, size)], sems.at[1 + n])
        cp.start()
        copies.append(cp)
    acc = stat_ref[6:12, :]
    more = acc[0:BT] * (1.0 + acc[BT:2 * BT])
    for t in range(BT):
        cols = slice(t * LANES, (t + 1) * LANES)
        exp_ref[cols] = more[t]
        for i in range(DRAFT):
            acc_ref[i:i + 1, cols] = acc[i * BT + t:i * BT + t + 1]
    for cp in copies:
        cp.wait()


def verify_local(hid, w_cols, q_rows, draft_tok):
    q = with_layout_constraint(q_rows.reshape(SEQ, DRAFT, TILES, LANES), Layout((0, 2, 1, 3)))
    q = q.transpose(0, 2, 1, 3).reshape(SEQ * TILES * DRAFT, 1, LANES)
    f32 = jnp.float32
    hbm = pl.BlockSpec(memory_space=pl.ANY)
    vmem = pl.BlockSpec(memory_space=pltpu.VMEM)
    dma = pltpu.SemaphoreType.DMA
    ex, bo, st = pl.pallas_call(
        kernel,
        out_shape=[
            jax.ShapeDtypeStruct((SHARD * BT * DRAFT, 1, LANES), f32),
            jax.ShapeDtypeStruct((ROWS_P, BATCH), f32),
            jax.ShapeDtypeStruct((16, LANES), f32),
        ],
        in_specs=[pl.BlockSpec(memory_space=pltpu.HBM)] * 4,
        out_specs=[hbm, hbm, vmem],
        scratch_shapes=[
            pltpu.VMEM((DRAFT, BATCH), jnp.int32),
            pltpu.VMEM((SEQ * TILES * DRAFT + 20, 1, LANES), f32),
            pltpu.VMEM((SHARD, DIM), jnp.bfloat16),
            pltpu.VMEM((SEQ, NPOS, DIM), jnp.bfloat16),
            pltpu.VMEM((DEV * HROWS, LANES), jnp.bfloat16),
            pltpu.VMEM((48 * PITCH, LANES), f32),
            pltpu.VMEM((COLS_P, DIM), jnp.bfloat16),
            pltpu.VMEM((ROWS_P, COLS_P), f32),
            pltpu.VMEM((DRAFT, DEV * BLK, LANES), f32),
            pltpu.VMEM((DRAFT, DEV * BLK, LANES), f32),
            pltpu.VMEM((SHARD * BT * DRAFT, 1, LANES), f32),
            pltpu.VMEM((24, LANES), f32),
            pltpu.VMEM((16, LANES), f32),
            pltpu.VMEM((16, LANES), f32),
            pltpu.VMEM((8 * STAT, 1, LANES), f32),
            pltpu.VMEM((16 * STAT, 1, LANES), f32),
            pltpu.VMEM((8 * STAT, 1, LANES), f32),
            pltpu.VMEM((16 * STAT, 1, LANES), f32),
            dma((4,)),
            dma((3, 3, 3)), dma((3, 3, 3)), dma((3,)), dma((3,)),
            dma((2,)), dma((2,)),
            dma((7,)), dma((7,)), dma((15,)), dma((15,)),
            dma((7,)), dma((7,)), dma((15,)), dma((15,)),
        ],
        compiler_params=pltpu.CompilerParams(vmem_limit_bytes=40 * 2 ** 20, has_side_effects=True, collective_id=0),
    )(*(pltpu.with_memory_space_constraint(x, pltpu.HBM) for x in (q, w_cols.T, hid, draft_tok.T)))
    res, bonus, acc, expected = pl.pallas_call(
        finish_kernel,
        out_shape=[
            jax.ShapeDtypeStruct((SHARD * BT * DRAFT, 1, LANES), f32),
            jax.ShapeDtypeStruct((SHARD, BATCH), f32),
            jax.ShapeDtypeStruct((DRAFT, BATCH), f32),
            jax.ShapeDtypeStruct((BATCH,), f32),
        ],
        in_specs=[vmem] * 3,
        out_specs=[hbm, hbm, vmem, vmem],
        scratch_shapes=[
            pltpu.VMEM((SHARD * BT * DRAFT, 1, LANES), f32),
            pltpu.VMEM((SHARD, BATCH), f32),
            dma((6,)),
        ],
        compiler_params=pltpu.CompilerParams(vmem_limit_bytes=12 * 2 ** 20),
    )(ex, bo, st)
    res = with_layout_constraint(res.reshape(SHARD, BT, DRAFT, LANES).transpose(0, 2, 1, 3), Layout((0, 2, 1, 3)))
    residual = res.reshape(SHARD, DRAFT, BATCH).transpose(2, 1, 0)
    return acc.T, expected, residual, bonus.T


def solution(mesh):
    return jax.shard_map(
        verify_local,
        mesh=mesh,
        in_specs=(P(('dp', 'tp'), None, None), P(None, 'tp'), P(('dp', 'tp'), None, None), P('dp', None)),
        out_specs=(P('dp', None), P('dp'), P('dp', None, 'tp'), P('dp', 'tp')),
        check_vma=False,
    )
```

```python
import jax
import jax.numpy as jnp
from jax import lax
from jax.experimental import pallas as pl
from jax.experimental.layout import Layout, with_layout_constraint
from jax.experimental.pallas import tpu as pltpu
from jax.sharding import PartitionSpec as P

INV_TEMP = 1.25
DEV = 128
SEQ = 3
NPOS = 3
DRAFT = 2
BATCH = 384
DIM = 2048
VOCAB = 128256
SHARD = VOCAB // DEV
LANES = 128
TILES = VOCAB // LANES
CHUNKS = 8
TAIL = SHARD - (CHUNKS - 1) * LANES
ROWS_P = 1008
TAIL_P = ROWS_P - (CHUNKS - 1) * LANES
KC = DIM // LANES
HROWS = SEQ * NPOS * KC
COLS = NPOS * BATCH
COLS_P = 1280
CT = COLS // LANES
BT = BATCH // LANES
BLK = SEQ * CHUNKS
PITCH = 49
NEG = -1e30
STAT = 18
MESH = pl.DeviceIdType.MESH


def remote(src, dst, ssem, rsem, dev):
    return pltpu.make_async_remote_copy(
        src_ref=src, dst_ref=dst, send_sem=ssem, recv_sem=rsem,
        device_id={'tp': dev}, device_id_type=MESH)


def reduce_stage(buf, slot, count, ssem, rsem, device, payload):
    buf.reshape(count * STAT, LANES)[pl.ds(slot * STAT, STAT), :] = payload
    here = buf.at[pl.ds(slot * STAT, STAT)]
    copies = []
    for r in range(1, count):
        cp = remote(here, here, ssem.at[r - 1], rsem.at[r - 1], device((slot + r) % count))
        cp.start()
        copies.append(cp)
    return copies


def finish(copies, buf):
    for cp in copies:
        cp.wait()
    count = len(copies) + 1
    rows = buf.reshape(count * STAT, LANES)
    return [rows[k * STAT:(k + 1) * STAT, :] for k in range(count)]


def merge_max_sum(parts):
    m = parts[0][0:CT]
    for p in parts[1:]:
        m = jnp.maximum(m, p[0:CT])
    s = parts[0][CT:2 * CT] * jnp.exp(parts[0][0:CT] - m)
    for p in parts[1:]:
        s = s + p[CT:2 * CT] * jnp.exp(p[0:CT] - m)
    return jnp.concatenate([m, s], axis=0)


def merge_add(parts):
    total = parts[0]
    for p in parts[1:]:
        total = total + p
    return total


def kernel(q_hbm, w_hbm, h_hbm, tok_hbm,
           ex_hbm, bo_hbm, out_ref,
           tok_ref, qbuf, wbuf, hloc, hidb, bounce, hmat, z, send, recv, exbuf, stat, peak, scale,
           a1, b1, a2, b2,
           lsem, ag_s, ag_r, d2d_s, d2d_r, qs_sem, qr_sem,
           sa1, ra1, sb1, rb1, sa2, ra2, sb2, rb2):
    scope = jax.named_scope
    me = lax.axis_index('tp')
    core = me % 2
    coord = (me // 32, (me // 8) % 4, (me // 2) % 4)
    unit = (32, 8, 2)
    partner = me + 1 - 2 * core
    hop = [[((coord[d] + r) % 4) * unit[d] for r in range(4)] for d in range(3)]

    def device(rz, ry, rx, rc):
        return hop[0][rz] + hop[1][ry] + hop[2][rx] + (core if rc == 0 else 1 - core)

    hcp = pltpu.make_async_copy(h_hbm, hloc, lsem.at[2])
    hcp.start()
    qcp = pltpu.make_async_copy(q_hbm, qbuf.at[pl.ds(0, SEQ * TILES * DRAFT)], lsem.at[0])
    qcp.start()
    wcp = pltpu.make_async_copy(w_hbm, wbuf, lsem.at[1])
    wcp.start()
    tcp = pltpu.make_async_copy(tok_hbm, tok_ref, lsem.at[3])
    tcp.start()
    barrier = pltpu.get_barrier_semaphore()
    peers = [partner]
    for d in range(3):
        for r in range(1, 4):
            steps = [0, 0, 0]
            steps[d] = r
            peers.append(device(*steps, 0))
    for dev in peers:
        pl.semaphore_signal(barrier, inc=1, device_id={'tp': dev}, device_id_type=MESH)

    with scope('hid'):
        hcp.wait()
        for s in range(SEQ):
            x = hloc[s].astype(jnp.float32)
            for kc in range(KC):
                bounce[pl.ds(s * 48 + kc, NPOS, stride=KC), :] = x[:, kc * LANES:(kc + 1) * LANES]
        hidb[pl.ds(pl.multiple_of(me * HROWS, 16), HROWS), :] = bounce[0:HROWS, :].astype(jnp.bfloat16)
    with scope('barrier'):
        pl.semaphore_wait(barrier, len(peers))

    hview = hidb.reshape(4, 4, 4, 2, SEQ, HROWS // SEQ, LANES)

    def ag_phase(phase):
        out = []
        for j in range(3):
            order = [(j + k) % 3 for k in range(3)]
            idx = list(coord)
            for d in order[:phase]:
                idx[d] = slice(None)
            view = hview.at[idx[0], idx[1], idx[2], core, j]
            for r in (1, 3, 2):
                steps = [0, 0, 0]
                steps[order[phase]] = r
                cp = remote(view, view, ag_s.at[phase, j, r - 1], ag_r.at[phase, j, r - 1], device(*steps, 0))
                cp.start()
                out.append(cp)
        return out

    qrows = qbuf.reshape(qbuf.shape[0], LANES)
    lane = lax.broadcasted_iota(jnp.int32, (8, LANES), 1)

    def pack(k, carry):
        first = (SHARD * k) // LANES
        off = (SHARD * k) % LANES
        shift = (LANES - off) % LANES
        keep = lane < LANES - off
        for i in range(DRAFT):
            for s in range(SEQ):
                base = (s * TILES + first) * DRAFT + i
                lo = qrows[pl.ds(base, 8, stride=2), :]
                hi = qrows[pl.ds(base + 2, 8, stride=2), :]
                lo = pltpu.roll(lo, shift, 1)
                hi = pltpu.roll(hi, shift, 1)
                send[i, pl.ds(pl.multiple_of(k * BLK + s * 8, 8), 8), :] = jnp.where(keep, lo, hi)
        return carry

    mine = pl.ds(pl.multiple_of(me * BLK, 8), BLK)

    def to(i, dev):
        remote(send.at[i, pl.ds(pl.multiple_of(dev * BLK, 8), BLK)], recv.at[i, mine],
               qs_sem.at[i], qr_sem.at[i], dev).start()

    def step(d, n):
        return ((coord[d] + n) % 4) * unit[d]

    def class0(i):
        pltpu.make_async_copy(send.at[i, mine], recv.at[i, mine], qr_sem.at[i]).start()
        to(i, partner)

    def class1(i, rc):
        last = core if rc == 0 else 1 - core
        for r in (1, 3, 2):
            for d in range(3):
                steps = [0, 0, 0]
                steps[d] = r
                to(i, device(*steps, rc))

    def class2(i, rc, lo=0, hi=9):
        last = core if rc == 0 else 1 - core

        def body(n, carry):
            a, b = n // 3 + 1, n % 3 + 1
            to(i, step(0, a) + step(1, b) + hop[2][0] + last)
            to(i, hop[0][0] + step(1, a) + step(2, b) + last)
            to(i, step(0, b) + hop[1][0] + step(2, a) + last)
            return carry

        lax.fori_loop(lo, hi, body, 0)

    def class3(i, rc, lo=0, hi=9):
        last = core if rc == 0 else 1 - core

        def body(n, carry):
            a, b = n // 3, n % 3
            for k in range(3):
                to(i, step(0, (a + k) % 3 + 1) + step(1, (b + k) % 3 + 1) + hop[2][k + 1] + last)
            return carry

        lax.fori_loop(lo, hi, body, 0)

    c0 = ag_phase(0)
    with scope('qwait'):
        qcp.wait()
    with scope('pack'):
        lax.fori_loop(0, DEV, pack, 0, unroll=8)
    with scope('ex0'):
        class0(0)
        class1(0, 0)
    with scope('ag0'):
        for cp in c0:
            cp.wait_recv()
    c1 = ag_phase(1)
    with scope('ex0a'):
        class1(0, 1)
        class2(0, 0)
    with scope('ag1'):
        for cp in c1:
            cp.wait_recv()
    c2 = ag_phase(2)
    d2d = []
    for j in range(3):
        with scope(f'ag2_{j}'):
            for cp in c2[3 * j:3 * j + 3]:
                cp.wait_recv()
        view = hview.at[:, :, :, core, j]
        cp = remote(view, view, d2d_s.at[j], d2d_r.at[j], partner)
        cp.start()
        d2d.append(cp)
    with scope('ex0b'):
        class3(0, 0)
        class3(0, 1)
        class2(0, 1)
        class3(1, 0)
    with scope('d2d'):
        for cp in d2d:
            cp.wait_recv()

    def relayout(n, carry):
        def up(b, c):
            x = hidb[pl.ds(pl.multiple_of((48 * n + b) * 48, 16), 48), :]
            bounce[pl.ds(b * PITCH, 48), :] = x.astype(jnp.float32)
            return c

        lax.fori_loop(0, 48, up, 0, unroll=4)
        for g in range(NPOS):
            for u in range(3):
                for kc in range(KC):
                    y = bounce[pl.ds(16 * u * PITCH + g * KC + kc, 16, stride=PITCH), :]
                    hmat[pl.ds(pl.multiple_of(g * BATCH + 48 * n + 16 * u, 16), 16),
                         kc * LANES:(kc + 1) * LANES] = y.astype(jnp.bfloat16)
        return carry

    with scope('relayout'):
        lax.fori_loop(0, 8, relayout, 0)
    wcp.wait()
    tcp.wait()

    z[SHARD:ROWS_P, :] = jnp.full((ROWS_P - SHARD, COLS_P), NEG, jnp.float32)

    def head(n, carry):
        hb = hmat[pl.ds(pl.multiple_of(n * 256, 256), 256), :]
        zt = lax.dot_general(wbuf[...], hb, (((1,), (1,)), ((), ())), preferred_element_type=jnp.float32)
        zt = zt * INV_TEMP
        z[0:SHARD, pl.ds(pl.multiple_of(n * 256, 256), 256)] = zt
        top = jnp.max(zt, axis=0, keepdims=True)
        peak[pl.ds(2 * n, 1), :] = top[:, 0:LANES]
        peak[pl.ds(2 * n + 1, 1), :] = top[:, LANES:]
        return carry

    with scope('head'):
        lax.fori_loop(0, COLS_P // 256, head, 0)

    def local_stats(t, carry):
        cols = pl.ds(pl.multiple_of(t * LANES, LANES), LANES)

        m = peak[pl.ds(t, 1), :]

        def expo(n, s):
            rows = pl.ds(pl.multiple_of(n * 112, 8), 112)
            x = jnp.exp(z[rows, cols] - m)
            z[rows, cols] = x
            return s + jnp.sum(x.reshape(14, 8, LANES), axis=0)

        s8 = lax.fori_loop(0, 9, expo, jnp.zeros((8, LANES), jnp.float32), unroll=3)
        stat[pl.ds(t, 1), :] = m
        stat[pl.ds(CT + t, 1), :] = jnp.sum(s8, axis=0, keepdims=True)
        return carry

    stat[...] = jnp.zeros_like(stat)
    with scope('stats'):
        lax.fori_loop(0, CT, local_stats, 0)
    bcp = pltpu.make_async_copy(z.at[:, DRAFT * BATCH:COLS], bo_hbm, lsem.at[2])
    bcp.start()

    slot, grp = me % 8, me // 8
    near = lambda k: grp * 8 + k
    far = lambda k: k * 8 + slot
    local = stat[0:STAT, :]
    copies = reduce_stage(a1, slot, 8, sa1, ra1, near, local)
    with scope('ex1a'):
        class3(1, 1, 0, 3)
    with scope('round1a'):
        parts = finish(copies, a1)
    copies = reduce_stage(b1, grp, 16, sb1, rb1, far, merge_max_sum(parts))
    with scope('ex1b'):
        class3(1, 1, 3, 9)
        class2(1, 1)
        class2(1, 0)
        class1(1, 1)
        class1(1, 0)
        class0(1)
    with scope('round1b'):
        parts = finish(copies, b1)
    tot = merge_max_sum(parts)
    fac = jnp.exp(local[0:CT] - tot[0:CT]) / tot[CT:2 * CT]
    scale[0:CT, :] = fac
    out_ref[12:16, :] = jnp.concatenate([fac[DRAFT * BT:CT], fac[0:1]], axis=0)

    exrows = exbuf.reshape(exbuf.shape[0], LANES)
    first_id = me * SHARD
    stat[...] = jnp.zeros_like(stat)
    for i in range(DRAFT):
        with scope(f'a2a_{i}'):
            pltpu.make_async_copy(recv.at[i], recv.at[i], qr_sem.at[i]).wait()
        for t in range(BT):
            row = i * BT + t
            sc = scale[row:row + 1, :]
            tok = tok_ref[i:i + 1, t * LANES:(t + 1) * LANES] - first_id
            col0 = i * BATCH + t * LANES

            def block(c, carry, size, valid):
                mass, pp, qp = carry
                q = recv[i, pl.ds(t * LANES * CHUNKS + c, LANES, stride=CHUNKS), :].T
                p = z[pl.ds(pl.multiple_of(c * LANES, LANES), size), col0:col0 + LANES] * sc
                ids = lax.broadcasted_iota(jnp.int32, (size, LANES), 0)
                q = q[0:size]
                if valid < size:
                    q = jnp.where(ids < valid, q, 0.0)
                x = jnp.maximum(p - q, 0.0)
                exrows[pl.ds(c * LANES * 6 + t * 2 + i, valid, stride=6), :] = x[0:valid]
                hit = ids == tok - c * LANES
                fold = lambda v: jnp.sum(v.reshape(size // 8, 8, LANES), axis=0)
                return (mass + fold(x), pp + fold(jnp.where(hit, p, 0.0)), qp + fold(jnp.where(hit, q, 0.0)))

            zero = jnp.zeros((8, LANES), jnp.float32)
            carry = lax.fori_loop(0, CHUNKS - 1, lambda c, v: block(c, v, LANES, LANES), (zero, zero, zero),
                                  unroll=CHUNKS - 1)
            mass, pp, qp = block(CHUNKS - 1, carry, TAIL_P, TAIL)
            stat[row:row + 1, :] = jnp.sum(mass, axis=0, keepdims=True)
            stat[6 + row:7 + row, :] = jnp.sum(pp, axis=0, keepdims=True)
            stat[12 + row:13 + row, :] = jnp.sum(qp, axis=0, keepdims=True)

    ecp = pltpu.make_async_copy(exbuf, ex_hbm, lsem.at[0])
    ecp.start()
    copies = reduce_stage(a2, slot, 8, sa2, ra2, near, stat[0:STAT, :])
    with scope('round2a'):
        parts = finish(copies, a2)
    copies = reduce_stage(b2, grp, 16, sb2, rb2, far, merge_add(parts))
    with scope('round2b'):
        parts = finish(copies, b2)
    tot = merge_add(parts)
    out_ref[0:6, :] = tot[0:6]
    out_ref[6:12, :] = jnp.minimum(tot[6:12] / tot[12:18], 1.0)
    with scope('tail'):
        ecp.wait()
        bcp.wait()
        for cp in c0 + c1 + c2 + d2d:
            cp.wait_send()
        for i in range(DRAFT):
            part = send.at[i, pl.ds(0, (DEV - 1) * BLK)]
            pltpu.make_async_copy(part, part, qs_sem.at[i]).wait()


def finish_kernel(ex_ref, bo_ref, stat_ref, res_hbm, bonus_hbm, acc_ref, exp_ref, res, bonus, sems):
    rows = ex_ref.reshape(ex_ref.shape[0], LANES)
    out = res.reshape(res.shape[0], LANES)
    copies = []
    fac = jnp.concatenate([stat_ref[12 + t:13 + t, :] for t in range(BT)], axis=1)
    step = 256
    for n in range(4):
        size = min(step, SHARD - n * step)
        bonus[n * step:n * step + size, :] = bo_ref[n * step:n * step + size, :] * fac
    cp = pltpu.make_async_copy(bonus, bonus_hbm, sems.at[0])
    cp.start()
    copies.append(cp)
    mass = jnp.concatenate([stat_ref[i * BT + t:i * BT + t + 1, :] for t in range(BT) for i in range(DRAFT)], axis=0)
    mass = jnp.concatenate([mass] * 4, axis=0)
    for n in range(5):
        def body(k, carry):
            at = pl.ds(pl.multiple_of(n * 1200 + k * 24, 8), 24)
            out[at, :] = rows[at, :] / mass
            return carry

        lax.fori_loop(0, 50, body, 0, unroll=5)
        size = 1200
        if n == 4:
            out[6000:6012, :] = rows[6000:6012, :] / mass[0:12]
            size = 1212
        cp = pltpu.make_async_copy(res.at[pl.ds(n * 1200, size)], res_hbm.at[pl.ds(n * 1200, size)], sems.at[1 + n])
        cp.start()
        copies.append(cp)
    acc = stat_ref[6:12, :]
    more = acc[0:BT] * (1.0 + acc[BT:2 * BT])
    for t in range(BT):
        cols = slice(t * LANES, (t + 1) * LANES)
        exp_ref[cols] = more[t]
        for i in range(DRAFT):
            acc_ref[i:i + 1, cols] = acc[i * BT + t:i * BT + t + 1]
    for cp in copies:
        cp.wait()


def verify_local(hid, w_cols, q_rows, draft_tok):
    q = with_layout_constraint(q_rows.reshape(SEQ, DRAFT, TILES, LANES), Layout((0, 2, 1, 3)))
    q = q.transpose(0, 2, 1, 3).reshape(SEQ * TILES * DRAFT, 1, LANES)
    f32 = jnp.float32
    hbm = pl.BlockSpec(memory_space=pl.ANY)
    vmem = pl.BlockSpec(memory_space=pltpu.VMEM)
    dma = pltpu.SemaphoreType.DMA
    ex, bo, st = pl.pallas_call(
        kernel,
        out_shape=[
            jax.ShapeDtypeStruct((SHARD * BT * DRAFT, 1, LANES), f32),
            jax.ShapeDtypeStruct((ROWS_P, BATCH), f32),
            jax.ShapeDtypeStruct((16, LANES), f32),
        ],
        in_specs=[pl.BlockSpec(memory_space=pltpu.HBM)] * 4,
        out_specs=[hbm, hbm, vmem],
        scratch_shapes=[
            pltpu.VMEM((DRAFT, BATCH), jnp.int32),
            pltpu.VMEM((SEQ * TILES * DRAFT + 20, 1, LANES), f32),
            pltpu.VMEM((SHARD, DIM), jnp.bfloat16),
            pltpu.VMEM((SEQ, NPOS, DIM), jnp.bfloat16),
            pltpu.VMEM((DEV * HROWS, LANES), jnp.bfloat16),
            pltpu.VMEM((48 * PITCH, LANES), f32),
            pltpu.VMEM((COLS_P, DIM), jnp.bfloat16),
            pltpu.VMEM((ROWS_P, COLS_P), f32),
            pltpu.VMEM((DRAFT, DEV * BLK, LANES), f32),
            pltpu.VMEM((DRAFT, DEV * BLK, LANES), f32),
            pltpu.VMEM((SHARD * BT * DRAFT, 1, LANES), f32),
            pltpu.VMEM((24, LANES), f32),
            pltpu.VMEM((16, LANES), f32),
            pltpu.VMEM((16, LANES), f32),
            pltpu.VMEM((8 * STAT, 1, LANES), f32),
            pltpu.VMEM((16 * STAT, 1, LANES), f32),
            pltpu.VMEM((8 * STAT, 1, LANES), f32),
            pltpu.VMEM((16 * STAT, 1, LANES), f32),
            dma((4,)),
            dma((3, 3, 3)), dma((3, 3, 3)), dma((3,)), dma((3,)),
            dma((2,)), dma((2,)),
            dma((7,)), dma((7,)), dma((15,)), dma((15,)),
            dma((7,)), dma((7,)), dma((15,)), dma((15,)),
        ],
        compiler_params=pltpu.CompilerParams(vmem_limit_bytes=40 * 2 ** 20, has_side_effects=True, collective_id=0),
    )(*(pltpu.with_memory_space_constraint(x, pltpu.HBM) for x in (q, w_cols.T, hid, draft_tok.T)))
    res, bonus, acc, expected = pl.pallas_call(
        finish_kernel,
        out_shape=[
            jax.ShapeDtypeStruct((SHARD * BT * DRAFT, 1, LANES), f32),
            jax.ShapeDtypeStruct((SHARD, BATCH), f32),
            jax.ShapeDtypeStruct((DRAFT, BATCH), f32),
            jax.ShapeDtypeStruct((BATCH,), f32),
        ],
        in_specs=[vmem] * 3,
        out_specs=[hbm, hbm, vmem, vmem],
        scratch_shapes=[
            pltpu.VMEM((SHARD * BT * DRAFT, 1, LANES), f32),
            pltpu.VMEM((SHARD, BATCH), f32),
            dma((6,)),
        ],
        compiler_params=pltpu.CompilerParams(vmem_limit_bytes=12 * 2 ** 20),
    )(ex, bo, st)
    res = with_layout_constraint(res.reshape(SHARD, BT, DRAFT, LANES).transpose(0, 2, 1, 3), Layout((0, 2, 1, 3)))
    residual = res.reshape(SHARD, DRAFT, BATCH).transpose(2, 1, 0)
    return acc.T, expected, residual, bonus.T


def solution(mesh):
    return jax.shard_map(
        verify_local,
        mesh=mesh,
        in_specs=(P(('dp', 'tp'), None, None), P(None, 'tp'), P(('dp', 'tp'), None, None), P('dp', None)),
        out_specs=(P('dp', None), P('dp'), P('dp', None, 'tp'), P('dp', 'tp')),
        check_vma=False,
    )
```

```python
import functools

import jax
import jax.numpy as jnp
from jax import lax
from jax.experimental import pallas as pl
from jax.experimental.layout import Layout, with_layout_constraint
from jax.experimental.pallas import tpu as pltpu
from jax.sharding import PartitionSpec as P

INV_TEMP = 1.25
DEV = 128
SEQ = 3
NPOS = 3
DRAFT = 2
BATCH = 384
DIM = 2048
VOCAB = 128256
SHARD = VOCAB // DEV
LANES = 128
TILES = VOCAB // LANES
CHUNKS = 8
TAIL = SHARD - (CHUNKS - 1) * LANES
ROWS_P = 1008
TAIL_P = ROWS_P - (CHUNKS - 1) * LANES
KC = DIM // LANES
HROWS = SEQ * NPOS * KC
COLS = NPOS * BATCH
COLS_P = 1280
CT = COLS // LANES
BT = BATCH // LANES
BLK = SEQ * CHUNKS
PITCH = 49
NEG = -1e30
STAT = 18
MESH = pl.DeviceIdType.MESH


def remote(src, dst, ssem, rsem, dev):
    return pltpu.make_async_remote_copy(
        src_ref=src, dst_ref=dst, send_sem=ssem, recv_sem=rsem,
        device_id={'tp': dev}, device_id_type=MESH)


def reduce_stage(buf, slot, count, ssem, rsem, device, payload):
    buf.reshape(count * STAT, LANES)[pl.ds(slot * STAT, STAT), :] = payload
    here = buf.at[pl.ds(slot * STAT, STAT)]
    for r in range(1, count):
        remote(here, here, ssem, rsem, device((slot + r) % count)).start()


def wait_rows(ref, rows, sem):
    part = ref.at[pl.ds(0, rows)]
    pltpu.make_async_copy(part, part, sem).wait()


def finish(buf, count, rsem):
    wait_rows(buf, (count - 1) * STAT, rsem)
    rows = buf.reshape(count * STAT, LANES)
    return [rows[k * STAT:(k + 1) * STAT, :] for k in range(count)]


def merge_max_sum(parts):
    m = parts[0][0:CT]
    for p in parts[1:]:
        m = jnp.maximum(m, p[0:CT])
    s = parts[0][CT:2 * CT] * jnp.exp(parts[0][0:CT] - m)
    for p in parts[1:]:
        s = s + p[CT:2 * CT] * jnp.exp(p[0:CT] - m)
    return jnp.concatenate([m, s], axis=0)


def merge_add(parts):
    total = parts[0]
    for p in parts[1:]:
        total = total + p
    return total


def kernel(q_hbm, w_hbm, h_hbm, tok_hbm,
           ex_hbm, bo_hbm, out_ref,
           tok_ref, qbuf, wbuf, hloc, hidb, bounce, hmat, z, send, recv, exbuf, stat, peak, scale,
           a1, b1, a2, b2,
           lsem, ag_s, ag_r, d2d_s, d2d_r, qs, qr_sem, rs, rr):
    scope = jax.named_scope
    me = lax.axis_index('tp')
    core = me % 2
    coord = (me // 32, (me // 8) % 4, (me // 2) % 4)
    unit = (32, 8, 2)
    partner = me + 1 - 2 * core
    hop = [[((coord[d] + r) % 4) * unit[d] for r in range(4)] for d in range(3)]

    def device(rz, ry, rx, rc):
        return hop[0][rz] + hop[1][ry] + hop[2][rx] + (core if rc == 0 else 1 - core)

    hcp = pltpu.make_async_copy(h_hbm, hloc, lsem.at[2])
    hcp.start()
    qcp = pltpu.make_async_copy(q_hbm, qbuf.at[pl.ds(0, SEQ * TILES * DRAFT)], lsem.at[0])
    qcp.start()
    wcp = pltpu.make_async_copy(w_hbm, wbuf, lsem.at[1])
    wcp.start()
    tcp = pltpu.make_async_copy(tok_hbm, tok_ref, lsem.at[3])
    tcp.start()
    barrier = pltpu.get_barrier_semaphore()
    peers = [partner]
    for d in range(3):
        for r in range(1, 4):
            steps = [0, 0, 0]
            steps[d] = r
            peers.append(device(*steps, 0))
    for dev in peers:
        pl.semaphore_signal(barrier, inc=1, device_id={'tp': dev}, device_id_type=MESH)

    with scope('hid'):
        hcp.wait()
        for s in range(SEQ):
            x = hloc[s].astype(jnp.float32)
            for kc in range(KC):
                bounce[pl.ds(s * 48 + kc, NPOS, stride=KC), :] = x[:, kc * LANES:(kc + 1) * LANES]
        hidb[pl.ds(pl.multiple_of(me * HROWS, 16), HROWS), :] = bounce[0:HROWS, :].astype(jnp.bfloat16)
    with scope('barrier'):
        pl.semaphore_wait(barrier, len(peers))

    hview = hidb.reshape(4, 4, 4, 2, SEQ, HROWS // SEQ, LANES)

    def ag_phase(phase):
        for j in range(3):
            order = [(j + k) % 3 for k in range(3)]
            idx = list(coord)
            for d in order[:phase]:
                idx[d] = slice(None)
            view = hview.at[idx[0], idx[1], idx[2], core, j]
            for r in (1, 3, 2):
                steps = [0, 0, 0]
                steps[order[phase]] = r
                remote(view, view, ag_s, ag_r.at[phase, j], device(*steps, 0)).start()

    def ag_wait(phase, j):
        wait_rows(hidb, 3 * 4 ** phase * (HROWS // SEQ), ag_r.at[phase, j])

    qrows = qbuf.reshape(qbuf.shape[0], LANES)
    lane = lax.broadcasted_iota(jnp.int32, (8, LANES), 1)

    def pack(i, k, carry):
        first = (SHARD * k) // LANES
        off = (SHARD * k) % LANES
        shift = (LANES - off) % LANES
        keep = lane < LANES - off
        for s in range(SEQ):
            base = (s * TILES + first) * DRAFT + i
            lo = qrows[pl.ds(base, 8, stride=2), :]
            hi = qrows[pl.ds(base + 2, 8, stride=2), :]
            lo = pltpu.roll(lo, shift, 1)
            hi = pltpu.roll(hi, shift, 1)
            send[i, pl.ds(pl.multiple_of(k * BLK + s * 8, 8), 8), :] = jnp.where(keep, lo, hi)
        return carry

    mine = pl.ds(pl.multiple_of(me * BLK, 8), BLK)

    def to(i, dev):
        remote(send.at[i, pl.ds(pl.multiple_of(dev * BLK, 8), BLK)], recv.at[i, mine],
               qs, qr_sem.at[i], dev).start()

    def step(d, n):
        return ((coord[d] + n) % 4) * unit[d]

    def class0(i):
        pltpu.make_async_copy(send.at[i, mine], recv.at[i, mine], qr_sem.at[i]).start()
        to(i, partner)

    def class1(i, rc):
        last = core if rc == 0 else 1 - core
        for r in (1, 3, 2):
            for d in range(3):
                steps = [0, 0, 0]
                steps[d] = r
                to(i, device(*steps, rc))

    def class2(i, rc, lo=0, hi=9):
        last = core if rc == 0 else 1 - core

        def body(n, carry):
            a, b = n // 3 + 1, n % 3 + 1
            to(i, step(0, a) + step(1, b) + hop[2][0] + last)
            to(i, hop[0][0] + step(1, a) + step(2, b) + last)
            to(i, step(0, b) + hop[1][0] + step(2, a) + last)
            return carry

        lax.fori_loop(lo, hi, body, 0)

    def class3(i, rc, lo=0, hi=9):
        last = core if rc == 0 else 1 - core

        def body(n, carry):
            a, b = n // 3, n % 3
            for k in range(3):
                to(i, step(0, (a + k) % 3 + 1) + step(1, (b + k) % 3 + 1) + hop[2][k + 1] + last)
            return carry

        lax.fori_loop(lo, hi, body, 0)

    ag_phase(0)
    with scope('qwait'):
        qcp.wait()
    with scope('pack'):
        lax.fori_loop(0, DEV, functools.partial(pack, 0), 0, unroll=16)
    with scope('ex0'):
        class0(0)
        class1(0, 0)
    with scope('ag0'):
        for j in range(3):
            ag_wait(0, j)
    ag_phase(1)
    with scope('ex0a'):
        class1(0, 1)
        class2(0, 0)
    with scope('pack2'):
        lax.fori_loop(0, DEV, functools.partial(pack, 1), 0, unroll=16)
    with scope('ag1'):
        for j in range(3):
            ag_wait(1, j)
    ag_phase(2)
    with scope('exag2'):
        class3(0, 0, 0, 3)
    d2d = []
    for j in range(3):
        with scope(f'ag2_{j}'):
            ag_wait(2, j)
        view = hview.at[:, :, :, core, j]
        cp = remote(view, view, d2d_s, d2d_r.at[j], partner)
        cp.start()
        d2d.append(cp)
    with scope('ex0b'):
        class3(0, 0, 3, 9)
        class3(0, 1)
        class2(0, 1)
        class3(1, 0)
    with scope('d2d'):
        for cp in d2d:
            cp.wait_recv()

    def relayout(n, carry):
        def up(b, c):
            x = hidb[pl.ds(pl.multiple_of((48 * n + b) * 48, 16), 48), :]
            bounce[pl.ds(b * PITCH, 48), :] = x.astype(jnp.float32)
            return c

        lax.fori_loop(0, 48, up, 0, unroll=4)
        for g in range(NPOS):
            for u in range(3):
                for kc in range(KC):
                    y = bounce[pl.ds(16 * u * PITCH + g * KC + kc, 16, stride=PITCH), :]
                    hmat[pl.ds(pl.multiple_of(g * BATCH + 48 * n + 16 * u, 16), 16),
                         kc * LANES:(kc + 1) * LANES] = y.astype(jnp.bfloat16)
        return carry

    with scope('relayout'):
        lax.fori_loop(0, 8, relayout, 0)
    wcp.wait()
    tcp.wait()

    z[SHARD:ROWS_P, :] = jnp.full((ROWS_P - SHARD, COLS_P), NEG, jnp.float32)

    def head(n, carry):
        hb = hmat[pl.ds(pl.multiple_of(n * 256, 256), 256), :]
        zt = lax.dot_general(wbuf[...], hb, (((1,), (1,)), ((), ())), preferred_element_type=jnp.float32)
        zt = zt * INV_TEMP
        z[0:SHARD, pl.ds(pl.multiple_of(n * 256, 256), 256)] = zt
        top = jnp.max(zt, axis=0, keepdims=True)
        peak[pl.ds(2 * n, 1), :] = top[:, 0:LANES]
        peak[pl.ds(2 * n + 1, 1), :] = top[:, LANES:]
        return carry

    with scope('head'):
        lax.fori_loop(0, COLS_P // 256, head, 0)

    def local_stats(t, carry):
        cols = pl.ds(pl.multiple_of(t * LANES, LANES), LANES)

        m = peak[pl.ds(t, 1), :]

        def expo(n, s):
            rows = pl.ds(pl.multiple_of(n * 112, 8), 112)
            x = jnp.exp(z[rows, cols] - m)
            z[rows, cols] = x
            return s + jnp.sum(x.reshape(14, 8, LANES), axis=0)

        s8 = lax.fori_loop(0, 9, expo, jnp.zeros((8, LANES), jnp.float32), unroll=3)
        stat[pl.ds(t, 1), :] = m
        stat[pl.ds(CT + t, 1), :] = jnp.sum(s8, axis=0, keepdims=True)
        return carry

    stat[...] = jnp.zeros_like(stat)
    with scope('stats'):
        lax.fori_loop(0, CT, local_stats, 0)
    bcp = pltpu.make_async_copy(z.at[:, DRAFT * BATCH:COLS], bo_hbm, lsem.at[2])
    bcp.start()

    slot, grp = me % 8, me // 8
    near = lambda k: grp * 8 + k
    far = lambda k: k * 8 + slot
    local = stat[0:STAT, :]
    reduce_stage(a1, slot, 8, rs, rr.at[0], near, local)
    with scope('ex1a'):
        class3(1, 1, 0, 3)
    with scope('round1a'):
        parts = finish(a1, 8, rr.at[0])
    reduce_stage(b1, grp, 16, rs, rr.at[1], far, merge_max_sum(parts))
    with scope('ex1b'):
        class3(1, 1, 3, 9)
        class2(1, 1)
        class2(1, 0)
        class1(1, 1)
        class1(1, 0)
        class0(1)
    with scope('round1b'):
        parts = finish(b1, 16, rr.at[1])
    tot = merge_max_sum(parts)
    fac = jnp.exp(local[0:CT] - tot[0:CT]) / tot[CT:2 * CT]
    scale[0:CT, :] = fac
    out_ref[12:16, :] = jnp.concatenate([fac[DRAFT * BT:CT], fac[0:1]], axis=0)

    exrows = exbuf.reshape(exbuf.shape[0], LANES)
    first_id = me * SHARD
    stat[...] = jnp.zeros_like(stat)
    for i in range(DRAFT):
        with scope(f'a2a_{i}'):
            pltpu.make_async_copy(recv.at[i], recv.at[i], qr_sem.at[i]).wait()
        for t in range(BT):
            row = i * BT + t
            sc = scale[row:row + 1, :]
            tok = tok_ref[i:i + 1, t * LANES:(t + 1) * LANES] - first_id
            col0 = i * BATCH + t * LANES

            def block(c, carry, size, valid):
                mass, pp, qp = carry
                q = recv[i, pl.ds(t * LANES * CHUNKS + c, LANES, stride=CHUNKS), :].T
                p = z[pl.ds(pl.multiple_of(c * LANES, LANES), size), col0:col0 + LANES] * sc
                ids = lax.broadcasted_iota(jnp.int32, (size, LANES), 0)
                q = q[0:size]
                if valid < size:
                    q = jnp.where(ids < valid, q, 0.0)
                x = jnp.maximum(p - q, 0.0)
                exrows[pl.ds(c * LANES * 6 + t * 2 + i, valid, stride=6), :] = x[0:valid]
                hit = ids == tok - c * LANES
                fold = lambda v: jnp.sum(v.reshape(size // 8, 8, LANES), axis=0)
                return (mass + fold(x), pp + fold(jnp.where(hit, p, 0.0)), qp + fold(jnp.where(hit, q, 0.0)))

            zero = jnp.zeros((8, LANES), jnp.float32)
            carry = lax.fori_loop(0, CHUNKS - 1, lambda c, v: block(c, v, LANES, LANES), (zero, zero, zero),
                                  unroll=CHUNKS - 1)
            mass, pp, qp = block(CHUNKS - 1, carry, TAIL_P, TAIL)
            stat[row:row + 1, :] = jnp.sum(mass, axis=0, keepdims=True)
            stat[6 + row:7 + row, :] = jnp.sum(pp, axis=0, keepdims=True)
            stat[12 + row:13 + row, :] = jnp.sum(qp, axis=0, keepdims=True)

    ecp = pltpu.make_async_copy(exbuf, ex_hbm, lsem.at[0])
    ecp.start()
    reduce_stage(a2, slot, 8, rs, rr.at[2], near, stat[0:STAT, :])
    with scope('round2a'):
        parts = finish(a2, 8, rr.at[2])
    reduce_stage(b2, grp, 16, rs, rr.at[3], far, merge_add(parts))
    with scope('round2b'):
        parts = finish(b2, 16, rr.at[3])
    tot = merge_add(parts)
    out_ref[0:6, :] = tot[0:6]
    out_ref[6:12, :] = jnp.minimum(tot[6:12] / tot[12:18], 1.0)
    with scope('tail'):
        ecp.wait()
        bcp.wait()
        wait_rows(hidb, 9 * 21 * (HROWS // SEQ), ag_s)
        wait_rows(hidb, DEV // 2 * HROWS, d2d_s)
        wait_rows(send.reshape(DRAFT * DEV * BLK, LANES), DRAFT * (DEV - 1) * BLK, qs)
        wait_rows(qbuf, 2 * (7 + 15) * STAT, rs)


def finish_kernel(ex_ref, bo_ref, stat_ref, res_hbm, bonus_hbm, acc_ref, exp_ref, res, bonus, sems):
    rows = ex_ref.reshape(ex_ref.shape[0], LANES)
    out = res.reshape(res.shape[0], LANES)
    copies = []
    fac = jnp.concatenate([stat_ref[12 + t:13 + t, :] for t in range(BT)], axis=1)
    step = 256
    for n in range(4):
        size = min(step, SHARD - n * step)
        bonus[n * step:n * step + size, :] = bo_ref[n * step:n * step + size, :] * fac
    cp = pltpu.make_async_copy(bonus, bonus_hbm, sems)
    cp.start()
    copies.append(cp)
    mass = jnp.concatenate([stat_ref[i * BT + t:i * BT + t + 1, :] for t in range(BT) for i in range(DRAFT)], axis=0)
    mass = jnp.concatenate([mass] * 4, axis=0)
    for n in range(5):
        def body(k, carry):
            at = pl.ds(pl.multiple_of(n * 1200 + k * 24, 8), 24)
            out[at, :] = rows[at, :] / mass
            return carry

        lax.fori_loop(0, 50, body, 0, unroll=5)
        size = 1200
        if n == 4:
            out[6000:6012, :] = rows[6000:6012, :] / mass[0:12]
            size = 1212
        cp = pltpu.make_async_copy(res.at[pl.ds(n * 1200, size)], res_hbm.at[pl.ds(n * 1200, size)], sems)
        cp.start()
        copies.append(cp)
    acc = stat_ref[6:12, :]
    more = acc[0:BT] * (1.0 + acc[BT:2 * BT])
    for t in range(BT):
        cols = slice(t * LANES, (t + 1) * LANES)
        exp_ref[cols] = more[t]
        for i in range(DRAFT):
            acc_ref[i:i + 1, cols] = acc[i * BT + t:i * BT + t + 1]
    for cp in copies:
        cp.wait()


def verify_local(hid, w_cols, q_rows, draft_tok):
    q = with_layout_constraint(q_rows.reshape(SEQ, DRAFT, TILES, LANES), Layout((0, 2, 1, 3)))
    q = q.transpose(0, 2, 1, 3).reshape(SEQ * TILES * DRAFT, 1, LANES)
    f32 = jnp.float32
    hbm = pl.BlockSpec(memory_space=pl.ANY)
    vmem = pl.BlockSpec(memory_space=pltpu.VMEM)
    dma = pltpu.SemaphoreType.DMA
    ex, bo, st = pl.pallas_call(
        kernel,
        out_shape=[
            jax.ShapeDtypeStruct((SHARD * BT * DRAFT, 1, LANES), f32),
            jax.ShapeDtypeStruct((ROWS_P, BATCH), f32),
            jax.ShapeDtypeStruct((16, LANES), f32),
        ],
        in_specs=[pl.BlockSpec(memory_space=pltpu.HBM)] * 4,
        out_specs=[hbm, hbm, vmem],
        scratch_shapes=[
            pltpu.VMEM((DRAFT, BATCH), jnp.int32),
            pltpu.VMEM((SEQ * TILES * DRAFT + 20, 1, LANES), f32),
            pltpu.VMEM((SHARD, DIM), jnp.bfloat16),
            pltpu.VMEM((SEQ, NPOS, DIM), jnp.bfloat16),
            pltpu.VMEM((DEV * HROWS, LANES), jnp.bfloat16),
            pltpu.VMEM((48 * PITCH, LANES), f32),
            pltpu.VMEM((COLS_P, DIM), jnp.bfloat16),
            pltpu.VMEM((ROWS_P, COLS_P), f32),
            pltpu.VMEM((DRAFT, DEV * BLK, LANES), f32),
            pltpu.VMEM((DRAFT, DEV * BLK, LANES), f32),
            pltpu.VMEM((SHARD * BT * DRAFT, 1, LANES), f32),
            pltpu.VMEM((24, LANES), f32),
            pltpu.VMEM((16, LANES), f32),
            pltpu.VMEM((16, LANES), f32),
            pltpu.VMEM((8 * STAT, 1, LANES), f32),
            pltpu.VMEM((16 * STAT, 1, LANES), f32),
            pltpu.VMEM((8 * STAT, 1, LANES), f32),
            pltpu.VMEM((16 * STAT, 1, LANES), f32),
            dma((4,)),
            dma, dma((3, 3)), dma, dma((3,)), dma, dma((2,)), dma, dma((4,)),
        ],
        compiler_params=pltpu.CompilerParams(vmem_limit_bytes=40 * 2 ** 20, has_side_effects=True, collective_id=0),
    )(*(pltpu.with_memory_space_constraint(x, pltpu.HBM) for x in (q, w_cols.T, hid, draft_tok.T)))
    res, bonus, acc, expected = pl.pallas_call(
        finish_kernel,
        out_shape=[
            jax.ShapeDtypeStruct((SHARD * BT * DRAFT, 1, LANES), f32),
            jax.ShapeDtypeStruct((SHARD, BATCH), f32),
            jax.ShapeDtypeStruct((DRAFT, BATCH), f32),
            jax.ShapeDtypeStruct((BATCH,), f32),
        ],
        in_specs=[vmem] * 3,
        out_specs=[hbm, hbm, vmem, vmem],
        scratch_shapes=[
            pltpu.VMEM((SHARD * BT * DRAFT, 1, LANES), f32),
            pltpu.VMEM((SHARD, BATCH), f32),
            dma,
        ],
        compiler_params=pltpu.CompilerParams(vmem_limit_bytes=12 * 2 ** 20),
    )(ex, bo, st)
    res = with_layout_constraint(res.reshape(SHARD, BT, DRAFT, LANES).transpose(0, 2, 1, 3), Layout((0, 2, 1, 3)))
    residual = res.reshape(SHARD, DRAFT, BATCH).transpose(2, 1, 0)
    return acc.T, expected, residual, bonus.T


def solution(mesh):
    return jax.shard_map(
        verify_local,
        mesh=mesh,
        in_specs=(P(('dp', 'tp'), None, None), P(None, 'tp'), P(('dp', 'tp'), None, None), P('dp', None)),
        out_specs=(P('dp', None), P('dp'), P('dp', None, 'tp'), P('dp', 'tp')),
        check_vma=False,
    )
```

```python
import functools

import jax
import jax.numpy as jnp
from jax import lax
from jax.experimental import pallas as pl
from jax.experimental.layout import Layout, with_layout_constraint
from jax.experimental.pallas import tpu as pltpu
from jax.sharding import PartitionSpec as P

INV_TEMP = 1.25
DEV = 128
SEQ = 3
NPOS = 3
DRAFT = 2
BATCH = 384
DIM = 2048
VOCAB = 128256
SHARD = VOCAB // DEV
LANES = 128
TILES = VOCAB // LANES
CHUNKS = 8
TAIL = SHARD - (CHUNKS - 1) * LANES
ROWS_P = 1008
TAIL_P = ROWS_P - (CHUNKS - 1) * LANES
KC = DIM // LANES
HROWS = SEQ * NPOS * KC
COLS = NPOS * BATCH
COLS_P = 1280
CT = COLS // LANES
BT = BATCH // LANES
BLK = SEQ * CHUNKS
PITCH = 49
NEG = -1e30
STAT = 18
MESH = pl.DeviceIdType.MESH


def remote(src, dst, ssem, rsem, dev):
    return pltpu.make_async_remote_copy(
        src_ref=src, dst_ref=dst, send_sem=ssem, recv_sem=rsem,
        device_id={'tp': dev}, device_id_type=MESH)


def reduce_stage(buf, slot, count, ssem, rsem, device, payload):
    buf.reshape(count * STAT, LANES)[pl.ds(slot * STAT, STAT), :] = payload
    here = buf.at[pl.ds(slot * STAT, STAT)]
    for r in range(1, count):
        remote(here, here, ssem, rsem, device((slot + r) % count)).start()


def wait_rows(ref, rows, sem):
    part = ref.at[pl.ds(0, rows)]
    pltpu.make_async_copy(part, part, sem).wait()


def finish(buf, count, rsem):
    wait_rows(buf, (count - 1) * STAT, rsem)
    rows = buf.reshape(count * STAT, LANES)
    return [rows[k * STAT:(k + 1) * STAT, :] for k in range(count)]


def merge_max_sum(parts):
    m = parts[0][0:CT]
    for p in parts[1:]:
        m = jnp.maximum(m, p[0:CT])
    s = parts[0][CT:2 * CT] * jnp.exp(parts[0][0:CT] - m)
    for p in parts[1:]:
        s = s + p[CT:2 * CT] * jnp.exp(p[0:CT] - m)
    return jnp.concatenate([m, s], axis=0)


def merge_add(parts):
    total = parts[0]
    for p in parts[1:]:
        total = total + p
    return total


def kernel(q_hbm, w_hbm, h_hbm, tok_hbm,
           ex_hbm, bo_hbm, out_ref,
           tok_ref, qbuf, wbuf, hloc, hidb, bounce, hmat, z, send, recv, exbuf, stat, peak, scale,
           a1, b1, a2, b2, c2,
           lsem, ag_s, ag_r, d2d_s, d2d_r, qs, qr_sem, rs, rr):
    scope = jax.named_scope
    me = lax.axis_index('tp')
    core = me % 2
    coord = (me // 32, (me // 8) % 4, (me // 2) % 4)
    unit = (32, 8, 2)
    partner = me + 1 - 2 * core
    hop = [[((coord[d] + r) % 4) * unit[d] for r in range(4)] for d in range(3)]

    def device(rz, ry, rx, rc):
        return hop[0][rz] + hop[1][ry] + hop[2][rx] + (core if rc == 0 else 1 - core)

    hcp = pltpu.make_async_copy(h_hbm, hloc, lsem.at[2])
    hcp.start()
    qcp = pltpu.make_async_copy(q_hbm, qbuf.at[pl.ds(0, SEQ * TILES * DRAFT)], lsem.at[0])
    qcp.start()
    wcp = pltpu.make_async_copy(w_hbm, wbuf, lsem.at[1])
    wcp.start()
    tcp = pltpu.make_async_copy(tok_hbm, tok_ref, lsem.at[3])
    tcp.start()
    barrier = pltpu.get_barrier_semaphore()
    peers = [partner]
    for d in range(3):
        for r in range(1, 4):
            steps = [0, 0, 0]
            steps[d] = r
            peers.append(device(*steps, 0))
    for dev in peers:
        pl.semaphore_signal(barrier, inc=1, device_id={'tp': dev}, device_id_type=MESH)

    with scope('hid'):
        hcp.wait()
        for s in range(SEQ):
            x = hloc[s].astype(jnp.float32)
            for kc in range(KC):
                bounce[pl.ds(s * 48 + kc, NPOS, stride=KC), :] = x[:, kc * LANES:(kc + 1) * LANES]
        hidb[pl.ds(pl.multiple_of(me * HROWS, 16), HROWS), :] = bounce[0:HROWS, :].astype(jnp.bfloat16)
    with scope('barrier'):
        pl.semaphore_wait(barrier, len(peers))

    hview = hidb.reshape(4, 4, 4, 2, SEQ, HROWS // SEQ, LANES)

    def ag_phase(phase):
        for j in range(3):
            order = [(j + k) % 3 for k in range(3)]
            idx = list(coord)
            for d in order[:phase]:
                idx[d] = slice(None)
            view = hview.at[idx[0], idx[1], idx[2], core, j]
            for r in (1, 3, 2):
                steps = [0, 0, 0]
                steps[order[phase]] = r
                remote(view, view, ag_s, ag_r.at[phase, j], device(*steps, 0)).start()

    def ag_wait(phase, j):
        wait_rows(hidb, 3 * 4 ** phase * (HROWS // SEQ), ag_r.at[phase, j])

    qrows = qbuf.reshape(qbuf.shape[0], LANES)
    lane = lax.broadcasted_iota(jnp.int32, (8, LANES), 1)

    def pack(i, k, carry):
        first = (SHARD * k) // LANES
        off = (SHARD * k) % LANES
        shift = (LANES - off) % LANES
        keep = lane < LANES - off
        for s in range(SEQ):
            base = (s * TILES + first) * DRAFT + i
            lo = qrows[pl.ds(base, 8, stride=2), :]
            hi = qrows[pl.ds(base + 2, 8, stride=2), :]
            lo = pltpu.roll(lo, shift, 1)
            hi = pltpu.roll(hi, shift, 1)
            send[i, pl.ds(pl.multiple_of(k * BLK + s * 8, 8), 8), :] = jnp.where(keep, lo, hi)
        return carry

    mine = pl.ds(pl.multiple_of(me * BLK, 8), BLK)

    def to(i, dev):
        remote(send.at[i, pl.ds(pl.multiple_of(dev * BLK, 8), BLK)], recv.at[i, mine],
               qs, qr_sem.at[i], dev).start()

    def step(d, n):
        return ((coord[d] + n) % 4) * unit[d]

    def class0(i):
        pltpu.make_async_copy(send.at[i, mine], recv.at[i, mine], qr_sem.at[i]).start()
        to(i, partner)

    def class1(i, rc):
        last = core if rc == 0 else 1 - core
        for r in (1, 3, 2):
            for d in range(3):
                steps = [0, 0, 0]
                steps[d] = r
                to(i, device(*steps, rc))

    def class2(i, rc, lo=0, hi=9):
        last = core if rc == 0 else 1 - core

        def body(n, carry):
            a, b = n // 3 + 1, n % 3 + 1
            to(i, step(0, a) + step(1, b) + hop[2][0] + last)
            to(i, hop[0][0] + step(1, a) + step(2, b) + last)
            to(i, step(0, b) + hop[1][0] + step(2, a) + last)
            return carry

        lax.fori_loop(lo, hi, body, 0)

    def class3(i, rc, lo=0, hi=9):
        last = core if rc == 0 else 1 - core

        def body(n, carry):
            a, b = n // 3, n % 3
            for k in range(3):
                to(i, step(0, (a + k) % 3 + 1) + step(1, (b + k) % 3 + 1) + hop[2][k + 1] + last)
            return carry

        lax.fori_loop(lo, hi, body, 0)

    ag_phase(0)
    with scope('qwait'):
        qcp.wait()
    with scope('pack'):
        lax.fori_loop(0, DEV, functools.partial(pack, 0), 0, unroll=16)
    with scope('ex0'):
        class0(0)
        class1(0, 0)
    with scope('ag0'):
        for j in range(3):
            ag_wait(0, j)
    ag_phase(1)
    with scope('ex0a'):
        class1(0, 1)
        class2(0, 0)
    with scope('pack2'):
        lax.fori_loop(0, DEV, functools.partial(pack, 1), 0, unroll=16)
    with scope('ag1'):
        for j in range(3):
            ag_wait(1, j)
    ag_phase(2)
    d2d = []
    for j in range(3):
        with scope(f'ag2_{j}'):
            ag_wait(2, j)
        view = hview.at[:, :, :, core, j]
        cp = remote(view, view, d2d_s, d2d_r.at[j], partner)
        cp.start()
        d2d.append(cp)
    with scope('ex0b'):
        class3(0, 0)
        class3(0, 1)
        class2(0, 1)
        class3(1, 0)
    with scope('d2d'):
        for cp in d2d:
            cp.wait_recv()

    def relayout(n, carry):
        def up(b, c):
            x = hidb[pl.ds(pl.multiple_of((48 * n + b) * 48, 16), 48), :]
            bounce[pl.ds(b * PITCH, 48), :] = x.astype(jnp.float32)
            return c

        lax.fori_loop(0, 48, up, 0, unroll=4)
        for g in range(NPOS):
            for u in range(3):
                for kc in range(KC):
                    y = bounce[pl.ds(16 * u * PITCH + g * KC + kc, 16, stride=PITCH), :]
                    hmat[pl.ds(pl.multiple_of(g * BATCH + 48 * n + 16 * u, 16), 16),
                         kc * LANES:(kc + 1) * LANES] = y.astype(jnp.bfloat16)
        return carry

    with scope('relayout'):
        lax.fori_loop(0, 8, relayout, 0)
    wcp.wait()
    tcp.wait()

    z[SHARD:ROWS_P, :] = jnp.full((ROWS_P - SHARD, COLS_P), NEG, jnp.float32)

    def head(n, carry):
        hb = hmat[pl.ds(pl.multiple_of(n * 256, 256), 256), :]
        zt = lax.dot_general(wbuf[...], hb, (((1,), (1,)), ((), ())), preferred_element_type=jnp.float32)
        zt = zt * INV_TEMP
        z[0:SHARD, pl.ds(pl.multiple_of(n * 256, 256), 256)] = zt
        top = jnp.max(zt, axis=0, keepdims=True)
        peak[pl.ds(2 * n, 1), :] = top[:, 0:LANES]
        peak[pl.ds(2 * n + 1, 1), :] = top[:, LANES:]
        return carry

    with scope('head'):
        lax.fori_loop(0, COLS_P // 256, head, 0)

    def local_stats(t, carry):
        cols = pl.ds(pl.multiple_of(t * LANES, LANES), LANES)

        m = peak[pl.ds(t, 1), :]

        def expo(n, s):
            rows = pl.ds(pl.multiple_of(n * 112, 8), 112)
            x = jnp.exp(z[rows, cols] - m)
            z[rows, cols] = x
            return s + jnp.sum(x.reshape(14, 8, LANES), axis=0)

        s8 = lax.fori_loop(0, 9, expo, jnp.zeros((8, LANES), jnp.float32), unroll=3)
        stat[pl.ds(t, 1), :] = m
        stat[pl.ds(CT + t, 1), :] = jnp.sum(s8, axis=0, keepdims=True)
        return carry

    stat[...] = jnp.zeros_like(stat)
    with scope('stats'):
        lax.fori_loop(0, CT, local_stats, 0)
    bcp = pltpu.make_async_copy(z.at[:, DRAFT * BATCH:COLS], bo_hbm, lsem.at[2])
    bcp.start()

    slot, grp = me % 8, me // 8
    near = lambda k: grp * 8 + k
    far = lambda k: k * 8 + slot
    local = stat[0:STAT, :]
    reduce_stage(a1, slot, 8, rs, rr.at[0], near, local)
    with scope('ex1a'):
        class3(1, 1, 0, 3)
    with scope('round1a'):
        parts = finish(a1, 8, rr.at[0])
    reduce_stage(b1, grp, 16, rs, rr.at[1], far, merge_max_sum(parts))
    with scope('ex1b'):
        class3(1, 1, 3, 9)
        class2(1, 1)
        class2(1, 0)
        class1(1, 1)
        class1(1, 0)
        class0(1)
    with scope('round1b'):
        parts = finish(b1, 16, rr.at[1])
    tot = merge_max_sum(parts)
    fac = jnp.exp(local[0:CT] - tot[0:CT]) / tot[CT:2 * CT]
    scale[0:CT, :] = fac
    out_ref[12:16, :] = jnp.concatenate([fac[DRAFT * BT:CT], fac[0:1]], axis=0)

    exrows = exbuf.reshape(exbuf.shape[0], LANES)
    first_id = me * SHARD
    stat[...] = jnp.zeros_like(stat)
    for i in range(DRAFT):
        with scope(f'a2a_{i}'):
            pltpu.make_async_copy(recv.at[i], recv.at[i], qr_sem.at[i]).wait()
        for t in range(BT):
            row = i * BT + t
            sc = scale[row:row + 1, :]
            tok = tok_ref[i:i + 1, t * LANES:(t + 1) * LANES] - first_id
            col0 = i * BATCH + t * LANES

            def block(c, carry, size, valid):
                mass, pp, qp = carry
                q = recv[i, pl.ds(t * LANES * CHUNKS + c, LANES, stride=CHUNKS), :].T
                p = z[pl.ds(pl.multiple_of(c * LANES, LANES), size), col0:col0 + LANES] * sc
                ids = lax.broadcasted_iota(jnp.int32, (size, LANES), 0)
                q = q[0:size]
                if valid < size:
                    q = jnp.where(ids < valid, q, 0.0)
                x = jnp.maximum(p - q, 0.0)
                exrows[pl.ds(c * LANES * 6 + t * 2 + i, valid, stride=6), :] = x[0:valid]
                hit = ids == tok - c * LANES
                fold = lambda v: jnp.sum(v.reshape(size // 8, 8, LANES), axis=0)
                return (mass + fold(x), pp + fold(jnp.where(hit, p, 0.0)), qp + fold(jnp.where(hit, q, 0.0)))

            zero = jnp.zeros((8, LANES), jnp.float32)
            carry = lax.fori_loop(0, CHUNKS - 1, lambda c, v: block(c, v, LANES, LANES), (zero, zero, zero),
                                  unroll=CHUNKS - 1)
            mass, pp, qp = block(CHUNKS - 1, carry, TAIL_P, TAIL)
            stat[row:row + 1, :] = jnp.sum(mass, axis=0, keepdims=True)
            stat[6 + row:7 + row, :] = jnp.sum(pp, axis=0, keepdims=True)
            stat[12 + row:13 + row, :] = jnp.sum(qp, axis=0, keepdims=True)

    ecp = pltpu.make_async_copy(exbuf, ex_hbm, lsem.at[0])
    ecp.start()
    reduce_stage(a2, slot, 8, rs, rr.at[2], near, stat[0:STAT, :])
    with scope('round2a'):
        parts = finish(a2, 8, rr.at[2])
    reduce_stage(b2, coord[1], 4, rs, rr.at[3], lambda k: coord[0] * 32 + k * 8 + slot, merge_add(parts))
    with scope('round2b'):
        parts = finish(b2, 4, rr.at[3])
    reduce_stage(c2, coord[0], 4, rs, rr.at[4], lambda k: k * 32 + coord[1] * 8 + slot, merge_add(parts))
    with scope('round2c'):
        parts = finish(c2, 4, rr.at[4])
    tot = merge_add(parts)
    out_ref[0:6, :] = tot[0:6]
    out_ref[6:12, :] = jnp.minimum(tot[6:12] / tot[12:18], 1.0)
    with scope('tail'):
        ecp.wait()
        bcp.wait()
        wait_rows(hidb, 9 * 21 * (HROWS // SEQ), ag_s)
        wait_rows(hidb, DEV // 2 * HROWS, d2d_s)
        wait_rows(send.reshape(DRAFT * DEV * BLK, LANES), DRAFT * (DEV - 1) * BLK, qs)
        wait_rows(qbuf, (7 + 15 + 7 + 3 + 3) * STAT, rs)


def finish_kernel(ex_ref, bo_ref, stat_ref, res_hbm, bonus_hbm, acc_ref, exp_ref, res, bonus, sems):
    rows = ex_ref.reshape(ex_ref.shape[0], LANES)
    out = res.reshape(res.shape[0], LANES)
    copies = []
    fac = jnp.concatenate([stat_ref[12 + t:13 + t, :] for t in range(BT)], axis=1)
    step = 256
    for n in range(4):
        size = min(step, SHARD - n * step)
        bonus[n * step:n * step + size, :] = bo_ref[n * step:n * step + size, :] * fac
    cp = pltpu.make_async_copy(bonus, bonus_hbm, sems)
    cp.start()
    copies.append(cp)
    mass = jnp.concatenate([stat_ref[i * BT + t:i * BT + t + 1, :] for t in range(BT) for i in range(DRAFT)], axis=0)
    mass = jnp.concatenate([mass] * 4, axis=0)
    for n in range(5):
        def body(k, carry):
            at = pl.ds(pl.multiple_of(n * 1200 + k * 24, 8), 24)
            out[at, :] = rows[at, :] / mass
            return carry

        lax.fori_loop(0, 50, body, 0, unroll=5)
        size = 1200
        if n == 4:
            out[6000:6012, :] = rows[6000:6012, :] / mass[0:12]
            size = 1212
        cp = pltpu.make_async_copy(res.at[pl.ds(n * 1200, size)], res_hbm.at[pl.ds(n * 1200, size)], sems)
        cp.start()
        copies.append(cp)
    acc = stat_ref[6:12, :]
    more = acc[0:BT] * (1.0 + acc[BT:2 * BT])
    for t in range(BT):
        cols = slice(t * LANES, (t + 1) * LANES)
        exp_ref[cols] = more[t]
        for i in range(DRAFT):
            acc_ref[i:i + 1, cols] = acc[i * BT + t:i * BT + t + 1]
    for cp in copies:
        cp.wait()


def verify_local(hid, w_cols, q_rows, draft_tok):
    q = with_layout_constraint(q_rows.reshape(SEQ, DRAFT, TILES, LANES), Layout((0, 2, 1, 3)))
    q = q.transpose(0, 2, 1, 3).reshape(SEQ * TILES * DRAFT, 1, LANES)
    f32 = jnp.float32
    hbm = pl.BlockSpec(memory_space=pl.ANY)
    vmem = pl.BlockSpec(memory_space=pltpu.VMEM)
    dma = pltpu.SemaphoreType.DMA
    ex, bo, st = pl.pallas_call(
        kernel,
        out_shape=[
            jax.ShapeDtypeStruct((SHARD * BT * DRAFT, 1, LANES), f32),
            jax.ShapeDtypeStruct((ROWS_P, BATCH), f32),
            jax.ShapeDtypeStruct((16, LANES), f32),
        ],
        in_specs=[pl.BlockSpec(memory_space=pltpu.HBM)] * 4,
        out_specs=[hbm, hbm, vmem],
        scratch_shapes=[
            pltpu.VMEM((DRAFT, BATCH), jnp.int32),
            pltpu.VMEM((SEQ * TILES * DRAFT + 20, 1, LANES), f32),
            pltpu.VMEM((SHARD, DIM), jnp.bfloat16),
            pltpu.VMEM((SEQ, NPOS, DIM), jnp.bfloat16),
            pltpu.VMEM((DEV * HROWS, LANES), jnp.bfloat16),
            pltpu.VMEM((48 * PITCH, LANES), f32),
            pltpu.VMEM((COLS_P, DIM), jnp.bfloat16),
            pltpu.VMEM((ROWS_P, COLS_P), f32),
            pltpu.VMEM((DRAFT, DEV * BLK, LANES), f32),
            pltpu.VMEM((DRAFT, DEV * BLK, LANES), f32),
            pltpu.VMEM((SHARD * BT * DRAFT, 1, LANES), f32),
            pltpu.VMEM((24, LANES), f32),
            pltpu.VMEM((16, LANES), f32),
            pltpu.VMEM((16, LANES), f32),
            pltpu.VMEM((8 * STAT, 1, LANES), f32),
            pltpu.VMEM((16 * STAT, 1, LANES), f32),
            pltpu.VMEM((8 * STAT, 1, LANES), f32),
            pltpu.VMEM((4 * STAT, 1, LANES), f32),
            pltpu.VMEM((4 * STAT, 1, LANES), f32),
            dma((4,)),
            dma, dma((3, 3)), dma, dma((3,)), dma, dma((2,)), dma, dma((5,)),
        ],
        compiler_params=pltpu.CompilerParams(vmem_limit_bytes=40 * 2 ** 20, has_side_effects=True, collective_id=0),
    )(*(pltpu.with_memory_space_constraint(x, pltpu.HBM) for x in (q, w_cols.T, hid, draft_tok.T)))
    res, bonus, acc, expected = pl.pallas_call(
        finish_kernel,
        out_shape=[
            jax.ShapeDtypeStruct((SHARD * BT * DRAFT, 1, LANES), f32),
            jax.ShapeDtypeStruct((SHARD, BATCH), f32),
            jax.ShapeDtypeStruct((DRAFT, BATCH), f32),
            jax.ShapeDtypeStruct((BATCH,), f32),
        ],
        in_specs=[vmem] * 3,
        out_specs=[hbm, hbm, vmem, vmem],
        scratch_shapes=[
            pltpu.VMEM((SHARD * BT * DRAFT, 1, LANES), f32),
            pltpu.VMEM((SHARD, BATCH), f32),
            dma,
        ],
        compiler_params=pltpu.CompilerParams(vmem_limit_bytes=12 * 2 ** 20),
    )(ex, bo, st)
    res = with_layout_constraint(res.reshape(SHARD, BT, DRAFT, LANES).transpose(0, 2, 1, 3), Layout((0, 2, 1, 3)))
    residual = res.reshape(SHARD, DRAFT, BATCH).transpose(2, 1, 0)
    return acc.T, expected, residual, bonus.T


def solution(mesh):
    return jax.shard_map(
        verify_local,
        mesh=mesh,
        in_specs=(P(('dp', 'tp'), None, None), P(None, 'tp'), P(('dp', 'tp'), None, None), P('dp', None)),
        out_specs=(P('dp', None), P('dp'), P('dp', None, 'tp'), P('dp', 'tp')),
        check_vma=False,
    )
```

```python
import functools

import jax
import jax.numpy as jnp
from jax import lax
from jax.experimental import pallas as pl
from jax.experimental.layout import Layout, with_layout_constraint
from jax.experimental.pallas import tpu as pltpu
from jax.sharding import PartitionSpec as P

INV_TEMP = 1.25
DEV = 128
SEQ = 3
NPOS = 3
DRAFT = 2
BATCH = 384
DIM = 2048
VOCAB = 128256
SHARD = VOCAB // DEV
LANES = 128
TILES = VOCAB // LANES
CHUNKS = 8
TAIL = SHARD - (CHUNKS - 1) * LANES
ROWS_P = 1008
TAIL_P = ROWS_P - (CHUNKS - 1) * LANES
KC = DIM // LANES
HROWS = SEQ * NPOS * KC
COLS = NPOS * BATCH
COLS_P = 1280
CT = COLS // LANES
BT = BATCH // LANES
BLK = SEQ * CHUNKS
PITCH = 49
NEG = -1e30
STAT = 18
MESH = pl.DeviceIdType.MESH


def remote(src, dst, ssem, rsem, dev):
    return pltpu.make_async_remote_copy(
        src_ref=src, dst_ref=dst, send_sem=ssem, recv_sem=rsem,
        device_id={'tp': dev}, device_id_type=MESH)


def reduce_stage(buf, slot, count, ssem, rsem, device, payload):
    buf.reshape(count * STAT, LANES)[pl.ds(slot * STAT, STAT), :] = payload
    here = buf.at[pl.ds(slot * STAT, STAT)]
    for r in range(1, count):
        remote(here, here, ssem, rsem, device((slot + r) % count)).start()


def wait_rows(ref, rows, sem):
    part = ref.at[pl.ds(0, rows)]
    pltpu.make_async_copy(part, part, sem).wait()


def finish(buf, count, rsem):
    wait_rows(buf, (count - 1) * STAT, rsem)
    rows = buf.reshape(count * STAT, LANES)
    return [rows[k * STAT:(k + 1) * STAT, :] for k in range(count)]


def merge_max_sum(parts):
    m = parts[0][0:CT]
    for p in parts[1:]:
        m = jnp.maximum(m, p[0:CT])
    s = parts[0][CT:2 * CT] * jnp.exp(parts[0][0:CT] - m)
    for p in parts[1:]:
        s = s + p[CT:2 * CT] * jnp.exp(p[0:CT] - m)
    return jnp.concatenate([m, s], axis=0)


def merge_add(parts):
    total = parts[0]
    for p in parts[1:]:
        total = total + p
    return total


def kernel(q_hbm, w_hbm, h_hbm, tok_hbm,
           ex_hbm, bo_hbm, out_ref,
           tok_ref, qbuf, wbuf, hloc, hidb, bounce, hmat, z, send, recv, exbuf, stat, peak, scale,
           a1, b1, a2, b2,
           lsem, ag_s, ag_r, d2d_s, d2d_r, qs, qr_sem, rs, rr):
    scope = jax.named_scope
    me = lax.axis_index('tp')
    core = me % 2
    coord = (me // 32, (me // 8) % 4, (me // 2) % 4)
    unit = (32, 8, 2)
    partner = me + 1 - 2 * core
    hop = [[((coord[d] + r) % 4) * unit[d] for r in range(4)] for d in range(3)]

    def device(rz, ry, rx, rc):
        return hop[0][rz] + hop[1][ry] + hop[2][rx] + (core if rc == 0 else 1 - core)

    hcp = pltpu.make_async_copy(h_hbm, hloc, lsem.at[2])
    hcp.start()
    qcp = pltpu.make_async_copy(q_hbm, qbuf.at[pl.ds(0, SEQ * TILES * DRAFT)], lsem.at[0])
    qcp.start()
    wcp = pltpu.make_async_copy(w_hbm, wbuf, lsem.at[1])
    wcp.start()
    tcp = pltpu.make_async_copy(tok_hbm, tok_ref, lsem.at[3])
    tcp.start()
    barrier = pltpu.get_barrier_semaphore()
    peers = [partner]
    for d in range(3):
        for r in range(1, 4):
            steps = [0, 0, 0]
            steps[d] = r
            peers.append(device(*steps, 0))
    for dev in peers:
        pl.semaphore_signal(barrier, inc=1, device_id={'tp': dev}, device_id_type=MESH)

    with scope('hid'):
        hcp.wait()
        for s in range(SEQ):
            x = hloc[s].astype(jnp.float32)
            for kc in range(KC):
                bounce[pl.ds(s * 48 + kc, NPOS, stride=KC), :] = x[:, kc * LANES:(kc + 1) * LANES]
        hidb[pl.ds(pl.multiple_of(me * HROWS, 16), HROWS), :] = bounce[0:HROWS, :].astype(jnp.bfloat16)
    with scope('barrier'):
        pl.semaphore_wait(barrier, len(peers))

    hview = hidb.reshape(4, 4, 4, 2, SEQ, HROWS // SEQ, LANES)

    def ag_phase(phase):
        for j in range(3):
            order = [(j + k) % 3 for k in range(3)]
            idx = list(coord)
            for d in order[:phase]:
                idx[d] = slice(None)
            view = hview.at[idx[0], idx[1], idx[2], core, j]
            for r in (1, 3, 2):
                steps = [0, 0, 0]
                steps[order[phase]] = r
                remote(view, view, ag_s, ag_r.at[phase, j], device(*steps, 0)).start()

    def ag_wait(phase, j):
        wait_rows(hidb, 3 * 4 ** phase * (HROWS // SEQ), ag_r.at[phase, j])

    qrows = qbuf.reshape(qbuf.shape[0], LANES)
    lane = lax.broadcasted_iota(jnp.int32, (8, LANES), 1)

    def pack(i, k, carry):
        first = (SHARD * k) // LANES
        off = (SHARD * k) % LANES
        shift = (LANES - off) % LANES
        keep = lane < LANES - off
        for s in range(SEQ):
            base = (s * TILES + first) * DRAFT + i
            lo = qrows[pl.ds(base, 8, stride=2), :]
            hi = qrows[pl.ds(base + 2, 8, stride=2), :]
            lo = pltpu.roll(lo, shift, 1)
            hi = pltpu.roll(hi, shift, 1)
            send[i, pl.ds(pl.multiple_of(k * BLK + s * 8, 8), 8), :] = jnp.where(keep, lo, hi)
        return carry

    mine = pl.ds(pl.multiple_of(me * BLK, 8), BLK)

    def to(i, dev):
        remote(send.at[i, pl.ds(pl.multiple_of(dev * BLK, 8), BLK)], recv.at[i, mine],
               qs, qr_sem.at[i], dev).start()

    def step(d, n):
        return ((coord[d] + n) % 4) * unit[d]

    def class0(i):
        pltpu.make_async_copy(send.at[i, mine], recv.at[i, mine], qr_sem.at[i]).start()
        to(i, partner)

    def class1(i, rc):
        last = core if rc == 0 else 1 - core
        for r in (1, 3, 2):
            for d in range(3):
                steps = [0, 0, 0]
                steps[d] = r
                to(i, device(*steps, rc))

    def class2(i, rc, lo=0, hi=9):
        last = core if rc == 0 else 1 - core

        def body(n, carry):
            a, b = n // 3 + 1, n % 3 + 1
            to(i, step(0, a) + step(1, b) + hop[2][0] + last)
            to(i, hop[0][0] + step(1, a) + step(2, b) + last)
            to(i, step(0, b) + hop[1][0] + step(2, a) + last)
            return carry

        lax.fori_loop(lo, hi, body, 0)

    def class3(i, rc, lo=0, hi=9):
        last = core if rc == 0 else 1 - core

        def body(n, carry):
            a, b = n // 3, n % 3
            for k in range(3):
                to(i, step(0, (a + k) % 3 + 1) + step(1, (b + k) % 3 + 1) + hop[2][k + 1] + last)
            return carry

        lax.fori_loop(lo, hi, body, 0)

    ag_phase(0)
    with scope('qwait'):
        qcp.wait()
    with scope('pack'):
        lax.fori_loop(0, DEV, functools.partial(pack, 0), 0, unroll=16)
    with scope('ex0'):
        class0(0)
        class1(0, 0)
    with scope('ag0'):
        for j in range(3):
            ag_wait(0, j)
    ag_phase(1)
    with scope('ex0a'):
        class1(0, 1)
        class2(0, 0)
    with scope('pack2'):
        lax.fori_loop(0, DEV, functools.partial(pack, 1), 0, unroll=16)
    with scope('ag1'):
        for j in range(3):
            ag_wait(1, j)
    ag_phase(2)
    d2d = []
    for j in range(3):
        with scope(f'ag2_{j}'):
            ag_wait(2, j)
        view = hview.at[:, :, :, core, j]
        cp = remote(view, view, d2d_s, d2d_r.at[j], partner)
        cp.start()
        d2d.append(cp)
    with scope('ex0b'):
        class3(0, 0)
        class3(0, 1)
        class2(0, 1)
        class3(1, 0, 0, 4)
    with scope('d2d'):
        for cp in d2d:
            cp.wait_recv()

    def relayout(n, carry):
        def up(b, c):
            x = hidb[pl.ds(pl.multiple_of((48 * n + b) * 48, 16), 48), :]
            bounce[pl.ds(b * PITCH, 48), :] = x.astype(jnp.float32)
            return c

        lax.fori_loop(0, 48, up, 0, unroll=4)
        for g in range(NPOS):
            for u in range(3):
                for kc in range(KC):
                    y = bounce[pl.ds(16 * u * PITCH + g * KC + kc, 16, stride=PITCH), :]
                    hmat[pl.ds(pl.multiple_of(g * BATCH + 48 * n + 16 * u, 16), 16),
                         kc * LANES:(kc + 1) * LANES] = y.astype(jnp.bfloat16)
        return carry

    with scope('relayout'):
        lax.fori_loop(0, 8, relayout, 0)
    wcp.wait()
    tcp.wait()

    z[SHARD:ROWS_P, :] = jnp.full((ROWS_P - SHARD, COLS_P), NEG, jnp.float32)

    def head(n, carry):
        hb = hmat[pl.ds(pl.multiple_of(n * 256, 256), 256), :]
        zt = lax.dot_general(wbuf[...], hb, (((1,), (1,)), ((), ())), preferred_element_type=jnp.float32)
        zt = zt * INV_TEMP
        z[0:SHARD, pl.ds(pl.multiple_of(n * 256, 256), 256)] = zt
        top = jnp.max(zt, axis=0, keepdims=True)
        peak[pl.ds(2 * n, 1), :] = top[:, 0:LANES]
        peak[pl.ds(2 * n + 1, 1), :] = top[:, LANES:]
        return carry

    with scope('head'):
        lax.fori_loop(0, COLS_P // 256, head, 0)

    def local_stats(t, carry):
        cols = pl.ds(pl.multiple_of(t * LANES, LANES), LANES)

        m = peak[pl.ds(t, 1), :]

        def expo(n, s):
            rows = pl.ds(pl.multiple_of(n * 112, 8), 112)
            x = jnp.exp(z[rows, cols] - m)
            z[rows, cols] = x
            return s + jnp.sum(x.reshape(14, 8, LANES), axis=0)

        s8 = lax.fori_loop(0, 9, expo, jnp.zeros((8, LANES), jnp.float32), unroll=3)
        stat[pl.ds(t, 1), :] = m
        stat[pl.ds(CT + t, 1), :] = jnp.sum(s8, axis=0, keepdims=True)
        return carry

    stat[...] = jnp.zeros_like(stat)
    with scope('stats'):
        lax.fori_loop(0, CT, local_stats, 0)
    bcp = pltpu.make_async_copy(z.at[:, DRAFT * BATCH:COLS], bo_hbm, lsem.at[2])
    bcp.start()

    slot, grp = me % 8, me // 8
    near = lambda k: grp * 8 + k
    far = lambda k: k * 8 + slot
    local = stat[0:STAT, :]
    reduce_stage(a1, slot, 8, rs, rr.at[0], near, local)
    with scope('ex1a'):
        class3(1, 0, 4, 9)
        class3(1, 1, 0, 3)
    with scope('round1a'):
        parts = finish(a1, 8, rr.at[0])
    reduce_stage(b1, grp, 16, rs, rr.at[1], far, merge_max_sum(parts))
    with scope('ex1b'):
        class3(1, 1, 3, 9)
        class2(1, 1)
        class2(1, 0)
        class1(1, 1)
        class1(1, 0)
        class0(1)
    with scope('round1b'):
        parts = finish(b1, 16, rr.at[1])
    tot = merge_max_sum(parts)
    fac = jnp.exp(local[0:CT] - tot[0:CT]) / tot[CT:2 * CT]
    scale[0:CT, :] = fac
    out_ref[12:16, :] = jnp.concatenate([fac[DRAFT * BT:CT], fac[0:1]], axis=0)

    exrows = exbuf.reshape(exbuf.shape[0], LANES)
    first_id = me * SHARD
    stat[...] = jnp.zeros_like(stat)
    for i in range(DRAFT):
        with scope(f'a2a_{i}'):
            pltpu.make_async_copy(recv.at[i], recv.at[i], qr_sem.at[i]).wait()
        for t in range(BT):
            row = i * BT + t
            sc = scale[row:row + 1, :]
            tok = tok_ref[i:i + 1, t * LANES:(t + 1) * LANES] - first_id
            col0 = i * BATCH + t * LANES

            def block(c, carry, size, valid):
                mass, pp, qp = carry
                q = recv[i, pl.ds(t * LANES * CHUNKS + c, LANES, stride=CHUNKS), :].T
                p = z[pl.ds(pl.multiple_of(c * LANES, LANES), size), col0:col0 + LANES] * sc
                ids = lax.broadcasted_iota(jnp.int32, (size, LANES), 0)
                q = q[0:size]
                if valid < size:
                    q = jnp.where(ids < valid, q, 0.0)
                x = jnp.maximum(p - q, 0.0)
                exrows[pl.ds(c * LANES * 6 + t * 2 + i, valid, stride=6), :] = x[0:valid]
                hit = ids == tok - c * LANES
                fold = lambda v: jnp.sum(v.reshape(size // 8, 8, LANES), axis=0)
                return (mass + fold(x), pp + fold(jnp.where(hit, p, 0.0)), qp + fold(jnp.where(hit, q, 0.0)))

            zero = jnp.zeros((8, LANES), jnp.float32)
            carry = lax.fori_loop(0, CHUNKS - 1, lambda c, v: block(c, v, LANES, LANES), (zero, zero, zero),
                                  unroll=CHUNKS - 1)
            mass, pp, qp = block(CHUNKS - 1, carry, TAIL_P, TAIL)
            stat[row:row + 1, :] = jnp.sum(mass, axis=0, keepdims=True)
            stat[6 + row:7 + row, :] = jnp.sum(pp, axis=0, keepdims=True)
            stat[12 + row:13 + row, :] = jnp.sum(qp, axis=0, keepdims=True)

    ecp = pltpu.make_async_copy(exbuf, ex_hbm, lsem.at[0])
    ecp.start()
    reduce_stage(a2, slot, 8, rs, rr.at[2], near, stat[0:STAT, :])
    with scope('round2a'):
        parts = finish(a2, 8, rr.at[2])
    reduce_stage(b2, grp, 16, rs, rr.at[3], far, merge_add(parts))
    with scope('round2b'):
        parts = finish(b2, 16, rr.at[3])
    tot = merge_add(parts)
    out_ref[0:6, :] = tot[0:6]
    out_ref[6:12, :] = jnp.minimum(tot[6:12] / tot[12:18], 1.0)
    with scope('tail'):
        ecp.wait()
        bcp.wait()
        wait_rows(hidb, 9 * 21 * (HROWS // SEQ), ag_s)
        wait_rows(hidb, DEV // 2 * HROWS, d2d_s)
        wait_rows(send.reshape(DRAFT * DEV * BLK, LANES), DRAFT * (DEV - 1) * BLK, qs)
        wait_rows(qbuf, 2 * (7 + 15) * STAT, rs)


def finish_kernel(ex_ref, bo_ref, stat_ref, res_hbm, bonus_hbm, acc_ref, exp_ref, res, bonus, sems):
    rows = ex_ref.reshape(ex_ref.shape[0], LANES)
    out = res.reshape(res.shape[0], LANES)
    copies = []
    fac = jnp.concatenate([stat_ref[12 + t:13 + t, :] for t in range(BT)], axis=1)
    step = 256
    for n in range(4):
        size = min(step, SHARD - n * step)
        bonus[n * step:n * step + size, :] = bo_ref[n * step:n * step + size, :] * fac
    cp = pltpu.make_async_copy(bonus, bonus_hbm, sems)
    cp.start()
    copies.append(cp)
    mass = jnp.concatenate([stat_ref[i * BT + t:i * BT + t + 1, :] for t in range(BT) for i in range(DRAFT)], axis=0)
    mass = jnp.concatenate([mass] * 4, axis=0)
    for n in range(5):
        def body(k, carry):
            at = pl.ds(pl.multiple_of(n * 1200 + k * 24, 8), 24)
            out[at, :] = rows[at, :] / mass
            return carry

        lax.fori_loop(0, 50, body, 0, unroll=5)
        size = 1200
        if n == 4:
            out[6000:6012, :] = rows[6000:6012, :] / mass[0:12]
            size = 1212
        cp = pltpu.make_async_copy(res.at[pl.ds(n * 1200, size)], res_hbm.at[pl.ds(n * 1200, size)], sems)
        cp.start()
        copies.append(cp)
    acc = stat_ref[6:12, :]
    more = acc[0:BT] * (1.0 + acc[BT:2 * BT])
    for t in range(BT):
        cols = slice(t * LANES, (t + 1) * LANES)
        exp_ref[cols] = more[t]
        for i in range(DRAFT):
            acc_ref[i:i + 1, cols] = acc[i * BT + t:i * BT + t + 1]
    for cp in copies:
        cp.wait()


def verify_local(hid, w_cols, q_rows, draft_tok):
    q = with_layout_constraint(q_rows.reshape(SEQ, DRAFT, TILES, LANES), Layout((0, 2, 1, 3)))
    q = q.transpose(0, 2, 1, 3).reshape(SEQ * TILES * DRAFT, 1, LANES)
    f32 = jnp.float32
    hbm = pl.BlockSpec(memory_space=pl.ANY)
    vmem = pl.BlockSpec(memory_space=pltpu.VMEM)
    dma = pltpu.SemaphoreType.DMA
    ex, bo, st = pl.pallas_call(
        kernel,
        out_shape=[
            jax.ShapeDtypeStruct((SHARD * BT * DRAFT, 1, LANES), f32),
            jax.ShapeDtypeStruct((ROWS_P, BATCH), f32),
            jax.ShapeDtypeStruct((16, LANES), f32),
        ],
        in_specs=[pl.BlockSpec(memory_space=pltpu.HBM)] * 4,
        out_specs=[hbm, hbm, vmem],
        scratch_shapes=[
            pltpu.VMEM((DRAFT, BATCH), jnp.int32),
            pltpu.VMEM((SEQ * TILES * DRAFT + 20, 1, LANES), f32),
            pltpu.VMEM((SHARD, DIM), jnp.bfloat16),
            pltpu.VMEM((SEQ, NPOS, DIM), jnp.bfloat16),
            pltpu.VMEM((DEV * HROWS, LANES), jnp.bfloat16),
            pltpu.VMEM((48 * PITCH, LANES), f32),
            pltpu.VMEM((COLS_P, DIM), jnp.bfloat16),
            pltpu.VMEM((ROWS_P, COLS_P), f32),
            pltpu.VMEM((DRAFT, DEV * BLK, LANES), f32),
            pltpu.VMEM((DRAFT, DEV * BLK, LANES), f32),
            pltpu.VMEM((SHARD * BT * DRAFT, 1, LANES), f32),
            pltpu.VMEM((24, LANES), f32),
            pltpu.VMEM((16, LANES), f32),
            pltpu.VMEM((16, LANES), f32),
            pltpu.VMEM((8 * STAT, 1, LANES), f32),
            pltpu.VMEM((16 * STAT, 1, LANES), f32),
            pltpu.VMEM((8 * STAT, 1, LANES), f32),
            pltpu.VMEM((16 * STAT, 1, LANES), f32),
            dma((4,)),
            dma, dma((3, 3)), dma, dma((3,)), dma, dma((2,)), dma, dma((4,)),
        ],
        compiler_params=pltpu.CompilerParams(vmem_limit_bytes=40 * 2 ** 20, has_side_effects=True, collective_id=0),
    )(*(pltpu.with_memory_space_constraint(x, pltpu.HBM) for x in (q, w_cols.T, hid, draft_tok.T)))
    res, bonus, acc, expected = pl.pallas_call(
        finish_kernel,
        out_shape=[
            jax.ShapeDtypeStruct((SHARD * BT * DRAFT, 1, LANES), f32),
            jax.ShapeDtypeStruct((SHARD, BATCH), f32),
            jax.ShapeDtypeStruct((DRAFT, BATCH), f32),
            jax.ShapeDtypeStruct((BATCH,), f32),
        ],
        in_specs=[vmem] * 3,
        out_specs=[hbm, hbm, vmem, vmem],
        scratch_shapes=[
            pltpu.VMEM((SHARD * BT * DRAFT, 1, LANES), f32),
            pltpu.VMEM((SHARD, BATCH), f32),
            dma,
        ],
        compiler_params=pltpu.CompilerParams(vmem_limit_bytes=12 * 2 ** 20),
    )(ex, bo, st)
    res = with_layout_constraint(res.reshape(SHARD, BT, DRAFT, LANES).transpose(0, 2, 1, 3), Layout((0, 2, 1, 3)))
    residual = res.reshape(SHARD, DRAFT, BATCH).transpose(2, 1, 0)
    return acc.T, expected, residual, bonus.T


def solution(mesh):
    return jax.shard_map(
        verify_local,
        mesh=mesh,
        in_specs=(P(('dp', 'tp'), None, None), P(None, 'tp'), P(('dp', 'tp'), None, None), P('dp', None)),
        out_specs=(P('dp', None), P('dp'), P('dp', None, 'tp'), P('dp', 'tp')),
        check_vma=False,
    )
```

```python
import functools

import jax
import jax.numpy as jnp
from jax import lax
from jax.experimental import pallas as pl
from jax.experimental.layout import Layout, with_layout_constraint
from jax.experimental.pallas import tpu as pltpu
from jax.sharding import PartitionSpec as P

INV_TEMP = 1.25
DEV = 128
SEQ = 3
NPOS = 3
DRAFT = 2
BATCH = 384
DIM = 2048
VOCAB = 128256
SHARD = VOCAB // DEV
LANES = 128
TILES = VOCAB // LANES
CHUNKS = 8
TAIL = SHARD - (CHUNKS - 1) * LANES
ROWS_P = 1008
TAIL_P = ROWS_P - (CHUNKS - 1) * LANES
KC = DIM // LANES
HROWS = SEQ * NPOS * KC
COLS = NPOS * BATCH
COLS_P = 1280
CT = COLS // LANES
BT = BATCH // LANES
BLK = SEQ * CHUNKS
PITCH = 49
NEG = -1e30
STAT = 18
MESH = pl.DeviceIdType.MESH


def remote(src, dst, ssem, rsem, dev):
    return pltpu.make_async_remote_copy(
        src_ref=src, dst_ref=dst, send_sem=ssem, recv_sem=rsem,
        device_id={'tp': dev}, device_id_type=MESH)


def reduce_stage(buf, slot, count, ssem, rsem, device, payload):
    buf.reshape(count * STAT, LANES)[pl.ds(slot * STAT, STAT), :] = payload
    here = buf.at[pl.ds(slot * STAT, STAT)]
    for r in range(1, count):
        remote(here, here, ssem, rsem, device((slot + r) % count)).start()


def wait_rows(ref, rows, sem):
    part = ref.at[pl.ds(0, rows)]
    pltpu.make_async_copy(part, part, sem).wait()


def finish(buf, count, rsem):
    wait_rows(buf, (count - 1) * STAT, rsem)
    rows = buf.reshape(count * STAT, LANES)
    return [rows[k * STAT:(k + 1) * STAT, :] for k in range(count)]


def merge_max_sum(parts):
    m = parts[0][0:CT]
    for p in parts[1:]:
        m = jnp.maximum(m, p[0:CT])
    s = parts[0][CT:2 * CT] * jnp.exp(parts[0][0:CT] - m)
    for p in parts[1:]:
        s = s + p[CT:2 * CT] * jnp.exp(p[0:CT] - m)
    return jnp.concatenate([m, s], axis=0)


def merge_add(parts):
    total = parts[0]
    for p in parts[1:]:
        total = total + p
    return total


def kernel(q_hbm, w_hbm, h_hbm, tok_hbm,
           ex_hbm, bo_hbm, out_ref,
           tok_ref, qbuf, wbuf, hloc, hidb, bounce, hmat, z, send, recv, exbuf, stat, peak, scale,
           a1, b1, a2, b2,
           lsem, ag_s, ag_r, d2d_s, d2d_r, qs, qr_sem, rs, rr):
    scope = jax.named_scope
    me = lax.axis_index('tp')
    core = me % 2
    coord = (me // 32, (me // 8) % 4, (me // 2) % 4)
    unit = (32, 8, 2)
    partner = me + 1 - 2 * core
    hop = [[((coord[d] + r) % 4) * unit[d] for r in range(4)] for d in range(3)]

    def device(rz, ry, rx, rc):
        return hop[0][rz] + hop[1][ry] + hop[2][rx] + (core if rc == 0 else 1 - core)

    hcp = pltpu.make_async_copy(h_hbm, hloc, lsem.at[2])
    hcp.start()
    qcp = pltpu.make_async_copy(q_hbm, qbuf.at[pl.ds(0, SEQ * TILES * DRAFT)], lsem.at[0])
    qcp.start()
    wcp = pltpu.make_async_copy(w_hbm, wbuf, lsem.at[1])
    wcp.start()
    tcp = pltpu.make_async_copy(tok_hbm, tok_ref, lsem.at[3])
    tcp.start()
    barrier = pltpu.get_barrier_semaphore()
    peers = [partner]
    for d in range(3):
        for r in range(1, 4):
            steps = [0, 0, 0]
            steps[d] = r
            peers.append(device(*steps, 0))
    for dev in peers:
        pl.semaphore_signal(barrier, inc=1, device_id={'tp': dev}, device_id_type=MESH)

    with scope('hid'):
        hcp.wait()
        for s in range(SEQ):
            x = hloc[s].astype(jnp.float32)
            for kc in range(KC):
                bounce[pl.ds(s * 48 + kc, NPOS, stride=KC), :] = x[:, kc * LANES:(kc + 1) * LANES]
        hidb[pl.ds(pl.multiple_of(me * HROWS, 16), HROWS), :] = bounce[0:HROWS, :].astype(jnp.bfloat16)
    with scope('barrier'):
        pl.semaphore_wait(barrier, len(peers))

    hview = hidb.reshape(4, 4, 4, 2, SEQ, HROWS // SEQ, LANES)

    def ag_phase(phase):
        for j in range(3):
            order = [(j + k) % 3 for k in range(3)]
            idx = list(coord)
            for d in order[:phase]:
                idx[d] = slice(None)
            view = hview.at[idx[0], idx[1], idx[2], core, j]
            for r in (1, 3, 2):
                steps = [0, 0, 0]
                steps[order[phase]] = r
                remote(view, view, ag_s, ag_r.at[phase, j], device(*steps, 0)).start()

    def ag_wait(phase, j):
        wait_rows(hidb, 3 * 4 ** phase * (HROWS // SEQ), ag_r.at[phase, j])

    qrows = qbuf.reshape(qbuf.shape[0], LANES)
    lane = lax.broadcasted_iota(jnp.int32, (8, LANES), 1)

    def pack(i, k, carry):
        first = (SHARD * k) // LANES
        off = (SHARD * k) % LANES
        shift = (LANES - off) % LANES
        keep = lane < LANES - off
        for s in range(SEQ):
            base = (s * TILES + first) * DRAFT + i
            lo = qrows[pl.ds(base, 8, stride=2), :]
            hi = qrows[pl.ds(base + 2, 8, stride=2), :]
            lo = pltpu.roll(lo, shift, 1)
            hi = pltpu.roll(hi, shift, 1)
            send[i, pl.ds(pl.multiple_of(k * BLK + s * 8, 8), 8), :] = jnp.where(keep, lo, hi)
        return carry

    mine = pl.ds(pl.multiple_of(me * BLK, 8), BLK)

    def to(i, dev):
        remote(send.at[i, pl.ds(pl.multiple_of(dev * BLK, 8), BLK)], recv.at[i, mine],
               qs, qr_sem.at[i], dev).start()

    def step(d, n):
        return ((coord[d] + n) % 4) * unit[d]

    def class0(i):
        pltpu.make_async_copy(send.at[i, mine], recv.at[i, mine], qr_sem.at[i]).start()
        to(i, partner)

    def class1(i, rc):
        last = core if rc == 0 else 1 - core
        for r in (1, 3, 2):
            for d in range(3):
                steps = [0, 0, 0]
                steps[d] = r
                to(i, device(*steps, rc))

    def class2(i, rc, lo=0, hi=9):
        last = core if rc == 0 else 1 - core

        def body(n, carry):
            a, b = n // 3 + 1, n % 3 + 1
            to(i, step(0, a) + step(1, b) + hop[2][0] + last)
            to(i, hop[0][0] + step(1, a) + step(2, b) + last)
            to(i, step(0, b) + hop[1][0] + step(2, a) + last)
            return carry

        lax.fori_loop(lo, hi, body, 0)

    def class3(i, rc, lo=0, hi=9):
        last = core if rc == 0 else 1 - core

        def body(n, carry):
            a, b = n // 3, n % 3
            for k in range(3):
                to(i, step(0, (a + k) % 3 + 1) + step(1, (b + k) % 3 + 1) + hop[2][k + 1] + last)
            return carry

        lax.fori_loop(lo, hi, body, 0)

    ag_phase(0)
    with scope('qwait'):
        qcp.wait()
    with scope('pack'):
        lax.fori_loop(0, DEV, functools.partial(pack, 0), 0, unroll=16)
    with scope('ex0'):
        class0(0)
        class1(0, 0)
    with scope('ag0'):
        for j in range(3):
            ag_wait(0, j)
    ag_phase(1)
    with scope('ex0a'):
        class1(0, 1)
        class2(0, 0)
    with scope('pack2'):
        lax.fori_loop(0, DEV, functools.partial(pack, 1), 0, unroll=16)
    with scope('ag1'):
        for j in range(3):
            ag_wait(1, j)
    ag_phase(2)
    d2d = []
    for j in range(3):
        with scope(f'ag2_{j}'):
            ag_wait(2, j)
        view = hview.at[:, :, :, core, j]
        cp = remote(view, view, d2d_s, d2d_r.at[j], partner)
        cp.start()
        d2d.append(cp)
    with scope('ex0b'):
        class3(0, 0, 0, 4)
    with scope('d2d'):
        for cp in d2d:
            cp.wait_recv()

    def relayout(n, carry):
        def up(b, c):
            x = hidb[pl.ds(pl.multiple_of((48 * n + b) * 48, 16), 48), :]
            bounce[pl.ds(b * PITCH, 48), :] = x.astype(jnp.float32)
            return c

        lax.fori_loop(0, 48, up, 0, unroll=4)
        for g in range(NPOS):
            for u in range(3):
                for kc in range(KC):
                    y = bounce[pl.ds(16 * u * PITCH + g * KC + kc, 16, stride=PITCH), :]
                    hmat[pl.ds(pl.multiple_of(g * BATCH + 48 * n + 16 * u, 16), 16),
                         kc * LANES:(kc + 1) * LANES] = y.astype(jnp.bfloat16)
        return carry

    with scope('relayout'):
        lax.fori_loop(0, 8, relayout, 0)
    with scope('ex0c'):
        class3(0, 0, 4, 9)
        class3(0, 1)
        class2(0, 1)
        class3(1, 0, 0, 4)
    wcp.wait()
    tcp.wait()

    z[SHARD:ROWS_P, :] = jnp.full((ROWS_P - SHARD, COLS_P), NEG, jnp.float32)

    def head(n, carry):
        hb = hmat[pl.ds(pl.multiple_of(n * 256, 256), 256), :]
        zt = lax.dot_general(wbuf[...], hb, (((1,), (1,)), ((), ())), preferred_element_type=jnp.float32)
        zt = zt * INV_TEMP
        z[0:SHARD, pl.ds(pl.multiple_of(n * 256, 256), 256)] = zt
        top = jnp.max(zt, axis=0, keepdims=True)
        peak[pl.ds(2 * n, 1), :] = top[:, 0:LANES]
        peak[pl.ds(2 * n + 1, 1), :] = top[:, LANES:]
        return carry

    with scope('head'):
        lax.fori_loop(0, COLS_P // 256, head, 0)

    def local_stats(t, carry):
        cols = pl.ds(pl.multiple_of(t * LANES, LANES), LANES)

        m = peak[pl.ds(t, 1), :]

        def expo(n, s):
            rows = pl.ds(pl.multiple_of(n * 112, 8), 112)
            x = jnp.exp(z[rows, cols] - m)
            z[rows, cols] = x
            return s + jnp.sum(x.reshape(14, 8, LANES), axis=0)

        s8 = lax.fori_loop(0, 9, expo, jnp.zeros((8, LANES), jnp.float32), unroll=3)
        stat[pl.ds(t, 1), :] = m
        stat[pl.ds(CT + t, 1), :] = jnp.sum(s8, axis=0, keepdims=True)
        return carry

    stat[...] = jnp.zeros_like(stat)
    with scope('stats'):
        lax.fori_loop(0, CT, local_stats, 0)
    bcp = pltpu.make_async_copy(z.at[:, DRAFT * BATCH:COLS], bo_hbm, lsem.at[2])
    bcp.start()

    slot, grp = me % 8, me // 8
    near = lambda k: grp * 8 + k
    far = lambda k: k * 8 + slot
    local = stat[0:STAT, :]
    reduce_stage(a1, slot, 8, rs, rr.at[0], near, local)
    with scope('ex1a'):
        class3(1, 0, 4, 9)
        class3(1, 1, 0, 3)
    with scope('round1a'):
        parts = finish(a1, 8, rr.at[0])
    reduce_stage(b1, grp, 16, rs, rr.at[1], far, merge_max_sum(parts))
    with scope('ex1b'):
        class3(1, 1, 3, 9)
        class2(1, 1)
        class2(1, 0)
        class1(1, 1)
        class1(1, 0)
        class0(1)
    with scope('round1b'):
        parts = finish(b1, 16, rr.at[1])
    tot = merge_max_sum(parts)
    fac = jnp.exp(local[0:CT] - tot[0:CT]) / tot[CT:2 * CT]
    scale[0:CT, :] = fac
    out_ref[12:16, :] = jnp.concatenate([fac[DRAFT * BT:CT], fac[0:1]], axis=0)

    exrows = exbuf.reshape(exbuf.shape[0], LANES)
    first_id = me * SHARD
    stat[...] = jnp.zeros_like(stat)
    for i in range(DRAFT):
        with scope(f'a2a_{i}'):
            pltpu.make_async_copy(recv.at[i], recv.at[i], qr_sem.at[i]).wait()
        for t in range(BT):
            row = i * BT + t
            sc = scale[row:row + 1, :]
            tok = tok_ref[i:i + 1, t * LANES:(t + 1) * LANES] - first_id
            col0 = i * BATCH + t * LANES

            def block(c, carry, size, valid):
                mass, pp, qp = carry
                q = recv[i, pl.ds(t * LANES * CHUNKS + c, LANES, stride=CHUNKS), :].T
                p = z[pl.ds(pl.multiple_of(c * LANES, LANES), size), col0:col0 + LANES] * sc
                ids = lax.broadcasted_iota(jnp.int32, (size, LANES), 0)
                q = q[0:size]
                if valid < size:
                    q = jnp.where(ids < valid, q, 0.0)
                x = jnp.maximum(p - q, 0.0)
                exrows[pl.ds(c * LANES * 6 + t * 2 + i, valid, stride=6), :] = x[0:valid]
                hit = ids == tok - c * LANES
                fold = lambda v: jnp.sum(v.reshape(size // 8, 8, LANES), axis=0)
                return (mass + fold(x), pp + fold(jnp.where(hit, p, 0.0)), qp + fold(jnp.where(hit, q, 0.0)))

            zero = jnp.zeros((8, LANES), jnp.float32)
            carry = lax.fori_loop(0, CHUNKS - 1, lambda c, v: block(c, v, LANES, LANES), (zero, zero, zero),
                                  unroll=CHUNKS - 1)
            mass, pp, qp = block(CHUNKS - 1, carry, TAIL_P, TAIL)
            stat[row:row + 1, :] = jnp.sum(mass, axis=0, keepdims=True)
            stat[6 + row:7 + row, :] = jnp.sum(pp, axis=0, keepdims=True)
            stat[12 + row:13 + row, :] = jnp.sum(qp, axis=0, keepdims=True)

    ecp = pltpu.make_async_copy(exbuf, ex_hbm, lsem.at[0])
    ecp.start()
    reduce_stage(a2, slot, 8, rs, rr.at[2], near, stat[0:STAT, :])
    with scope('round2a'):
        parts = finish(a2, 8, rr.at[2])
    reduce_stage(b2, grp, 16, rs, rr.at[3], far, merge_add(parts))
    with scope('round2b'):
        parts = finish(b2, 16, rr.at[3])
    tot = merge_add(parts)
    out_ref[0:6, :] = tot[0:6]
    out_ref[6:12, :] = jnp.minimum(tot[6:12] / tot[12:18], 1.0)
    with scope('tail'):
        ecp.wait()
        bcp.wait()
        wait_rows(hidb, 9 * 21 * (HROWS // SEQ), ag_s)
        wait_rows(hidb, DEV // 2 * HROWS, d2d_s)
        wait_rows(send.reshape(DRAFT * DEV * BLK, LANES), DRAFT * (DEV - 1) * BLK, qs)
        wait_rows(qbuf, 2 * (7 + 15) * STAT, rs)


def finish_kernel(ex_ref, bo_ref, stat_ref, res_hbm, bonus_hbm, acc_ref, exp_ref, res, bonus, sems):
    rows = ex_ref.reshape(ex_ref.shape[0], LANES)
    out = res.reshape(res.shape[0], LANES)
    copies = []
    fac = jnp.concatenate([stat_ref[12 + t:13 + t, :] for t in range(BT)], axis=1)
    step = 256
    for n in range(4):
        size = min(step, SHARD - n * step)
        bonus[n * step:n * step + size, :] = bo_ref[n * step:n * step + size, :] * fac
    cp = pltpu.make_async_copy(bonus, bonus_hbm, sems)
    cp.start()
    copies.append(cp)
    mass = jnp.concatenate([stat_ref[i * BT + t:i * BT + t + 1, :] for t in range(BT) for i in range(DRAFT)], axis=0)
    mass = jnp.concatenate([mass] * 4, axis=0)
    for n in range(5):
        def body(k, carry):
            at = pl.ds(pl.multiple_of(n * 1200 + k * 24, 8), 24)
            out[at, :] = rows[at, :] / mass
            return carry

        lax.fori_loop(0, 50, body, 0, unroll=5)
        size = 1200
        if n == 4:
            out[6000:6012, :] = rows[6000:6012, :] / mass[0:12]
            size = 1212
        cp = pltpu.make_async_copy(res.at[pl.ds(n * 1200, size)], res_hbm.at[pl.ds(n * 1200, size)], sems)
        cp.start()
        copies.append(cp)
    acc = stat_ref[6:12, :]
    more = acc[0:BT] * (1.0 + acc[BT:2 * BT])
    for t in range(BT):
        cols = slice(t * LANES, (t + 1) * LANES)
        exp_ref[cols] = more[t]
        for i in range(DRAFT):
            acc_ref[i:i + 1, cols] = acc[i * BT + t:i * BT + t + 1]
    for cp in copies:
        cp.wait()


def verify_local(hid, w_cols, q_rows, draft_tok):
    q = with_layout_constraint(q_rows.reshape(SEQ, DRAFT, TILES, LANES), Layout((0, 2, 1, 3)))
    q = q.transpose(0, 2, 1, 3).reshape(SEQ * TILES * DRAFT, 1, LANES)
    f32 = jnp.float32
    hbm = pl.BlockSpec(memory_space=pl.ANY)
    vmem = pl.BlockSpec(memory_space=pltpu.VMEM)
    dma = pltpu.SemaphoreType.DMA
    ex, bo, st = pl.pallas_call(
        kernel,
        out_shape=[
            jax.ShapeDtypeStruct((SHARD * BT * DRAFT, 1, LANES), f32),
            jax.ShapeDtypeStruct((ROWS_P, BATCH), f32),
            jax.ShapeDtypeStruct((16, LANES), f32),
        ],
        in_specs=[pl.BlockSpec(memory_space=pltpu.HBM)] * 4,
        out_specs=[hbm, hbm, vmem],
        scratch_shapes=[
            pltpu.VMEM((DRAFT, BATCH), jnp.int32),
            pltpu.VMEM((SEQ * TILES * DRAFT + 20, 1, LANES), f32),
            pltpu.VMEM((SHARD, DIM), jnp.bfloat16),
            pltpu.VMEM((SEQ, NPOS, DIM), jnp.bfloat16),
            pltpu.VMEM((DEV * HROWS, LANES), jnp.bfloat16),
            pltpu.VMEM((48 * PITCH, LANES), f32),
            pltpu.VMEM((COLS_P, DIM), jnp.bfloat16),
            pltpu.VMEM((ROWS_P, COLS_P), f32),
            pltpu.VMEM((DRAFT, DEV * BLK, LANES), f32),
            pltpu.VMEM((DRAFT, DEV * BLK, LANES), f32),
            pltpu.VMEM((SHARD * BT * DRAFT, 1, LANES), f32),
            pltpu.VMEM((24, LANES), f32),
            pltpu.VMEM((16, LANES), f32),
            pltpu.VMEM((16, LANES), f32),
            pltpu.VMEM((8 * STAT, 1, LANES), f32),
            pltpu.VMEM((16 * STAT, 1, LANES), f32),
            pltpu.VMEM((8 * STAT, 1, LANES), f32),
            pltpu.VMEM((16 * STAT, 1, LANES), f32),
            dma((4,)),
            dma, dma((3, 3)), dma, dma((3,)), dma, dma((2,)), dma, dma((4,)),
        ],
        compiler_params=pltpu.CompilerParams(vmem_limit_bytes=40 * 2 ** 20, has_side_effects=True, collective_id=0),
    )(*(pltpu.with_memory_space_constraint(x, pltpu.HBM) for x in (q, w_cols.T, hid, draft_tok.T)))
    res, bonus, acc, expected = pl.pallas_call(
        finish_kernel,
        out_shape=[
            jax.ShapeDtypeStruct((SHARD * BT * DRAFT, 1, LANES), f32),
            jax.ShapeDtypeStruct((SHARD, BATCH), f32),
            jax.ShapeDtypeStruct((DRAFT, BATCH), f32),
            jax.ShapeDtypeStruct((BATCH,), f32),
        ],
        in_specs=[vmem] * 3,
        out_specs=[hbm, hbm, vmem, vmem],
        scratch_shapes=[
            pltpu.VMEM((SHARD * BT * DRAFT, 1, LANES), f32),
            pltpu.VMEM((SHARD, BATCH), f32),
            dma,
        ],
        compiler_params=pltpu.CompilerParams(vmem_limit_bytes=12 * 2 ** 20),
    )(ex, bo, st)
    res = with_layout_constraint(res.reshape(SHARD, BT, DRAFT, LANES).transpose(0, 2, 1, 3), Layout((0, 2, 1, 3)))
    residual = res.reshape(SHARD, DRAFT, BATCH).transpose(2, 1, 0)
    return acc.T, expected, residual, bonus.T


def solution(mesh):
    return jax.shard_map(
        verify_local,
        mesh=mesh,
        in_specs=(P(('dp', 'tp'), None, None), P(None, 'tp'), P(('dp', 'tp'), None, None), P('dp', None)),
        out_specs=(P('dp', None), P('dp'), P('dp', None, 'tp'), P('dp', 'tp')),
        check_vma=False,
    )
```

```python
import functools

import jax
import jax.numpy as jnp
from jax import lax
from jax.experimental import pallas as pl
from jax.experimental.layout import Layout, with_layout_constraint
from jax.experimental.pallas import tpu as pltpu
from jax.sharding import PartitionSpec as P

INV_TEMP = 1.25
DEV = 128
SEQ = 3
NPOS = 3
DRAFT = 2
BATCH = 384
DIM = 2048
VOCAB = 128256
SHARD = VOCAB // DEV
LANES = 128
TILES = VOCAB // LANES
CHUNKS = 8
TAIL = SHARD - (CHUNKS - 1) * LANES
ROWS_P = 1008
TAIL_P = ROWS_P - (CHUNKS - 1) * LANES
KC = DIM // LANES
HROWS = SEQ * NPOS * KC
COLS = NPOS * BATCH
COLS_P = 1280
CT = COLS // LANES
BT = BATCH // LANES
BLK = SEQ * CHUNKS
PITCH = 49
NEG = -1e30
STAT = 18
MESH = pl.DeviceIdType.MESH


def remote(src, dst, ssem, rsem, dev):
    return pltpu.make_async_remote_copy(
        src_ref=src, dst_ref=dst, send_sem=ssem, recv_sem=rsem,
        device_id={'tp': dev}, device_id_type=MESH)


def reduce_stage(buf, slot, count, ssem, rsem, device, payload):
    buf.reshape(count * STAT, LANES)[pl.ds(slot * STAT, STAT), :] = payload
    here = buf.at[pl.ds(slot * STAT, STAT)]
    for r in range(1, count):
        remote(here, here, ssem, rsem, device((slot + r) % count)).start()


def wait_rows(ref, rows, sem):
    part = ref.at[pl.ds(0, rows)]
    pltpu.make_async_copy(part, part, sem).wait()


def finish(buf, count, rsem):
    wait_rows(buf, (count - 1) * STAT, rsem)
    rows = buf.reshape(count * STAT, LANES)
    return [rows[k * STAT:(k + 1) * STAT, :] for k in range(count)]


def merge_max_sum(parts):
    m = parts[0][0:CT]
    for p in parts[1:]:
        m = jnp.maximum(m, p[0:CT])
    s = parts[0][CT:2 * CT] * jnp.exp(parts[0][0:CT] - m)
    for p in parts[1:]:
        s = s + p[CT:2 * CT] * jnp.exp(p[0:CT] - m)
    return jnp.concatenate([m, s], axis=0)


def merge_add(parts):
    total = parts[0]
    for p in parts[1:]:
        total = total + p
    return total


def kernel(q_hbm, w_hbm, h_hbm, tok_hbm,
           ex_hbm, bo_hbm, out_ref,
           tok_ref, qbuf, wbuf, hloc, hidb, bounce, hmat, z, send, recv, exbuf, stat, peak, scale,
           a1, b1, a2, b2,
           lsem, ag_s, ag_r, d2d_s, d2d_r, qs, qr_sem, rs, rr):
    scope = jax.named_scope
    me = lax.axis_index('tp')
    core = me % 2
    coord = (me // 32, (me // 8) % 4, (me // 2) % 4)
    unit = (32, 8, 2)
    partner = me + 1 - 2 * core
    hop = [[((coord[d] + r) % 4) * unit[d] for r in range(4)] for d in range(3)]

    def device(rz, ry, rx, rc):
        return hop[0][rz] + hop[1][ry] + hop[2][rx] + (core if rc == 0 else 1 - core)

    hcp = pltpu.make_async_copy(h_hbm, hloc, lsem.at[2])
    hcp.start()
    qcp = pltpu.make_async_copy(q_hbm, qbuf.at[pl.ds(0, SEQ * TILES * DRAFT)], lsem.at[0])
    qcp.start()
    wcp = pltpu.make_async_copy(w_hbm, wbuf, lsem.at[1])
    wcp.start()
    tcp = pltpu.make_async_copy(tok_hbm, tok_ref, lsem.at[3])
    tcp.start()
    barrier = pltpu.get_barrier_semaphore()
    peers = [partner]
    for d in range(3):
        for r in range(1, 4):
            steps = [0, 0, 0]
            steps[d] = r
            peers.append(device(*steps, 0))
    for dev in peers:
        pl.semaphore_signal(barrier, inc=1, device_id={'tp': dev}, device_id_type=MESH)

    with scope('hid'):
        hcp.wait()
        for s in range(SEQ):
            x = hloc[s].astype(jnp.float32)
            for kc in range(KC):
                bounce[pl.ds(s * 48 + kc, NPOS, stride=KC), :] = x[:, kc * LANES:(kc + 1) * LANES]
        hidb[pl.ds(pl.multiple_of(me * HROWS, 16), HROWS), :] = bounce[0:HROWS, :].astype(jnp.bfloat16)
    with scope('barrier'):
        pl.semaphore_wait(barrier, len(peers))

    hview = hidb.reshape(4, 4, 4, 2, SEQ, HROWS // SEQ, LANES)

    def ag_phase(phase):
        for j in range(3):
            order = [(j + k) % 3 for k in range(3)]
            idx = list(coord)
            for d in order[:phase]:
                idx[d] = slice(None)
            view = hview.at[idx[0], idx[1], idx[2], core, j]
            for r in (1, 3, 2):
                steps = [0, 0, 0]
                steps[order[phase]] = r
                remote(view, view, ag_s, ag_r.at[phase, j], device(*steps, 0)).start()

    def ag_wait(phase, j):
        wait_rows(hidb, 3 * 4 ** phase * (HROWS // SEQ), ag_r.at[phase, j])

    qrows = qbuf.reshape(qbuf.shape[0], LANES)
    lane = lax.broadcasted_iota(jnp.int32, (8, LANES), 1)

    def pack(i, k, carry):
        first = (SHARD * k) // LANES
        off = (SHARD * k) % LANES
        shift = (LANES - off) % LANES
        keep = lane < LANES - off
        for s in range(SEQ):
            base = (s * TILES + first) * DRAFT + i
            lo = qrows[pl.ds(base, 8, stride=2), :]
            hi = qrows[pl.ds(base + 2, 8, stride=2), :]
            lo = pltpu.roll(lo, shift, 1)
            hi = pltpu.roll(hi, shift, 1)
            send[i, pl.ds(pl.multiple_of(k * BLK + s * 8, 8), 8), :] = jnp.where(keep, lo, hi)
        return carry

    mine = pl.ds(pl.multiple_of(me * BLK, 8), BLK)

    def to(i, dev):
        remote(send.at[i, pl.ds(pl.multiple_of(dev * BLK, 8), BLK)], recv.at[i, mine],
               qs, qr_sem.at[i], dev).start()

    def step(d, n):
        return ((coord[d] + n) % 4) * unit[d]

    def class0(i):
        pltpu.make_async_copy(send.at[i, mine], recv.at[i, mine], qr_sem.at[i]).start()
        to(i, partner)

    def class1(i, rc):
        last = core if rc == 0 else 1 - core
        for r in (1, 3, 2):
            for d in range(3):
                steps = [0, 0, 0]
                steps[d] = r
                to(i, device(*steps, rc))

    def class2(i, rc, lo=0, hi=9):
        last = core if rc == 0 else 1 - core

        def body(n, carry):
            a, b = n // 3 + 1, n % 3 + 1
            to(i, step(0, a) + step(1, b) + hop[2][0] + last)
            to(i, hop[0][0] + step(1, a) + step(2, b) + last)
            to(i, step(0, b) + hop[1][0] + step(2, a) + last)
            return carry

        lax.fori_loop(lo, hi, body, 0)

    def class3(i, rc, lo=0, hi=9):
        last = core if rc == 0 else 1 - core

        def body(n, carry):
            a, b = n // 3, n % 3
            for k in range(3):
                to(i, step(0, (a + k) % 3 + 1) + step(1, (b + k) % 3 + 1) + hop[2][k + 1] + last)
            return carry

        lax.fori_loop(lo, hi, body, 0)

    ag_phase(0)
    with scope('qwait'):
        qcp.wait()
    with scope('pack'):
        lax.fori_loop(0, DEV, functools.partial(pack, 0), 0, unroll=16)
    with scope('ex0'):
        class0(0)
        class1(0, 0)
    with scope('ag0'):
        for j in range(3):
            ag_wait(0, j)
    ag_phase(1)
    with scope('ex0a'):
        class1(0, 1)
        class2(0, 0)
    with scope('pack2'):
        lax.fori_loop(0, DEV, functools.partial(pack, 1), 0, unroll=16)
    with scope('ag1'):
        for j in range(3):
            ag_wait(1, j)
    ag_phase(2)
    with scope('exag2'):
        class0(1)
        class1(1, 0)
        class1(1, 1)
    d2d = []
    for j in (2, 1, 0):
        with scope(f'ag2_{j}'):
            ag_wait(2, j)
        view = hview.at[:, :, :, core, j]
        cp = remote(view, view, d2d_s, d2d_r.at[j], partner)
        cp.start()
        d2d.append(cp)
    with scope('ex0b'):
        class3(0, 0)
        class3(0, 1)
        class2(0, 1)
        class3(1, 0, 0, 4)
    with scope('d2d'):
        for cp in d2d:
            cp.wait_recv()

    def relayout(n, carry):
        def up(b, c):
            x = hidb[pl.ds(pl.multiple_of((48 * n + b) * 48, 16), 48), :]
            bounce[pl.ds(b * PITCH, 48), :] = x.astype(jnp.float32)
            return c

        lax.fori_loop(0, 48, up, 0, unroll=4)
        for g in range(NPOS):
            for u in range(3):
                for kc in range(KC):
                    y = bounce[pl.ds(16 * u * PITCH + g * KC + kc, 16, stride=PITCH), :]
                    hmat[pl.ds(pl.multiple_of(g * BATCH + 48 * n + 16 * u, 16), 16),
                         kc * LANES:(kc + 1) * LANES] = y.astype(jnp.bfloat16)
        return carry

    with scope('relayout'):
        lax.fori_loop(0, 8, relayout, 0)
    wcp.wait()
    tcp.wait()

    z[SHARD:ROWS_P, :] = jnp.full((ROWS_P - SHARD, COLS_P), NEG, jnp.float32)

    def head(n, carry):
        hb = hmat[pl.ds(pl.multiple_of(n * 256, 256), 256), :]
        zt = lax.dot_general(wbuf[...], hb, (((1,), (1,)), ((), ())), preferred_element_type=jnp.float32)
        zt = zt * INV_TEMP
        z[0:SHARD, pl.ds(pl.multiple_of(n * 256, 256), 256)] = zt
        top = jnp.max(zt, axis=0, keepdims=True)
        peak[pl.ds(2 * n, 1), :] = top[:, 0:LANES]
        peak[pl.ds(2 * n + 1, 1), :] = top[:, LANES:]
        return carry

    with scope('head'):
        lax.fori_loop(0, COLS_P // 256, head, 0)

    def local_stats(t, carry):
        cols = pl.ds(pl.multiple_of(t * LANES, LANES), LANES)

        m = peak[pl.ds(t, 1), :]

        def expo(n, s):
            rows = pl.ds(pl.multiple_of(n * 112, 8), 112)
            x = jnp.exp(z[rows, cols] - m)
            z[rows, cols] = x
            return s + jnp.sum(x.reshape(14, 8, LANES), axis=0)

        s8 = lax.fori_loop(0, 9, expo, jnp.zeros((8, LANES), jnp.float32), unroll=3)
        stat[pl.ds(t, 1), :] = m
        stat[pl.ds(CT + t, 1), :] = jnp.sum(s8, axis=0, keepdims=True)
        return carry

    stat[...] = jnp.zeros_like(stat)
    with scope('stats'):
        lax.fori_loop(0, CT, local_stats, 0)
    bcp = pltpu.make_async_copy(z.at[:, DRAFT * BATCH:COLS], bo_hbm, lsem.at[2])
    bcp.start()

    slot, grp = me % 8, me // 8
    near = lambda k: grp * 8 + k
    far = lambda k: k * 8 + slot
    local = stat[0:STAT, :]
    reduce_stage(a1, slot, 8, rs, rr.at[0], near, local)
    with scope('ex1a'):
        class3(1, 0, 4, 9)
        class3(1, 1, 0, 3)
    with scope('round1a'):
        parts = finish(a1, 8, rr.at[0])
    reduce_stage(b1, grp, 16, rs, rr.at[1], far, merge_max_sum(parts))
    with scope('ex1b'):
        class3(1, 1, 3, 9)
        class2(1, 1)
        class2(1, 0)
    with scope('round1b'):
        parts = finish(b1, 16, rr.at[1])
    tot = merge_max_sum(parts)
    fac = jnp.exp(local[0:CT] - tot[0:CT]) / tot[CT:2 * CT]
    scale[0:CT, :] = fac
    out_ref[12:16, :] = jnp.concatenate([fac[DRAFT * BT:CT], fac[0:1]], axis=0)

    exrows = exbuf.reshape(exbuf.shape[0], LANES)
    first_id = me * SHARD
    stat[...] = jnp.zeros_like(stat)
    for i in range(DRAFT):
        with scope(f'a2a_{i}'):
            pltpu.make_async_copy(recv.at[i], recv.at[i], qr_sem.at[i]).wait()
        for t in range(BT):
            row = i * BT + t
            sc = scale[row:row + 1, :]
            tok = tok_ref[i:i + 1, t * LANES:(t + 1) * LANES] - first_id
            col0 = i * BATCH + t * LANES

            def block(c, carry, size, valid):
                mass, pp, qp = carry
                q = recv[i, pl.ds(t * LANES * CHUNKS + c, LANES, stride=CHUNKS), :].T
                p = z[pl.ds(pl.multiple_of(c * LANES, LANES), size), col0:col0 + LANES] * sc
                ids = lax.broadcasted_iota(jnp.int32, (size, LANES), 0)
                q = q[0:size]
                if valid < size:
                    q = jnp.where(ids < valid, q, 0.0)
                x = jnp.maximum(p - q, 0.0)
                exrows[pl.ds(c * LANES * 6 + t * 2 + i, valid, stride=6), :] = x[0:valid]
                hit = ids == tok - c * LANES
                fold = lambda v: jnp.sum(v.reshape(size // 8, 8, LANES), axis=0)
                return (mass + fold(x), pp + fold(jnp.where(hit, p, 0.0)), qp + fold(jnp.where(hit, q, 0.0)))

            zero = jnp.zeros((8, LANES), jnp.float32)
            carry = lax.fori_loop(0, CHUNKS - 1, lambda c, v: block(c, v, LANES, LANES), (zero, zero, zero),
                                  unroll=CHUNKS - 1)
            mass, pp, qp = block(CHUNKS - 1, carry, TAIL_P, TAIL)
            stat[row:row + 1, :] = jnp.sum(mass, axis=0, keepdims=True)
            stat[6 + row:7 + row, :] = jnp.sum(pp, axis=0, keepdims=True)
            stat[12 + row:13 + row, :] = jnp.sum(qp, axis=0, keepdims=True)

    ecp = pltpu.make_async_copy(exbuf, ex_hbm, lsem.at[0])
    ecp.start()
    reduce_stage(a2, slot, 8, rs, rr.at[2], near, stat[0:STAT, :])
    with scope('round2a'):
        parts = finish(a2, 8, rr.at[2])
    reduce_stage(b2, grp, 16, rs, rr.at[3], far, merge_add(parts))
    with scope('round2b'):
        parts = finish(b2, 16, rr.at[3])
    tot = merge_add(parts)
    out_ref[0:6, :] = tot[0:6]
    out_ref[6:12, :] = jnp.minimum(tot[6:12] / tot[12:18], 1.0)
    with scope('tail'):
        ecp.wait()
        bcp.wait()
        wait_rows(hidb, 9 * 21 * (HROWS // SEQ), ag_s)
        wait_rows(hidb, DEV // 2 * HROWS, d2d_s)
        wait_rows(send.reshape(DRAFT * DEV * BLK, LANES), DRAFT * (DEV - 1) * BLK, qs)
        wait_rows(qbuf, 2 * (7 + 15) * STAT, rs)


def finish_kernel(ex_ref, bo_ref, stat_ref, res_hbm, bonus_hbm, acc_ref, exp_ref, res, bonus, sems):
    rows = ex_ref.reshape(ex_ref.shape[0], LANES)
    out = res.reshape(res.shape[0], LANES)
    copies = []
    fac = jnp.concatenate([stat_ref[12 + t:13 + t, :] for t in range(BT)], axis=1)
    step = 256
    for n in range(4):
        size = min(step, SHARD - n * step)
        bonus[n * step:n * step + size, :] = bo_ref[n * step:n * step + size, :] * fac
    cp = pltpu.make_async_copy(bonus, bonus_hbm, sems)
    cp.start()
    copies.append(cp)
    mass = jnp.concatenate([stat_ref[i * BT + t:i * BT + t + 1, :] for t in range(BT) for i in range(DRAFT)], axis=0)
    mass = jnp.concatenate([mass] * 4, axis=0)
    for n in range(5):
        def body(k, carry):
            at = pl.ds(pl.multiple_of(n * 1200 + k * 24, 8), 24)
            out[at, :] = rows[at, :] / mass
            return carry

        lax.fori_loop(0, 50, body, 0, unroll=5)
        size = 1200
        if n == 4:
            out[6000:6012, :] = rows[6000:6012, :] / mass[0:12]
            size = 1212
        cp = pltpu.make_async_copy(res.at[pl.ds(n * 1200, size)], res_hbm.at[pl.ds(n * 1200, size)], sems)
        cp.start()
        copies.append(cp)
    acc = stat_ref[6:12, :]
    more = acc[0:BT] * (1.0 + acc[BT:2 * BT])
    for t in range(BT):
        cols = slice(t * LANES, (t + 1) * LANES)
        exp_ref[cols] = more[t]
        for i in range(DRAFT):
            acc_ref[i:i + 1, cols] = acc[i * BT + t:i * BT + t + 1]
    for cp in copies:
        cp.wait()


def verify_local(hid, w_cols, q_rows, draft_tok):
    q = with_layout_constraint(q_rows.reshape(SEQ, DRAFT, TILES, LANES), Layout((0, 2, 1, 3)))
    q = q.transpose(0, 2, 1, 3).reshape(SEQ * TILES * DRAFT, 1, LANES)
    f32 = jnp.float32
    hbm = pl.BlockSpec(memory_space=pl.ANY)
    vmem = pl.BlockSpec(memory_space=pltpu.VMEM)
    dma = pltpu.SemaphoreType.DMA
    ex, bo, st = pl.pallas_call(
        kernel,
        out_shape=[
            jax.ShapeDtypeStruct((SHARD * BT * DRAFT, 1, LANES), f32),
            jax.ShapeDtypeStruct((ROWS_P, BATCH), f32),
            jax.ShapeDtypeStruct((16, LANES), f32),
        ],
        in_specs=[pl.BlockSpec(memory_space=pltpu.HBM)] * 4,
        out_specs=[hbm, hbm, vmem],
        scratch_shapes=[
            pltpu.VMEM((DRAFT, BATCH), jnp.int32),
            pltpu.VMEM((SEQ * TILES * DRAFT + 20, 1, LANES), f32),
            pltpu.VMEM((SHARD, DIM), jnp.bfloat16),
            pltpu.VMEM((SEQ, NPOS, DIM), jnp.bfloat16),
            pltpu.VMEM((DEV * HROWS, LANES), jnp.bfloat16),
            pltpu.VMEM((48 * PITCH, LANES), f32),
            pltpu.VMEM((COLS_P, DIM), jnp.bfloat16),
            pltpu.VMEM((ROWS_P, COLS_P), f32),
            pltpu.VMEM((DRAFT, DEV * BLK, LANES), f32),
            pltpu.VMEM((DRAFT, DEV * BLK, LANES), f32),
            pltpu.VMEM((SHARD * BT * DRAFT, 1, LANES), f32),
            pltpu.VMEM((24, LANES), f32),
            pltpu.VMEM((16, LANES), f32),
            pltpu.VMEM((16, LANES), f32),
            pltpu.VMEM((8 * STAT, 1, LANES), f32),
            pltpu.VMEM((16 * STAT, 1, LANES), f32),
            pltpu.VMEM((8 * STAT, 1, LANES), f32),
            pltpu.VMEM((16 * STAT, 1, LANES), f32),
            dma((4,)),
            dma, dma((3, 3)), dma, dma((3,)), dma, dma((2,)), dma, dma((4,)),
        ],
        compiler_params=pltpu.CompilerParams(vmem_limit_bytes=40 * 2 ** 20, has_side_effects=True, collective_id=0),
    )(*(pltpu.with_memory_space_constraint(x, pltpu.HBM) for x in (q, w_cols.T, hid, draft_tok.T)))
    res, bonus, acc, expected = pl.pallas_call(
        finish_kernel,
        out_shape=[
            jax.ShapeDtypeStruct((SHARD * BT * DRAFT, 1, LANES), f32),
            jax.ShapeDtypeStruct((SHARD, BATCH), f32),
            jax.ShapeDtypeStruct((DRAFT, BATCH), f32),
            jax.ShapeDtypeStruct((BATCH,), f32),
        ],
        in_specs=[vmem] * 3,
        out_specs=[hbm, hbm, vmem, vmem],
        scratch_shapes=[
            pltpu.VMEM((SHARD * BT * DRAFT, 1, LANES), f32),
            pltpu.VMEM((SHARD, BATCH), f32),
            dma,
        ],
        compiler_params=pltpu.CompilerParams(vmem_limit_bytes=12 * 2 ** 20),
    )(ex, bo, st)
    res = with_layout_constraint(res.reshape(SHARD, BT, DRAFT, LANES).transpose(0, 2, 1, 3), Layout((0, 2, 1, 3)))
    residual = res.reshape(SHARD, DRAFT, BATCH).transpose(2, 1, 0)
    return acc.T, expected, residual, bonus.T


def solution(mesh):
    return jax.shard_map(
        verify_local,
        mesh=mesh,
        in_specs=(P(('dp', 'tp'), None, None), P(None, 'tp'), P(('dp', 'tp'), None, None), P('dp', None)),
        out_specs=(P('dp', None), P('dp'), P('dp', None, 'tp'), P('dp', 'tp')),
        check_vma=False,
    )
```

```python
import functools

import jax
import jax.numpy as jnp
from jax import lax
from jax.experimental import pallas as pl
from jax.experimental.layout import Layout, with_layout_constraint
from jax.experimental.pallas import tpu as pltpu
from jax.sharding import PartitionSpec as P

INV_TEMP = 1.25
DEV = 128
SEQ = 3
NPOS = 3
DRAFT = 2
BATCH = 384
DIM = 2048
VOCAB = 128256
SHARD = VOCAB // DEV
LANES = 128
TILES = VOCAB // LANES
CHUNKS = 8
TAIL = SHARD - (CHUNKS - 1) * LANES
ROWS_P = 1008
TAIL_P = ROWS_P - (CHUNKS - 1) * LANES
KC = DIM // LANES
HROWS = SEQ * NPOS * KC
COLS = NPOS * BATCH
COLS_P = 1280
CT = COLS // LANES
BT = BATCH // LANES
BLK = SEQ * CHUNKS
PITCH = 49
NEG = -1e30
STAT = 18
MESH = pl.DeviceIdType.MESH


def remote(src, dst, ssem, rsem, dev):
    return pltpu.make_async_remote_copy(
        src_ref=src, dst_ref=dst, send_sem=ssem, recv_sem=rsem,
        device_id={'tp': dev}, device_id_type=MESH)


def reduce_stage(buf, slot, count, ssem, rsem, device, payload):
    buf.reshape(count * STAT, LANES)[pl.ds(slot * STAT, STAT), :] = payload
    here = buf.at[pl.ds(slot * STAT, STAT)]
    for r in range(1, count):
        remote(here, here, ssem, rsem, device((slot + r) % count)).start()


def wait_rows(ref, rows, sem):
    part = ref.at[pl.ds(0, rows)]
    pltpu.make_async_copy(part, part, sem).wait()


def finish(buf, count, rsem):
    wait_rows(buf, (count - 1) * STAT, rsem)
    rows = buf.reshape(count * STAT, LANES)
    return [rows[k * STAT:(k + 1) * STAT, :] for k in range(count)]


def merge_max_sum(parts):
    m = parts[0][0:CT]
    for p in parts[1:]:
        m = jnp.maximum(m, p[0:CT])
    s = parts[0][CT:2 * CT] * jnp.exp(parts[0][0:CT] - m)
    for p in parts[1:]:
        s = s + p[CT:2 * CT] * jnp.exp(p[0:CT] - m)
    return jnp.concatenate([m, s], axis=0)


def merge_add(parts):
    total = parts[0]
    for p in parts[1:]:
        total = total + p
    return total


def kernel(q_hbm, w_hbm, h_hbm, tok_hbm,
           ex_hbm, bo_hbm, out_ref,
           tok_ref, qbuf, wbuf, hloc, hidb, bounce, hmat, z, send, recv, exbuf, stat, peak, scale,
           a1, b1, a2, b2,
           lsem, ag_s, ag_r, ag_r2, d2d_s, d2d_r, qs, qr_sem, rs, rr):
    scope = jax.named_scope
    me = lax.axis_index('tp')
    core = me % 2
    coord = (me // 32, (me // 8) % 4, (me // 2) % 4)
    unit = (32, 8, 2)
    partner = me + 1 - 2 * core
    hop = [[((coord[d] + r) % 4) * unit[d] for r in range(4)] for d in range(3)]

    def device(rz, ry, rx, rc):
        return hop[0][rz] + hop[1][ry] + hop[2][rx] + (core if rc == 0 else 1 - core)

    hcp = pltpu.make_async_copy(h_hbm, hloc, lsem.at[2])
    hcp.start()
    qcp = pltpu.make_async_copy(q_hbm, qbuf.at[pl.ds(0, SEQ * TILES * DRAFT)], lsem.at[0])
    qcp.start()
    wcp = pltpu.make_async_copy(w_hbm, wbuf, lsem.at[1])
    wcp.start()
    tcp = pltpu.make_async_copy(tok_hbm, tok_ref, lsem.at[3])
    tcp.start()
    barrier = pltpu.get_barrier_semaphore()
    peers = [partner]
    for d in range(3):
        for r in range(1, 4):
            steps = [0, 0, 0]
            steps[d] = r
            peers.append(device(*steps, 0))
    for dev in peers:
        pl.semaphore_signal(barrier, inc=1, device_id={'tp': dev}, device_id_type=MESH)

    with scope('hid'):
        hcp.wait()
        for s in range(SEQ):
            x = hloc[s].astype(jnp.float32)
            for kc in range(KC):
                bounce[pl.ds(s * 48 + kc, NPOS, stride=KC), :] = x[:, kc * LANES:(kc + 1) * LANES]
        hidb[pl.ds(pl.multiple_of(me * HROWS, 16), HROWS), :] = bounce[0:HROWS, :].astype(jnp.bfloat16)
    with scope('barrier'):
        pl.semaphore_wait(barrier, len(peers))

    hview = hidb.reshape(4, 4, 4, 2, SEQ, HROWS // SEQ, LANES)

    def ag_phase(phase):
        for j in range(3):
            order = [(j + k) % 3 for k in range(3)]
            idx = list(coord)
            for d in order[:phase]:
                idx[d] = slice(None)
            view = hview.at[idx[0], idx[1], idx[2], core, j]
            for r in (1, 3, 2):
                steps = [0, 0, 0]
                steps[order[phase]] = r
                remote(view, view, ag_s, ag_r.at[phase, j], device(*steps, 0)).start()

    def ag_wait(phase, j):
        wait_rows(hidb, 3 * 4 ** phase * (HROWS // SEQ), ag_r.at[phase, j])

    def half(j, off, part):
        order = [(j + k) % 3 for k in range(3)]
        idx = [slice(None)] * 3
        idx[order[2]] = (coord[order[2]] + off) % 4
        idx[order[0]] = slice(2 * part, 2 * part + 2)
        return hview.at[idx[0], idx[1], idx[2], core, j]

    def ag_half(j, off, part, sem, r):
        steps = [0, 0, 0]
        steps[(j + 2) % 3] = r
        view = half(j, off, part)
        remote(view, view, ag_s, ag_r2.at[j, sem], device(*steps, 0)).start()

    HALF = 8 * HROWS // SEQ
    qrows = qbuf.reshape(qbuf.shape[0], LANES)
    lane = lax.broadcasted_iota(jnp.int32, (8, LANES), 1)

    def pack(i, k, carry):
        first = (SHARD * k) // LANES
        off = (SHARD * k) % LANES
        shift = (LANES - off) % LANES
        keep = lane < LANES - off
        for s in range(SEQ):
            base = (s * TILES + first) * DRAFT + i
            lo = qrows[pl.ds(base, 8, stride=2), :]
            hi = qrows[pl.ds(base + 2, 8, stride=2), :]
            lo = pltpu.roll(lo, shift, 1)
            hi = pltpu.roll(hi, shift, 1)
            send[i, pl.ds(pl.multiple_of(k * BLK + s * 8, 8), 8), :] = jnp.where(keep, lo, hi)
        return carry

    mine = pl.ds(pl.multiple_of(me * BLK, 8), BLK)

    def to(i, dev):
        remote(send.at[i, pl.ds(pl.multiple_of(dev * BLK, 8), BLK)], recv.at[i, mine],
               qs, qr_sem.at[i], dev).start()

    def step(d, n):
        return ((coord[d] + n) % 4) * unit[d]

    def class0(i):
        pltpu.make_async_copy(send.at[i, mine], recv.at[i, mine], qr_sem.at[i]).start()
        to(i, partner)

    def class1(i, rc):
        last = core if rc == 0 else 1 - core
        for r in (1, 3, 2):
            for d in range(3):
                steps = [0, 0, 0]
                steps[d] = r
                to(i, device(*steps, rc))

    def class2(i, rc, lo=0, hi=9):
        last = core if rc == 0 else 1 - core

        def body(n, carry):
            a, b = n // 3 + 1, n % 3 + 1
            to(i, step(0, a) + step(1, b) + hop[2][0] + last)
            to(i, hop[0][0] + step(1, a) + step(2, b) + last)
            to(i, step(0, b) + hop[1][0] + step(2, a) + last)
            return carry

        lax.fori_loop(lo, hi, body, 0)

    def class3(i, rc, lo=0, hi=9):
        last = core if rc == 0 else 1 - core

        def body(n, carry):
            a, b = n // 3, n % 3
            for k in range(3):
                to(i, step(0, (a + k) % 3 + 1) + step(1, (b + k) % 3 + 1) + hop[2][k + 1] + last)
            return carry

        lax.fori_loop(lo, hi, body, 0)

    ag_phase(0)
    with scope('qwait'):
        qcp.wait()
    with scope('pack'):
        lax.fori_loop(0, DEV, functools.partial(pack, 0), 0, unroll=16)
    with scope('ex0'):
        class0(0)
        class1(0, 0)
    with scope('ag0'):
        for j in range(3):
            ag_wait(0, j)
    ag_phase(1)
    with scope('ex0a'):
        class1(0, 1)
        class2(0, 0)
    with scope('pack2'):
        lax.fori_loop(0, DEV, functools.partial(pack, 1), 0, unroll=16)
    with scope('ag1'):
        for j in range(3):
            ag_wait(1, j)
    for j in range(3):
        ag_half(j, 0, 0, 0, 1)
        ag_half(j, 0, 1, 1, 3)
    for j in range(3):
        ag_half(j, 0, 1, 2, 1)
        ag_half(j, 0, 0, 2, 3)
    with scope('relay'):
        for j in range(3):
            wait_rows(hidb, HALF, ag_r2.at[j, 0])
            ag_half(j, 3, 0, 2, 1)
            wait_rows(hidb, HALF, ag_r2.at[j, 1])
            ag_half(j, 1, 1, 2, 3)
    with scope('exag2'):
        class0(1)
        class1(1, 0)
        class1(1, 1)
    d2d = []
    for j in (2, 1, 0):
        with scope(f'ag2_{j}'):
            wait_rows(hidb, 4 * HALF, ag_r2.at[j, 2])
        view = hview.at[:, :, :, core, j]
        cp = remote(view, view, d2d_s, d2d_r.at[j], partner)
        cp.start()
        d2d.append(cp)
    with scope('ex0b'):
        class3(0, 0)
        class3(0, 1)
        class2(0, 1)
        class3(1, 0, 0, 4)
    with scope('d2d'):
        for cp in d2d:
            cp.wait_recv()

    def relayout(n, carry):
        def up(b, c):
            x = hidb[pl.ds(pl.multiple_of((48 * n + b) * 48, 16), 48), :]
            bounce[pl.ds(b * PITCH, 48), :] = x.astype(jnp.float32)
            return c

        lax.fori_loop(0, 48, up, 0, unroll=4)
        for g in range(NPOS):
            for u in range(3):
                for kc in range(KC):
                    y = bounce[pl.ds(16 * u * PITCH + g * KC + kc, 16, stride=PITCH), :]
                    hmat[pl.ds(pl.multiple_of(g * BATCH + 48 * n + 16 * u, 16), 16),
                         kc * LANES:(kc + 1) * LANES] = y.astype(jnp.bfloat16)
        return carry

    with scope('relayout'):
        lax.fori_loop(0, 8, relayout, 0)
    wcp.wait()
    tcp.wait()

    z[SHARD:ROWS_P, :] = jnp.full((ROWS_P - SHARD, COLS_P), NEG, jnp.float32)

    def head(n, carry):
        hb = hmat[pl.ds(pl.multiple_of(n * 256, 256), 256), :]
        zt = lax.dot_general(wbuf[...], hb, (((1,), (1,)), ((), ())), preferred_element_type=jnp.float32)
        zt = zt * INV_TEMP
        z[0:SHARD, pl.ds(pl.multiple_of(n * 256, 256), 256)] = zt
        top = jnp.max(zt, axis=0, keepdims=True)
        peak[pl.ds(2 * n, 1), :] = top[:, 0:LANES]
        peak[pl.ds(2 * n + 1, 1), :] = top[:, LANES:]
        return carry

    with scope('head'):
        lax.fori_loop(0, COLS_P // 256, head, 0)

    def local_stats(t, carry):
        cols = pl.ds(pl.multiple_of(t * LANES, LANES), LANES)

        m = peak[pl.ds(t, 1), :]

        def expo(n, s):
            rows = pl.ds(pl.multiple_of(n * 112, 8), 112)
            x = jnp.exp(z[rows, cols] - m)
            z[rows, cols] = x
            return s + jnp.sum(x.reshape(14, 8, LANES), axis=0)

        s8 = lax.fori_loop(0, 9, expo, jnp.zeros((8, LANES), jnp.float32), unroll=3)
        stat[pl.ds(t, 1), :] = m
        stat[pl.ds(CT + t, 1), :] = jnp.sum(s8, axis=0, keepdims=True)
        return carry

    stat[...] = jnp.zeros_like(stat)
    with scope('stats'):
        lax.fori_loop(0, CT, local_stats, 0)
    bcp = pltpu.make_async_copy(z.at[:, DRAFT * BATCH:COLS], bo_hbm, lsem.at[2])
    bcp.start()

    slot, grp = me % 8, me // 8
    near = lambda k: grp * 8 + k
    far = lambda k: k * 8 + slot
    local = stat[0:STAT, :]
    reduce_stage(a1, slot, 8, rs, rr.at[0], near, local)
    with scope('ex1a'):
        class3(1, 0, 4, 9)
        class3(1, 1, 0, 3)
    with scope('round1a'):
        parts = finish(a1, 8, rr.at[0])
    reduce_stage(b1, grp, 16, rs, rr.at[1], far, merge_max_sum(parts))
    with scope('ex1b'):
        class3(1, 1, 3, 9)
        class2(1, 1)
        class2(1, 0)
    with scope('round1b'):
        parts = finish(b1, 16, rr.at[1])
    tot = merge_max_sum(parts)
    fac = jnp.exp(local[0:CT] - tot[0:CT]) / tot[CT:2 * CT]
    scale[0:CT, :] = fac
    out_ref[12:16, :] = jnp.concatenate([fac[DRAFT * BT:CT], fac[0:1]], axis=0)

    exrows = exbuf.reshape(exbuf.shape[0], LANES)
    first_id = me * SHARD
    stat[...] = jnp.zeros_like(stat)
    for i in range(DRAFT):
        with scope(f'a2a_{i}'):
            pltpu.make_async_copy(recv.at[i], recv.at[i], qr_sem.at[i]).wait()
        for t in range(BT):
            row = i * BT + t
            sc = scale[row:row + 1, :]
            tok = tok_ref[i:i + 1, t * LANES:(t + 1) * LANES] - first_id
            col0 = i * BATCH + t * LANES

            def block(c, carry, size, valid):
                mass, pp, qp = carry
                q = recv[i, pl.ds(t * LANES * CHUNKS + c, LANES, stride=CHUNKS), :].T
                p = z[pl.ds(pl.multiple_of(c * LANES, LANES), size), col0:col0 + LANES] * sc
                ids = lax.broadcasted_iota(jnp.int32, (size, LANES), 0)
                q = q[0:size]
                if valid < size:
                    q = jnp.where(ids < valid, q, 0.0)
                x = jnp.maximum(p - q, 0.0)
                exrows[pl.ds(c * LANES * 6 + t * 2 + i, valid, stride=6), :] = x[0:valid]
                hit = ids == tok - c * LANES
                fold = lambda v: jnp.sum(v.reshape(size // 8, 8, LANES), axis=0)
                return (mass + fold(x), pp + fold(jnp.where(hit, p, 0.0)), qp + fold(jnp.where(hit, q, 0.0)))

            zero = jnp.zeros((8, LANES), jnp.float32)
            carry = lax.fori_loop(0, CHUNKS - 1, lambda c, v: block(c, v, LANES, LANES), (zero, zero, zero),
                                  unroll=CHUNKS - 1)
            mass, pp, qp = block(CHUNKS - 1, carry, TAIL_P, TAIL)
            stat[row:row + 1, :] = jnp.sum(mass, axis=0, keepdims=True)
            stat[6 + row:7 + row, :] = jnp.sum(pp, axis=0, keepdims=True)
            stat[12 + row:13 + row, :] = jnp.sum(qp, axis=0, keepdims=True)

    ecp = pltpu.make_async_copy(exbuf, ex_hbm, lsem.at[0])
    ecp.start()
    reduce_stage(a2, slot, 8, rs, rr.at[2], near, stat[0:STAT, :])
    with scope('round2a'):
        parts = finish(a2, 8, rr.at[2])
    reduce_stage(b2, grp, 16, rs, rr.at[3], far, merge_add(parts))
    with scope('round2b'):
        parts = finish(b2, 16, rr.at[3])
    tot = merge_add(parts)
    out_ref[0:6, :] = tot[0:6]
    out_ref[6:12, :] = jnp.minimum(tot[6:12] / tot[12:18], 1.0)
    with scope('tail'):
        ecp.wait()
        bcp.wait()
        wait_rows(hidb, 9 * 21 * (HROWS // SEQ), ag_s)
        wait_rows(hidb, DEV // 2 * HROWS, d2d_s)
        wait_rows(send.reshape(DRAFT * DEV * BLK, LANES), DRAFT * (DEV - 1) * BLK, qs)
        wait_rows(qbuf, 2 * (7 + 15) * STAT, rs)


def finish_kernel(ex_ref, bo_ref, stat_ref, res_hbm, bonus_hbm, acc_ref, exp_ref, res, bonus, sems):
    rows = ex_ref.reshape(ex_ref.shape[0], LANES)
    out = res.reshape(res.shape[0], LANES)
    copies = []
    fac = jnp.concatenate([stat_ref[12 + t:13 + t, :] for t in range(BT)], axis=1)
    step = 256
    for n in range(4):
        size = min(step, SHARD - n * step)
        bonus[n * step:n * step + size, :] = bo_ref[n * step:n * step + size, :] * fac
    cp = pltpu.make_async_copy(bonus, bonus_hbm, sems)
    cp.start()
    copies.append(cp)
    mass = jnp.concatenate([stat_ref[i * BT + t:i * BT + t + 1, :] for t in range(BT) for i in range(DRAFT)], axis=0)
    mass = jnp.concatenate([mass] * 4, axis=0)
    for n in range(5):
        def body(k, carry):
            at = pl.ds(pl.multiple_of(n * 1200 + k * 24, 8), 24)
            out[at, :] = rows[at, :] / mass
            return carry

        lax.fori_loop(0, 50, body, 0, unroll=5)
        size = 1200
        if n == 4:
            out[6000:6012, :] = rows[6000:6012, :] / mass[0:12]
            size = 1212
        cp = pltpu.make_async_copy(res.at[pl.ds(n * 1200, size)], res_hbm.at[pl.ds(n * 1200, size)], sems)
        cp.start()
        copies.append(cp)
    acc = stat_ref[6:12, :]
    more = acc[0:BT] * (1.0 + acc[BT:2 * BT])
    for t in range(BT):
        cols = slice(t * LANES, (t + 1) * LANES)
        exp_ref[cols] = more[t]
        for i in range(DRAFT):
            acc_ref[i:i + 1, cols] = acc[i * BT + t:i * BT + t + 1]
    for cp in copies:
        cp.wait()


def verify_local(hid, w_cols, q_rows, draft_tok):
    q = with_layout_constraint(q_rows.reshape(SEQ, DRAFT, TILES, LANES), Layout((0, 2, 1, 3)))
    q = q.transpose(0, 2, 1, 3).reshape(SEQ * TILES * DRAFT, 1, LANES)
    f32 = jnp.float32
    hbm = pl.BlockSpec(memory_space=pl.ANY)
    vmem = pl.BlockSpec(memory_space=pltpu.VMEM)
    dma = pltpu.SemaphoreType.DMA
    ex, bo, st = pl.pallas_call(
        kernel,
        out_shape=[
            jax.ShapeDtypeStruct((SHARD * BT * DRAFT, 1, LANES), f32),
            jax.ShapeDtypeStruct((ROWS_P, BATCH), f32),
            jax.ShapeDtypeStruct((16, LANES), f32),
        ],
        in_specs=[pl.BlockSpec(memory_space=pltpu.HBM)] * 4,
        out_specs=[hbm, hbm, vmem],
        scratch_shapes=[
            pltpu.VMEM((DRAFT, BATCH), jnp.int32),
            pltpu.VMEM((SEQ * TILES * DRAFT + 20, 1, LANES), f32),
            pltpu.VMEM((SHARD, DIM), jnp.bfloat16),
            pltpu.VMEM((SEQ, NPOS, DIM), jnp.bfloat16),
            pltpu.VMEM((DEV * HROWS, LANES), jnp.bfloat16),
            pltpu.VMEM((48 * PITCH, LANES), f32),
            pltpu.VMEM((COLS_P, DIM), jnp.bfloat16),
            pltpu.VMEM((ROWS_P, COLS_P), f32),
            pltpu.VMEM((DRAFT, DEV * BLK, LANES), f32),
            pltpu.VMEM((DRAFT, DEV * BLK, LANES), f32),
            pltpu.VMEM((SHARD * BT * DRAFT, 1, LANES), f32),
            pltpu.VMEM((24, LANES), f32),
            pltpu.VMEM((16, LANES), f32),
            pltpu.VMEM((16, LANES), f32),
            pltpu.VMEM((8 * STAT, 1, LANES), f32),
            pltpu.VMEM((16 * STAT, 1, LANES), f32),
            pltpu.VMEM((8 * STAT, 1, LANES), f32),
            pltpu.VMEM((16 * STAT, 1, LANES), f32),
            dma((4,)),
            dma, dma((2, 3)), dma((3, 3)), dma, dma((3,)), dma, dma((2,)), dma, dma((4,)),
        ],
        compiler_params=pltpu.CompilerParams(vmem_limit_bytes=40 * 2 ** 20, has_side_effects=True, collective_id=0),
    )(*(pltpu.with_memory_space_constraint(x, pltpu.HBM) for x in (q, w_cols.T, hid, draft_tok.T)))
    res, bonus, acc, expected = pl.pallas_call(
        finish_kernel,
        out_shape=[
            jax.ShapeDtypeStruct((SHARD * BT * DRAFT, 1, LANES), f32),
            jax.ShapeDtypeStruct((SHARD, BATCH), f32),
            jax.ShapeDtypeStruct((DRAFT, BATCH), f32),
            jax.ShapeDtypeStruct((BATCH,), f32),
        ],
        in_specs=[vmem] * 3,
        out_specs=[hbm, hbm, vmem, vmem],
        scratch_shapes=[
            pltpu.VMEM((SHARD * BT * DRAFT, 1, LANES), f32),
            pltpu.VMEM((SHARD, BATCH), f32),
            dma,
        ],
        compiler_params=pltpu.CompilerParams(vmem_limit_bytes=12 * 2 ** 20),
    )(ex, bo, st)
    res = with_layout_constraint(res.reshape(SHARD, BT, DRAFT, LANES).transpose(0, 2, 1, 3), Layout((0, 2, 1, 3)))
    residual = res.reshape(SHARD, DRAFT, BATCH).transpose(2, 1, 0)
    return acc.T, expected, residual, bonus.T


def solution(mesh):
    return jax.shard_map(
        verify_local,
        mesh=mesh,
        in_specs=(P(('dp', 'tp'), None, None), P(None, 'tp'), P(('dp', 'tp'), None, None), P('dp', None)),
        out_specs=(P('dp', None), P('dp'), P('dp', None, 'tp'), P('dp', 'tp')),
        check_vma=False,
    )
```

```python
import functools

import jax
import jax.numpy as jnp
from jax import lax
from jax.experimental import pallas as pl
from jax.experimental.layout import Layout, with_layout_constraint
from jax.experimental.pallas import tpu as pltpu
from jax.sharding import PartitionSpec as P

INV_TEMP = 1.25
DEV = 128
SEQ = 3
NPOS = 3
DRAFT = 2
BATCH = 384
DIM = 2048
VOCAB = 128256
SHARD = VOCAB // DEV
LANES = 128
TILES = VOCAB // LANES
CHUNKS = 8
TAIL = SHARD - (CHUNKS - 1) * LANES
ROWS_P = 1008
TAIL_P = ROWS_P - (CHUNKS - 1) * LANES
KC = DIM // LANES
HROWS = SEQ * NPOS * KC
COLS = NPOS * BATCH
COLS_P = 1280
CT = COLS // LANES
BT = BATCH // LANES
BLK = SEQ * CHUNKS
PITCH = 49
NEG = -1e30
STAT = 18
MESH = pl.DeviceIdType.MESH


def remote(src, dst, ssem, rsem, dev):
    return pltpu.make_async_remote_copy(
        src_ref=src, dst_ref=dst, send_sem=ssem, recv_sem=rsem,
        device_id={'tp': dev}, device_id_type=MESH)


def reduce_stage(buf, slot, count, ssem, rsem, device, payload):
    buf.reshape(count * STAT, LANES)[pl.ds(slot * STAT, STAT), :] = payload
    here = buf.at[pl.ds(slot * STAT, STAT)]
    for r in range(1, count):
        remote(here, here, ssem, rsem, device((slot + r) % count)).start()


def wait_rows(ref, rows, sem):
    part = ref.at[pl.ds(0, rows)]
    pltpu.make_async_copy(part, part, sem).wait()


def finish(buf, count, rsem):
    wait_rows(buf, (count - 1) * STAT, rsem)
    rows = buf.reshape(count * STAT, LANES)
    return [rows[k * STAT:(k + 1) * STAT, :] for k in range(count)]


def merge_max_sum(parts):
    m = parts[0][0:CT]
    for p in parts[1:]:
        m = jnp.maximum(m, p[0:CT])
    s = parts[0][CT:2 * CT] * jnp.exp(parts[0][0:CT] - m)
    for p in parts[1:]:
        s = s + p[CT:2 * CT] * jnp.exp(p[0:CT] - m)
    return jnp.concatenate([m, s], axis=0)


def merge_add(parts):
    total = parts[0]
    for p in parts[1:]:
        total = total + p
    return total


def kernel(q_hbm, w_hbm, h_hbm, tok_hbm,
           ex_hbm, bo_hbm, out_ref,
           tok_ref, qbuf, wbuf, hloc, hidb, bounce, hmat, z, send, recv, exbuf, stat, peak, scale,
           a1, b1, a2, b2,
           lsem, ag_s, ag_r, ag_r2, d2d_s, d2d_r, qs, qr_sem, rs, rr):
    scope = jax.named_scope
    me = lax.axis_index('tp')
    core = me % 2
    coord = (me // 32, (me // 8) % 4, (me // 2) % 4)
    unit = (32, 8, 2)
    partner = me + 1 - 2 * core
    hop = [[((coord[d] + r) % 4) * unit[d] for r in range(4)] for d in range(3)]

    def device(rz, ry, rx, rc):
        return hop[0][rz] + hop[1][ry] + hop[2][rx] + (core if rc == 0 else 1 - core)

    hcp = pltpu.make_async_copy(h_hbm, hloc, lsem.at[2])
    hcp.start()
    qcp = pltpu.make_async_copy(q_hbm, qbuf.at[pl.ds(0, SEQ * TILES * DRAFT)], lsem.at[0])
    qcp.start()
    wcp = pltpu.make_async_copy(w_hbm, wbuf, lsem.at[1])
    wcp.start()
    tcp = pltpu.make_async_copy(tok_hbm, tok_ref, lsem.at[3])
    tcp.start()
    barrier = pltpu.get_barrier_semaphore()
    peers = [partner]
    for d in range(3):
        for r in range(1, 4):
            steps = [0, 0, 0]
            steps[d] = r
            peers.append(device(*steps, 0))
    for dev in peers:
        pl.semaphore_signal(barrier, inc=1, device_id={'tp': dev}, device_id_type=MESH)

    with scope('hid'):
        hcp.wait()
        for s in range(SEQ):
            x = hloc[s].astype(jnp.float32)
            for kc in range(KC):
                bounce[pl.ds(s * 48 + kc, NPOS, stride=KC), :] = x[:, kc * LANES:(kc + 1) * LANES]
        hidb[pl.ds(pl.multiple_of(me * HROWS, 16), HROWS), :] = bounce[0:HROWS, :].astype(jnp.bfloat16)
    with scope('barrier'):
        pl.semaphore_wait(barrier, len(peers))

    hview = hidb.reshape(4, 4, 4, 2, SEQ, HROWS // SEQ, LANES)

    def ag_phase(phase):
        for j in range(3):
            order = [(j + k) % 3 for k in range(3)]
            idx = list(coord)
            for d in order[:phase]:
                idx[d] = slice(None)
            view = hview.at[idx[0], idx[1], idx[2], core, j]
            for r in (1, 3, 2):
                steps = [0, 0, 0]
                steps[order[phase]] = r
                remote(view, view, ag_s, ag_r.at[phase, j], device(*steps, 0)).start()

    def ag_wait(phase, j):
        wait_rows(hidb, 3 * 4 ** phase * (HROWS // SEQ), ag_r.at[phase, j])

    def half(j, off, part):
        order = [(j + k) % 3 for k in range(3)]
        idx = [slice(None)] * 3
        idx[order[2]] = (coord[order[2]] + off) % 4
        idx[order[0]] = slice(2 * part, 2 * part + 2)
        return hview.at[idx[0], idx[1], idx[2], core, j]

    def ag_half(j, off, part, sem, r):
        steps = [0, 0, 0]
        steps[(j + 2) % 3] = r
        view = half(j, off, part)
        remote(view, view, ag_s, ag_r2.at[j, sem], device(*steps, 0)).start()

    HALF = 8 * HROWS // SEQ
    qrows = qbuf.reshape(qbuf.shape[0], LANES)
    lane = lax.broadcasted_iota(jnp.int32, (8, LANES), 1)

    def pack(i, k, carry):
        first = (SHARD * k) // LANES
        off = (SHARD * k) % LANES
        shift = (LANES - off) % LANES
        keep = lane < LANES - off
        for s in range(SEQ):
            base = (s * TILES + first) * DRAFT + i
            lo = qrows[pl.ds(base, 8, stride=2), :]
            hi = qrows[pl.ds(base + 2, 8, stride=2), :]
            lo = pltpu.roll(lo, shift, 1)
            hi = pltpu.roll(hi, shift, 1)
            send[i, pl.ds(pl.multiple_of(k * BLK + s * 8, 8), 8), :] = jnp.where(keep, lo, hi)
        return carry

    mine = pl.ds(pl.multiple_of(me * BLK, 8), BLK)

    def to(i, dev):
        remote(send.at[i, pl.ds(pl.multiple_of(dev * BLK, 8), BLK)], recv.at[i, mine],
               qs, qr_sem.at[i], dev).start()

    def step(d, n):
        return ((coord[d] + n) % 4) * unit[d]

    def class0(i):
        pltpu.make_async_copy(send.at[i, mine], recv.at[i, mine], qr_sem.at[i]).start()
        to(i, partner)

    def class1(i, rc):
        last = core if rc == 0 else 1 - core
        for r in (1, 3, 2):
            for d in range(3):
                steps = [0, 0, 0]
                steps[d] = r
                to(i, device(*steps, rc))

    def class2(i, rc, lo=0, hi=9):
        last = core if rc == 0 else 1 - core

        def body(n, carry):
            a, b = n // 3 + 1, n % 3 + 1
            to(i, step(0, a) + step(1, b) + hop[2][0] + last)
            to(i, hop[0][0] + step(1, a) + step(2, b) + last)
            to(i, step(0, b) + hop[1][0] + step(2, a) + last)
            return carry

        lax.fori_loop(lo, hi, body, 0)

    def class3(i, rc, lo=0, hi=9):
        last = core if rc == 0 else 1 - core

        def body(n, carry):
            a, b = n // 3, n % 3
            for k in range(3):
                to(i, step(0, (a + k) % 3 + 1) + step(1, (b + k) % 3 + 1) + hop[2][k + 1] + last)
            return carry

        lax.fori_loop(lo, hi, body, 0)

    ag_phase(0)
    with scope('qwait'):
        qcp.wait()
    with scope('pack'):
        lax.fori_loop(0, DEV, functools.partial(pack, 0), 0, unroll=16)
    with scope('ex0'):
        class0(0)
        class1(0, 0)
    with scope('ag0'):
        for j in range(3):
            ag_wait(0, j)
    ag_phase(1)
    with scope('ex0a'):
        class1(0, 1)
        class2(0, 0)
    with scope('pack2'):
        lax.fori_loop(0, DEV, functools.partial(pack, 1), 0, unroll=16)
    with scope('ag1'):
        for j in range(3):
            ag_wait(1, j)
    for j in range(3):
        ag_half(j, 0, 0, 0, 1)
        ag_half(j, 0, 1, 1, 3)
    for j in range(3):
        ag_half(j, 0, 1, 2, 1)
        ag_half(j, 0, 0, 2, 3)
    with scope('relay'):
        for j in range(3):
            wait_rows(hidb, HALF, ag_r2.at[j, 0])
            ag_half(j, 3, 0, 2, 1)
            wait_rows(hidb, HALF, ag_r2.at[j, 1])
            ag_half(j, 1, 1, 2, 3)
    d2d = []
    for j in (2, 1, 0):
        with scope(f'ag2_{j}'):
            wait_rows(hidb, 4 * HALF, ag_r2.at[j, 2])
        view = hview.at[:, :, :, core, j]
        cp = remote(view, view, d2d_s, d2d_r.at[j], partner)
        cp.start()
        d2d.append(cp)
    with scope('ex0b'):
        class3(0, 0)
        class3(0, 1)
        class2(0, 1)
        class3(1, 0, 0, 4)
    with scope('d2d'):
        for cp in d2d:
            cp.wait_recv()

    def relayout(n, carry):
        def up(b, c):
            x = hidb[pl.ds(pl.multiple_of((48 * n + b) * 48, 16), 48), :]
            bounce[pl.ds(b * PITCH, 48), :] = x.astype(jnp.float32)
            return c

        lax.fori_loop(0, 48, up, 0, unroll=4)
        for g in range(NPOS):
            for u in range(3):
                for kc in range(KC):
                    y = bounce[pl.ds(16 * u * PITCH + g * KC + kc, 16, stride=PITCH), :]
                    hmat[pl.ds(pl.multiple_of(g * BATCH + 48 * n + 16 * u, 16), 16),
                         kc * LANES:(kc + 1) * LANES] = y.astype(jnp.bfloat16)
        return carry

    with scope('relayout'):
        lax.fori_loop(0, 8, relayout, 0)
    wcp.wait()
    tcp.wait()

    z[SHARD:ROWS_P, :] = jnp.full((ROWS_P - SHARD, COLS_P), NEG, jnp.float32)

    def head(n, carry):
        hb = hmat[pl.ds(pl.multiple_of(n * 256, 256), 256), :]
        zt = lax.dot_general(wbuf[...], hb, (((1,), (1,)), ((), ())), preferred_element_type=jnp.float32)
        zt = zt * INV_TEMP
        z[0:SHARD, pl.ds(pl.multiple_of(n * 256, 256), 256)] = zt
        top = jnp.max(zt, axis=0, keepdims=True)
        peak[pl.ds(2 * n, 1), :] = top[:, 0:LANES]
        peak[pl.ds(2 * n + 1, 1), :] = top[:, LANES:]
        return carry

    with scope('head'):
        lax.fori_loop(0, COLS_P // 256, head, 0)

    def local_stats(t, carry):
        cols = pl.ds(pl.multiple_of(t * LANES, LANES), LANES)

        m = peak[pl.ds(t, 1), :]

        def expo(n, s):
            rows = pl.ds(pl.multiple_of(n * 112, 8), 112)
            x = jnp.exp(z[rows, cols] - m)
            z[rows, cols] = x
            return s + jnp.sum(x.reshape(14, 8, LANES), axis=0)

        s8 = lax.fori_loop(0, 9, expo, jnp.zeros((8, LANES), jnp.float32), unroll=3)
        stat[pl.ds(t, 1), :] = m
        stat[pl.ds(CT + t, 1), :] = jnp.sum(s8, axis=0, keepdims=True)
        return carry

    stat[...] = jnp.zeros_like(stat)
    with scope('stats'):
        lax.fori_loop(0, CT, local_stats, 0)
    bcp = pltpu.make_async_copy(z.at[:, DRAFT * BATCH:COLS], bo_hbm, lsem.at[2])
    bcp.start()

    slot, grp = me % 8, me // 8
    near = lambda k: grp * 8 + k
    far = lambda k: k * 8 + slot
    local = stat[0:STAT, :]
    reduce_stage(a1, slot, 8, rs, rr.at[0], near, local)
    with scope('ex1a'):
        class3(1, 0, 4, 9)
        class3(1, 1, 0, 3)
    with scope('round1a'):
        parts = finish(a1, 8, rr.at[0])
    reduce_stage(b1, grp, 16, rs, rr.at[1], far, merge_max_sum(parts))
    with scope('ex1b'):
        class3(1, 1, 3, 9)
        class2(1, 1)
        class2(1, 0)
        class1(1, 1)
        class1(1, 0)
        class0(1)
    with scope('round1b'):
        parts = finish(b1, 16, rr.at[1])
    tot = merge_max_sum(parts)
    fac = jnp.exp(local[0:CT] - tot[0:CT]) / tot[CT:2 * CT]
    scale[0:CT, :] = fac
    out_ref[12:16, :] = jnp.concatenate([fac[DRAFT * BT:CT], fac[0:1]], axis=0)

    exrows = exbuf.reshape(exbuf.shape[0], LANES)
    first_id = me * SHARD
    stat[...] = jnp.zeros_like(stat)
    for i in range(DRAFT):
        with scope(f'a2a_{i}'):
            pltpu.make_async_copy(recv.at[i], recv.at[i], qr_sem.at[i]).wait()
        for t in range(BT):
            row = i * BT + t
            sc = scale[row:row + 1, :]
            tok = tok_ref[i:i + 1, t * LANES:(t + 1) * LANES] - first_id
            col0 = i * BATCH + t * LANES

            def block(c, carry, size, valid):
                mass, pp, qp = carry
                q = recv[i, pl.ds(t * LANES * CHUNKS + c, LANES, stride=CHUNKS), :].T
                p = z[pl.ds(pl.multiple_of(c * LANES, LANES), size), col0:col0 + LANES] * sc
                ids = lax.broadcasted_iota(jnp.int32, (size, LANES), 0)
                q = q[0:size]
                if valid < size:
                    q = jnp.where(ids < valid, q, 0.0)
                x = jnp.maximum(p - q, 0.0)
                exrows[pl.ds(c * LANES * 6 + t * 2 + i, valid, stride=6), :] = x[0:valid]
                hit = ids == tok - c * LANES
                fold = lambda v: jnp.sum(v.reshape(size // 8, 8, LANES), axis=0)
                return (mass + fold(x), pp + fold(jnp.where(hit, p, 0.0)), qp + fold(jnp.where(hit, q, 0.0)))

            zero = jnp.zeros((8, LANES), jnp.float32)
            carry = lax.fori_loop(0, CHUNKS - 1, lambda c, v: block(c, v, LANES, LANES), (zero, zero, zero),
                                  unroll=CHUNKS - 1)
            mass, pp, qp = block(CHUNKS - 1, carry, TAIL_P, TAIL)
            stat[row:row + 1, :] = jnp.sum(mass, axis=0, keepdims=True)
            stat[6 + row:7 + row, :] = jnp.sum(pp, axis=0, keepdims=True)
            stat[12 + row:13 + row, :] = jnp.sum(qp, axis=0, keepdims=True)

    ecp = pltpu.make_async_copy(exbuf, ex_hbm, lsem.at[0])
    ecp.start()
    reduce_stage(a2, slot, 8, rs, rr.at[2], near, stat[0:STAT, :])
    with scope('round2a'):
        parts = finish(a2, 8, rr.at[2])
    reduce_stage(b2, grp, 16, rs, rr.at[3], far, merge_add(parts))
    with scope('round2b'):
        parts = finish(b2, 16, rr.at[3])
    tot = merge_add(parts)
    out_ref[0:6, :] = tot[0:6]
    out_ref[6:12, :] = jnp.minimum(tot[6:12] / tot[12:18], 1.0)
    with scope('tail'):
        ecp.wait()
        bcp.wait()
        wait_rows(hidb, 9 * 21 * (HROWS // SEQ), ag_s)
        wait_rows(hidb, DEV // 2 * HROWS, d2d_s)
        wait_rows(send.reshape(DRAFT * DEV * BLK, LANES), DRAFT * (DEV - 1) * BLK, qs)
        wait_rows(qbuf, 2 * (7 + 15) * STAT, rs)


def finish_kernel(ex_ref, bo_ref, stat_ref, res_hbm, bonus_hbm, acc_ref, exp_ref, res, bonus, sems):
    rows = ex_ref.reshape(ex_ref.shape[0], LANES)
    out = res.reshape(res.shape[0], LANES)
    copies = []
    fac = jnp.concatenate([stat_ref[12 + t:13 + t, :] for t in range(BT)], axis=1)
    step = 256
    for n in range(4):
        size = min(step, SHARD - n * step)
        bonus[n * step:n * step + size, :] = bo_ref[n * step:n * step + size, :] * fac
    cp = pltpu.make_async_copy(bonus, bonus_hbm, sems)
    cp.start()
    copies.append(cp)
    mass = jnp.concatenate([stat_ref[i * BT + t:i * BT + t + 1, :] for t in range(BT) for i in range(DRAFT)], axis=0)
    mass = jnp.concatenate([mass] * 4, axis=0)
    for n in range(5):
        def body(k, carry):
            at = pl.ds(pl.multiple_of(n * 1200 + k * 24, 8), 24)
            out[at, :] = rows[at, :] / mass
            return carry

        lax.fori_loop(0, 50, body, 0, unroll=5)
        size = 1200
        if n == 4:
            out[6000:6012, :] = rows[6000:6012, :] / mass[0:12]
            size = 1212
        cp = pltpu.make_async_copy(res.at[pl.ds(n * 1200, size)], res_hbm.at[pl.ds(n * 1200, size)], sems)
        cp.start()
        copies.append(cp)
    acc = stat_ref[6:12, :]
    more = acc[0:BT] * (1.0 + acc[BT:2 * BT])
    for t in range(BT):
        cols = slice(t * LANES, (t + 1) * LANES)
        exp_ref[cols] = more[t]
        for i in range(DRAFT):
            acc_ref[i:i + 1, cols] = acc[i * BT + t:i * BT + t + 1]
    for cp in copies:
        cp.wait()


def verify_local(hid, w_cols, q_rows, draft_tok):
    q = with_layout_constraint(q_rows.reshape(SEQ, DRAFT, TILES, LANES), Layout((0, 2, 1, 3)))
    q = q.transpose(0, 2, 1, 3).reshape(SEQ * TILES * DRAFT, 1, LANES)
    f32 = jnp.float32
    hbm = pl.BlockSpec(memory_space=pl.ANY)
    vmem = pl.BlockSpec(memory_space=pltpu.VMEM)
    dma = pltpu.SemaphoreType.DMA
    ex, bo, st = pl.pallas_call(
        kernel,
        out_shape=[
            jax.ShapeDtypeStruct((SHARD * BT * DRAFT, 1, LANES), f32),
            jax.ShapeDtypeStruct((ROWS_P, BATCH), f32),
            jax.ShapeDtypeStruct((16, LANES), f32),
        ],
        in_specs=[pl.BlockSpec(memory_space=pltpu.HBM)] * 4,
        out_specs=[hbm, hbm, vmem],
        scratch_shapes=[
            pltpu.VMEM((DRAFT, BATCH), jnp.int32),
            pltpu.VMEM((SEQ * TILES * DRAFT + 20, 1, LANES), f32),
            pltpu.VMEM((SHARD, DIM), jnp.bfloat16),
            pltpu.VMEM((SEQ, NPOS, DIM), jnp.bfloat16),
            pltpu.VMEM((DEV * HROWS, LANES), jnp.bfloat16),
            pltpu.VMEM((48 * PITCH, LANES), f32),
            pltpu.VMEM((COLS_P, DIM), jnp.bfloat16),
            pltpu.VMEM((ROWS_P, COLS_P), f32),
            pltpu.VMEM((DRAFT, DEV * BLK, LANES), f32),
            pltpu.VMEM((DRAFT, DEV * BLK, LANES), f32),
            pltpu.VMEM((SHARD * BT * DRAFT, 1, LANES), f32),
            pltpu.VMEM((24, LANES), f32),
            pltpu.VMEM((16, LANES), f32),
            pltpu.VMEM((16, LANES), f32),
            pltpu.VMEM((8 * STAT, 1, LANES), f32),
            pltpu.VMEM((16 * STAT, 1, LANES), f32),
            pltpu.VMEM((8 * STAT, 1, LANES), f32),
            pltpu.VMEM((16 * STAT, 1, LANES), f32),
            dma((4,)),
            dma, dma((2, 3)), dma((3, 3)), dma, dma((3,)), dma, dma((2,)), dma, dma((4,)),
        ],
        compiler_params=pltpu.CompilerParams(vmem_limit_bytes=40 * 2 ** 20, has_side_effects=True, collective_id=0),
    )(*(pltpu.with_memory_space_constraint(x, pltpu.HBM) for x in (q, w_cols.T, hid, draft_tok.T)))
    res, bonus, acc, expected = pl.pallas_call(
        finish_kernel,
        out_shape=[
            jax.ShapeDtypeStruct((SHARD * BT * DRAFT, 1, LANES), f32),
            jax.ShapeDtypeStruct((SHARD, BATCH), f32),
            jax.ShapeDtypeStruct((DRAFT, BATCH), f32),
            jax.ShapeDtypeStruct((BATCH,), f32),
        ],
        in_specs=[vmem] * 3,
        out_specs=[hbm, hbm, vmem, vmem],
        scratch_shapes=[
            pltpu.VMEM((SHARD * BT * DRAFT, 1, LANES), f32),
            pltpu.VMEM((SHARD, BATCH), f32),
            dma,
        ],
        compiler_params=pltpu.CompilerParams(vmem_limit_bytes=12 * 2 ** 20),
    )(ex, bo, st)
    res = with_layout_constraint(res.reshape(SHARD, BT, DRAFT, LANES).transpose(0, 2, 1, 3), Layout((0, 2, 1, 3)))
    residual = res.reshape(SHARD, DRAFT, BATCH).transpose(2, 1, 0)
    return acc.T, expected, residual, bonus.T


def solution(mesh):
    return jax.shard_map(
        verify_local,
        mesh=mesh,
        in_specs=(P(('dp', 'tp'), None, None), P(None, 'tp'), P(('dp', 'tp'), None, None), P('dp', None)),
        out_specs=(P('dp', None), P('dp'), P('dp', None, 'tp'), P('dp', 'tp')),
        check_vma=False,
    )
```

```python
import functools

import jax
import jax.numpy as jnp
from jax import lax
from jax.experimental import pallas as pl
from jax.experimental.layout import Layout, with_layout_constraint
from jax.experimental.pallas import tpu as pltpu
from jax.sharding import PartitionSpec as P

INV_TEMP = 1.25
DEV = 128
SEQ = 3
NPOS = 3
DRAFT = 2
BATCH = 384
DIM = 2048
VOCAB = 128256
SHARD = VOCAB // DEV
LANES = 128
TILES = VOCAB // LANES
CHUNKS = 8
TAIL = SHARD - (CHUNKS - 1) * LANES
ROWS_P = 1008
TAIL_P = ROWS_P - (CHUNKS - 1) * LANES
KC = DIM // LANES
HROWS = SEQ * NPOS * KC
COLS = NPOS * BATCH
COLS_P = 1280
CT = COLS // LANES
BT = BATCH // LANES
BLK = SEQ * CHUNKS
PITCH = 49
NEG = -1e30
STAT = 18
MESH = pl.DeviceIdType.MESH


def remote(src, dst, ssem, rsem, dev):
    return pltpu.make_async_remote_copy(
        src_ref=src, dst_ref=dst, send_sem=ssem, recv_sem=rsem,
        device_id={'tp': dev}, device_id_type=MESH)


def reduce_stage(buf, slot, count, ssem, rsem, device, payload):
    buf.reshape(count * STAT, LANES)[pl.ds(slot * STAT, STAT), :] = payload
    here = buf.at[pl.ds(slot * STAT, STAT)]
    for r in range(1, count):
        remote(here, here, ssem, rsem, device((slot + r) % count)).start()


def wait_rows(ref, rows, sem):
    part = ref.at[pl.ds(0, rows)]
    pltpu.make_async_copy(part, part, sem).wait()


def finish(buf, count, rsem):
    wait_rows(buf, (count - 1) * STAT, rsem)
    rows = buf.reshape(count * STAT, LANES)
    return [rows[k * STAT:(k + 1) * STAT, :] for k in range(count)]


def merge_max_sum(parts):
    m = parts[0][0:CT]
    for p in parts[1:]:
        m = jnp.maximum(m, p[0:CT])
    s = parts[0][CT:2 * CT] * jnp.exp(parts[0][0:CT] - m)
    for p in parts[1:]:
        s = s + p[CT:2 * CT] * jnp.exp(p[0:CT] - m)
    return jnp.concatenate([m, s], axis=0)


def merge_add(parts):
    total = parts[0]
    for p in parts[1:]:
        total = total + p
    return total


def kernel(q_hbm, w_hbm, h_hbm, tok_hbm,
           ex_hbm, bo_hbm, out_ref,
           tok_ref, qbuf, wbuf, hloc, hidb, bounce, hmat, z, send, recv, exbuf, stat, peak, scale,
           a1, b1, a2, b2,
           lsem, ag_s, ag_r, ag_r2, d2d_s, d2d_r, qs, qr_sem, rs, rr):
    scope = jax.named_scope
    me = lax.axis_index('tp')
    core = me % 2
    coord = (me // 32, (me // 8) % 4, (me // 2) % 4)
    unit = (32, 8, 2)
    partner = me + 1 - 2 * core
    hop = [[((coord[d] + r) % 4) * unit[d] for r in range(4)] for d in range(3)]

    def device(rz, ry, rx, rc):
        return hop[0][rz] + hop[1][ry] + hop[2][rx] + (core if rc == 0 else 1 - core)

    hcp = pltpu.make_async_copy(h_hbm, hloc, lsem.at[2])
    hcp.start()
    qcp = pltpu.make_async_copy(q_hbm, qbuf.at[pl.ds(0, SEQ * TILES * DRAFT)], lsem.at[0])
    qcp.start()
    wcp = pltpu.make_async_copy(w_hbm, wbuf, lsem.at[1])
    wcp.start()
    tcp = pltpu.make_async_copy(tok_hbm, tok_ref, lsem.at[3])
    tcp.start()
    barrier = pltpu.get_barrier_semaphore()
    peers = [partner]
    for d in range(3):
        for r in range(1, 4):
            steps = [0, 0, 0]
            steps[d] = r
            peers.append(device(*steps, 0))
    for dev in peers:
        pl.semaphore_signal(barrier, inc=1, device_id={'tp': dev}, device_id_type=MESH)

    with scope('hid'):
        hcp.wait()
        for s in range(SEQ):
            x = hloc[s].astype(jnp.float32)
            for kc in range(KC):
                bounce[pl.ds(s * 48 + kc, NPOS, stride=KC), :] = x[:, kc * LANES:(kc + 1) * LANES]
        hidb[pl.ds(pl.multiple_of(me * HROWS, 16), HROWS), :] = bounce[0:HROWS, :].astype(jnp.bfloat16)
    with scope('barrier'):
        pl.semaphore_wait(barrier, len(peers))

    hview = hidb.reshape(4, 4, 4, 2, SEQ, HROWS // SEQ, LANES)

    def ag_phase(phase):
        for j in range(3):
            order = [(j + k) % 3 for k in range(3)]
            idx = list(coord)
            for d in order[:phase]:
                idx[d] = slice(None)
            view = hview.at[idx[0], idx[1], idx[2], core, j]
            for r in (1, 3, 2):
                steps = [0, 0, 0]
                steps[order[phase]] = r
                remote(view, view, ag_s, ag_r.at[phase, j], device(*steps, 0)).start()

    def ag_wait(phase, j):
        wait_rows(hidb, 3 * 4 ** phase * (HROWS // SEQ), ag_r.at[phase, j])

    def half(j, off, part):
        order = [(j + k) % 3 for k in range(3)]
        idx = [slice(None)] * 3
        idx[order[2]] = (coord[order[2]] + off) % 4
        idx[order[0]] = slice(2 * part, 2 * part + 2)
        return hview.at[idx[0], idx[1], idx[2], core, j]

    def ag_half(j, off, part, sem, r):
        steps = [0, 0, 0]
        steps[(j + 2) % 3] = r
        view = half(j, off, part)
        remote(view, view, ag_s, ag_r2.at[j, sem], device(*steps, 0)).start()

    HALF = 8 * HROWS // SEQ
    qrows = qbuf.reshape(qbuf.shape[0], LANES)
    lane = lax.broadcasted_iota(jnp.int32, (8, LANES), 1)

    def pack(i, k, carry):
        first = (SHARD * k) // LANES
        off = (SHARD * k) % LANES
        shift = (LANES - off) % LANES
        keep = lane < LANES - off
        for s in range(SEQ):
            base = (s * TILES + first) * DRAFT + i
            lo = qrows[pl.ds(base, 8, stride=2), :]
            hi = qrows[pl.ds(base + 2, 8, stride=2), :]
            lo = pltpu.roll(lo, shift, 1)
            hi = pltpu.roll(hi, shift, 1)
            send[i, pl.ds(pl.multiple_of(k * BLK + s * 8, 8), 8), :] = jnp.where(keep, lo, hi)
        return carry

    mine = pl.ds(pl.multiple_of(me * BLK, 8), BLK)

    def to(i, dev):
        remote(send.at[i, pl.ds(pl.multiple_of(dev * BLK, 8), BLK)], recv.at[i, mine],
               qs, qr_sem.at[i], dev).start()

    def step(d, n):
        return ((coord[d] + n) % 4) * unit[d]

    def class0(i):
        pltpu.make_async_copy(send.at[i, mine], recv.at[i, mine], qr_sem.at[i]).start()
        to(i, partner)

    def class1(i, rc):
        last = core if rc == 0 else 1 - core
        for r in (1, 3, 2):
            for d in range(3):
                steps = [0, 0, 0]
                steps[d] = r
                to(i, device(*steps, rc))

    def class2(i, rc, lo=0, hi=9):
        last = core if rc == 0 else 1 - core

        def body(n, carry):
            a, b = n // 3 + 1, n % 3 + 1
            to(i, step(0, a) + step(1, b) + hop[2][0] + last)
            to(i, hop[0][0] + step(1, a) + step(2, b) + last)
            to(i, step(0, b) + hop[1][0] + step(2, a) + last)
            return carry

        lax.fori_loop(lo, hi, body, 0)

    def class3(i, rc, lo=0, hi=9):
        last = core if rc == 0 else 1 - core

        def body(n, carry):
            a, b = n // 3, n % 3
            for k in range(3):
                to(i, step(0, (a + k) % 3 + 1) + step(1, (b + k) % 3 + 1) + hop[2][k + 1] + last)
            return carry

        lax.fori_loop(lo, hi, body, 0)

    ag_phase(0)
    with scope('qwait'):
        qcp.wait()
    with scope('pack'):
        lax.fori_loop(0, DEV, functools.partial(pack, 0), 0, unroll=16)
    with scope('ex0'):
        class0(0)
        class1(0, 0)
    with scope('ag0'):
        for j in range(3):
            ag_wait(0, j)
    ag_phase(1)
    with scope('ex0a'):
        class1(0, 1)
        class2(0, 0)
    with scope('pack2'):
        lax.fori_loop(0, DEV, functools.partial(pack, 1), 0, unroll=16)
    with scope('ag1'):
        for j in range(3):
            ag_wait(1, j)
    for j in range(3):
        ag_half(j, 0, 0, 0, 1)
        ag_half(j, 0, 1, 1, 3)
    for j in range(3):
        ag_half(j, 0, 1, 2, 1)
        ag_half(j, 0, 0, 2, 3)
    with scope('relay'):
        for j in range(3):
            wait_rows(hidb, HALF, ag_r2.at[j, 0])
            ag_half(j, 3, 0, 2, 1)
            wait_rows(hidb, HALF, ag_r2.at[j, 1])
            ag_half(j, 1, 1, 2, 3)
    with scope('exag2'):
        class0(1)
        class1(1, 0)
        class1(1, 1)
        class2(0, 1)
    d2d = []
    for j in (2, 1, 0):
        with scope(f'ag2_{j}'):
            wait_rows(hidb, 4 * HALF, ag_r2.at[j, 2])
        view = hview.at[:, :, :, core, j]
        cp = remote(view, view, d2d_s, d2d_r.at[j], partner)
        cp.start()
        d2d.append(cp)
    with scope('ex0b'):
        class3(0, 0)
        class3(0, 1)
        class3(1, 0)
    with scope('d2d'):
        for cp in d2d:
            cp.wait_recv()

    def relayout(n, carry):
        def up(b, c):
            x = hidb[pl.ds(pl.multiple_of((48 * n + b) * 48, 16), 48), :]
            bounce[pl.ds(b * PITCH, 48), :] = x.astype(jnp.float32)
            return c

        lax.fori_loop(0, 48, up, 0, unroll=4)
        for g in range(NPOS):
            for u in range(3):
                for kc in range(KC):
                    y = bounce[pl.ds(16 * u * PITCH + g * KC + kc, 16, stride=PITCH), :]
                    hmat[pl.ds(pl.multiple_of(g * BATCH + 48 * n + 16 * u, 16), 16),
                         kc * LANES:(kc + 1) * LANES] = y.astype(jnp.bfloat16)
        return carry

    with scope('relayout'):
        lax.fori_loop(0, 8, relayout, 0)
    wcp.wait()
    tcp.wait()

    z[SHARD:ROWS_P, :] = jnp.full((ROWS_P - SHARD, COLS_P), NEG, jnp.float32)

    def head(n, carry):
        hb = hmat[pl.ds(pl.multiple_of(n * 256, 256), 256), :]
        zt = lax.dot_general(wbuf[...], hb, (((1,), (1,)), ((), ())), preferred_element_type=jnp.float32)
        zt = zt * INV_TEMP
        z[0:SHARD, pl.ds(pl.multiple_of(n * 256, 256), 256)] = zt
        top = jnp.max(zt, axis=0, keepdims=True)
        peak[pl.ds(2 * n, 1), :] = top[:, 0:LANES]
        peak[pl.ds(2 * n + 1, 1), :] = top[:, LANES:]
        return carry

    with scope('head'):
        lax.fori_loop(0, COLS_P // 256, head, 0)

    def local_stats(t, carry):
        cols = pl.ds(pl.multiple_of(t * LANES, LANES), LANES)

        m = peak[pl.ds(t, 1), :]

        def expo(n, s):
            rows = pl.ds(pl.multiple_of(n * 112, 8), 112)
            x = jnp.exp(z[rows, cols] - m)
            z[rows, cols] = x
            return s + jnp.sum(x.reshape(14, 8, LANES), axis=0)

        s8 = lax.fori_loop(0, 9, expo, jnp.zeros((8, LANES), jnp.float32), unroll=3)
        stat[pl.ds(t, 1), :] = m
        stat[pl.ds(CT + t, 1), :] = jnp.sum(s8, axis=0, keepdims=True)
        return carry

    stat[...] = jnp.zeros_like(stat)
    with scope('stats'):
        lax.fori_loop(0, CT, local_stats, 0)
    bcp = pltpu.make_async_copy(z.at[:, DRAFT * BATCH:COLS], bo_hbm, lsem.at[2])
    bcp.start()

    slot, grp = me % 8, me // 8
    near = lambda k: grp * 8 + k
    far = lambda k: k * 8 + slot
    local = stat[0:STAT, :]
    reduce_stage(a1, slot, 8, rs, rr.at[0], near, local)
    with scope('ex1a'):
        class3(1, 1, 0, 8)
    with scope('round1a'):
        parts = finish(a1, 8, rr.at[0])
    reduce_stage(b1, grp, 16, rs, rr.at[1], far, merge_max_sum(parts))
    with scope('ex1b'):
        class3(1, 1, 8, 9)
        class2(1, 1)
        class2(1, 0)
    with scope('round1b'):
        parts = finish(b1, 16, rr.at[1])
    tot = merge_max_sum(parts)
    fac = jnp.exp(local[0:CT] - tot[0:CT]) / tot[CT:2 * CT]
    scale[0:CT, :] = fac
    out_ref[12:16, :] = jnp.concatenate([fac[DRAFT * BT:CT], fac[0:1]], axis=0)

    exrows = exbuf.reshape(exbuf.shape[0], LANES)
    first_id = me * SHARD
    stat[...] = jnp.zeros_like(stat)
    for i in range(DRAFT):
        with scope(f'a2a_{i}'):
            pltpu.make_async_copy(recv.at[i], recv.at[i], qr_sem.at[i]).wait()
        for t in range(BT):
            row = i * BT + t
            sc = scale[row:row + 1, :]
            tok = tok_ref[i:i + 1, t * LANES:(t + 1) * LANES] - first_id
            col0 = i * BATCH + t * LANES

            def block(c, carry, size, valid):
                mass, pp, qp = carry
                q = recv[i, pl.ds(t * LANES * CHUNKS + c, LANES, stride=CHUNKS), :].T
                p = z[pl.ds(pl.multiple_of(c * LANES, LANES), size), col0:col0 + LANES] * sc
                ids = lax.broadcasted_iota(jnp.int32, (size, LANES), 0)
                q = q[0:size]
                if valid < size:
                    q = jnp.where(ids < valid, q, 0.0)
                x = jnp.maximum(p - q, 0.0)
                exrows[pl.ds(c * LANES * 6 + t * 2 + i, valid, stride=6), :] = x[0:valid]
                hit = ids == tok - c * LANES
                fold = lambda v: jnp.sum(v.reshape(size // 8, 8, LANES), axis=0)
                return (mass + fold(x), pp + fold(jnp.where(hit, p, 0.0)), qp + fold(jnp.where(hit, q, 0.0)))

            zero = jnp.zeros((8, LANES), jnp.float32)
            carry = lax.fori_loop(0, CHUNKS - 1, lambda c, v: block(c, v, LANES, LANES), (zero, zero, zero),
                                  unroll=CHUNKS - 1)
            mass, pp, qp = block(CHUNKS - 1, carry, TAIL_P, TAIL)
            stat[row:row + 1, :] = jnp.sum(mass, axis=0, keepdims=True)
            stat[6 + row:7 + row, :] = jnp.sum(pp, axis=0, keepdims=True)
            stat[12 + row:13 + row, :] = jnp.sum(qp, axis=0, keepdims=True)

    ecp = pltpu.make_async_copy(exbuf, ex_hbm, lsem.at[0])
    ecp.start()
    reduce_stage(a2, slot, 8, rs, rr.at[2], near, stat[0:STAT, :])
    with scope('round2a'):
        parts = finish(a2, 8, rr.at[2])
    reduce_stage(b2, grp, 16, rs, rr.at[3], far, merge_add(parts))
    with scope('round2b'):
        parts = finish(b2, 16, rr.at[3])
    tot = merge_add(parts)
    out_ref[0:6, :] = tot[0:6]
    out_ref[6:12, :] = jnp.minimum(tot[6:12] / tot[12:18], 1.0)
    with scope('tail'):
        ecp.wait()
        bcp.wait()
        wait_rows(hidb, 9 * 21 * (HROWS // SEQ), ag_s)
        wait_rows(hidb, DEV // 2 * HROWS, d2d_s)
        wait_rows(send.reshape(DRAFT * DEV * BLK, LANES), DRAFT * (DEV - 1) * BLK, qs)
        wait_rows(qbuf, 2 * (7 + 15) * STAT, rs)


def finish_kernel(ex_ref, bo_ref, stat_ref, res_hbm, bonus_hbm, acc_ref, exp_ref, res, bonus, sems):
    rows = ex_ref.reshape(ex_ref.shape[0], LANES)
    out = res.reshape(res.shape[0], LANES)
    copies = []
    fac = jnp.concatenate([stat_ref[12 + t:13 + t, :] for t in range(BT)], axis=1)
    step = 256
    for n in range(4):
        size = min(step, SHARD - n * step)
        bonus[n * step:n * step + size, :] = bo_ref[n * step:n * step + size, :] * fac
    cp = pltpu.make_async_copy(bonus, bonus_hbm, sems)
    cp.start()
    copies.append(cp)
    mass = jnp.concatenate([stat_ref[i * BT + t:i * BT + t + 1, :] for t in range(BT) for i in range(DRAFT)], axis=0)
    mass = jnp.concatenate([mass] * 4, axis=0)
    for n in range(5):
        def body(k, carry):
            at = pl.ds(pl.multiple_of(n * 1200 + k * 24, 8), 24)
            out[at, :] = rows[at, :] / mass
            return carry

        lax.fori_loop(0, 50, body, 0, unroll=5)
        size = 1200
        if n == 4:
            out[6000:6012, :] = rows[6000:6012, :] / mass[0:12]
            size = 1212
        cp = pltpu.make_async_copy(res.at[pl.ds(n * 1200, size)], res_hbm.at[pl.ds(n * 1200, size)], sems)
        cp.start()
        copies.append(cp)
    acc = stat_ref[6:12, :]
    more = acc[0:BT] * (1.0 + acc[BT:2 * BT])
    for t in range(BT):
        cols = slice(t * LANES, (t + 1) * LANES)
        exp_ref[cols] = more[t]
        for i in range(DRAFT):
            acc_ref[i:i + 1, cols] = acc[i * BT + t:i * BT + t + 1]
    for cp in copies:
        cp.wait()


def verify_local(hid, w_cols, q_rows, draft_tok):
    q = with_layout_constraint(q_rows.reshape(SEQ, DRAFT, TILES, LANES), Layout((0, 2, 1, 3)))
    q = q.transpose(0, 2, 1, 3).reshape(SEQ * TILES * DRAFT, 1, LANES)
    f32 = jnp.float32
    hbm = pl.BlockSpec(memory_space=pl.ANY)
    vmem = pl.BlockSpec(memory_space=pltpu.VMEM)
    dma = pltpu.SemaphoreType.DMA
    ex, bo, st = pl.pallas_call(
        kernel,
        out_shape=[
            jax.ShapeDtypeStruct((SHARD * BT * DRAFT, 1, LANES), f32),
            jax.ShapeDtypeStruct((ROWS_P, BATCH), f32),
            jax.ShapeDtypeStruct((16, LANES), f32),
        ],
        in_specs=[pl.BlockSpec(memory_space=pltpu.HBM)] * 4,
        out_specs=[hbm, hbm, vmem],
        scratch_shapes=[
            pltpu.VMEM((DRAFT, BATCH), jnp.int32),
            pltpu.VMEM((SEQ * TILES * DRAFT + 20, 1, LANES), f32),
            pltpu.VMEM((SHARD, DIM), jnp.bfloat16),
            pltpu.VMEM((SEQ, NPOS, DIM), jnp.bfloat16),
            pltpu.VMEM((DEV * HROWS, LANES), jnp.bfloat16),
            pltpu.VMEM((48 * PITCH, LANES), f32),
            pltpu.VMEM((COLS_P, DIM), jnp.bfloat16),
            pltpu.VMEM((ROWS_P, COLS_P), f32),
            pltpu.VMEM((DRAFT, DEV * BLK, LANES), f32),
            pltpu.VMEM((DRAFT, DEV * BLK, LANES), f32),
            pltpu.VMEM((SHARD * BT * DRAFT, 1, LANES), f32),
            pltpu.VMEM((24, LANES), f32),
            pltpu.VMEM((16, LANES), f32),
            pltpu.VMEM((16, LANES), f32),
            pltpu.VMEM((8 * STAT, 1, LANES), f32),
            pltpu.VMEM((16 * STAT, 1, LANES), f32),
            pltpu.VMEM((8 * STAT, 1, LANES), f32),
            pltpu.VMEM((16 * STAT, 1, LANES), f32),
            dma((4,)),
            dma, dma((2, 3)), dma((3, 3)), dma, dma((3,)), dma, dma((2,)), dma, dma((4,)),
        ],
        compiler_params=pltpu.CompilerParams(vmem_limit_bytes=40 * 2 ** 20, has_side_effects=True, collective_id=0),
    )(*(pltpu.with_memory_space_constraint(x, pltpu.HBM) for x in (q, w_cols.T, hid, draft_tok.T)))
    res, bonus, acc, expected = pl.pallas_call(
        finish_kernel,
        out_shape=[
            jax.ShapeDtypeStruct((SHARD * BT * DRAFT, 1, LANES), f32),
            jax.ShapeDtypeStruct((SHARD, BATCH), f32),
            jax.ShapeDtypeStruct((DRAFT, BATCH), f32),
            jax.ShapeDtypeStruct((BATCH,), f32),
        ],
        in_specs=[vmem] * 3,
        out_specs=[hbm, hbm, vmem, vmem],
        scratch_shapes=[
            pltpu.VMEM((SHARD * BT * DRAFT, 1, LANES), f32),
            pltpu.VMEM((SHARD, BATCH), f32),
            dma,
        ],
        compiler_params=pltpu.CompilerParams(vmem_limit_bytes=12 * 2 ** 20),
    )(ex, bo, st)
    res = with_layout_constraint(res.reshape(SHARD, BT, DRAFT, LANES).transpose(0, 2, 1, 3), Layout((0, 2, 1, 3)))
    residual = res.reshape(SHARD, DRAFT, BATCH).transpose(2, 1, 0)
    return acc.T, expected, residual, bonus.T


def solution(mesh):
    return jax.shard_map(
        verify_local,
        mesh=mesh,
        in_specs=(P(('dp', 'tp'), None, None), P(None, 'tp'), P(('dp', 'tp'), None, None), P('dp', None)),
        out_specs=(P('dp', None), P('dp'), P('dp', None, 'tp'), P('dp', 'tp')),
        check_vma=False,
    )
```

```python
import functools

import jax
import jax.numpy as jnp
from jax import lax
from jax.experimental import pallas as pl
from jax.experimental.layout import Layout, with_layout_constraint
from jax.experimental.pallas import tpu as pltpu
from jax.sharding import PartitionSpec as P

INV_TEMP = 1.25
DEV = 128
SEQ = 3
NPOS = 3
DRAFT = 2
BATCH = 384
DIM = 2048
VOCAB = 128256
SHARD = VOCAB // DEV
LANES = 128
TILES = VOCAB // LANES
CHUNKS = 8
TAIL = SHARD - (CHUNKS - 1) * LANES
ROWS_P = 1008
TAIL_P = ROWS_P - (CHUNKS - 1) * LANES
KC = DIM // LANES
HROWS = SEQ * NPOS * KC
COLS = NPOS * BATCH
COLS_P = 1280
CT = COLS // LANES
BT = BATCH // LANES
BLK = SEQ * CHUNKS
PITCH = 49
NEG = -1e30
STAT = 18
MESH = pl.DeviceIdType.MESH


def remote(src, dst, ssem, rsem, dev):
    return pltpu.make_async_remote_copy(
        src_ref=src, dst_ref=dst, send_sem=ssem, recv_sem=rsem,
        device_id={'tp': dev}, device_id_type=MESH)


def reduce_stage(buf, slot, count, ssem, rsem, device, payload):
    buf.reshape(count * STAT, LANES)[pl.ds(slot * STAT, STAT), :] = payload
    here = buf.at[pl.ds(slot * STAT, STAT)]
    for r in range(1, count):
        remote(here, here, ssem, rsem, device((slot + r) % count)).start()


def wait_rows(ref, rows, sem):
    part = ref.at[pl.ds(0, rows)]
    pltpu.make_async_copy(part, part, sem).wait()


def finish(buf, count, rsem):
    wait_rows(buf, (count - 1) * STAT, rsem)
    rows = buf.reshape(count * STAT, LANES)
    return [rows[k * STAT:(k + 1) * STAT, :] for k in range(count)]


def merge_max_sum(parts):
    m = parts[0][0:CT]
    for p in parts[1:]:
        m = jnp.maximum(m, p[0:CT])
    s = parts[0][CT:2 * CT] * jnp.exp(parts[0][0:CT] - m)
    for p in parts[1:]:
        s = s + p[CT:2 * CT] * jnp.exp(p[0:CT] - m)
    return jnp.concatenate([m, s], axis=0)


def merge_add(parts):
    total = parts[0]
    for p in parts[1:]:
        total = total + p
    return total


def kernel(q_hbm, w_hbm, h_hbm, tok_hbm,
           ex_hbm, bo_hbm, out_ref,
           tok_ref, qbuf, wbuf, hloc, hidb, bounce, hmat, z, send, recv, exbuf, stat, peak, scale,
           a1, b1, a2, b2,
           lsem, ag_s, ag_r, ag_r2, d2d_s, d2d_r, qs, qr_sem, rs, rr):
    scope = jax.named_scope
    me = lax.axis_index('tp')
    core = me % 2
    coord = (me // 32, (me // 8) % 4, (me // 2) % 4)
    unit = (32, 8, 2)
    partner = me + 1 - 2 * core
    hop = [[((coord[d] + r) % 4) * unit[d] for r in range(4)] for d in range(3)]

    def device(rz, ry, rx, rc):
        return hop[0][rz] + hop[1][ry] + hop[2][rx] + (core if rc == 0 else 1 - core)

    hcp = pltpu.make_async_copy(h_hbm, hloc, lsem.at[2])
    hcp.start()
    qcp = pltpu.make_async_copy(q_hbm, qbuf.at[pl.ds(0, SEQ * TILES * DRAFT)], lsem.at[0])
    qcp.start()
    wcp = pltpu.make_async_copy(w_hbm, wbuf, lsem.at[1])
    wcp.start()
    tcp = pltpu.make_async_copy(tok_hbm, tok_ref, lsem.at[3])
    tcp.start()
    barrier = pltpu.get_barrier_semaphore()
    peers = [partner]
    for d in range(3):
        for r in range(1, 4):
            steps = [0, 0, 0]
            steps[d] = r
            peers.append(device(*steps, 0))
    for dev in peers:
        pl.semaphore_signal(barrier, inc=1, device_id={'tp': dev}, device_id_type=MESH)

    with scope('hid'):
        hcp.wait()
        for s in range(SEQ):
            x = hloc[s].astype(jnp.float32)
            for kc in range(KC):
                bounce[pl.ds(s * 48 + kc, NPOS, stride=KC), :] = x[:, kc * LANES:(kc + 1) * LANES]
        hidb[pl.ds(pl.multiple_of(me * HROWS, 16), HROWS), :] = bounce[0:HROWS, :].astype(jnp.bfloat16)
    with scope('barrier'):
        pl.semaphore_wait(barrier, len(peers))

    hview = hidb.reshape(4, 4, 4, 2, SEQ, HROWS // SEQ, LANES)

    def ag_phase(phase):
        for j in range(3):
            order = [(j + k) % 3 for k in range(3)]
            idx = list(coord)
            for d in order[:phase]:
                idx[d] = slice(None)
            view = hview.at[idx[0], idx[1], idx[2], core, j]
            for r in (1, 3, 2):
                steps = [0, 0, 0]
                steps[order[phase]] = r
                remote(view, view, ag_s, ag_r.at[phase, j], device(*steps, 0)).start()

    def ag_wait(phase, j):
        wait_rows(hidb, 3 * 4 ** phase * (HROWS // SEQ), ag_r.at[phase, j])

    def half(j, off, part):
        order = [(j + k) % 3 for k in range(3)]
        idx = [slice(None)] * 3
        idx[order[2]] = (coord[order[2]] + off) % 4
        idx[order[0]] = slice(2 * part, 2 * part + 2)
        return hview.at[idx[0], idx[1], idx[2], core, j]

    def ag_half(j, off, part, sem, r):
        steps = [0, 0, 0]
        steps[(j + 2) % 3] = r
        view = half(j, off, part)
        remote(view, view, ag_s, ag_r2.at[j, sem], device(*steps, 0)).start()

    HALF = 8 * HROWS // SEQ
    qrows = qbuf.reshape(qbuf.shape[0], LANES)
    lane = lax.broadcasted_iota(jnp.int32, (8, LANES), 1)

    def pack(i, k, carry):
        first = (SHARD * k) // LANES
        off = (SHARD * k) % LANES
        shift = (LANES - off) % LANES
        keep = lane < LANES - off
        for s in range(SEQ):
            base = (s * TILES + first) * DRAFT + i
            lo = qrows[pl.ds(base, 8, stride=2), :]
            hi = qrows[pl.ds(base + 2, 8, stride=2), :]
            lo = pltpu.roll(lo, shift, 1)
            hi = pltpu.roll(hi, shift, 1)
            send[i, pl.ds(pl.multiple_of(k * BLK + s * 8, 8), 8), :] = jnp.where(keep, lo, hi)
        return carry

    mine = pl.ds(pl.multiple_of(me * BLK, 8), BLK)

    def to(i, dev):
        remote(send.at[i, pl.ds(pl.multiple_of(dev * BLK, 8), BLK)], recv.at[i, mine],
               qs, qr_sem.at[i], dev).start()

    def step(d, n):
        return ((coord[d] + n) % 4) * unit[d]

    def class0(i):
        pltpu.make_async_copy(send.at[i, mine], recv.at[i, mine], qr_sem.at[i]).start()
        to(i, partner)

    def class1(i, rc):
        last = core if rc == 0 else 1 - core
        for r in (1, 3, 2):
            for d in range(3):
                steps = [0, 0, 0]
                steps[d] = r
                to(i, device(*steps, rc))

    def class2(i, rc, lo=0, hi=9):
        last = core if rc == 0 else 1 - core

        def body(n, carry):
            a, b = n // 3 + 1, n % 3 + 1
            to(i, step(0, a) + step(1, b) + hop[2][0] + last)
            to(i, hop[0][0] + step(1, a) + step(2, b) + last)
            to(i, step(0, b) + hop[1][0] + step(2, a) + last)
            return carry

        lax.fori_loop(lo, hi, body, 0)

    def class3(i, rc, lo=0, hi=9):
        last = core if rc == 0 else 1 - core

        def body(n, carry):
            a, b = n // 3, n % 3
            for k in range(3):
                to(i, step(0, (a + k) % 3 + 1) + step(1, (b + k) % 3 + 1) + hop[2][k + 1] + last)
            return carry

        lax.fori_loop(lo, hi, body, 0)

    ag_phase(0)
    with scope('qwait'):
        qcp.wait()
    with scope('pack'):
        lax.fori_loop(0, DEV, functools.partial(pack, 0), 0, unroll=16)
    with scope('ex0'):
        class0(0)
        class1(0, 0)
    with scope('ag0'):
        for j in range(3):
            ag_wait(0, j)
    ag_phase(1)
    with scope('ex0a'):
        class1(0, 1)
        class2(0, 0)
    with scope('pack2'):
        lax.fori_loop(0, DEV, functools.partial(pack, 1), 0, unroll=16)
    with scope('ag1'):
        for j in range(3):
            ag_wait(1, j)
    for j in range(3):
        ag_half(j, 0, 0, 0, 1)
        ag_half(j, 0, 1, 1, 3)
    for j in range(3):
        ag_half(j, 0, 1, 2, 1)
        ag_half(j, 0, 0, 2, 3)
    with scope('relay'):
        for j in range(3):
            wait_rows(hidb, HALF, ag_r2.at[j, 0])
            ag_half(j, 3, 0, 2, 1)
            wait_rows(hidb, HALF, ag_r2.at[j, 1])
            ag_half(j, 1, 1, 2, 3)
    with scope('exag2'):
        class0(1)
        class1(1, 0)
        class1(1, 1)
        class2(0, 1)
        class3(0, 0, 0, 5)
    d2d = []
    for j in (2, 1, 0):
        with scope(f'ag2_{j}'):
            wait_rows(hidb, 4 * HALF, ag_r2.at[j, 2])
        view = hview.at[:, :, :, core, j]
        cp = remote(view, view, d2d_s, d2d_r.at[j], partner)
        cp.start()
        d2d.append(cp)
    with scope('ex0b'):
        class3(0, 0, 5, 9)
        class3(0, 1)
        class3(1, 0)
        class3(1, 1, 0, 4)
    with scope('d2d'):
        for cp in d2d:
            cp.wait_recv()

    def relayout(n, carry):
        def up(b, c):
            x = hidb[pl.ds(pl.multiple_of((48 * n + b) * 48, 16), 48), :]
            bounce[pl.ds(b * PITCH, 48), :] = x.astype(jnp.float32)
            return c

        lax.fori_loop(0, 48, up, 0, unroll=4)
        for g in range(NPOS):
            for u in range(3):
                for kc in range(KC):
                    y = bounce[pl.ds(16 * u * PITCH + g * KC + kc, 16, stride=PITCH), :]
                    hmat[pl.ds(pl.multiple_of(g * BATCH + 48 * n + 16 * u, 16), 16),
                         kc * LANES:(kc + 1) * LANES] = y.astype(jnp.bfloat16)
        return carry

    with scope('relayout'):
        lax.fori_loop(0, 8, relayout, 0)
    wcp.wait()
    tcp.wait()

    z[SHARD:ROWS_P, :] = jnp.full((ROWS_P - SHARD, COLS_P), NEG, jnp.float32)

    def head(n, carry):
        hb = hmat[pl.ds(pl.multiple_of(n * 256, 256), 256), :]
        zt = lax.dot_general(wbuf[...], hb, (((1,), (1,)), ((), ())), preferred_element_type=jnp.float32)
        zt = zt * INV_TEMP
        z[0:SHARD, pl.ds(pl.multiple_of(n * 256, 256), 256)] = zt
        top = jnp.max(zt, axis=0, keepdims=True)
        peak[pl.ds(2 * n, 1), :] = top[:, 0:LANES]
        peak[pl.ds(2 * n + 1, 1), :] = top[:, LANES:]
        return carry

    with scope('head'):
        lax.fori_loop(0, COLS_P // 256, head, 0)

    def local_stats(t, carry):
        cols = pl.ds(pl.multiple_of(t * LANES, LANES), LANES)

        m = peak[pl.ds(t, 1), :]

        def expo(n, s):
            rows = pl.ds(pl.multiple_of(n * 112, 8), 112)
            x = jnp.exp(z[rows, cols] - m)
            z[rows, cols] = x
            return s + jnp.sum(x.reshape(14, 8, LANES), axis=0)

        s8 = lax.fori_loop(0, 9, expo, jnp.zeros((8, LANES), jnp.float32), unroll=3)
        stat[pl.ds(t, 1), :] = m
        stat[pl.ds(CT + t, 1), :] = jnp.sum(s8, axis=0, keepdims=True)
        return carry

    stat[...] = jnp.zeros_like(stat)
    with scope('stats'):
        lax.fori_loop(0, CT, local_stats, 0)
    bcp = pltpu.make_async_copy(z.at[:, DRAFT * BATCH:COLS], bo_hbm, lsem.at[2])
    bcp.start()

    slot, grp = me % 8, me // 8
    near = lambda k: grp * 8 + k
    far = lambda k: k * 8 + slot
    local = stat[0:STAT, :]
    reduce_stage(a1, slot, 8, rs, rr.at[0], near, local)
    with scope('ex1a'):
        class3(1, 1, 4, 9)
        class2(1, 1, 0, 3)
    with scope('round1a'):
        parts = finish(a1, 8, rr.at[0])
    reduce_stage(b1, grp, 16, rs, rr.at[1], far, merge_max_sum(parts))
    with scope('ex1b'):
        class2(1, 1, 3, 9)
        class2(1, 0)
    with scope('round1b'):
        parts = finish(b1, 16, rr.at[1])
    tot = merge_max_sum(parts)
    fac = jnp.exp(local[0:CT] - tot[0:CT]) / tot[CT:2 * CT]
    scale[0:CT, :] = fac
    out_ref[12:16, :] = jnp.concatenate([fac[DRAFT * BT:CT], fac[0:1]], axis=0)

    exrows = exbuf.reshape(exbuf.shape[0], LANES)
    first_id = me * SHARD
    stat[...] = jnp.zeros_like(stat)
    for i in range(DRAFT):
        with scope(f'a2a_{i}'):
            pltpu.make_async_copy(recv.at[i], recv.at[i], qr_sem.at[i]).wait()
        for t in range(BT):
            row = i * BT + t
            sc = scale[row:row + 1, :]
            tok = tok_ref[i:i + 1, t * LANES:(t + 1) * LANES] - first_id
            col0 = i * BATCH + t * LANES

            def block(c, carry, size, valid):
                mass, pp, qp = carry
                q = recv[i, pl.ds(t * LANES * CHUNKS + c, LANES, stride=CHUNKS), :].T
                p = z[pl.ds(pl.multiple_of(c * LANES, LANES), size), col0:col0 + LANES] * sc
                ids = lax.broadcasted_iota(jnp.int32, (size, LANES), 0)
                q = q[0:size]
                if valid < size:
                    q = jnp.where(ids < valid, q, 0.0)
                x = jnp.maximum(p - q, 0.0)
                exrows[pl.ds(c * LANES * 6 + t * 2 + i, valid, stride=6), :] = x[0:valid]
                hit = ids == tok - c * LANES
                fold = lambda v: jnp.sum(v.reshape(size // 8, 8, LANES), axis=0)
                return (mass + fold(x), pp + fold(jnp.where(hit, p, 0.0)), qp + fold(jnp.where(hit, q, 0.0)))

            zero = jnp.zeros((8, LANES), jnp.float32)
            carry = lax.fori_loop(0, CHUNKS - 1, lambda c, v: block(c, v, LANES, LANES), (zero, zero, zero),
                                  unroll=CHUNKS - 1)
            mass, pp, qp = block(CHUNKS - 1, carry, TAIL_P, TAIL)
            stat[row:row + 1, :] = jnp.sum(mass, axis=0, keepdims=True)
            stat[6 + row:7 + row, :] = jnp.sum(pp, axis=0, keepdims=True)
            stat[12 + row:13 + row, :] = jnp.sum(qp, axis=0, keepdims=True)

    ecp = pltpu.make_async_copy(exbuf, ex_hbm, lsem.at[0])
    ecp.start()
    reduce_stage(a2, slot, 8, rs, rr.at[2], near, stat[0:STAT, :])
    with scope('round2a'):
        parts = finish(a2, 8, rr.at[2])
    reduce_stage(b2, grp, 16, rs, rr.at[3], far, merge_add(parts))
    with scope('round2b'):
        parts = finish(b2, 16, rr.at[3])
    tot = merge_add(parts)
    out_ref[0:6, :] = tot[0:6]
    out_ref[6:12, :] = jnp.minimum(tot[6:12] / tot[12:18], 1.0)
    with scope('tail'):
        ecp.wait()
        bcp.wait()
        wait_rows(hidb, 9 * 21 * (HROWS // SEQ), ag_s)
        wait_rows(hidb, DEV // 2 * HROWS, d2d_s)
        wait_rows(send.reshape(DRAFT * DEV * BLK, LANES), DRAFT * (DEV - 1) * BLK, qs)
        wait_rows(qbuf, 2 * (7 + 15) * STAT, rs)


def finish_kernel(ex_ref, bo_ref, stat_ref, res_hbm, bonus_hbm, acc_ref, exp_ref, res, bonus, sems):
    rows = ex_ref.reshape(ex_ref.shape[0], LANES)
    out = res.reshape(res.shape[0], LANES)
    copies = []
    fac = jnp.concatenate([stat_ref[12 + t:13 + t, :] for t in range(BT)], axis=1)
    step = 256
    for n in range(4):
        size = min(step, SHARD - n * step)
        bonus[n * step:n * step + size, :] = bo_ref[n * step:n * step + size, :] * fac
    cp = pltpu.make_async_copy(bonus, bonus_hbm, sems)
    cp.start()
    copies.append(cp)
    mass = jnp.concatenate([stat_ref[i * BT + t:i * BT + t + 1, :] for t in range(BT) for i in range(DRAFT)], axis=0)
    mass = jnp.concatenate([mass] * 4, axis=0)
    for n in range(5):
        def body(k, carry):
            at = pl.ds(pl.multiple_of(n * 1200 + k * 24, 8), 24)
            out[at, :] = rows[at, :] / mass
            return carry

        lax.fori_loop(0, 50, body, 0, unroll=5)
        size = 1200
        if n == 4:
            out[6000:6012, :] = rows[6000:6012, :] / mass[0:12]
            size = 1212
        cp = pltpu.make_async_copy(res.at[pl.ds(n * 1200, size)], res_hbm.at[pl.ds(n * 1200, size)], sems)
        cp.start()
        copies.append(cp)
    acc = stat_ref[6:12, :]
    more = acc[0:BT] * (1.0 + acc[BT:2 * BT])
    for t in range(BT):
        cols = slice(t * LANES, (t + 1) * LANES)
        exp_ref[cols] = more[t]
        for i in range(DRAFT):
            acc_ref[i:i + 1, cols] = acc[i * BT + t:i * BT + t + 1]
    for cp in copies:
        cp.wait()


def verify_local(hid, w_cols, q_rows, draft_tok):
    q = with_layout_constraint(q_rows.reshape(SEQ, DRAFT, TILES, LANES), Layout((0, 2, 1, 3)))
    q = q.transpose(0, 2, 1, 3).reshape(SEQ * TILES * DRAFT, 1, LANES)
    f32 = jnp.float32
    hbm = pl.BlockSpec(memory_space=pl.ANY)
    vmem = pl.BlockSpec(memory_space=pltpu.VMEM)
    dma = pltpu.SemaphoreType.DMA
    ex, bo, st = pl.pallas_call(
        kernel,
        out_shape=[
            jax.ShapeDtypeStruct((SHARD * BT * DRAFT, 1, LANES), f32),
            jax.ShapeDtypeStruct((ROWS_P, BATCH), f32),
            jax.ShapeDtypeStruct((16, LANES), f32),
        ],
        in_specs=[pl.BlockSpec(memory_space=pltpu.HBM)] * 4,
        out_specs=[hbm, hbm, vmem],
        scratch_shapes=[
            pltpu.VMEM((DRAFT, BATCH), jnp.int32),
            pltpu.VMEM((SEQ * TILES * DRAFT + 20, 1, LANES), f32),
            pltpu.VMEM((SHARD, DIM), jnp.bfloat16),
            pltpu.VMEM((SEQ, NPOS, DIM), jnp.bfloat16),
            pltpu.VMEM((DEV * HROWS, LANES), jnp.bfloat16),
            pltpu.VMEM((48 * PITCH, LANES), f32),
            pltpu.VMEM((COLS_P, DIM), jnp.bfloat16),
            pltpu.VMEM((ROWS_P, COLS_P), f32),
            pltpu.VMEM((DRAFT, DEV * BLK, LANES), f32),
            pltpu.VMEM((DRAFT, DEV * BLK, LANES), f32),
            pltpu.VMEM((SHARD * BT * DRAFT, 1, LANES), f32),
            pltpu.VMEM((24, LANES), f32),
            pltpu.VMEM((16, LANES), f32),
            pltpu.VMEM((16, LANES), f32),
            pltpu.VMEM((8 * STAT, 1, LANES), f32),
            pltpu.VMEM((16 * STAT, 1, LANES), f32),
            pltpu.VMEM((8 * STAT, 1, LANES), f32),
            pltpu.VMEM((16 * STAT, 1, LANES), f32),
            dma((4,)),
            dma, dma((2, 3)), dma((3, 3)), dma, dma((3,)), dma, dma((2,)), dma, dma((4,)),
        ],
        compiler_params=pltpu.CompilerParams(vmem_limit_bytes=40 * 2 ** 20, has_side_effects=True, collective_id=0),
    )(*(pltpu.with_memory_space_constraint(x, pltpu.HBM) for x in (q, w_cols.T, hid, draft_tok.T)))
    res, bonus, acc, expected = pl.pallas_call(
        finish_kernel,
        out_shape=[
            jax.ShapeDtypeStruct((SHARD * BT * DRAFT, 1, LANES), f32),
            jax.ShapeDtypeStruct((SHARD, BATCH), f32),
            jax.ShapeDtypeStruct((DRAFT, BATCH), f32),
            jax.ShapeDtypeStruct((BATCH,), f32),
        ],
        in_specs=[vmem] * 3,
        out_specs=[hbm, hbm, vmem, vmem],
        scratch_shapes=[
            pltpu.VMEM((SHARD * BT * DRAFT, 1, LANES), f32),
            pltpu.VMEM((SHARD, BATCH), f32),
            dma,
        ],
        compiler_params=pltpu.CompilerParams(vmem_limit_bytes=12 * 2 ** 20),
    )(ex, bo, st)
    res = with_layout_constraint(res.reshape(SHARD, BT, DRAFT, LANES).transpose(0, 2, 1, 3), Layout((0, 2, 1, 3)))
    residual = res.reshape(SHARD, DRAFT, BATCH).transpose(2, 1, 0)
    return acc.T, expected, residual, bonus.T


def solution(mesh):
    return jax.shard_map(
        verify_local,
        mesh=mesh,
        in_specs=(P(('dp', 'tp'), None, None), P(None, 'tp'), P(('dp', 'tp'), None, None), P('dp', None)),
        out_specs=(P('dp', None), P('dp'), P('dp', None, 'tp'), P('dp', 'tp')),
        check_vma=False,
    )
```

```python
import functools

import jax
import jax.numpy as jnp
from jax import lax
from jax.experimental import pallas as pl
from jax.experimental.layout import Layout, with_layout_constraint
from jax.experimental.pallas import tpu as pltpu
from jax.sharding import PartitionSpec as P

INV_TEMP = 1.25
DEV = 128
SEQ = 3
NPOS = 3
DRAFT = 2
BATCH = 384
DIM = 2048
VOCAB = 128256
SHARD = VOCAB // DEV
LANES = 128
TILES = VOCAB // LANES
CHUNKS = 8
TAIL = SHARD - (CHUNKS - 1) * LANES
ROWS_P = 1008
TAIL_P = ROWS_P - (CHUNKS - 1) * LANES
KC = DIM // LANES
HROWS = SEQ * NPOS * KC
COLS = NPOS * BATCH
COLS_P = 1280
CT = COLS // LANES
BT = BATCH // LANES
BLK = SEQ * CHUNKS
PITCH = 49
NEG = -1e30
STAT = 18
MESH = pl.DeviceIdType.MESH


def remote(src, dst, ssem, rsem, dev):
    return pltpu.make_async_remote_copy(
        src_ref=src, dst_ref=dst, send_sem=ssem, recv_sem=rsem,
        device_id={'tp': dev}, device_id_type=MESH)


def reduce_stage(buf, slot, count, ssem, rsem, device, payload):
    buf.reshape(count * STAT, LANES)[pl.ds(slot * STAT, STAT), :] = payload
    here = buf.at[pl.ds(slot * STAT, STAT)]
    for r in range(1, count):
        remote(here, here, ssem, rsem, device((slot + r) % count)).start()


def wait_rows(ref, rows, sem):
    part = ref.at[pl.ds(0, rows)]
    pltpu.make_async_copy(part, part, sem).wait()


def finish(buf, count, rsem):
    wait_rows(buf, (count - 1) * STAT, rsem)
    rows = buf.reshape(count * STAT, LANES)
    return [rows[k * STAT:(k + 1) * STAT, :] for k in range(count)]


def merge_max_sum(parts):
    m = parts[0][0:CT]
    for p in parts[1:]:
        m = jnp.maximum(m, p[0:CT])
    s = parts[0][CT:2 * CT] * jnp.exp(parts[0][0:CT] - m)
    for p in parts[1:]:
        s = s + p[CT:2 * CT] * jnp.exp(p[0:CT] - m)
    return jnp.concatenate([m, s], axis=0)


def merge_add(parts):
    total = parts[0]
    for p in parts[1:]:
        total = total + p
    return total


def kernel(q_hbm, w_hbm, h_hbm, tok_hbm,
           ex_hbm, bo_hbm, out_ref,
           tok_ref, qbuf, wbuf, hloc, hidb, bounce, hmat, z, send, recv, exbuf, stat, peak, scale,
           a1, b1, a2, b2,
           lsem, ag_s, ag_r, ag_r2, d2d_s, d2d_r, qs, qr_sem, rs, rr):
    scope = jax.named_scope
    me = lax.axis_index('tp')
    core = me % 2
    coord = (me // 32, (me // 8) % 4, (me // 2) % 4)
    unit = (32, 8, 2)
    partner = me + 1 - 2 * core
    hop = [[((coord[d] + r) % 4) * unit[d] for r in range(4)] for d in range(3)]

    def device(rz, ry, rx, rc):
        return hop[0][rz] + hop[1][ry] + hop[2][rx] + (core if rc == 0 else 1 - core)

    hcp = pltpu.make_async_copy(h_hbm, hloc, lsem.at[2])
    hcp.start()
    qcp = pltpu.make_async_copy(q_hbm, qbuf.at[pl.ds(0, SEQ * TILES * DRAFT)], lsem.at[0])
    qcp.start()
    wcp = pltpu.make_async_copy(w_hbm, wbuf, lsem.at[1])
    wcp.start()
    tcp = pltpu.make_async_copy(tok_hbm, tok_ref, lsem.at[3])
    tcp.start()
    barrier = pltpu.get_barrier_semaphore()
    peers = [partner]
    for d in range(3):
        for r in range(1, 4):
            steps = [0, 0, 0]
            steps[d] = r
            peers.append(device(*steps, 0))
    for dev in peers:
        pl.semaphore_signal(barrier, inc=1, device_id={'tp': dev}, device_id_type=MESH)

    with scope('hid'):
        hcp.wait()
        for s in range(SEQ):
            x = hloc[s].astype(jnp.float32)
            for kc in range(KC):
                bounce[pl.ds(s * 48 + kc, NPOS, stride=KC), :] = x[:, kc * LANES:(kc + 1) * LANES]
        hidb[pl.ds(pl.multiple_of(me * HROWS, 16), HROWS), :] = bounce[0:HROWS, :].astype(jnp.bfloat16)
    with scope('barrier'):
        pl.semaphore_wait(barrier, len(peers))

    hview = hidb.reshape(4, 4, 4, 2, SEQ, HROWS // SEQ, LANES)

    def ag_phase(phase):
        for j in range(3):
            order = [(j + k) % 3 for k in range(3)]
            idx = list(coord)
            for d in order[:phase]:
                idx[d] = slice(None)
            view = hview.at[idx[0], idx[1], idx[2], core, j]
            for r in (1, 3, 2):
                steps = [0, 0, 0]
                steps[order[phase]] = r
                remote(view, view, ag_s, ag_r.at[phase, j], device(*steps, 0)).start()

    def ag_wait(phase, j):
        wait_rows(hidb, 3 * 4 ** phase * (HROWS // SEQ), ag_r.at[phase, j])

    def half(j, off, part):
        order = [(j + k) % 3 for k in range(3)]
        idx = [slice(None)] * 3
        idx[order[2]] = (coord[order[2]] + off) % 4
        idx[order[0]] = slice(2 * part, 2 * part + 2)
        return hview.at[idx[0], idx[1], idx[2], core, j]

    def ag_half(j, off, part, sem, r):
        steps = [0, 0, 0]
        steps[(j + 2) % 3] = r
        view = half(j, off, part)
        remote(view, view, ag_s, ag_r2.at[j, sem], device(*steps, 0)).start()

    HALF = 8 * HROWS // SEQ
    qrows = qbuf.reshape(qbuf.shape[0], LANES)
    lane = lax.broadcasted_iota(jnp.int32, (8, LANES), 1)

    def pack(i, k, carry):
        first = (SHARD * k) // LANES
        off = (SHARD * k) % LANES
        shift = (LANES - off) % LANES
        keep = lane < LANES - off
        for s in range(SEQ):
            base = (s * TILES + first) * DRAFT + i
            lo = qrows[pl.ds(base, 8, stride=2), :]
            hi = qrows[pl.ds(base + 2, 8, stride=2), :]
            lo = pltpu.roll(lo, shift, 1)
            hi = pltpu.roll(hi, shift, 1)
            send[i, pl.ds(pl.multiple_of(k * BLK + s * 8, 8), 8), :] = jnp.where(keep, lo, hi)
        return carry

    mine = pl.ds(pl.multiple_of(me * BLK, 8), BLK)

    def to(i, dev):
        remote(send.at[i, pl.ds(pl.multiple_of(dev * BLK, 8), BLK)], recv.at[i, mine],
               qs, qr_sem.at[i], dev).start()

    def step(d, n):
        return ((coord[d] + n) % 4) * unit[d]

    def class0(i):
        pltpu.make_async_copy(send.at[i, mine], recv.at[i, mine], qr_sem.at[i]).start()
        to(i, partner)

    def class1(i, rc):
        last = core if rc == 0 else 1 - core
        for r in (1, 3, 2):
            for d in range(3):
                steps = [0, 0, 0]
                steps[d] = r
                to(i, device(*steps, rc))

    def class2(i, rc, lo=0, hi=9):
        last = core if rc == 0 else 1 - core

        def body(n, carry):
            a, b = n // 3 + 1, n % 3 + 1
            to(i, step(0, a) + step(1, b) + hop[2][0] + last)
            to(i, hop[0][0] + step(1, a) + step(2, b) + last)
            to(i, step(0, b) + hop[1][0] + step(2, a) + last)
            return carry

        lax.fori_loop(lo, hi, body, 0)

    def class3(i, rc, lo=0, hi=9):
        last = core if rc == 0 else 1 - core

        def body(n, carry):
            a, b = n // 3, n % 3
            for k in range(3):
                to(i, step(0, (a + k) % 3 + 1) + step(1, (b + k) % 3 + 1) + hop[2][k + 1] + last)
            return carry

        lax.fori_loop(lo, hi, body, 0)

    ag_phase(0)
    with scope('qwait'):
        qcp.wait()
    with scope('pack'):
        lax.fori_loop(0, DEV, functools.partial(pack, 0), 0, unroll=16)
    with scope('ex0'):
        class0(0)
        class1(0, 0)
    with scope('ag0'):
        for j in range(3):
            ag_wait(0, j)
    ag_phase(1)
    with scope('ex0a'):
        class1(0, 1)
        class2(0, 0)
    with scope('pack2'):
        lax.fori_loop(0, DEV, functools.partial(pack, 1), 0, unroll=16)
    with scope('ag1'):
        for j in range(3):
            ag_wait(1, j)
    for j in range(3):
        ag_half(j, 0, 0, 0, 1)
        ag_half(j, 0, 1, 1, 3)
    for j in range(3):
        ag_half(j, 0, 1, 2, 1)
        ag_half(j, 0, 0, 2, 3)
    with scope('relay'):
        for j in range(3):
            wait_rows(hidb, HALF, ag_r2.at[j, 0])
            ag_half(j, 3, 0, 2, 1)
            wait_rows(hidb, HALF, ag_r2.at[j, 1])
            ag_half(j, 1, 1, 2, 3)
    with scope('exag2'):
        class0(1)
        class1(1, 0)
        class1(1, 1)
        class2(0, 1)
        class3(0, 0)
    d2d = []
    for j in (2, 1, 0):
        with scope(f'ag2_{j}'):
            wait_rows(hidb, 4 * HALF, ag_r2.at[j, 2])
        view = hview.at[:, :, :, core, j]
        cp = remote(view, view, d2d_s, d2d_r.at[j], partner)
        cp.start()
        d2d.append(cp)
    with scope('ex0b'):
        class3(0, 1)
        class3(1, 0)
        class3(1, 1, 0, 4)
    with scope('d2d'):
        for cp in d2d:
            cp.wait_recv()

    def relayout(n, carry):
        def up(b, c):
            x = hidb[pl.ds(pl.multiple_of((48 * n + b) * 48, 16), 48), :]
            bounce[pl.ds(b * PITCH, 48), :] = x.astype(jnp.float32)
            return c

        lax.fori_loop(0, 48, up, 0, unroll=4)
        for g in range(NPOS):
            for u in range(3):
                for kc in range(KC):
                    y = bounce[pl.ds(16 * u * PITCH + g * KC + kc, 16, stride=PITCH), :]
                    hmat[pl.ds(pl.multiple_of(g * BATCH + 48 * n + 16 * u, 16), 16),
                         kc * LANES:(kc + 1) * LANES] = y.astype(jnp.bfloat16)
        return carry

    with scope('relayout'):
        lax.fori_loop(0, 8, relayout, 0)
    wcp.wait()
    tcp.wait()

    z[SHARD:ROWS_P, :] = jnp.full((ROWS_P - SHARD, COLS_P), NEG, jnp.float32)

    def head(n, carry):
        hb = hmat[pl.ds(pl.multiple_of(n * 256, 256), 256), :]
        zt = lax.dot_general(wbuf[...], hb, (((1,), (1,)), ((), ())), preferred_element_type=jnp.float32)
        zt = zt * INV_TEMP
        z[0:SHARD, pl.ds(pl.multiple_of(n * 256, 256), 256)] = zt
        top = jnp.max(zt, axis=0, keepdims=True)
        peak[pl.ds(2 * n, 1), :] = top[:, 0:LANES]
        peak[pl.ds(2 * n + 1, 1), :] = top[:, LANES:]
        return carry

    with scope('head'):
        lax.fori_loop(0, COLS_P // 256, head, 0)

    def local_stats(t, carry):
        cols = pl.ds(pl.multiple_of(t * LANES, LANES), LANES)

        m = peak[pl.ds(t, 1), :]

        def expo(n, s):
            rows = pl.ds(pl.multiple_of(n * 112, 8), 112)
            x = jnp.exp(z[rows, cols] - m)
            z[rows, cols] = x
            return s + jnp.sum(x.reshape(14, 8, LANES), axis=0)

        s8 = lax.fori_loop(0, 9, expo, jnp.zeros((8, LANES), jnp.float32), unroll=3)
        stat[pl.ds(t, 1), :] = m
        stat[pl.ds(CT + t, 1), :] = jnp.sum(s8, axis=0, keepdims=True)
        return carry

    stat[...] = jnp.zeros_like(stat)
    with scope('stats'):
        lax.fori_loop(0, CT, local_stats, 0)
    bcp = pltpu.make_async_copy(z.at[:, DRAFT * BATCH:COLS], bo_hbm, lsem.at[2])
    bcp.start()

    slot, grp = me % 8, me // 8
    near = lambda k: grp * 8 + k
    far = lambda k: k * 8 + slot
    local = stat[0:STAT, :]
    reduce_stage(a1, slot, 8, rs, rr.at[0], near, local)
    with scope('ex1a'):
        class3(1, 1, 4, 9)
        class2(1, 1, 0, 3)
    with scope('round1a'):
        parts = finish(a1, 8, rr.at[0])
    reduce_stage(b1, grp, 16, rs, rr.at[1], far, merge_max_sum(parts))
    with scope('ex1b'):
        class2(1, 1, 3, 9)
        class2(1, 0)
    with scope('round1b'):
        parts = finish(b1, 16, rr.at[1])
    tot = merge_max_sum(parts)
    fac = jnp.exp(local[0:CT] - tot[0:CT]) / tot[CT:2 * CT]
    scale[0:CT, :] = fac
    out_ref[12:16, :] = jnp.concatenate([fac[DRAFT * BT:CT], fac[0:1]], axis=0)

    exrows = exbuf.reshape(exbuf.shape[0], LANES)
    first_id = me * SHARD
    stat[...] = jnp.zeros_like(stat)
    for i in range(DRAFT):
        with scope(f'a2a_{i}'):
            pltpu.make_async_copy(recv.at[i], recv.at[i], qr_sem.at[i]).wait()
        for t in range(BT):
            row = i * BT + t
            sc = scale[row:row + 1, :]
            tok = tok_ref[i:i + 1, t * LANES:(t + 1) * LANES] - first_id
            col0 = i * BATCH + t * LANES

            def block(c, carry, size, valid):
                mass, pp, qp = carry
                q = recv[i, pl.ds(t * LANES * CHUNKS + c, LANES, stride=CHUNKS), :].T
                p = z[pl.ds(pl.multiple_of(c * LANES, LANES), size), col0:col0 + LANES] * sc
                ids = lax.broadcasted_iota(jnp.int32, (size, LANES), 0)
                q = q[0:size]
                if valid < size:
                    q = jnp.where(ids < valid, q, 0.0)
                x = jnp.maximum(p - q, 0.0)
                exrows[pl.ds(c * LANES * 6 + t * 2 + i, valid, stride=6), :] = x[0:valid]
                hit = ids == tok - c * LANES
                fold = lambda v: jnp.sum(v.reshape(size // 8, 8, LANES), axis=0)
                return (mass + fold(x), pp + fold(jnp.where(hit, p, 0.0)), qp + fold(jnp.where(hit, q, 0.0)))

            zero = jnp.zeros((8, LANES), jnp.float32)
            carry = lax.fori_loop(0, CHUNKS - 1, lambda c, v: block(c, v, LANES, LANES), (zero, zero, zero),
                                  unroll=CHUNKS - 1)
            mass, pp, qp = block(CHUNKS - 1, carry, TAIL_P, TAIL)
            stat[row:row + 1, :] = jnp.sum(mass, axis=0, keepdims=True)
            stat[6 + row:7 + row, :] = jnp.sum(pp, axis=0, keepdims=True)
            stat[12 + row:13 + row, :] = jnp.sum(qp, axis=0, keepdims=True)

    ecp = pltpu.make_async_copy(exbuf, ex_hbm, lsem.at[0])
    ecp.start()
    reduce_stage(a2, slot, 8, rs, rr.at[2], near, stat[0:STAT, :])
    with scope('round2a'):
        parts = finish(a2, 8, rr.at[2])
    reduce_stage(b2, grp, 16, rs, rr.at[3], far, merge_add(parts))
    with scope('round2b'):
        parts = finish(b2, 16, rr.at[3])
    tot = merge_add(parts)
    out_ref[0:6, :] = tot[0:6]
    out_ref[6:12, :] = jnp.minimum(tot[6:12] / tot[12:18], 1.0)
    with scope('tail'):
        ecp.wait()
        bcp.wait()
        wait_rows(hidb, 9 * 21 * (HROWS // SEQ), ag_s)
        wait_rows(hidb, DEV // 2 * HROWS, d2d_s)
        wait_rows(send.reshape(DRAFT * DEV * BLK, LANES), DRAFT * (DEV - 1) * BLK, qs)
        wait_rows(qbuf, 2 * (7 + 15) * STAT, rs)


def finish_kernel(ex_ref, bo_ref, stat_ref, res_hbm, bonus_hbm, acc_ref, exp_ref, res, bonus, sems):
    rows = ex_ref.reshape(ex_ref.shape[0], LANES)
    out = res.reshape(res.shape[0], LANES)
    copies = []
    fac = jnp.concatenate([stat_ref[12 + t:13 + t, :] for t in range(BT)], axis=1)
    step = 256
    for n in range(4):
        size = min(step, SHARD - n * step)
        bonus[n * step:n * step + size, :] = bo_ref[n * step:n * step + size, :] * fac
    cp = pltpu.make_async_copy(bonus, bonus_hbm, sems)
    cp.start()
    copies.append(cp)
    mass = jnp.concatenate([stat_ref[i * BT + t:i * BT + t + 1, :] for t in range(BT) for i in range(DRAFT)], axis=0)
    mass = jnp.concatenate([mass] * 4, axis=0)
    for n in range(5):
        def body(k, carry):
            at = pl.ds(pl.multiple_of(n * 1200 + k * 24, 8), 24)
            out[at, :] = rows[at, :] / mass
            return carry

        lax.fori_loop(0, 50, body, 0, unroll=5)
        size = 1200
        if n == 4:
            out[6000:6012, :] = rows[6000:6012, :] / mass[0:12]
            size = 1212
        cp = pltpu.make_async_copy(res.at[pl.ds(n * 1200, size)], res_hbm.at[pl.ds(n * 1200, size)], sems)
        cp.start()
        copies.append(cp)
    acc = stat_ref[6:12, :]
    more = acc[0:BT] * (1.0 + acc[BT:2 * BT])
    for t in range(BT):
        cols = slice(t * LANES, (t + 1) * LANES)
        exp_ref[cols] = more[t]
        for i in range(DRAFT):
            acc_ref[i:i + 1, cols] = acc[i * BT + t:i * BT + t + 1]
    for cp in copies:
        cp.wait()


def verify_local(hid, w_cols, q_rows, draft_tok):
    q = with_layout_constraint(q_rows.reshape(SEQ, DRAFT, TILES, LANES), Layout((0, 2, 1, 3)))
    q = q.transpose(0, 2, 1, 3).reshape(SEQ * TILES * DRAFT, 1, LANES)
    f32 = jnp.float32
    hbm = pl.BlockSpec(memory_space=pl.ANY)
    vmem = pl.BlockSpec(memory_space=pltpu.VMEM)
    dma = pltpu.SemaphoreType.DMA
    ex, bo, st = pl.pallas_call(
        kernel,
        out_shape=[
            jax.ShapeDtypeStruct((SHARD * BT * DRAFT, 1, LANES), f32),
            jax.ShapeDtypeStruct((ROWS_P, BATCH), f32),
            jax.ShapeDtypeStruct((16, LANES), f32),
        ],
        in_specs=[pl.BlockSpec(memory_space=pltpu.HBM)] * 4,
        out_specs=[hbm, hbm, vmem],
        scratch_shapes=[
            pltpu.VMEM((DRAFT, BATCH), jnp.int32),
            pltpu.VMEM((SEQ * TILES * DRAFT + 20, 1, LANES), f32),
            pltpu.VMEM((SHARD, DIM), jnp.bfloat16),
            pltpu.VMEM((SEQ, NPOS, DIM), jnp.bfloat16),
            pltpu.VMEM((DEV * HROWS, LANES), jnp.bfloat16),
            pltpu.VMEM((48 * PITCH, LANES), f32),
            pltpu.VMEM((COLS_P, DIM), jnp.bfloat16),
            pltpu.VMEM((ROWS_P, COLS_P), f32),
            pltpu.VMEM((DRAFT, DEV * BLK, LANES), f32),
            pltpu.VMEM((DRAFT, DEV * BLK, LANES), f32),
            pltpu.VMEM((SHARD * BT * DRAFT, 1, LANES), f32),
            pltpu.VMEM((24, LANES), f32),
            pltpu.VMEM((16, LANES), f32),
            pltpu.VMEM((16, LANES), f32),
            pltpu.VMEM((8 * STAT, 1, LANES), f32),
            pltpu.VMEM((16 * STAT, 1, LANES), f32),
            pltpu.VMEM((8 * STAT, 1, LANES), f32),
            pltpu.VMEM((16 * STAT, 1, LANES), f32),
            dma((4,)),
            dma, dma((2, 3)), dma((3, 3)), dma, dma((3,)), dma, dma((2,)), dma, dma((4,)),
        ],
        compiler_params=pltpu.CompilerParams(vmem_limit_bytes=40 * 2 ** 20, has_side_effects=True, collective_id=0),
    )(*(pltpu.with_memory_space_constraint(x, pltpu.HBM) for x in (q, w_cols.T, hid, draft_tok.T)))
    res, bonus, acc, expected = pl.pallas_call(
        finish_kernel,
        out_shape=[
            jax.ShapeDtypeStruct((SHARD * BT * DRAFT, 1, LANES), f32),
            jax.ShapeDtypeStruct((SHARD, BATCH), f32),
            jax.ShapeDtypeStruct((DRAFT, BATCH), f32),
            jax.ShapeDtypeStruct((BATCH,), f32),
        ],
        in_specs=[vmem] * 3,
        out_specs=[hbm, hbm, vmem, vmem],
        scratch_shapes=[
            pltpu.VMEM((SHARD * BT * DRAFT, 1, LANES), f32),
            pltpu.VMEM((SHARD, BATCH), f32),
            dma,
        ],
        compiler_params=pltpu.CompilerParams(vmem_limit_bytes=12 * 2 ** 20),
    )(ex, bo, st)
    res = with_layout_constraint(res.reshape(SHARD, BT, DRAFT, LANES).transpose(0, 2, 1, 3), Layout((0, 2, 1, 3)))
    residual = res.reshape(SHARD, DRAFT, BATCH).transpose(2, 1, 0)
    return acc.T, expected, residual, bonus.T


def solution(mesh):
    return jax.shard_map(
        verify_local,
        mesh=mesh,
        in_specs=(P(('dp', 'tp'), None, None), P(None, 'tp'), P(('dp', 'tp'), None, None), P('dp', None)),
        out_specs=(P('dp', None), P('dp'), P('dp', None, 'tp'), P('dp', 'tp')),
        check_vma=False,
    )
```
